32 devices in a mesh: dp: 4 (over x, core), seq: 8 (over z, y).
Axes of the slice: x: 2, y: 2, z: 4, core: 2. Of those that a mesh axis runs over, the one named last changes fastest.
Arguments:
- frames: float32 [32, 768, 512], P('dp', 'seq'), may hold values from -6 to 6
- lengths: int32 [32], replicated, may hold values from 192 to 768, as said below
- cotangent: float32 [32, 768, 512], P('dp', 'seq'), may hold values from -6 to 6
- gains: bfloat16 [1, 6, 512], P(None, None, ('dp', 'seq')), may hold values from 0.5 to 1.5
- shifts: bfloat16 [1, 6, 512], P(None, None, ('dp', 'seq')), may hold values from -3 to 3
- rel_bias: bfloat16 [1, 2, 512], P(None, None, ('dp', 'seq')), may hold values from -3 to 3
- ffn_up: bfloat16 [1, 2, 512, 2048], P(None, None, ('dp', 'seq')), may hold values from -0.25 to 0.25
- ffn_down: bfloat16 [1, 2, 2048, 512], P(None, None, ('dp', 'seq')), may hold values from -0.125 to 0.125
- attn_in: bfloat16 [1, 512, 1536], P(None, ('dp', 'seq')), may hold values from -1 to 1
- attn_out: bfloat16 [1, 512, 512], P(None, ('dp', 'seq')), may hold values from -1 to 1
- pos_proj: bfloat16 [1, 512, 512], P(None, ('dp', 'seq')), may hold values from -0.25 to 0.25
- conv_in: bfloat16 [1, 512, 1024], P(None, ('dp', 'seq')), may hold values from -0.25 to 0.25
- depthwise: bfloat16 [1, 512, 31], P(None, ('dp', 'seq')), may hold values from -1 to 1
- conv_out: bfloat16 [1, 512, 512], P(None, ('dp', 'seq')), may hold values from -0.25 to 0.25
Outputs:
- mixed: float32 [32, 768, 512], P('dp', 'seq')
- grad_frames: float32 [32, 768, 512], P('dp', 'seq')
- grad_gains: float32 [1, 6, 512], P(None, None, ('dp', 'seq'))
- grad_shifts: float32 [1, 6, 512], P(None, None, ('dp', 'seq'))
- grad_rel_bias: float32 [1, 2, 512], P(None, None, ('dp', 'seq'))
- grad_ffn_up: float32 [1, 2, 512, 2048], P(None, None, ('dp', 'seq'))
- grad_ffn_down: float32 [1, 2, 2048, 512], P(None, None, ('dp', 'seq'))
- grad_attn_in: float32 [1, 512, 1536], P(None, ('dp', 'seq'))
- grad_attn_out: float32 [1, 512, 512], P(None, ('dp', 'seq'))
- grad_pos_proj: float32 [1, 512, 512], P(None, ('dp', 'seq'))
- grad_conv_in: float32 [1, 512, 1024], P(None, ('dp', 'seq'))
- grad_depthwise: float32 [1, 512, 31], P(None, ('dp', 'seq'))
- grad_conv_out: float32 [1, 512, 512], P(None, ('dp', 'seq'))
The draws below stay inside these ranges and needn't reach their ends.
Inputs may be any that keep to these rules, and one draw needn't show every extreme that they name: `lengths`: some utterance has exactly 768 valid frames and some exactly 192.
All inputs are finite; a program needn't handle non-finite values.
Results may differ from the reference program's by a relative error of at most 0.019.
Values may be sent and summed in bfloat16 or wider, within the bound.
A program may use at most 384 MiB of HBM per device.

```python
import math
from functools import partial
import jax
import jax.numpy as jnp
from jax import lax

D = 512
FF = 2048
H = 8
DH = 64
KW = 31
NL = 1
MB = 2
U = 4
LEN = 768
B = 32
N_DP = 4


def draw_lengths(key, part):
    key_a, key_b, key_c = jax.random.split(key, 3)
    drawn_len = jax.random.randint(key_a, (B,), LEN // 4, LEN + 1, dtype=jnp.int32)
    full_at = jax.random.randint(key_b, (), 0, B, dtype=jnp.int32)
    short_at = jax.random.randint(key_c, (), 0, B - 1, dtype=jnp.int32)
    short_at = short_at + (short_at >= full_at).astype(jnp.int32)
    drawn_len = drawn_len.at[full_at].set(LEN)
    return drawn_len.at[short_at].set(LEN // 4)


def draw_frames(key, part):
    key_n = jax.random.fold_in(jax.random.fold_in(key, 17), 0)
    drawn = jnp.clip(jax.random.normal(key_n, (B, LEN, D), dtype=jnp.float32), -6.0, 6.0)
    return drawn


def draw_attn_in(key, part):
    key_w = jax.random.fold_in(key, 23)
    deviation = D ** (-0.5)
    matrix = jnp.clip(jax.random.normal(key_w, (NL, D, 3 * D), dtype=jnp.float32) * deviation, -6.0 * deviation, 6.0 * deviation)
    return matrix.astype(jnp.bfloat16)


def shard_levels(stream_key, dims, pieces, least, top_value):
    def one(axis_at, blocks):
        draws = jax.random.uniform(jax.random.fold_in(jax.random.fold_in(stream_key, 6), axis_at), (blocks,), jnp.float32, least / len(pieces), top_value / len(pieces))
        return jnp.repeat(jnp.exp(draws), dims[axis_at] // blocks).reshape((-1,) + (1,) * (len(dims) - axis_at - 1))

    factor_of = one(*pieces[0])
    for cut in pieces[1:]:
        factor_of = factor_of * one(*cut)
    return factor_of


def bell_draw(stream_key, dims, scale, reach, cuts=(), held_as=jnp.bfloat16):
    values = jax.random.normal(stream_key, dims, jnp.float32) * scale
    if len(cuts) > 0:
        values = shard_levels(stream_key, dims, cuts, -0.22, 0.18) * values
    return jnp.clip(values, min=-reach, max=reach).astype(held_as)


def setup_inputs(seed: int = 0) -> dict:
    streams_of = jax.random.split(jax.random.key(seed), 15)
    return {
        "frames": draw_frames(jax.random.fold_in(streams_of[14], 71), 0),
        "lengths": draw_lengths(jax.random.fold_in(streams_of[14], 71), 0),
        "cotangent": bell_draw(streams_of[2], (B, LEN, D), 1.0, 6.0, ((0, 4), (1, 8)), jnp.float32),
        "gains": jnp.clip(1.0 + 0.1 * jax.random.normal(streams_of[3], (NL, 6, D), jnp.float32), 0.5, 1.5).astype(jnp.bfloat16),
        "shifts": bell_draw(streams_of[4], (NL, 6, D), 0.5, 3.0, ((2, 32),)),
        "rel_bias": bell_draw(streams_of[5], (NL, 2, D), 0.5, 3.0, ((2, 32),)),
        "ffn_up": bell_draw(streams_of[6], (NL, 2, D, FF), D ** -0.5, 0.25, ((2, 32),)),
        "ffn_down": bell_draw(streams_of[7], (NL, 2, FF, D), FF ** -0.5, 0.125, ((2, 32),)),
        "attn_in": draw_attn_in(jax.random.fold_in(streams_of[14], 71), 0),
        "attn_out": bell_draw(streams_of[9], (NL, D, D), (D // 16) ** -0.5, 1.0, ((1, 32),)),
        "pos_proj": bell_draw(streams_of[10], (NL, D, D), D ** -0.5, 0.25, ((1, 32),)),
        "conv_in": bell_draw(streams_of[11], (NL, D, 2 * D), D ** -0.5, 0.25, ((1, 32),)),
        "depthwise": bell_draw(streams_of[12], (NL, D, KW), KW ** -0.5, 1.0, ((1, 32),)),
        "conv_out": bell_draw(streams_of[13], (NL, D, D), D ** -0.5, 0.25, ((1, 32),)),
    }


HIGHEST_PREC = lax.Precision.HIGHEST

@jax.custom_vjp
def low(v):
    return lax.optimization_barrier(v.astype(jnp.bfloat16)).astype(jnp.float32)

@jax.custom_vjp
def low_back(v):
    return v

def low_keep(v):
    return (low(v), None)

def low_pass(kept, grad):
    return (grad,)

def back_keep(v):
    return (v, None)

def back_low(kept, grad):
    return (low(grad),)
low.defvjp(low_keep, low_pass)
low_back.defvjp(back_keep, back_low)

def matmul(left, right):
    return jnp.dot(left, right, precision=HIGHEST_PREC, preferred_element_type=jnp.float32)

def layer_norm(values, gain_row, shift_row):
    centred = values - lax.optimization_barrier(jnp.mean(values, axis=-1, keepdims=True))
    spread = lax.optimization_barrier(jnp.mean(centred * centred, axis=-1, keepdims=True))
    return centred * lax.rsqrt(spread + 1e-05) * gain_row + shift_row

def sinusoid(offsets, model_width):
    half_width = model_width // 2
    frequency = jnp.exp(jnp.arange(half_width, dtype=jnp.float32) * (-2.0 * math.log(10000.0) / model_width))
    angles = offsets.astype(jnp.float32)[:, None] * frequency[None, :]
    return jnp.concatenate([jnp.sin(angles), jnp.cos(angles)], axis=1)

def skew_rows(raw_pos, key_count):
    row_count = raw_pos.shape[-2]
    col_count = raw_pos.shape[-1]
    lead = raw_pos.shape[:-2]
    flat_rows = raw_pos.reshape(lead + (row_count * col_count,))
    flat_rows = flat_rows[..., row_count - 1:row_count - 1 + row_count * (col_count - 1)]
    return flat_rows.reshape(lead + (row_count, col_count - 1))[..., :key_count]

def glu_gate(gate_pair):
    half_width = gate_pair.shape[-1] // 2
    return gate_pair[..., :half_width] * jax.nn.sigmoid(gate_pair[..., half_width:])

def feed_forward(values, gain_row, shift_row, w_up, w_down):
    normed = low(layer_norm(values, gain_row, shift_row))
    hidden = low_back(matmul(normed, w_up))
    active = low(jax.nn.silu(hidden))
    return values + 0.5 * low_back(matmul(active, w_down))

def attend_one(inputs, pos_rows):
    query_u, query_v, key_rows, value_rows, key_valid = inputs
    content = jnp.einsum('fhd,lhd->hfl', query_u, key_rows, precision=HIGHEST_PREC)
    raw_pos = jnp.einsum('fhd,whd->hfw', query_v, pos_rows, precision=HIGHEST_PREC)
    logits = low_back((content + skew_rows(raw_pos, LEN)) * 0.125)
    logits = jnp.where(key_valid[None, None, :], logits, -1e+30)
    top_score = lax.optimization_barrier(jnp.max(logits, axis=-1, keepdims=True))
    exp_scores = jnp.exp(logits - top_score)
    prob_rows = exp_scores / lax.optimization_barrier(jnp.sum(exp_scores, axis=-1, keepdims=True))
    context = jnp.einsum('hfl,lhd->fhd', low(prob_rows), value_rows, precision=HIGHEST_PREC)
    return low(low_back(context))

def self_attention(values, key_valid, gain_row, shift_row, bias_u, bias_v, w_in, w_out, w_pos, pos_table):
    normed = low(layer_norm(values, gain_row, shift_row))
    proj_rows = low_back(matmul(normed, w_in))
    utt_count = values.shape[0]
    query_rows = proj_rows[..., :D].reshape(utt_count, LEN, H, DH)
    key_rows = low(proj_rows[..., D:2 * D]).reshape(utt_count, LEN, H, DH)
    value_rows = low(proj_rows[..., 2 * D:]).reshape(utt_count, LEN, H, DH)
    query_u = low(query_rows + bias_u.reshape(H, DH))
    query_v = low(query_rows + bias_v.reshape(H, DH))
    pos_rows = low(matmul(pos_table, w_pos)).reshape(2 * LEN - 1, H, DH)
    context = lax.map(jax.checkpoint(partial(attend_one, pos_rows=pos_rows)), (query_u, query_v, key_rows, value_rows, key_valid))
    context = context.reshape(utt_count, LEN, D)
    return values + low_back(matmul(context, w_out))

def convolution(values, frame_mask, frame_count, gain_row, shift_row, w_in, kernel, bn_gain, bn_shift, w_out):
    normed = low(layer_norm(values, gain_row, shift_row))
    gate_pair = low_back(matmul(normed, w_in))
    gated = low(glu_gate(gate_pair) * frame_mask[..., None])
    halo_reach = (KW - 1) // 2
    padded = jnp.pad(gated, ((0, 0), (halo_reach, halo_reach), (0, 0)))
    depth_out = padded[:, 0:LEN] * kernel[:, 0]
    for tap_idx in range(1, KW):
        depth_out = depth_out + padded[:, tap_idx:tap_idx + LEN] * kernel[:, tap_idx]
    depth_out = low_back(depth_out)
    weight_mask = frame_mask[..., None]
    sum_all = lax.optimization_barrier(jnp.sum(depth_out * weight_mask, axis=(0, 1)))
    square_all = lax.optimization_barrier(jnp.sum(depth_out * depth_out * weight_mask, axis=(0, 1)))
    mean_val = sum_all / frame_count
    variance = square_all / frame_count - mean_val * mean_val
    normal = (depth_out - mean_val) * lax.rsqrt(variance + 1e-05) * bn_gain + bn_shift
    active = low(jax.nn.silu(normal))
    return values + low_back(matmul(active, w_out))

def conformer_layer(values, params, frame_mask, key_valid, frame_count, pos_table):
    gains, shifts, rel_bias, ffn_up, ffn_down, attn_in, attn_out, pos_proj, conv_in, depthwise, conv_out = params
    values = feed_forward(values, gains[0], shifts[0], ffn_up[0], ffn_down[0])
    values = self_attention(values, key_valid, gains[1], shifts[1], rel_bias[0], rel_bias[1], attn_in, attn_out, pos_proj, pos_table)
    values = convolution(values, frame_mask, frame_count, gains[2], shifts[2], conv_in, depthwise, gains[5], shifts[5], conv_out)
    values = feed_forward(values, gains[3], shifts[3], ffn_up[1], ffn_down[1])
    return layer_norm(values, gains[4], shifts[4])

def forward_pass(values, params, frame_mask, key_valid, frame_count, pos_table):
    for layer_idx in range(NL):
        layer_params = tuple((member[layer_idx] for member in params))
        values = conformer_layer(values, layer_params, frame_mask, key_valid, frame_count, pos_table)
    return values

def reference(frames, lengths, cotangent, gains, shifts, rel_bias, ffn_up, ffn_down, attn_in, attn_out, pos_proj, conv_in, depthwise, conv_out):
    params = tuple((member.astype(jnp.float32) for member in (gains, shifts, rel_bias, ffn_up, ffn_down, attn_in, attn_out, pos_proj, conv_in, depthwise, conv_out)))
    offsets = LEN - 1 - jnp.arange(2 * LEN - 1, dtype=jnp.int32)
    pos_table = low(sinusoid(offsets, D))
    grid_in = frames.reshape(N_DP, MB, U, LEN, D)
    grid_cot = cotangent.reshape(N_DP, MB, U, LEN, D)
    grid_len = lengths.reshape(N_DP, MB, U)
    positions = jnp.arange(LEN, dtype=jnp.int32)
    result_list = []
    grad_list = []
    summed = None
    for micro_idx in range(MB):
        values = grid_in[:, micro_idx].reshape(N_DP * U, LEN, D)
        lens_here = grid_len[:, micro_idx].reshape(N_DP * U)
        key_valid = positions[None, :] < lens_here[:, None]
        frame_mask = key_valid.astype(jnp.float32)
        frame_count = jnp.sum(lens_here).astype(jnp.float32)

        def run_layers(val_in, par_in):
            return forward_pass(val_in, par_in, frame_mask, key_valid, frame_count, pos_table)
        result, pullback = jax.vjp(run_layers, values, params)
        grad_in, grad_par = pullback(grid_cot[:, micro_idx].reshape(N_DP * U, LEN, D))
        result_list.append(result.reshape(N_DP, U, LEN, D))
        grad_list.append(grad_in.reshape(N_DP, U, LEN, D))
        if summed is None:
            summed = grad_par
        else:
            summed = jax.tree.map(jnp.add, summed, grad_par)
    mixed = jnp.stack(result_list, axis=1).reshape(N_DP * MB * U, LEN, D)
    grad_frames = jnp.stack(grad_list, axis=1).reshape(N_DP * MB * U, LEN, D)
    return (mixed, grad_frames, summed[0], summed[1], summed[2], summed[3], summed[4], summed[5], summed[6], summed[7], summed[8], summed[9], summed[10])
```

```python
import math

import jax
import jax.numpy as jnp
import numpy as np
from jax import lax
from jax.experimental import pallas as pl
from jax.experimental.pallas import tpu as pltpu
from jax.sharding import PartitionSpec as P

H = 8
DH = 64
NL = 1
MB = 2


HIGHEST_PREC = lax.Precision.HIGHEST


def extended(cells, sides, width):
    for axis, dim in sides:
        count = lax.axis_size(axis)
        ends = count - 1
        head = lax.slice_in_dim(cells, 0, width, axis=dim)
        tail = lax.slice_in_dim(cells, cells.shape[dim] - width, cells.shape[dim], axis=dim)
        cells = jnp.concatenate(
            [
                lax.ppermute(tail, axis, [(i, (i + 1) % count) for i in range(ends)]),
                cells,
                lax.ppermute(head, axis, [((i + 1) % count, i) for i in range(ends)]),
            ],
            axis=dim,
        )
    return cells


def layer_norm(values, gain_row, shift_row):
    centred = values - jnp.mean(values, axis=-1, keepdims=True)
    spread = jnp.mean(centred * centred, axis=-1, keepdims=True)
    return centred * lax.rsqrt(spread + 1e-05) * gain_row + shift_row


def sinusoid(offsets, model_width):
    half_width = model_width // 2
    frequency = jnp.exp(
        jnp.arange(half_width, dtype=jnp.float32) * (-2.0 * math.log(10000.0) / model_width)
    )
    angles = offsets.astype(jnp.float32)[:, None] * frequency[None, :]
    return jnp.concatenate([jnp.sin(angles), jnp.cos(angles)], axis=1)


def skew_rows(raw_pos, key_count):
    row_count = raw_pos.shape[-2]
    col_count = raw_pos.shape[-1]
    lead = raw_pos.shape[:-2]
    flat_rows = raw_pos.reshape(lead + (row_count * col_count,))
    flat_rows = flat_rows[..., row_count - 1 : row_count - 1 + row_count * (col_count - 1)]
    return flat_rows.reshape(lead + (row_count, col_count - 1))[..., :key_count]


def skew_back(grad_skew, raw_shape, key_count):
    zero_raw = jnp.zeros(raw_shape, jnp.float32)
    return jax.vjp(lambda raw_pos: skew_rows(raw_pos, key_count), zero_raw)[1](grad_skew)[0]


def glu_gate(gate_pair):
    half_width = gate_pair.shape[-1] // 2
    return gate_pair[..., :half_width] * jax.nn.sigmoid(gate_pair[..., half_width:])


def matmul_low(left, right):
    return jnp.dot(left, right, preferred_element_type=jnp.float32)


def matmul_back(grad_low, weight):
    return lax.dot_general(
        grad_low, weight, (((1,), (1,)), ((), ())), preferred_element_type=jnp.float32
    )


def weight_grad(inputs_low, grad_low):
    return lax.dot_general(
        inputs_low, grad_low, (((0,), (0,)), ((), ())), preferred_element_type=jnp.float32
    )


def ffn_forward(row_data, gain_row, shift_row, w_up, w_down):
    normed_b = layer_norm(row_data, gain_row, shift_row).astype(jnp.bfloat16)
    hidden = matmul_low(normed_b, w_up)
    active_b = jax.nn.silu(hidden).astype(jnp.bfloat16)
    branch = matmul_low(active_b, w_down)
    return (row_data + 0.5 * branch, (row_data, normed_b, hidden, active_b))


def ffn_backward(grad_rows, kept_data, gain_row, shift_row, w_up, w_down):
    row_data, normed_b, hidden, active_b = kept_data
    grad_out_b = (0.5 * grad_rows).astype(jnp.bfloat16)
    g_down = weight_grad(active_b, grad_out_b)
    grad_active = matmul_back(grad_out_b, w_down)
    grad_hidden_b = jax.vjp(jax.nn.silu, hidden)[1](grad_active)[0].astype(jnp.bfloat16)
    g_up = weight_grad(normed_b, grad_hidden_b)
    grad_normed = matmul_back(grad_hidden_b, w_up)
    grad_ln, g_gain, g_shift = jax.vjp(layer_norm, row_data, gain_row, shift_row)[1](grad_normed)
    return (grad_rows + grad_ln, (g_gain, g_shift, g_up, g_down))


def attention_logits(query_u_b, query_v_b, key_heads, pos_heads, key_valid):
    content = jnp.einsum(
        "ufhd,ulhd->uhfl", query_u_b, key_heads, preferred_element_type=jnp.float32
    )
    raw_pos = jnp.einsum("ufhd,whd->uhfw", query_v_b, pos_heads, preferred_element_type=jnp.float32)
    logits = (content + skew_rows(raw_pos, key_heads.shape[1])) * 0.125
    return jnp.where(key_valid[:, None, None, :], logits, -1e30)


def attn_forward(
    row_data,
    utt_count,
    gain_row,
    shift_row,
    bias_u,
    bias_v,
    w_in,
    w_out,
    w_pos,
    key_valid,
    pos_table_b,
):
    model_width = row_data.shape[1]
    frame_len = row_data.shape[0] // utt_count
    normed_b = layer_norm(row_data, gain_row, shift_row).astype(jnp.bfloat16)
    proj_rows = matmul_low(normed_b, w_in)
    query_rows = proj_rows[:, :model_width].reshape(utt_count, frame_len, H, DH)
    key_b = (
        proj_rows[:, model_width : 2 * model_width]
        .astype(jnp.bfloat16)
        .reshape(utt_count, frame_len, model_width)
    )
    value_b = (
        proj_rows[:, 2 * model_width :]
        .astype(jnp.bfloat16)
        .reshape(utt_count, frame_len, model_width)
    )
    all_keys, all_values = (
        lax.all_gather(key_b, "seq", axis=1, tiled=True),
        lax.all_gather(value_b, "seq", axis=1, tiled=True),
    )
    key_heads = all_keys.reshape(utt_count, -1, H, DH)
    value_heads = all_values.reshape(utt_count, -1, H, DH)
    query_u_b = (query_rows + bias_u.reshape(H, DH)).astype(jnp.bfloat16)
    query_v_b = (query_rows + bias_v.reshape(H, DH)).astype(jnp.bfloat16)
    pos_heads = matmul_low(pos_table_b, w_pos).astype(jnp.bfloat16).reshape(-1, H, DH)
    logits = attention_logits(query_u_b, query_v_b, key_heads, pos_heads, key_valid)
    top_score = jnp.max(logits, axis=-1, keepdims=True)
    exp_scores = jnp.exp(logits - top_score)
    row_total = jnp.sum(exp_scores, axis=-1, keepdims=True)
    prob_b = (exp_scores / row_total).astype(jnp.bfloat16)
    log_total = top_score + jnp.log(row_total)
    context = jnp.einsum("uhfl,ulhd->ufhd", prob_b, value_heads, preferred_element_type=jnp.float32)
    context_b = context.astype(jnp.bfloat16).reshape(-1, model_width)
    branch = matmul_low(context_b, w_out)
    kept_data = (
        row_data,
        normed_b,
        query_u_b,
        query_v_b,
        key_heads,
        value_heads,
        pos_heads,
        log_total,
        context_b,
    )
    return (row_data + branch, kept_data)


def attn_backward(grad_rows, kept_data, gain_row, shift_row, w_in, w_out, key_valid, pos_table_b):
    (
        row_data,
        normed_b,
        query_u_b,
        query_v_b,
        key_heads,
        value_heads,
        pos_heads,
        log_total,
        context_b,
    ) = kept_data
    utt_count = query_u_b.shape[0]
    frame_len = query_u_b.shape[1]
    model_width = row_data.shape[1]
    key_len = key_heads.shape[1]
    grad_out_b = grad_rows.astype(jnp.bfloat16)
    g_out = weight_grad(context_b, grad_out_b)
    grad_context_b = (
        matmul_back(grad_out_b, w_out).astype(jnp.bfloat16).reshape(utt_count, frame_len, H, DH)
    )
    logits = attention_logits(query_u_b, query_v_b, key_heads, pos_heads, key_valid)
    prob_rows = jnp.exp(logits - log_total)
    grad_probs = jnp.einsum(
        "ufhd,ulhd->uhfl", grad_context_b, value_heads, preferred_element_type=jnp.float32
    )
    inner_sum = jnp.sum(grad_probs * prob_rows, axis=-1, keepdims=True)
    grad_logits_b = (prob_rows * (grad_probs - inner_sum)).astype(jnp.bfloat16) * 0.125
    grad_query_u = jnp.einsum(
        "uhfl,ulhd->ufhd", grad_logits_b, key_heads, preferred_element_type=jnp.float32
    )
    raw_shape = (utt_count, H, frame_len, pos_heads.shape[0])
    grad_raw_b = skew_back(grad_logits_b.astype(jnp.float32), raw_shape, key_len).astype(
        jnp.bfloat16
    )
    grad_query_v = jnp.einsum(
        "uhfw,whd->ufhd", grad_raw_b, pos_heads, preferred_element_type=jnp.float32
    )
    grad_pos = jnp.einsum(
        "uhfw,ufhd->whd", grad_raw_b, query_v_b, preferred_element_type=jnp.float32
    )
    grad_pos = grad_pos.reshape(-1, model_width)
    g_pos = lax.dot_general(
        pos_table_b.astype(jnp.float32),
        grad_pos,
        (((0,), (0,)), ((), ())),
        precision=HIGHEST_PREC,
        preferred_element_type=jnp.float32,
    )
    prob_b = prob_rows.astype(jnp.bfloat16)
    grad_values = jnp.einsum(
        "uhfl,ufhd->ulhd", prob_b, grad_context_b, preferred_element_type=jnp.float32
    )
    grad_keys = jnp.einsum(
        "uhfl,ufhd->ulhd", grad_logits_b, query_u_b, preferred_element_type=jnp.float32
    )
    own_keys, own_values = (
        lax.psum_scatter(
            grad_keys.reshape(utt_count, key_len, model_width),
            "seq",
            scatter_dimension=1,
            tiled=True,
        ),
        lax.psum_scatter(
            grad_values.reshape(utt_count, key_len, model_width),
            "seq",
            scatter_dimension=1,
            tiled=True,
        ),
    )
    g_bias_u = jnp.sum(grad_query_u, axis=(0, 1)).reshape(-1)
    g_bias_v = jnp.sum(grad_query_v, axis=(0, 1)).reshape(-1)
    grad_proj_b = jnp.concatenate(
        [
            (grad_query_u + grad_query_v).reshape(-1, model_width),
            own_keys.reshape(-1, model_width),
            own_values.reshape(-1, model_width),
        ],
        axis=1,
    ).astype(jnp.bfloat16)
    g_in = weight_grad(normed_b, grad_proj_b)
    grad_normed = matmul_back(grad_proj_b, w_in)
    grad_ln, g_gain, g_shift = jax.vjp(layer_norm, row_data, gain_row, shift_row)[1](grad_normed)
    return (grad_rows + grad_ln, (g_gain, g_shift, g_bias_u, g_bias_v, g_in, g_out, g_pos))


def conv_forward(
    row_data,
    utt_count,
    gain_row,
    shift_row,
    w_in,
    kernel,
    bn_gain,
    bn_shift,
    w_out,
    frame_mask,
    frame_count,
):
    model_width = row_data.shape[1]
    frame_len = row_data.shape[0] // utt_count
    normed_b = layer_norm(row_data, gain_row, shift_row).astype(jnp.bfloat16)
    gate_pair = matmul_low(normed_b, w_in)
    mask_rows = frame_mask.reshape(-1, 1)
    gated_b = (
        (glu_gate(gate_pair) * mask_rows)
        .astype(jnp.bfloat16)
        .reshape(utt_count, frame_len, model_width)
    )
    halo_reach = (kernel.shape[1] - 1) // 2
    padded = extended(gated_b, (("seq", 1),), halo_reach)
    kernel_f = kernel.astype(jnp.float32)
    depth_out = padded[:, 0:frame_len].astype(jnp.float32) * kernel_f[:, 0]
    for tap_idx in range(1, kernel.shape[1]):
        depth_out = (
            depth_out
            + padded[:, tap_idx : tap_idx + frame_len].astype(jnp.float32) * kernel_f[:, tap_idx]
        )
    weight_mask = frame_mask[:, :, None]
    sum_local = jnp.sum(depth_out * weight_mask, axis=(0, 1))
    square_local = jnp.sum(depth_out * depth_out * weight_mask, axis=(0, 1))
    sum_all, square_all = lax.psum((sum_local, square_local), ("dp", "seq"))
    mean_val = sum_all / frame_count
    variance = square_all / frame_count - mean_val * mean_val
    inv_std = lax.rsqrt(variance + 1e-05)
    normal = (depth_out - mean_val) * inv_std * bn_gain + bn_shift
    active_b = jax.nn.silu(normal).astype(jnp.bfloat16).reshape(-1, model_width)
    branch = matmul_low(active_b, w_out)
    kept_data = (
        row_data,
        normed_b,
        gate_pair,
        padded,
        depth_out,
        mean_val,
        inv_std,
        normal,
        active_b,
    )
    return (row_data + branch, kept_data)


def conv_backward(
    grad_rows, kept_data, gain_row, shift_row, w_in, kernel, bn_gain, w_out, frame_mask, frame_count
):
    row_data, normed_b, gate_pair, padded, depth_out, mean_val, inv_std, normal, active_b = (
        kept_data
    )
    frame_len = depth_out.shape[1]
    model_width = depth_out.shape[2]
    grad_out_b = grad_rows.astype(jnp.bfloat16)
    g_out = weight_grad(active_b, grad_out_b)
    grad_active = matmul_back(grad_out_b, w_out).reshape(depth_out.shape)
    grad_normal = jax.vjp(jax.nn.silu, normal)[1](grad_active)[0]
    centred_hat = (depth_out - mean_val) * inv_std
    g_bn_gain = jnp.sum(grad_normal * centred_hat, axis=(0, 1))
    g_bn_shift = jnp.sum(grad_normal, axis=(0, 1))
    grad_hat = grad_normal * bn_gain
    part_one = jnp.sum(grad_hat, axis=(0, 1))
    part_two = jnp.sum(grad_hat * depth_out, axis=(0, 1))
    part_one, part_two = lax.psum((part_one, part_two), ("dp", "seq"))
    grad_inv = part_two - mean_val * part_one
    grad_var = -0.5 * inv_std * inv_std * inv_std * grad_inv
    grad_mean = -inv_std * part_one - 2.0 * mean_val * grad_var
    weight_mask = frame_mask[:, :, None]
    grad_depth_b = (
        grad_hat * inv_std
        + weight_mask * (grad_mean / frame_count + 2.0 * depth_out * grad_var / frame_count)
    ).astype(jnp.bfloat16)
    halo_reach = (kernel.shape[1] - 1) // 2
    grad_padded = extended(grad_depth_b, (("seq", 1),), halo_reach)
    kernel_f = kernel.astype(jnp.float32)
    grad_depth_f = grad_depth_b.astype(jnp.float32)
    grad_gated = jnp.zeros(depth_out.shape, jnp.float32)
    kernel_cols = []
    for tap_idx in range(kernel.shape[1]):
        begin_at = 2 * halo_reach - tap_idx
        grad_gated = (
            grad_gated
            + grad_padded[:, begin_at : begin_at + frame_len].astype(jnp.float32)
            * kernel_f[:, tap_idx]
        )
        kernel_cols.append(
            jnp.sum(
                padded[:, tap_idx : tap_idx + frame_len].astype(jnp.float32) * grad_depth_f,
                axis=(0, 1),
            )
        )
    g_kernel = jnp.stack(kernel_cols, axis=1)
    grad_gate_b = jax.vjp(glu_gate, gate_pair)[1](
        (grad_gated * weight_mask).reshape(-1, model_width)
    )[0]
    grad_gate_b = grad_gate_b.astype(jnp.bfloat16)
    g_in = weight_grad(normed_b, grad_gate_b)
    grad_normed = matmul_back(grad_gate_b, w_in)
    grad_ln, g_gain, g_shift = jax.vjp(layer_norm, row_data, gain_row, shift_row)[1](grad_normed)
    return (grad_rows + grad_ln, (g_gain, g_shift, g_in, g_kernel, g_bn_gain, g_bn_shift, g_out))


def layer_forward(values, weights, frame_mask, key_valid, frame_count, pos_table_b):
    (
        gain_set,
        shift_set,
        rel_set,
        up_pair,
        down_pair,
        attn_in_w,
        attn_out_w,
        pos_w,
        conv_in_w,
        kernel,
        conv_out_w,
    ) = weights
    gain_f = gain_set.astype(jnp.float32)
    shift_f = shift_set.astype(jnp.float32)
    rel_f = rel_set.astype(jnp.float32)
    utt_count = values.shape[0]
    row_data = values.reshape(-1, values.shape[2])
    row_data, kept_one = ffn_forward(row_data, gain_f[0], shift_f[0], up_pair[0], down_pair[0])
    row_data, kept_attn = attn_forward(
        row_data,
        utt_count,
        gain_f[1],
        shift_f[1],
        rel_f[0],
        rel_f[1],
        attn_in_w,
        attn_out_w,
        pos_w,
        key_valid,
        pos_table_b,
    )
    row_data, kept_conv = conv_forward(
        row_data,
        utt_count,
        gain_f[2],
        shift_f[2],
        conv_in_w,
        kernel,
        gain_f[5],
        shift_f[5],
        conv_out_w,
        frame_mask,
        frame_count,
    )
    row_data, kept_two = ffn_forward(row_data, gain_f[3], shift_f[3], up_pair[1], down_pair[1])
    result = layer_norm(row_data, gain_f[4], shift_f[4])
    return (result.reshape(values.shape), (kept_one, kept_attn, kept_conv, kept_two, row_data))


def layer_backward(
    grad_values, kept_data, weights, frame_mask, key_valid, frame_count, pos_table_b
):
    (
        gain_set,
        shift_set,
        rel_set,
        up_pair,
        down_pair,
        attn_in_w,
        attn_out_w,
        pos_w,
        conv_in_w,
        kernel,
        conv_out_w,
    ) = weights
    gain_f = gain_set.astype(jnp.float32)
    shift_f = shift_set.astype(jnp.float32)
    kept_one, kept_attn, kept_conv, kept_two, last_rows = kept_data
    grad_rows = grad_values.reshape(-1, grad_values.shape[2])
    grad_rows, g_gain_last, g_shift_last = jax.vjp(layer_norm, last_rows, gain_f[4], shift_f[4])[1](
        grad_rows
    )
    grad_rows, two_grads = ffn_backward(
        grad_rows, kept_two, gain_f[3], shift_f[3], up_pair[1], down_pair[1]
    )
    grad_rows, conv_grads = conv_backward(
        grad_rows,
        kept_conv,
        gain_f[2],
        shift_f[2],
        conv_in_w,
        kernel,
        gain_f[5],
        conv_out_w,
        frame_mask,
        frame_count,
    )
    grad_rows, attn_grads = attn_backward(
        grad_rows, kept_attn, gain_f[1], shift_f[1], attn_in_w, attn_out_w, key_valid, pos_table_b
    )
    grad_rows, one_grads = ffn_backward(
        grad_rows, kept_one, gain_f[0], shift_f[0], up_pair[0], down_pair[0]
    )
    grad_gains = jnp.stack(
        [one_grads[0], attn_grads[0], conv_grads[0], two_grads[0], g_gain_last, conv_grads[4]]
    )
    grad_shifts = jnp.stack(
        [one_grads[1], attn_grads[1], conv_grads[1], two_grads[1], g_shift_last, conv_grads[5]]
    )
    grad_rel = jnp.stack([attn_grads[2], attn_grads[3]])
    grad_up = jnp.stack([one_grads[2], two_grads[2]])
    grad_down = jnp.stack([one_grads[3], two_grads[3]])
    layer_grads = (
        grad_gains,
        grad_shifts,
        grad_rel,
        grad_up,
        grad_down,
        attn_grads[4],
        attn_grads[5],
        attn_grads[6],
        conv_grads[2],
        conv_grads[3],
        conv_grads[6],
    )
    return (grad_rows.reshape(grad_values.shape), layer_grads)


def gather_forward(shards, layer_idx):
    pieces = tuple((member[layer_idx] for member in shards))
    return (
        lax.all_gather(pieces[0], ("dp", "seq"), axis=1, tiled=True),
        lax.all_gather(pieces[1], ("dp", "seq"), axis=1, tiled=True),
        lax.all_gather(pieces[2], ("dp", "seq"), axis=1, tiled=True),
        lax.all_gather(pieces[3], ("dp", "seq"), axis=1, tiled=True),
        lax.all_gather(pieces[4], ("dp", "seq"), axis=1, tiled=True),
        lax.all_gather(pieces[5], ("dp", "seq"), axis=0, tiled=True),
        lax.all_gather(pieces[6], ("dp", "seq"), axis=0, tiled=True),
        lax.all_gather(pieces[7], ("dp", "seq"), axis=0, tiled=True),
        lax.all_gather(pieces[8], ("dp", "seq"), axis=0, tiled=True),
        lax.all_gather(pieces[9], ("dp", "seq"), axis=0, tiled=True),
        lax.all_gather(pieces[10], ("dp", "seq"), axis=0, tiled=True),
    )


def gather_backward(shards, layer_idx):
    pieces = tuple((member[layer_idx] for member in shards))
    return (
        lax.all_gather(pieces[0], ("dp", "seq"), axis=1, tiled=True),
        lax.all_gather(pieces[1], ("dp", "seq"), axis=1, tiled=True),
        lax.all_gather(pieces[2], ("dp", "seq"), axis=1, tiled=True),
        lax.all_gather(pieces[3], ("dp", "seq"), axis=1, tiled=True),
        lax.all_gather(pieces[4], ("dp", "seq"), axis=1, tiled=True),
        lax.all_gather(pieces[5], ("dp", "seq"), axis=0, tiled=True),
        lax.all_gather(pieces[6], ("dp", "seq"), axis=0, tiled=True),
        lax.all_gather(pieces[7], ("dp", "seq"), axis=0, tiled=True),
        lax.all_gather(pieces[8], ("dp", "seq"), axis=0, tiled=True),
        lax.all_gather(pieces[9], ("dp", "seq"), axis=0, tiled=True),
        lax.all_gather(pieces[10], ("dp", "seq"), axis=0, tiled=True),
    )


def local_general(
    frames,
    lengths,
    cotangent,
    gains,
    shifts,
    rel_bias,
    ffn_up,
    ffn_down,
    attn_in,
    attn_out,
    pos_proj,
    conv_in,
    depthwise,
    conv_out,
):
    shards = (
        gains,
        shifts,
        rel_bias,
        ffn_up,
        ffn_down,
        attn_in,
        attn_out,
        pos_proj,
        conv_in,
        depthwise,
        conv_out,
    )
    groups = lax.axis_size("dp")
    seq_devices = lax.axis_size("seq")
    local_utts = frames.shape[0]
    frame_len = frames.shape[1]
    model_width = frames.shape[2]
    utt_per = local_utts // MB
    length = frame_len * seq_devices
    seq_start = lax.axis_index("seq") * frame_len
    first_utt = lax.axis_index("dp") * local_utts
    own_lengths = lax.dynamic_slice_in_dim(lengths, first_utt, local_utts)
    lengths_grid = lengths.reshape(groups, MB, utt_per)
    offsets = seq_start + frame_len - 1 - jnp.arange(length + frame_len - 1, dtype=jnp.int32)
    pos_table_b = sinusoid(offsets, model_width).astype(jnp.bfloat16)
    frame_pos = seq_start + jnp.arange(frame_len, dtype=jnp.int32)
    key_pos = jnp.arange(length, dtype=jnp.int32)
    result_list = []
    grad_list = []
    full_sums = [None] * NL
    for micro_idx in range(MB):
        lens_here = own_lengths[micro_idx * utt_per : (micro_idx + 1) * utt_per]
        frame_mask = (frame_pos[None, :] < lens_here[:, None]).astype(jnp.float32)
        key_valid = key_pos[None, :] < lens_here[:, None]
        frame_count = jnp.sum(lengths_grid[:, micro_idx]).astype(jnp.float32)
        values = frames[micro_idx * utt_per : (micro_idx + 1) * utt_per]
        held_weights = []
        layer_idx = 0
        weights = gather_forward(shards, layer_idx)
        values, kept_data = layer_forward(
            values, weights, frame_mask, key_valid, frame_count, pos_table_b
        )
        saved_acts = [kept_data]
        held_weights.append(weights)
        result_list.append(values)
        grad_values = cotangent[micro_idx * utt_per : (micro_idx + 1) * utt_per]
        for layer_idx in reversed(range(NL)):
            weights = gather_backward(shards, layer_idx)
            grad_values, layer_grads = layer_backward(
                grad_values,
                saved_acts[layer_idx],
                weights,
                frame_mask,
                key_valid,
                frame_count,
                pos_table_b,
            )
            if full_sums[layer_idx] is None:
                full_sums[layer_idx] = layer_grads
            else:
                full_sums[layer_idx] = jax.tree.map(jnp.add, full_sums[layer_idx], layer_grads)
        grad_list.append(grad_values)
    stacked = tuple((jnp.stack([full_sums[0][member]]) for member in range(11)))
    final_grads = (
        lax.psum_scatter(stacked[0], ("dp", "seq"), scatter_dimension=2, tiled=True),
        lax.psum_scatter(stacked[1], ("dp", "seq"), scatter_dimension=2, tiled=True),
        lax.psum_scatter(stacked[2], ("dp", "seq"), scatter_dimension=2, tiled=True),
        lax.psum_scatter(stacked[3], ("dp", "seq"), scatter_dimension=2, tiled=True),
        lax.psum_scatter(stacked[4], ("dp", "seq"), scatter_dimension=2, tiled=True),
        lax.psum_scatter(stacked[5], ("dp", "seq"), scatter_dimension=1, tiled=True),
        lax.psum_scatter(stacked[6], ("dp", "seq"), scatter_dimension=1, tiled=True),
        lax.psum_scatter(stacked[7], ("dp", "seq"), scatter_dimension=1, tiled=True),
        lax.psum_scatter(stacked[8], ("dp", "seq"), scatter_dimension=1, tiled=True),
        lax.psum_scatter(stacked[9], ("dp", "seq"), scatter_dimension=1, tiled=True),
        lax.psum_scatter(stacked[10], ("dp", "seq"), scatter_dimension=1, tiled=True),
    )
    mixed = jnp.concatenate(result_list, axis=0)
    grad_frames = jnp.concatenate(grad_list, axis=0)
    return (
        mixed,
        grad_frames,
        final_grads[0],
        final_grads[1],
        final_grads[2],
        final_grads[3],
        final_grads[4],
        final_grads[5],
        final_grads[6],
        final_grads[7],
        final_grads[8],
        final_grads[9],
        final_grads[10],
    )


NT = (((1,), (1,)), ((), ()))
TN = (((0,), (0,)), ((), ()))
NN = (((1,), (0,)), ((), ()))
MESH = pl.DeviceIdType.MESH
UTTS = 4
COLS = (2048, 2048, 1536, 512, 512, 1024, 512, 128)
VMEM_LIMIT = 60 * 1024 * 1024


def fits_whole(mesh):
    return mesh.shape["dp"] == 4 and mesh.shape["seq"] == MB * UTTS


def dotf(left, right, dims=NN):
    return lax.dot_general(left, right, dims, preferred_element_type=jnp.float32)


def place():
    dp = lax.axis_index("dp")
    sq = lax.axis_index("seq")
    return dp, sq, lax.div(dp, 2), lax.rem(dp, 2), lax.div(sq, 2), lax.rem(sq, 2)


def flip_if(value, bit):
    return 1 - value if bit else value


def partners():
    dp, sq, x, c, z, y = place()
    even = c == 0
    core = (x * 2 + 1 - c, sq)
    xdev = ((1 - x) * 2 + c, sq)
    ydev = (dp, z * 2 + 1 - y)
    first = (jnp.where(even, ydev[0], xdev[0]), jnp.where(even, ydev[1], xdev[1]))
    second = (jnp.where(even, xdev[0], ydev[0]), jnp.where(even, xdev[1], ydev[1]))
    return core, xdev, first, second


def rank_of(color, a, b, k):
    _, _, x, _, z, y = place()
    even = color == 0
    xx = jnp.where(even, x + a * (1 - 2 * x), x + b * (1 - 2 * x))
    yy = jnp.where(even, y + b * (1 - 2 * y), y + a * (1 - 2 * y))
    return xx * 16 + color * 8 + lax.rem(z + k, 4) * 2 + yy


def greet(devices):
    barrier = pltpu.get_barrier_semaphore()
    for device in devices:
        pl.semaphore_signal(barrier, inc=1, device_id=device, device_id_type=MESH)
    pl.semaphore_wait(barrier, len(devices))


def seq_peers(dp, sq, count):
    return [(dp, lax.rem(sq + k, count)) for k in range(1, count)]


def remote(src, dst, send, recv, device):
    return pltpu.make_async_remote_copy(
        src_ref=src, dst_ref=dst, send_sem=send, recv_sem=recv, device_id=device, device_id_type=MESH
    )


def gather_kernel(
    w_ref, d_ref, f_ref, c_ref, w_all, d_all, f_all, c_all, send, recv, row_send, row_recv, own
):
    dp, sq, x, c, z, y = place()
    core, xdev, first, second = partners()
    count = f_ref.shape[0]
    greet(seq_peers(dp, sq, count) + [core, xdev])
    wr = w_ref.shape[0]
    dr = d_ref.shape[1]

    def rows_of(rank):
        return (
            w_all.at[pl.ds(pl.multiple_of(rank * wr, 16), wr), :],
            d_all.at[:, pl.ds(pl.multiple_of(rank * dr, 16), dr), :],
        )

    def pair(rank, device, slot, landing, mine=False):
        w_dst, d_dst = rows_of(rank)
        w_src, d_src = (w_ref, d_ref) if mine else (w_dst, d_dst)
        return (
            remote(w_src, w_dst, send.at[0, slot], recv.at[0, landing], device),
            remote(d_src, d_dst, send.at[1, slot], recv.at[1, landing], device),
        )

    started = []

    def ship(*args, **kwargs):
        for copy in pair(*args, **kwargs):
            copy.start()
            started.append(copy)

    def arrive(color, a, b, k):
        slot = a * 8 + b * 4 + k + (0 if color is c else 16)
        for copy in pair(rank_of(color, a, b, k), core, 0, slot):
            copy.wait_recv()

    def row_copy(src, dst, which, k):
        to = lax.rem(sq + k, count)
        return remote(
            src.at[to], dst.at[sq], row_send.at[which, k - 1], row_recv.at[which, count - 1 - k], (dp, to)
        )

    for k in range(1, count):
        copy = row_copy(f_ref, f_all, 0, k)
        copy.start()
        started.append(copy)
    mine = rank_of(c, 0, 0, 0)
    ship(mine, second, 15, 8, mine=True)
    ship(mine, first, 3, 4, mine=True)
    for k in (1, 3, 2):
        ship(mine, (dp, lax.rem(z + k, 4) * 2 + y), k - 1, 4 - k, mine=True)
    ship(mine, core, 16, 16, mine=True)
    w_own, d_own = rows_of(mine)
    locals_ = [
        pltpu.make_async_copy(w_ref, w_own, own.at[0]),
        pltpu.make_async_copy(d_ref, d_own, own.at[1]),
        pltpu.make_async_copy(f_ref.at[sq], f_all.at[sq], own.at[2]),
        pltpu.make_async_copy(c_ref.at[sq], c_all.at[sq], own.at[3]),
    ]
    for copy in locals_:
        copy.start()
    for k in range(1, count):
        copy = row_copy(c_ref, c_all, 1, k)
        copy.start()
        started.append(copy)

    def to_core(a, b, k):
        ship(rank_of(c, a, b, k), core, 16 + a * 8 + b * 4 + k - (1 if a * 8 + b * 4 + k > 15 else 0), 16 + a * 8 + b * 4 + k)

    rounds = (0, 1, 3, 2)
    last = None
    for k in rounds:
        if k:
            arrive(c, 0, 0, k)
            ship(rank_of(c, 0, 0, k), second, 8 + k - 1, 8 + k)
            ship(rank_of(c, 0, 0, k), first, 4 + k - 1, 4 + k)
            to_core(0, 0, k)
        arrive(c, 0, 1, k)
        ship(rank_of(c, 0, 1, k), second, 11 + k, 12 + k)
        to_core(0, 1, k)
        if last is not None:
            for b in (0, 1):
                arrive(c, 1, b, last)
                to_core(1, b, last)
        last = k
    for b in (0, 1):
        arrive(c, 1, b, last)
        to_core(1, b, last)
    other = 1 - c
    for k in rounds:
        for a, b in ((0, 0), (0, 1), (1, 0), (1, 1)):
            arrive(other, a, b, k)
    for which, (src, dst) in enumerate(((f_ref, f_all), (c_ref, c_all))):
        for k in range(1, count):
            remote(
                src.at[sq], dst.at[lax.rem(sq + k, count)], row_send.at[which, k - 1], row_recv.at[which, k - 1], core
            ).wait_recv()
    for copy in locals_:
        copy.wait()
    for copy in started:
        copy.wait_send()


def gather_all(w, d, f, c):
    count = f.shape[0]
    vm = pl.BlockSpec(memory_space=pltpu.VMEM)
    hbm = pl.BlockSpec(memory_space=pl.ANY)
    return pl.pallas_call(
        gather_kernel,
        in_specs=[vm] * 4,
        out_specs=[hbm] * 4,
        out_shape=[
            jax.ShapeDtypeStruct((w.shape[0] * 32, w.shape[1]), w.dtype),
            jax.ShapeDtypeStruct((d.shape[0], d.shape[1] * 32, d.shape[2]), d.dtype),
            jax.ShapeDtypeStruct(f.shape, f.dtype),
            jax.ShapeDtypeStruct(c.shape, c.dtype),
        ],
        scratch_shapes=[
            pltpu.SemaphoreType.DMA((2, 32)),
            pltpu.SemaphoreType.DMA((2, 32)),
            pltpu.SemaphoreType.DMA((2, count - 1)),
            pltpu.SemaphoreType.DMA((2, count - 1)),
            pltpu.SemaphoreType.DMA((4,)),
        ],
        compiler_params=pltpu.CompilerParams(collective_id=0, has_side_effects=True),
        name="gather_all",
    )(w, d, f, c)


def scatter_kernel(
    w_ref, d_ref, m_ref, g_ref, w_out, d_out, m_all, g_all,
    w0, d0, w1, d1, w2, d2, w3, d3, send, recv, row_send, row_recv, own,
):
    dp, sq, x, c, z, y = place()
    core, xdev, first, second = partners()
    count = m_all.shape[0]
    width = m_all.shape[1]
    greet(seq_peers(dp, sq, count) + [core, xdev])
    wr = w_out.shape[0]
    dr = d_out.shape[1]

    def w_rows(rank):
        return pl.ds(pl.multiple_of(rank * wr, 16), wr)

    def d_rows(rank):
        return pl.ds(pl.multiple_of(rank * dr, 16), dr)

    def row_copy(src, dst, which, k):
        to = lax.rem(sq + k, count)
        return remote(
            src.at[pl.ds(pl.multiple_of(to * width, 16), width), :],
            dst.at[sq],
            row_send.at[which, k - 1],
            row_recv.at[which, count - 1 - k],
            (dp, to),
        )

    def core_copies(slot):
        rank = rank_of(1 - c, lax.div(slot, 8), lax.rem(lax.div(slot, 4), 2), lax.rem(slot, 4))
        return (
            remote(w_ref.at[w_rows(rank), :], w0.at[slot], send.at[0, slot], recv.at[0, slot], core),
            remote(d_ref.at[:, d_rows(rank), :], d0.at[slot], send.at[1, slot], recv.at[1, slot], core),
        )

    def second_copies(slot):
        return (
            remote(w0.at[8 + slot], w1.at[slot], send.at[0, 16 + slot], recv.at[0, 16 + slot], second),
            remote(d0.at[8 + slot], d1.at[slot], send.at[1, 16 + slot], recv.at[1, 16 + slot], second),
        )

    def first_copies(slot):
        return (
            remote(w0.at[4 + slot], w2.at[slot], send.at[0, 24 + slot], recv.at[0, 24 + slot], first),
            remote(d0.at[4 + slot], d2.at[slot], send.at[1, 24 + slot], recv.at[1, 24 + slot], first),
        )

    def z_copies(k):
        to = (dp, lax.rem(z + k, 4) * 2 + y)
        return (
            remote(w0.at[k], w3.at[3 - k], send.at[0, 27 + k], recv.at[0, 31 - k], to),
            remote(d0.at[k], d3.at[3 - k], send.at[1, 27 + k], recv.at[1, 31 - k], to),
        )

    def begin(copies):
        for copy in copies:
            copy.start()

    def landed(copies):
        for copy in copies:
            copy.wait_recv()

    def add_w(slot, other):
        w0[slot] = (w0[slot].astype(jnp.float32) + other.astype(jnp.float32)).astype(jnp.bfloat16)

    def add_d(slot, other):
        d0[slot] = (d0[slot].astype(jnp.float32) + other.astype(jnp.float32)).astype(jnp.bfloat16)

    @pl.loop(0, 16)
    def _(step):
        begin(core_copies(15 - step))

    for which, (src, dst) in enumerate(((g_ref, g_all), (m_ref, m_all))):
        for k in range(1, count):
            row_copy(src, dst, which, k).start()
    here = pl.ds(pl.multiple_of(sq * width, 16), width)
    locals_ = [
        pltpu.make_async_copy(m_ref.at[here, :], m_all.at[sq], own.at[0]),
        pltpu.make_async_copy(g_ref.at[here, :], g_all.at[sq], own.at[1]),
    ]
    begin(locals_)

    def take_core(slot):
        landed(core_copies(slot))
        rank = rank_of(c, lax.div(slot, 8), lax.rem(lax.div(slot, 4), 2), lax.rem(slot, 4))
        add_w(slot, w_ref[w_rows(rank), :])
        add_d(slot, d_ref[:, d_rows(rank), :])

    @pl.loop(0, 8)
    def _(step):
        take_core(15 - step)
        begin(second_copies(7 - step))

    @pl.loop(0, 4)
    def _(step):
        slot = 7 - step
        take_core(slot)
        landed(second_copies(slot))
        add_w(slot, w1[slot])
        add_d(slot, d1[slot])
        begin(first_copies(slot - 4))

    @pl.loop(0, 3)
    def _(step):
        slot = 3 - step
        take_core(slot)
        landed(second_copies(slot))
        add_w(slot, w1[slot])
        add_d(slot, d1[slot])
        landed(first_copies(slot))
        add_w(slot, w2[slot])
        add_d(slot, d2[slot])
        begin(z_copies(slot))

    take_core(0)
    landed(second_copies(0))
    landed(first_copies(0))
    for k in (1, 2, 3):
        landed(z_copies(k))

    def total(base, parts):
        value = base.astype(jnp.float32)
        for part in parts:
            value = value + part.astype(jnp.float32)
        return value

    w_out[...] = total(w0[0], (w1[0], w2[0], w3[0], w3[1], w3[2]))
    d_out[...] = total(d0[0], (d1[0], d2[0], d3[0], d3[1], d3[2]))
    for which, dst in enumerate((g_all, m_all)):
        for k in range(1, count):
            remote(
                m_ref.at[here, :], dst.at[lax.rem(sq + k, count)], row_send.at[which, k - 1], row_recv.at[which, k - 1], core
            ).wait_recv()

    def sent(copies):
        for copy in copies:
            copy.wait_send()

    @pl.loop(0, 16)
    def _(slot):
        sent(core_copies(slot))

    @pl.loop(0, 8)
    def _(slot):
        sent(second_copies(slot))

    @pl.loop(0, 4)
    def _(slot):
        sent(first_copies(slot))

    for k in (1, 2, 3):
        sent(z_copies(k))
    for which, (src, dst) in enumerate(((g_ref, g_all), (m_ref, m_all))):
        for k in range(1, count):
            row_copy(src, dst, which, k).wait_send()
    for copy in locals_:
        copy.wait()


def scatter_all(w, d, m, g, count):
    vm = pl.BlockSpec(memory_space=pltpu.VMEM)
    hbm = pl.BlockSpec(memory_space=pl.ANY)
    wr, wc = w.shape[0] // 32, w.shape[1]
    dr, dc = d.shape[1] // 32, d.shape[2]
    rows = m.shape[0] // count
    bf = jnp.bfloat16
    scratch = []
    for n in (16, 8, 4, 3):
        scratch += [pltpu.VMEM((n, wr, wc), bf), pltpu.VMEM((n, d.shape[0], dr, dc), bf)]
    row_shape = jax.ShapeDtypeStruct((count, rows, m.shape[1]), bf)
    return pl.pallas_call(
        scatter_kernel,
        in_specs=[vm] * 4,
        out_specs=[vm, vm, hbm, hbm],
        out_shape=[
            jax.ShapeDtypeStruct((wr, wc), jnp.float32),
            jax.ShapeDtypeStruct((d.shape[0], dr, dc), jnp.float32),
            row_shape,
            row_shape,
        ],
        scratch_shapes=scratch
        + [
            pltpu.SemaphoreType.DMA((2, 32)),
            pltpu.SemaphoreType.DMA((2, 32)),
            pltpu.SemaphoreType.DMA((2, count - 1)),
            pltpu.SemaphoreType.DMA((2, count - 1)),
            pltpu.SemaphoreType.DMA((2,)),
        ],
        compiler_params=pltpu.CompilerParams(
            collective_id=1, has_side_effects=True, vmem_limit_bytes=VMEM_LIMIT
        ),
        name="scatter_all",
    )(w, d, m, g)


def batch_sum_kernel(s_ref, o_ref, buf, send, recv):
    dp, sq, *_ = place()
    base = lax.div(sq, UTTS) * UTTS
    me = dp * UTTS + lax.rem(sq, UTTS)
    size = buf.shape[0]

    def device(j):
        r = lax.rem(me + j, size)
        return (lax.div(r, UTTS), base + lax.rem(r, UTTS))

    def copy(j):
        return remote(s_ref, buf.at[me], send.at[j - 1], recv.at[size - 1 - j], device(j))

    greet([device(j) for j in range(1, size)])
    for j in range(1, size):
        copy(j).start()
    buf[me] = s_ref[...]
    for j in range(1, size):
        remote(s_ref, buf.at[lax.rem(me + j, size)], send.at[j - 1], recv.at[j - 1], device(j)).wait_recv()
    o_ref[...] = jnp.sum(buf[...], axis=0)
    for j in range(1, size):
        copy(j).wait_send()


def batch_sum(sums, ident):
    vm = pl.BlockSpec(memory_space=pltpu.VMEM)
    size = 4 * UTTS
    return pl.pallas_call(
        batch_sum_kernel,
        in_specs=[vm],
        out_specs=vm,
        out_shape=jax.ShapeDtypeStruct(sums.shape, jnp.float32),
        scratch_shapes=[
            pltpu.VMEM((size,) + sums.shape, jnp.float32),
            pltpu.SemaphoreType.DMA((size - 1,)),
            pltpu.SemaphoreType.DMA((size - 1,)),
        ],
        compiler_params=pltpu.CompilerParams(collective_id=ident, has_side_effects=True),
        name="batch_sum",
    )(sums)


def att_fwd_kernel(len_ref, qu_ref, qv_ref, k_ref, v_ref, t_ref, ctx_ref, p_ref, *, tq):
    keys = k_ref.shape[0]
    span = keys + tq
    valid = lax.broadcasted_iota(jnp.int32, (1, keys), 1) < len_ref[0]
    for h in range(2):
        cols = slice(h * DH, (h + 1) * DH)
        k = k_ref[:, cols]
        v = v_ref[:, cols]
        for i in range(keys // tq):
            rows = slice(i * tq, (i + 1) * tq)
            start = keys - tq - i * tq
            content = dotf(qu_ref[rows, cols], k, NT)
            raw = dotf(qv_ref[rows, cols], t_ref[start : start + span, cols], NT)
            pos = pltpu.roll(raw, keys + 1, 1, stride=1, stride_axis=0)[:, :keys]
            s = jnp.where(valid, (content + pos) * 0.125, -1e30)
            e = jnp.exp(s - jnp.max(s, axis=1, keepdims=True))
            p = (e * (1.0 / jnp.sum(e, axis=1, keepdims=True))).astype(jnp.bfloat16)
            p_ref[h, rows, :] = p
            ctx_ref[rows, cols] = dotf(p, v).astype(jnp.bfloat16)


def att_fwd(length, qu, qv, k, v, table, tq=128):
    rows, width = qu.shape
    blk = pl.BlockSpec((rows, 128), lambda h, *_: (0, h))
    tab = pl.BlockSpec((2 * rows, 128), lambda h, *_: (0, h))
    return pl.pallas_call(
        lambda *refs: att_fwd_kernel(*refs, tq=tq),
        grid_spec=pltpu.PrefetchScalarGridSpec(
            num_scalar_prefetch=1,
            grid=(width // 128,),
            in_specs=[blk] * 4 + [tab],
            out_specs=[blk, pl.BlockSpec((2, rows, rows), lambda h, *_: (h, 0, 0))],
        ),
        out_shape=[
            jax.ShapeDtypeStruct((rows, width), jnp.bfloat16),
            jax.ShapeDtypeStruct((width // DH, rows, rows), jnp.bfloat16),
        ],
        name="att_fwd",
    )(length, qu, qv, k, v, table)


def att_bwd_kernel(
    p_ref, g_ref, qu_ref, qv_ref, k_ref, v_ref, t_ref,
    dqu_ref, dqv_ref, dk_ref, dv_ref, dt_ref, ds_sc, dt_sc, *, tq,
):
    keys = k_ref.shape[0]
    span = keys + tq
    low = jnp.bfloat16
    flip = (
        lax.broadcasted_iota(jnp.int32, (tq, tq), 0) + lax.broadcasted_iota(jnp.int32, (tq, tq), 1) == tq - 1
    ).astype(low)
    pad = jnp.zeros((tq, tq), jnp.float32)
    for h in range(2):
        cols = slice(h * DH, (h + 1) * DH)
        k = k_ref[:, cols]
        v = v_ref[:, cols]
        dt_sc[...] = jnp.zeros_like(dt_sc)
        for i in range(keys // tq):
            rows = slice(i * tq, (i + 1) * tq)
            start = keys - tq - i * tq
            dp = dotf(g_ref[rows, cols], v, NT)
            pf = p_ref[h, rows, :].astype(jnp.float32)
            ds = (pf * (dp - jnp.sum(dp * pf, axis=1, keepdims=True))).astype(low)
            ds_sc[rows, :] = ds
            dqu_ref[rows, cols] = dotf(ds, k) * 0.125
            back = jnp.concatenate([dotf(flip, ds), pad], axis=1)
            raw = pltpu.roll(back, 0, 1, stride=1, stride_axis=0).astype(low)
            dqv = dotf(raw, t_ref[start : start + span, cols]).astype(low)
            dqv_ref[rows, cols] = dotf(flip, dqv) * 0.125
            qv = dotf(flip, qv_ref[rows, cols]).astype(low)
            dt_sc[start : start + span, :] += dotf(raw, qv, TN)
        dt_ref[:, cols] = (dt_sc[...] * 0.125).astype(low)
        dk_ref[:, cols] = dotf(ds_sc[...], qu_ref[:, cols], TN) * 0.125
        dv_ref[:, cols] = dotf(p_ref[h], g_ref[:, cols], TN)


def att_bwd(p, g, qu, qv, k, v, table, tq=128):
    rows, width = qu.shape
    blk = pl.BlockSpec((rows, 128), lambda h: (0, h))
    tab = pl.BlockSpec((2 * rows, 128), lambda h: (0, h))
    out = jax.ShapeDtypeStruct((rows, width), jnp.float32)
    return pl.pallas_call(
        lambda *refs: att_bwd_kernel(*refs, tq=tq),
        grid=(width // 128,),
        in_specs=[pl.BlockSpec((2, rows, rows), lambda h: (h, 0, 0))] + [blk] * 5 + [tab],
        out_specs=[blk] * 4 + [tab],
        out_shape=[out] * 4 + [jax.ShapeDtypeStruct((2 * rows, width), jnp.bfloat16)],
        scratch_shapes=[pltpu.VMEM((rows, rows), jnp.bfloat16), pltpu.VMEM((2 * rows, DH), jnp.float32)],
        name="att_bwd",
    )(p, g, qu, qv, k, v, table)


def position_table(length, width):
    offsets = (length - 1 - np.arange(2 * length)).astype(np.float32)
    half = width // 2
    steps = np.arange(half, dtype=np.float32) * np.float32(-2.0 * math.log(10000.0) / width)
    angles = (offsets[:, None] * np.exp(steps)[None, :]).astype(np.float64)
    table = np.concatenate([np.sin(angles), np.cos(angles)], axis=1)
    return jnp.asarray(table.astype(np.float32)).astype(jnp.bfloat16)


def shifted_sum(values, kernel_f, reverse):
    taps = kernel_f.shape[1]
    reach = (taps - 1) // 2
    padded = jnp.pad(values, ((reach, reach), (0, 0)))
    rows = values.shape[0]
    total = None
    for k in range(taps):
        at = taps - 1 - k if reverse else k
        term = padded[at : at + rows].astype(jnp.float32) * kernel_f[:, k]
        total = term if total is None else total + term
    return total


def tap_grads(values, grad, taps):
    reach = (taps - 1) // 2
    padded = jnp.pad(values, ((reach, reach), (0, 0)))
    rows = values.shape[0]
    grad_f = grad.astype(jnp.float32)
    return jnp.stack(
        [jnp.sum(padded[k : k + rows].astype(jnp.float32) * grad_f, axis=0) for k in range(taps)]
    )


def local_whole(
    frames,
    lengths,
    cotangent,
    gains,
    shifts,
    rel_bias,
    ffn_up,
    ffn_down,
    attn_in,
    attn_out,
    pos_proj,
    conv_in,
    depthwise,
    conv_out,
):
    low = jnp.bfloat16
    dp, sq = lax.axis_index("dp"), lax.axis_index("seq")
    count, width_rows, model = frames.shape
    length = count * 0 + width_rows * lax.axis_size("seq")
    taps = depthwise.shape[2]
    small = jnp.concatenate([gains[0], shifts[0], rel_bias[0]], axis=0).T
    small = jnp.concatenate([small, depthwise[0]], axis=1)
    small = jnp.pad(small, ((0, 0), (0, COLS[-1] - small.shape[1])))
    packed = jnp.concatenate(
        [ffn_up[0, 0], ffn_up[0, 1], attn_in[0], attn_out[0], pos_proj[0], conv_in[0], conv_out[0], small],
        axis=1,
    )
    w_all, down, f_all, c_all = gather_all(
        packed, ffn_down[0], frames.astype(low), cotangent.astype(low)
    )
    cuts = np.cumsum((0,) + COLS)
    up_0, up_1, w_attn_in, w_attn_out, w_pos, w_conv_in, w_conv_out, small = (
        w_all[:, int(lo) : int(hi)] for lo, hi in zip(cuts[:-1], cuts[1:])
    )
    small = small.astype(jnp.float32).T
    gain, shift, rel = small[0:6], small[6:12], small[12:14]
    kernel_f = small[14 : 14 + taps].T
    own_length = lax.dynamic_slice_in_dim(lengths, dp * count + sq, 1)
    grid = lengths.reshape(lax.axis_size("dp"), MB, UTTS)
    per_batch = jnp.sum(grid, axis=(0, 2)).astype(jnp.float32)
    frame_count = lax.dynamic_slice_in_dim(per_batch, lax.div(sq, UTTS), 1)[0]
    mask = (jnp.arange(length, dtype=jnp.int32) < own_length[0]).astype(jnp.float32)[:, None]
    table_in = position_table(length, model)

    x0 = f_all.reshape(length, model).astype(jnp.float32)
    x1, kept_one = ffn_forward(x0, gain[0], shift[0], up_0, down[0])
    a1 = layer_norm(x1, gain[1], shift[1]).astype(low)
    proj = matmul_low(a1, w_attn_in)
    query = proj[:, :model]
    qu = (query + rel[0]).astype(low)
    qv = (query + rel[1]).astype(low)
    key = proj[:, model : 2 * model].astype(low)
    value = proj[:, 2 * model :].astype(low)
    table = matmul_low(table_in, w_pos).astype(low)
    ctx, probs = att_fwd(own_length, qu, qv, key, value, table)
    x2 = x1 + matmul_low(ctx, w_attn_out)

    a2 = layer_norm(x2, gain[2], shift[2]).astype(low)
    gate = matmul_low(a2, w_conv_in)
    gated = (glu_gate(gate) * mask).astype(low)
    depth = shifted_sum(gated, kernel_f, False)
    sums = jnp.stack([jnp.sum(depth * mask, axis=0), jnp.sum(depth * depth * mask, axis=0)])
    sums = batch_sum(sums, 2)
    mean = sums[0] / frame_count
    var = sums[1] / frame_count - mean * mean
    inv = lax.rsqrt(var + 1e-05)
    normal = (depth - mean) * inv * gain[5] + shift[5]
    active = jax.nn.silu(normal).astype(low)
    x3 = x2 + matmul_low(active, w_conv_out)
    x4, kept_two = ffn_forward(x3, gain[3], shift[3], up_1, down[1])
    mixed = layer_norm(x4, gain[4], shift[4])

    cot = c_all.reshape(length, model).astype(jnp.float32)
    grad, g_gain4, g_shift4 = jax.vjp(layer_norm, x4, gain[4], shift[4])[1](cot)
    grad, (g_gain3, g_shift3, g_up1, g_down1) = ffn_backward(
        grad, kept_two, gain[3], shift[3], up_1, down[1]
    )
    grad_b = grad.astype(low)
    g_conv_out = weight_grad(active, grad_b)
    grad_active = matmul_back(grad_b, w_conv_out)
    grad_normal = jax.vjp(jax.nn.silu, normal)[1](grad_active)[0]
    g_gain5 = jnp.sum(grad_normal * ((depth - mean) * inv), axis=0)
    g_shift5 = jnp.sum(grad_normal, axis=0)
    hat = grad_normal * gain[5]
    sums = batch_sum(jnp.stack([jnp.sum(hat, axis=0), jnp.sum(hat * depth, axis=0)]), 3)
    grad_var = -0.5 * inv * inv * inv * (sums[1] - mean * sums[0])
    grad_mean = -inv * sums[0] - 2.0 * mean * grad_var
    grad_depth = (
        hat * inv + mask * (grad_mean / frame_count + 2.0 * depth * grad_var / frame_count)
    ).astype(low)
    grad_gated = shifted_sum(grad_depth, kernel_f, True) * mask
    g_kernel = tap_grads(gated, grad_depth, taps)
    grad_gate = jax.vjp(glu_gate, gate)[1](grad_gated)[0].astype(low)
    g_conv_in = weight_grad(a2, grad_gate)
    grad_ln, g_gain2, g_shift2 = jax.vjp(layer_norm, x2, gain[2], shift[2])[1](
        matmul_back(grad_gate, w_conv_in)
    )
    grad = grad + grad_ln

    grad_b = grad.astype(low)
    g_attn_out = weight_grad(ctx, grad_b)
    grad_ctx = matmul_back(grad_b, w_attn_out).astype(low)
    dqu, dqv, dkey, dvalue, dtable = att_bwd(probs, grad_ctx, qu, qv, key, value, table)
    g_rel = jnp.stack([jnp.sum(dqu, axis=0), jnp.sum(dqv, axis=0)])
    grad_proj = jnp.concatenate([dqu + dqv, dkey, dvalue], axis=1).astype(low)
    g_pos = weight_grad(table_in, dtable)
    g_attn_in = weight_grad(a1, grad_proj)
    grad_ln, g_gain1, g_shift1 = jax.vjp(layer_norm, x1, gain[1], shift[1])[1](
        matmul_back(grad_proj, w_attn_in)
    )
    grad = grad + grad_ln
    grad, (g_gain0, g_shift0, g_up0, g_down0) = ffn_backward(
        grad, kept_one, gain[0], shift[0], up_0, down[0]
    )

    g_small = jnp.concatenate(
        [
            jnp.stack([g_gain0, g_gain1, g_gain2, g_gain3, g_gain4, g_gain5]),
            jnp.stack([g_shift0, g_shift1, g_shift2, g_shift3, g_shift4, g_shift5]),
            g_rel,
            g_kernel,
        ]
    )
    g_small = jnp.pad(g_small, ((0, COLS[-1] - g_small.shape[0]), (0, 0))).T
    g_packed = jnp.concatenate(
        [
            member.astype(low)
            for member in (g_up0, g_up1, g_attn_in, g_attn_out, g_pos, g_conv_in, g_conv_out, g_small)
        ],
        axis=1,
    )
    g_down = jnp.stack([g_down0, g_down1]).astype(low)
    w_sum, d_sum, m_all, g_all = scatter_all(g_packed, g_down, mixed.astype(low), grad.astype(low), count)
    parts = [w_sum[:, int(lo) : int(hi)] for lo, hi in zip(cuts[:-1], cuts[1:])]
    tail = parts[7][:, : 14 + taps]
    rows = tail[:, :14].T
    return (
        m_all.astype(jnp.float32),
        g_all.astype(jnp.float32),
        rows[None, 0:6],
        rows[None, 6:12],
        rows[None, 12:14],
        jnp.stack([parts[0], parts[1]])[None],
        d_sum[None],
        parts[2][None],
        parts[3][None],
        parts[4][None],
        parts[5][None],
        tail[None, :, 14:],
        parts[6][None],
    )


def solution(mesh):
    body = local_whole if fits_whole(mesh) else local_general
    in_specs = (
        P("dp", "seq", None),
        P(),
        P("dp", "seq", None),
        P(None, None, ("dp", "seq")),
        P(None, None, ("dp", "seq")),
        P(None, None, ("dp", "seq")),
        P(None, None, ("dp", "seq"), None),
        P(None, None, ("dp", "seq"), None),
        P(None, ("dp", "seq"), None),
        P(None, ("dp", "seq"), None),
        P(None, ("dp", "seq"), None),
        P(None, ("dp", "seq"), None),
        P(None, ("dp", "seq"), None),
        P(None, ("dp", "seq"), None),
    )
    out_specs = (
        P("dp", "seq", None),
        P("dp", "seq", None),
        P(None, None, ("dp", "seq")),
        P(None, None, ("dp", "seq")),
        P(None, None, ("dp", "seq")),
        P(None, None, ("dp", "seq"), None),
        P(None, None, ("dp", "seq"), None),
        P(None, ("dp", "seq"), None),
        P(None, ("dp", "seq"), None),
        P(None, ("dp", "seq"), None),
        P(None, ("dp", "seq"), None),
        P(None, ("dp", "seq"), None),
        P(None, ("dp", "seq"), None),
    )
    return jax.shard_map(body, mesh=mesh, in_specs=in_specs, out_specs=out_specs, check_vma=False)
```

```python
import math

import jax
import jax.numpy as jnp
import numpy as np
from jax import lax
from jax.experimental import pallas as pl
from jax.experimental.pallas import tpu as pltpu
from jax.sharding import PartitionSpec as P

H = 8
DH = 64
NL = 1
MB = 2


HIGHEST_PREC = lax.Precision.HIGHEST


def extended(cells, sides, width):
    for axis, dim in sides:
        count = lax.axis_size(axis)
        ends = count - 1
        head = lax.slice_in_dim(cells, 0, width, axis=dim)
        tail = lax.slice_in_dim(cells, cells.shape[dim] - width, cells.shape[dim], axis=dim)
        cells = jnp.concatenate(
            [
                lax.ppermute(tail, axis, [(i, (i + 1) % count) for i in range(ends)]),
                cells,
                lax.ppermute(head, axis, [((i + 1) % count, i) for i in range(ends)]),
            ],
            axis=dim,
        )
    return cells


def layer_norm(values, gain_row, shift_row):
    centred = values - jnp.mean(values, axis=-1, keepdims=True)
    spread = jnp.mean(centred * centred, axis=-1, keepdims=True)
    return centred * lax.rsqrt(spread + 1e-05) * gain_row + shift_row


def sinusoid(offsets, model_width):
    half_width = model_width // 2
    frequency = jnp.exp(
        jnp.arange(half_width, dtype=jnp.float32) * (-2.0 * math.log(10000.0) / model_width)
    )
    angles = offsets.astype(jnp.float32)[:, None] * frequency[None, :]
    return jnp.concatenate([jnp.sin(angles), jnp.cos(angles)], axis=1)


def skew_rows(raw_pos, key_count):
    row_count = raw_pos.shape[-2]
    col_count = raw_pos.shape[-1]
    lead = raw_pos.shape[:-2]
    flat_rows = raw_pos.reshape(lead + (row_count * col_count,))
    flat_rows = flat_rows[..., row_count - 1 : row_count - 1 + row_count * (col_count - 1)]
    return flat_rows.reshape(lead + (row_count, col_count - 1))[..., :key_count]


def skew_back(grad_skew, raw_shape, key_count):
    zero_raw = jnp.zeros(raw_shape, jnp.float32)
    return jax.vjp(lambda raw_pos: skew_rows(raw_pos, key_count), zero_raw)[1](grad_skew)[0]


def glu_gate(gate_pair):
    half_width = gate_pair.shape[-1] // 2
    return gate_pair[..., :half_width] * jax.nn.sigmoid(gate_pair[..., half_width:])


def matmul_low(left, right):
    return jnp.dot(left, right, preferred_element_type=jnp.float32)


def matmul_back(grad_low, weight):
    return lax.dot_general(
        grad_low, weight, (((1,), (1,)), ((), ())), preferred_element_type=jnp.float32
    )


def weight_grad(inputs_low, grad_low):
    return lax.dot_general(
        inputs_low, grad_low, (((0,), (0,)), ((), ())), preferred_element_type=jnp.float32
    )


def ffn_forward(row_data, gain_row, shift_row, w_up, w_down):
    normed_b = layer_norm(row_data, gain_row, shift_row).astype(jnp.bfloat16)
    hidden = matmul_low(normed_b, w_up)
    active_b = jax.nn.silu(hidden).astype(jnp.bfloat16)
    branch = matmul_low(active_b, w_down)
    return (row_data + 0.5 * branch, (row_data, normed_b, hidden, active_b))


def ffn_backward(grad_rows, kept_data, gain_row, shift_row, w_up, w_down):
    row_data, normed_b, hidden, active_b = kept_data
    grad_out_b = (0.5 * grad_rows).astype(jnp.bfloat16)
    g_down = weight_grad(active_b, grad_out_b)
    grad_active = matmul_back(grad_out_b, w_down)
    grad_hidden_b = jax.vjp(jax.nn.silu, hidden)[1](grad_active)[0].astype(jnp.bfloat16)
    g_up = weight_grad(normed_b, grad_hidden_b)
    grad_normed = matmul_back(grad_hidden_b, w_up)
    grad_ln, g_gain, g_shift = jax.vjp(layer_norm, row_data, gain_row, shift_row)[1](grad_normed)
    return (grad_rows + grad_ln, (g_gain, g_shift, g_up, g_down))


def attention_logits(query_u_b, query_v_b, key_heads, pos_heads, key_valid):
    content = jnp.einsum(
        "ufhd,ulhd->uhfl", query_u_b, key_heads, preferred_element_type=jnp.float32
    )
    raw_pos = jnp.einsum("ufhd,whd->uhfw", query_v_b, pos_heads, preferred_element_type=jnp.float32)
    logits = (content + skew_rows(raw_pos, key_heads.shape[1])) * 0.125
    return jnp.where(key_valid[:, None, None, :], logits, -1e30)


def attn_forward(
    row_data,
    utt_count,
    gain_row,
    shift_row,
    bias_u,
    bias_v,
    w_in,
    w_out,
    w_pos,
    key_valid,
    pos_table_b,
):
    model_width = row_data.shape[1]
    frame_len = row_data.shape[0] // utt_count
    normed_b = layer_norm(row_data, gain_row, shift_row).astype(jnp.bfloat16)
    proj_rows = matmul_low(normed_b, w_in)
    query_rows = proj_rows[:, :model_width].reshape(utt_count, frame_len, H, DH)
    key_b = (
        proj_rows[:, model_width : 2 * model_width]
        .astype(jnp.bfloat16)
        .reshape(utt_count, frame_len, model_width)
    )
    value_b = (
        proj_rows[:, 2 * model_width :]
        .astype(jnp.bfloat16)
        .reshape(utt_count, frame_len, model_width)
    )
    all_keys, all_values = (
        lax.all_gather(key_b, "seq", axis=1, tiled=True),
        lax.all_gather(value_b, "seq", axis=1, tiled=True),
    )
    key_heads = all_keys.reshape(utt_count, -1, H, DH)
    value_heads = all_values.reshape(utt_count, -1, H, DH)
    query_u_b = (query_rows + bias_u.reshape(H, DH)).astype(jnp.bfloat16)
    query_v_b = (query_rows + bias_v.reshape(H, DH)).astype(jnp.bfloat16)
    pos_heads = matmul_low(pos_table_b, w_pos).astype(jnp.bfloat16).reshape(-1, H, DH)
    logits = attention_logits(query_u_b, query_v_b, key_heads, pos_heads, key_valid)
    top_score = jnp.max(logits, axis=-1, keepdims=True)
    exp_scores = jnp.exp(logits - top_score)
    row_total = jnp.sum(exp_scores, axis=-1, keepdims=True)
    prob_b = (exp_scores / row_total).astype(jnp.bfloat16)
    log_total = top_score + jnp.log(row_total)
    context = jnp.einsum("uhfl,ulhd->ufhd", prob_b, value_heads, preferred_element_type=jnp.float32)
    context_b = context.astype(jnp.bfloat16).reshape(-1, model_width)
    branch = matmul_low(context_b, w_out)
    kept_data = (
        row_data,
        normed_b,
        query_u_b,
        query_v_b,
        key_heads,
        value_heads,
        pos_heads,
        log_total,
        context_b,
    )
    return (row_data + branch, kept_data)


def attn_backward(grad_rows, kept_data, gain_row, shift_row, w_in, w_out, key_valid, pos_table_b):
    (
        row_data,
        normed_b,
        query_u_b,
        query_v_b,
        key_heads,
        value_heads,
        pos_heads,
        log_total,
        context_b,
    ) = kept_data
    utt_count = query_u_b.shape[0]
    frame_len = query_u_b.shape[1]
    model_width = row_data.shape[1]
    key_len = key_heads.shape[1]
    grad_out_b = grad_rows.astype(jnp.bfloat16)
    g_out = weight_grad(context_b, grad_out_b)
    grad_context_b = (
        matmul_back(grad_out_b, w_out).astype(jnp.bfloat16).reshape(utt_count, frame_len, H, DH)
    )
    logits = attention_logits(query_u_b, query_v_b, key_heads, pos_heads, key_valid)
    prob_rows = jnp.exp(logits - log_total)
    grad_probs = jnp.einsum(
        "ufhd,ulhd->uhfl", grad_context_b, value_heads, preferred_element_type=jnp.float32
    )
    inner_sum = jnp.sum(grad_probs * prob_rows, axis=-1, keepdims=True)
    grad_logits_b = (prob_rows * (grad_probs - inner_sum)).astype(jnp.bfloat16) * 0.125
    grad_query_u = jnp.einsum(
        "uhfl,ulhd->ufhd", grad_logits_b, key_heads, preferred_element_type=jnp.float32
    )
    raw_shape = (utt_count, H, frame_len, pos_heads.shape[0])
    grad_raw_b = skew_back(grad_logits_b.astype(jnp.float32), raw_shape, key_len).astype(
        jnp.bfloat16
    )
    grad_query_v = jnp.einsum(
        "uhfw,whd->ufhd", grad_raw_b, pos_heads, preferred_element_type=jnp.float32
    )
    grad_pos = jnp.einsum(
        "uhfw,ufhd->whd", grad_raw_b, query_v_b, preferred_element_type=jnp.float32
    )
    grad_pos = grad_pos.reshape(-1, model_width)
    g_pos = lax.dot_general(
        pos_table_b.astype(jnp.float32),
        grad_pos,
        (((0,), (0,)), ((), ())),
        precision=HIGHEST_PREC,
        preferred_element_type=jnp.float32,
    )
    prob_b = prob_rows.astype(jnp.bfloat16)
    grad_values = jnp.einsum(
        "uhfl,ufhd->ulhd", prob_b, grad_context_b, preferred_element_type=jnp.float32
    )
    grad_keys = jnp.einsum(
        "uhfl,ufhd->ulhd", grad_logits_b, query_u_b, preferred_element_type=jnp.float32
    )
    own_keys, own_values = (
        lax.psum_scatter(
            grad_keys.reshape(utt_count, key_len, model_width),
            "seq",
            scatter_dimension=1,
            tiled=True,
        ),
        lax.psum_scatter(
            grad_values.reshape(utt_count, key_len, model_width),
            "seq",
            scatter_dimension=1,
            tiled=True,
        ),
    )
    g_bias_u = jnp.sum(grad_query_u, axis=(0, 1)).reshape(-1)
    g_bias_v = jnp.sum(grad_query_v, axis=(0, 1)).reshape(-1)
    grad_proj_b = jnp.concatenate(
        [
            (grad_query_u + grad_query_v).reshape(-1, model_width),
            own_keys.reshape(-1, model_width),
            own_values.reshape(-1, model_width),
        ],
        axis=1,
    ).astype(jnp.bfloat16)
    g_in = weight_grad(normed_b, grad_proj_b)
    grad_normed = matmul_back(grad_proj_b, w_in)
    grad_ln, g_gain, g_shift = jax.vjp(layer_norm, row_data, gain_row, shift_row)[1](grad_normed)
    return (grad_rows + grad_ln, (g_gain, g_shift, g_bias_u, g_bias_v, g_in, g_out, g_pos))


def conv_forward(
    row_data,
    utt_count,
    gain_row,
    shift_row,
    w_in,
    kernel,
    bn_gain,
    bn_shift,
    w_out,
    frame_mask,
    frame_count,
):
    model_width = row_data.shape[1]
    frame_len = row_data.shape[0] // utt_count
    normed_b = layer_norm(row_data, gain_row, shift_row).astype(jnp.bfloat16)
    gate_pair = matmul_low(normed_b, w_in)
    mask_rows = frame_mask.reshape(-1, 1)
    gated_b = (
        (glu_gate(gate_pair) * mask_rows)
        .astype(jnp.bfloat16)
        .reshape(utt_count, frame_len, model_width)
    )
    halo_reach = (kernel.shape[1] - 1) // 2
    padded = extended(gated_b, (("seq", 1),), halo_reach)
    kernel_f = kernel.astype(jnp.float32)
    depth_out = padded[:, 0:frame_len].astype(jnp.float32) * kernel_f[:, 0]
    for tap_idx in range(1, kernel.shape[1]):
        depth_out = (
            depth_out
            + padded[:, tap_idx : tap_idx + frame_len].astype(jnp.float32) * kernel_f[:, tap_idx]
        )
    weight_mask = frame_mask[:, :, None]
    sum_local = jnp.sum(depth_out * weight_mask, axis=(0, 1))
    square_local = jnp.sum(depth_out * depth_out * weight_mask, axis=(0, 1))
    sum_all, square_all = lax.psum((sum_local, square_local), ("dp", "seq"))
    mean_val = sum_all / frame_count
    variance = square_all / frame_count - mean_val * mean_val
    inv_std = lax.rsqrt(variance + 1e-05)
    normal = (depth_out - mean_val) * inv_std * bn_gain + bn_shift
    active_b = jax.nn.silu(normal).astype(jnp.bfloat16).reshape(-1, model_width)
    branch = matmul_low(active_b, w_out)
    kept_data = (
        row_data,
        normed_b,
        gate_pair,
        padded,
        depth_out,
        mean_val,
        inv_std,
        normal,
        active_b,
    )
    return (row_data + branch, kept_data)


def conv_backward(
    grad_rows, kept_data, gain_row, shift_row, w_in, kernel, bn_gain, w_out, frame_mask, frame_count
):
    row_data, normed_b, gate_pair, padded, depth_out, mean_val, inv_std, normal, active_b = (
        kept_data
    )
    frame_len = depth_out.shape[1]
    model_width = depth_out.shape[2]
    grad_out_b = grad_rows.astype(jnp.bfloat16)
    g_out = weight_grad(active_b, grad_out_b)
    grad_active = matmul_back(grad_out_b, w_out).reshape(depth_out.shape)
    grad_normal = jax.vjp(jax.nn.silu, normal)[1](grad_active)[0]
    centred_hat = (depth_out - mean_val) * inv_std
    g_bn_gain = jnp.sum(grad_normal * centred_hat, axis=(0, 1))
    g_bn_shift = jnp.sum(grad_normal, axis=(0, 1))
    grad_hat = grad_normal * bn_gain
    part_one = jnp.sum(grad_hat, axis=(0, 1))
    part_two = jnp.sum(grad_hat * depth_out, axis=(0, 1))
    part_one, part_two = lax.psum((part_one, part_two), ("dp", "seq"))
    grad_inv = part_two - mean_val * part_one
    grad_var = -0.5 * inv_std * inv_std * inv_std * grad_inv
    grad_mean = -inv_std * part_one - 2.0 * mean_val * grad_var
    weight_mask = frame_mask[:, :, None]
    grad_depth_b = (
        grad_hat * inv_std
        + weight_mask * (grad_mean / frame_count + 2.0 * depth_out * grad_var / frame_count)
    ).astype(jnp.bfloat16)
    halo_reach = (kernel.shape[1] - 1) // 2
    grad_padded = extended(grad_depth_b, (("seq", 1),), halo_reach)
    kernel_f = kernel.astype(jnp.float32)
    grad_depth_f = grad_depth_b.astype(jnp.float32)
    grad_gated = jnp.zeros(depth_out.shape, jnp.float32)
    kernel_cols = []
    for tap_idx in range(kernel.shape[1]):
        begin_at = 2 * halo_reach - tap_idx
        grad_gated = (
            grad_gated
            + grad_padded[:, begin_at : begin_at + frame_len].astype(jnp.float32)
            * kernel_f[:, tap_idx]
        )
        kernel_cols.append(
            jnp.sum(
                padded[:, tap_idx : tap_idx + frame_len].astype(jnp.float32) * grad_depth_f,
                axis=(0, 1),
            )
        )
    g_kernel = jnp.stack(kernel_cols, axis=1)
    grad_gate_b = jax.vjp(glu_gate, gate_pair)[1](
        (grad_gated * weight_mask).reshape(-1, model_width)
    )[0]
    grad_gate_b = grad_gate_b.astype(jnp.bfloat16)
    g_in = weight_grad(normed_b, grad_gate_b)
    grad_normed = matmul_back(grad_gate_b, w_in)
    grad_ln, g_gain, g_shift = jax.vjp(layer_norm, row_data, gain_row, shift_row)[1](grad_normed)
    return (grad_rows + grad_ln, (g_gain, g_shift, g_in, g_kernel, g_bn_gain, g_bn_shift, g_out))


def layer_forward(values, weights, frame_mask, key_valid, frame_count, pos_table_b):
    (
        gain_set,
        shift_set,
        rel_set,
        up_pair,
        down_pair,
        attn_in_w,
        attn_out_w,
        pos_w,
        conv_in_w,
        kernel,
        conv_out_w,
    ) = weights
    gain_f = gain_set.astype(jnp.float32)
    shift_f = shift_set.astype(jnp.float32)
    rel_f = rel_set.astype(jnp.float32)
    utt_count = values.shape[0]
    row_data = values.reshape(-1, values.shape[2])
    row_data, kept_one = ffn_forward(row_data, gain_f[0], shift_f[0], up_pair[0], down_pair[0])
    row_data, kept_attn = attn_forward(
        row_data,
        utt_count,
        gain_f[1],
        shift_f[1],
        rel_f[0],
        rel_f[1],
        attn_in_w,
        attn_out_w,
        pos_w,
        key_valid,
        pos_table_b,
    )
    row_data, kept_conv = conv_forward(
        row_data,
        utt_count,
        gain_f[2],
        shift_f[2],
        conv_in_w,
        kernel,
        gain_f[5],
        shift_f[5],
        conv_out_w,
        frame_mask,
        frame_count,
    )
    row_data, kept_two = ffn_forward(row_data, gain_f[3], shift_f[3], up_pair[1], down_pair[1])
    result = layer_norm(row_data, gain_f[4], shift_f[4])
    return (result.reshape(values.shape), (kept_one, kept_attn, kept_conv, kept_two, row_data))


def layer_backward(
    grad_values, kept_data, weights, frame_mask, key_valid, frame_count, pos_table_b
):
    (
        gain_set,
        shift_set,
        rel_set,
        up_pair,
        down_pair,
        attn_in_w,
        attn_out_w,
        pos_w,
        conv_in_w,
        kernel,
        conv_out_w,
    ) = weights
    gain_f = gain_set.astype(jnp.float32)
    shift_f = shift_set.astype(jnp.float32)
    kept_one, kept_attn, kept_conv, kept_two, last_rows = kept_data
    grad_rows = grad_values.reshape(-1, grad_values.shape[2])
    grad_rows, g_gain_last, g_shift_last = jax.vjp(layer_norm, last_rows, gain_f[4], shift_f[4])[1](
        grad_rows
    )
    grad_rows, two_grads = ffn_backward(
        grad_rows, kept_two, gain_f[3], shift_f[3], up_pair[1], down_pair[1]
    )
    grad_rows, conv_grads = conv_backward(
        grad_rows,
        kept_conv,
        gain_f[2],
        shift_f[2],
        conv_in_w,
        kernel,
        gain_f[5],
        conv_out_w,
        frame_mask,
        frame_count,
    )
    grad_rows, attn_grads = attn_backward(
        grad_rows, kept_attn, gain_f[1], shift_f[1], attn_in_w, attn_out_w, key_valid, pos_table_b
    )
    grad_rows, one_grads = ffn_backward(
        grad_rows, kept_one, gain_f[0], shift_f[0], up_pair[0], down_pair[0]
    )
    grad_gains = jnp.stack(
        [one_grads[0], attn_grads[0], conv_grads[0], two_grads[0], g_gain_last, conv_grads[4]]
    )
    grad_shifts = jnp.stack(
        [one_grads[1], attn_grads[1], conv_grads[1], two_grads[1], g_shift_last, conv_grads[5]]
    )
    grad_rel = jnp.stack([attn_grads[2], attn_grads[3]])
    grad_up = jnp.stack([one_grads[2], two_grads[2]])
    grad_down = jnp.stack([one_grads[3], two_grads[3]])
    layer_grads = (
        grad_gains,
        grad_shifts,
        grad_rel,
        grad_up,
        grad_down,
        attn_grads[4],
        attn_grads[5],
        attn_grads[6],
        conv_grads[2],
        conv_grads[3],
        conv_grads[6],
    )
    return (grad_rows.reshape(grad_values.shape), layer_grads)


def gather_forward(shards, layer_idx):
    pieces = tuple((member[layer_idx] for member in shards))
    return (
        lax.all_gather(pieces[0], ("dp", "seq"), axis=1, tiled=True),
        lax.all_gather(pieces[1], ("dp", "seq"), axis=1, tiled=True),
        lax.all_gather(pieces[2], ("dp", "seq"), axis=1, tiled=True),
        lax.all_gather(pieces[3], ("dp", "seq"), axis=1, tiled=True),
        lax.all_gather(pieces[4], ("dp", "seq"), axis=1, tiled=True),
        lax.all_gather(pieces[5], ("dp", "seq"), axis=0, tiled=True),
        lax.all_gather(pieces[6], ("dp", "seq"), axis=0, tiled=True),
        lax.all_gather(pieces[7], ("dp", "seq"), axis=0, tiled=True),
        lax.all_gather(pieces[8], ("dp", "seq"), axis=0, tiled=True),
        lax.all_gather(pieces[9], ("dp", "seq"), axis=0, tiled=True),
        lax.all_gather(pieces[10], ("dp", "seq"), axis=0, tiled=True),
    )


def gather_backward(shards, layer_idx):
    pieces = tuple((member[layer_idx] for member in shards))
    return (
        lax.all_gather(pieces[0], ("dp", "seq"), axis=1, tiled=True),
        lax.all_gather(pieces[1], ("dp", "seq"), axis=1, tiled=True),
        lax.all_gather(pieces[2], ("dp", "seq"), axis=1, tiled=True),
        lax.all_gather(pieces[3], ("dp", "seq"), axis=1, tiled=True),
        lax.all_gather(pieces[4], ("dp", "seq"), axis=1, tiled=True),
        lax.all_gather(pieces[5], ("dp", "seq"), axis=0, tiled=True),
        lax.all_gather(pieces[6], ("dp", "seq"), axis=0, tiled=True),
        lax.all_gather(pieces[7], ("dp", "seq"), axis=0, tiled=True),
        lax.all_gather(pieces[8], ("dp", "seq"), axis=0, tiled=True),
        lax.all_gather(pieces[9], ("dp", "seq"), axis=0, tiled=True),
        lax.all_gather(pieces[10], ("dp", "seq"), axis=0, tiled=True),
    )


def local_general(
    frames,
    lengths,
    cotangent,
    gains,
    shifts,
    rel_bias,
    ffn_up,
    ffn_down,
    attn_in,
    attn_out,
    pos_proj,
    conv_in,
    depthwise,
    conv_out,
):
    shards = (
        gains,
        shifts,
        rel_bias,
        ffn_up,
        ffn_down,
        attn_in,
        attn_out,
        pos_proj,
        conv_in,
        depthwise,
        conv_out,
    )
    groups = lax.axis_size("dp")
    seq_devices = lax.axis_size("seq")
    local_utts = frames.shape[0]
    frame_len = frames.shape[1]
    model_width = frames.shape[2]
    utt_per = local_utts // MB
    length = frame_len * seq_devices
    seq_start = lax.axis_index("seq") * frame_len
    first_utt = lax.axis_index("dp") * local_utts
    own_lengths = lax.dynamic_slice_in_dim(lengths, first_utt, local_utts)
    lengths_grid = lengths.reshape(groups, MB, utt_per)
    offsets = seq_start + frame_len - 1 - jnp.arange(length + frame_len - 1, dtype=jnp.int32)
    pos_table_b = sinusoid(offsets, model_width).astype(jnp.bfloat16)
    frame_pos = seq_start + jnp.arange(frame_len, dtype=jnp.int32)
    key_pos = jnp.arange(length, dtype=jnp.int32)
    result_list = []
    grad_list = []
    full_sums = [None] * NL
    for micro_idx in range(MB):
        lens_here = own_lengths[micro_idx * utt_per : (micro_idx + 1) * utt_per]
        frame_mask = (frame_pos[None, :] < lens_here[:, None]).astype(jnp.float32)
        key_valid = key_pos[None, :] < lens_here[:, None]
        frame_count = jnp.sum(lengths_grid[:, micro_idx]).astype(jnp.float32)
        values = frames[micro_idx * utt_per : (micro_idx + 1) * utt_per]
        held_weights = []
        layer_idx = 0
        weights = gather_forward(shards, layer_idx)
        values, kept_data = layer_forward(
            values, weights, frame_mask, key_valid, frame_count, pos_table_b
        )
        saved_acts = [kept_data]
        held_weights.append(weights)
        result_list.append(values)
        grad_values = cotangent[micro_idx * utt_per : (micro_idx + 1) * utt_per]
        for layer_idx in reversed(range(NL)):
            weights = gather_backward(shards, layer_idx)
            grad_values, layer_grads = layer_backward(
                grad_values,
                saved_acts[layer_idx],
                weights,
                frame_mask,
                key_valid,
                frame_count,
                pos_table_b,
            )
            if full_sums[layer_idx] is None:
                full_sums[layer_idx] = layer_grads
            else:
                full_sums[layer_idx] = jax.tree.map(jnp.add, full_sums[layer_idx], layer_grads)
        grad_list.append(grad_values)
    stacked = tuple((jnp.stack([full_sums[0][member]]) for member in range(11)))
    final_grads = (
        lax.psum_scatter(stacked[0], ("dp", "seq"), scatter_dimension=2, tiled=True),
        lax.psum_scatter(stacked[1], ("dp", "seq"), scatter_dimension=2, tiled=True),
        lax.psum_scatter(stacked[2], ("dp", "seq"), scatter_dimension=2, tiled=True),
        lax.psum_scatter(stacked[3], ("dp", "seq"), scatter_dimension=2, tiled=True),
        lax.psum_scatter(stacked[4], ("dp", "seq"), scatter_dimension=2, tiled=True),
        lax.psum_scatter(stacked[5], ("dp", "seq"), scatter_dimension=1, tiled=True),
        lax.psum_scatter(stacked[6], ("dp", "seq"), scatter_dimension=1, tiled=True),
        lax.psum_scatter(stacked[7], ("dp", "seq"), scatter_dimension=1, tiled=True),
        lax.psum_scatter(stacked[8], ("dp", "seq"), scatter_dimension=1, tiled=True),
        lax.psum_scatter(stacked[9], ("dp", "seq"), scatter_dimension=1, tiled=True),
        lax.psum_scatter(stacked[10], ("dp", "seq"), scatter_dimension=1, tiled=True),
    )
    mixed = jnp.concatenate(result_list, axis=0)
    grad_frames = jnp.concatenate(grad_list, axis=0)
    return (
        mixed,
        grad_frames,
        final_grads[0],
        final_grads[1],
        final_grads[2],
        final_grads[3],
        final_grads[4],
        final_grads[5],
        final_grads[6],
        final_grads[7],
        final_grads[8],
        final_grads[9],
        final_grads[10],
    )


NT = (((1,), (1,)), ((), ()))
TN = (((0,), (0,)), ((), ()))
NN = (((1,), (0,)), ((), ()))
MESH = pl.DeviceIdType.MESH
UTTS = 4
COLS = (2048, 2048, 1536, 512, 512, 1024, 512, 128)
VMEM_LIMIT = 60 * 1024 * 1024


def fits_whole(mesh):
    return mesh.shape["dp"] == 4 and mesh.shape["seq"] == MB * UTTS


def dotf(left, right, dims=NN):
    return lax.dot_general(left, right, dims, preferred_element_type=jnp.float32)


def place():
    dp = lax.axis_index("dp")
    sq = lax.axis_index("seq")
    return dp, sq, lax.div(dp, 2), lax.rem(dp, 2), lax.div(sq, 2), lax.rem(sq, 2)


def flip_if(value, bit):
    return 1 - value if bit else value


def partners():
    dp, sq, x, c, z, y = place()
    even = c == 0
    core = (x * 2 + 1 - c, sq)
    xdev = ((1 - x) * 2 + c, sq)
    ydev = (dp, z * 2 + 1 - y)
    first = (jnp.where(even, ydev[0], xdev[0]), jnp.where(even, ydev[1], xdev[1]))
    second = (jnp.where(even, xdev[0], ydev[0]), jnp.where(even, xdev[1], ydev[1]))
    return core, xdev, first, second


def rank_of(color, a, b, k):
    _, _, x, _, z, y = place()
    even = color == 0
    xx = jnp.where(even, x + a * (1 - 2 * x), x + b * (1 - 2 * x))
    yy = jnp.where(even, y + b * (1 - 2 * y), y + a * (1 - 2 * y))
    return xx * 16 + color * 8 + lax.rem(z + k, 4) * 2 + yy


def greet(devices):
    barrier = pltpu.get_barrier_semaphore()
    for device in devices:
        pl.semaphore_signal(barrier, inc=1, device_id=device, device_id_type=MESH)
    pl.semaphore_wait(barrier, len(devices))


def seq_peers(dp, sq, count):
    return [(dp, lax.rem(sq + k, count)) for k in range(1, count)]


def remote(src, dst, send, recv, device):
    return pltpu.make_async_remote_copy(
        src_ref=src, dst_ref=dst, send_sem=send, recv_sem=recv, device_id=device, device_id_type=MESH
    )


def gather_kernel(
    w_ref, d_ref, f_ref, w_all, d_all, f_all, send, recv, row_send, row_recv, own
):
    dp, sq, x, c, z, y = place()
    core, xdev, first, second = partners()
    count = f_ref.shape[0]
    greet(seq_peers(dp, sq, count) + [core, xdev])
    wr = w_ref.shape[0]
    dr = d_ref.shape[1]

    def rows_of(rank):
        return (
            w_all.at[pl.ds(pl.multiple_of(rank * wr, 16), wr), :],
            d_all.at[:, pl.ds(pl.multiple_of(rank * dr, 16), dr), :],
        )

    def pair(rank, device, slot, landing, mine=False):
        w_dst, d_dst = rows_of(rank)
        w_src, d_src = (w_ref, d_ref) if mine else (w_dst, d_dst)
        return (
            remote(w_src, w_dst, send.at[0, slot], recv.at[0, landing], device),
            remote(d_src, d_dst, send.at[1, slot], recv.at[1, landing], device),
        )

    started = []

    def ship(*args, **kwargs):
        for copy in pair(*args, **kwargs):
            copy.start()
            started.append(copy)

    def arrive(color, a, b, k):
        slot = a * 8 + b * 4 + k + (0 if color is c else 16)
        for copy in pair(rank_of(color, a, b, k), core, 0, slot):
            copy.wait_recv()

    mine = rank_of(c, 0, 0, 0)
    ship(mine, second, 15, 8, mine=True)
    ship(mine, first, 3, 4, mine=True)
    for k in (1, 3, 2):
        ship(mine, (dp, lax.rem(z + k, 4) * 2 + y), k - 1, 4 - k, mine=True)
    ship(mine, core, 16, 16, mine=True)
    w_own, d_own = rows_of(mine)
    locals_ = [
        pltpu.make_async_copy(w_ref, w_own, own.at[0]),
        pltpu.make_async_copy(d_ref, d_own, own.at[1]),
        pltpu.make_async_copy(f_ref.at[sq], f_all.at[sq], own.at[2]),
    ]
    for copy in locals_:
        copy.start()
    for k in range(1, count):
        copy = row_copy(f_ref, f_all, row_send, row_recv, k)
        copy.start()
        started.append(copy)

    def to_core(a, b, k):
        ship(rank_of(c, a, b, k), core, 16 + a * 8 + b * 4 + k - (1 if a * 8 + b * 4 + k > 15 else 0), 16 + a * 8 + b * 4 + k)

    rounds = (0, 1, 3, 2)
    last = None
    for k in rounds:
        if k:
            arrive(c, 0, 0, k)
            ship(rank_of(c, 0, 0, k), second, 8 + k - 1, 8 + k)
            ship(rank_of(c, 0, 0, k), first, 4 + k - 1, 4 + k)
            to_core(0, 0, k)
        arrive(c, 0, 1, k)
        ship(rank_of(c, 0, 1, k), second, 11 + k, 12 + k)
        to_core(0, 1, k)
        if last is not None:
            for b in (0, 1):
                arrive(c, 1, b, last)
                to_core(1, b, last)
        last = k
    for b in (0, 1):
        arrive(c, 1, b, last)
        to_core(1, b, last)
    other = 1 - c
    for k in rounds:
        for a, b in ((0, 0), (0, 1), (1, 0), (1, 1)):
            arrive(other, a, b, k)
    for k in range(1, count):
        landing(f_ref, f_all, row_send, row_recv, k).wait_recv()
    for copy in locals_:
        copy.wait()
    for copy in started:
        copy.wait_send()


def gather_all(w, d, f):
    count = f.shape[0]
    vm = pl.BlockSpec(memory_space=pltpu.VMEM)
    hbm = pl.BlockSpec(memory_space=pl.ANY)
    return pl.pallas_call(
        gather_kernel,
        in_specs=[vm] * 3,
        out_specs=[hbm] * 3,
        out_shape=[
            jax.ShapeDtypeStruct((w.shape[0] * 32, w.shape[1]), w.dtype),
            jax.ShapeDtypeStruct((d.shape[0], d.shape[1] * 32, d.shape[2]), d.dtype),
            jax.ShapeDtypeStruct(f.shape, f.dtype),
        ],
        scratch_shapes=[
            pltpu.SemaphoreType.DMA((2, 32)),
            pltpu.SemaphoreType.DMA((2, 32)),
            pltpu.SemaphoreType.DMA((count - 1,)),
            pltpu.SemaphoreType.DMA((count - 1,)),
            pltpu.SemaphoreType.DMA((3,)),
        ],
        compiler_params=pltpu.CompilerParams(collective_id=0, has_side_effects=True),
        name="gather_all",
    )(w, d, f)


def scatter_kernel(
    w_ref, d_ref, g_ref, w_out, d_out, g_all,
    w0, d0, w1, d1, w2, d2, w3, d3, send, recv, row_send, row_recv, own,
):
    dp, sq, x, c, z, y = place()
    core, xdev, first, second = partners()
    count = g_all.shape[0]
    greet(seq_peers(dp, sq, count) + [core, xdev])
    wr = w_out.shape[0]
    dr = d_out.shape[1]

    def w_rows(rank):
        return pl.ds(pl.multiple_of(rank * wr, 16), wr)

    def d_rows(rank):
        return pl.ds(pl.multiple_of(rank * dr, 16), dr)

    def core_copies(slot):
        rank = rank_of(1 - c, lax.div(slot, 8), lax.rem(lax.div(slot, 4), 2), lax.rem(slot, 4))
        return (
            remote(w_ref.at[w_rows(rank), :], w0.at[slot], send.at[0, slot], recv.at[0, slot], core),
            remote(d_ref.at[:, d_rows(rank), :], d0.at[slot], send.at[1, slot], recv.at[1, slot], core),
        )

    def second_copies(slot):
        return (
            remote(w0.at[8 + slot], w1.at[slot], send.at[0, 16 + slot], recv.at[0, 16 + slot], second),
            remote(d0.at[8 + slot], d1.at[slot], send.at[1, 16 + slot], recv.at[1, 16 + slot], second),
        )

    def first_copies(slot):
        return (
            remote(w0.at[4 + slot], w2.at[slot], send.at[0, 24 + slot], recv.at[0, 24 + slot], first),
            remote(d0.at[4 + slot], d2.at[slot], send.at[1, 24 + slot], recv.at[1, 24 + slot], first),
        )

    def z_copies(k):
        to = (dp, lax.rem(z + k, 4) * 2 + y)
        return (
            remote(w0.at[k], w3.at[3 - k], send.at[0, 27 + k], recv.at[0, 31 - k], to),
            remote(d0.at[k], d3.at[3 - k], send.at[1, 27 + k], recv.at[1, 31 - k], to),
        )

    def begin(copies):
        for copy in copies:
            copy.start()

    def landed(copies):
        for copy in copies:
            copy.wait_recv()

    def add_w(slot, other):
        w0[slot] = (w0[slot].astype(jnp.float32) + other.astype(jnp.float32)).astype(jnp.bfloat16)

    def add_d(slot, other):
        d0[slot] = (d0[slot].astype(jnp.float32) + other.astype(jnp.float32)).astype(jnp.bfloat16)

    @pl.loop(0, 16)
    def _(step):
        begin(core_copies(15 - step))

    def take_core(slot):
        landed(core_copies(slot))
        rank = rank_of(c, lax.div(slot, 8), lax.rem(lax.div(slot, 4), 2), lax.rem(slot, 4))
        add_w(slot, w_ref[w_rows(rank), :])
        add_d(slot, d_ref[:, d_rows(rank), :])

    @pl.loop(0, 8)
    def _(step):
        take_core(15 - step)
        begin(second_copies(7 - step))

    for k in range(1, count):
        row_copy(g_ref, g_all, row_send, row_recv, k).start()
    mine = pltpu.make_async_copy(g_ref.at[sq], g_all.at[sq], own)
    mine.start()

    @pl.loop(0, 4)
    def _(step):
        slot = 7 - step
        take_core(slot)
        landed(second_copies(slot))
        add_w(slot, w1[slot])
        add_d(slot, d1[slot])
        begin(first_copies(slot - 4))

    @pl.loop(0, 3)
    def _(step):
        slot = 3 - step
        take_core(slot)
        landed(second_copies(slot))
        add_w(slot, w1[slot])
        add_d(slot, d1[slot])
        landed(first_copies(slot))
        add_w(slot, w2[slot])
        add_d(slot, d2[slot])
        begin(z_copies(slot))

    take_core(0)
    landed(second_copies(0))
    landed(first_copies(0))
    for k in (1, 2, 3):
        landed(z_copies(k))

    def total(base, parts):
        value = base.astype(jnp.float32)
        for part in parts:
            value = value + part.astype(jnp.float32)
        return value

    w_out[...] = total(w0[0], (w1[0], w2[0], w3[0], w3[1], w3[2]))
    d_out[...] = total(d0[0], (d1[0], d2[0], d3[0], d3[1], d3[2]))
    for k in range(1, count):
        landing(g_ref, g_all, row_send, row_recv, k).wait_recv()

    def sent(copies):
        for copy in copies:
            copy.wait_send()

    @pl.loop(0, 16)
    def _(slot):
        sent(core_copies(slot))

    @pl.loop(0, 8)
    def _(slot):
        sent(second_copies(slot))

    @pl.loop(0, 4)
    def _(slot):
        sent(first_copies(slot))

    for k in (1, 2, 3):
        sent(z_copies(k))
    for k in range(1, count):
        row_copy(g_ref, g_all, row_send, row_recv, k).wait_send()
    mine.wait()


def scatter_all(w, d, g):
    count = g.shape[0]
    vm = pl.BlockSpec(memory_space=pltpu.VMEM)
    hbm = pl.BlockSpec(memory_space=pl.ANY)
    wr, wc = w.shape[0] // 32, w.shape[1]
    dr, dc = d.shape[1] // 32, d.shape[2]
    bf = jnp.bfloat16
    scratch = []
    for n in (16, 8, 4, 3):
        scratch += [pltpu.VMEM((n, wr, wc), bf), pltpu.VMEM((n, d.shape[0], dr, dc), bf)]
    return pl.pallas_call(
        scatter_kernel,
        in_specs=[vm] * 3,
        out_specs=[vm, vm, hbm],
        out_shape=[
            jax.ShapeDtypeStruct((wr, wc), jnp.float32),
            jax.ShapeDtypeStruct((d.shape[0], dr, dc), jnp.float32),
            jax.ShapeDtypeStruct(g.shape, bf),
        ],
        scratch_shapes=scratch
        + [
            pltpu.SemaphoreType.DMA((2, 32)),
            pltpu.SemaphoreType.DMA((2, 32)),
            pltpu.SemaphoreType.DMA((count - 1,)),
            pltpu.SemaphoreType.DMA((count - 1,)),
            pltpu.SemaphoreType.DMA,
        ],
        compiler_params=pltpu.CompilerParams(
            collective_id=1, has_side_effects=True, vmem_limit_bytes=VMEM_LIMIT
        ),
        name="scatter_all",
    )(w, d, g)


def batch_sum_kernel(s_ref, o_ref, buf, send, recv):
    dp, sq, *_ = place()
    base = lax.div(sq, UTTS) * UTTS
    me = dp * UTTS + lax.rem(sq, UTTS)
    size = buf.shape[0]

    def device(j):
        r = lax.rem(me + j, size)
        return (lax.div(r, UTTS), base + lax.rem(r, UTTS))

    def copy(j):
        return remote(s_ref, buf.at[me], send.at[j - 1], recv.at[size - 1 - j], device(j))

    greet([device(j) for j in range(1, size)])
    for j in range(1, size):
        copy(j).start()
    buf[me] = s_ref[...]
    for j in range(1, size):
        remote(s_ref, buf.at[lax.rem(me + j, size)], send.at[j - 1], recv.at[j - 1], device(j)).wait_recv()
    o_ref[...] = jnp.sum(buf[...], axis=0)
    for j in range(1, size):
        copy(j).wait_send()


def batch_sum(sums, ident):
    vm = pl.BlockSpec(memory_space=pltpu.VMEM)
    size = 4 * UTTS
    return pl.pallas_call(
        batch_sum_kernel,
        in_specs=[vm],
        out_specs=vm,
        out_shape=jax.ShapeDtypeStruct(sums.shape, jnp.float32),
        scratch_shapes=[
            pltpu.VMEM((size,) + sums.shape, jnp.float32),
            pltpu.SemaphoreType.DMA((size - 1,)),
            pltpu.SemaphoreType.DMA((size - 1,)),
        ],
        compiler_params=pltpu.CompilerParams(collective_id=ident, has_side_effects=True),
        name="batch_sum",
    )(sums)


def rows_begin(src, dst, send, recv, own):
    dp, sq, *_ = place()
    count = dst.shape[0]
    greet(seq_peers(dp, sq, count))
    for k in range(1, count):
        row_copy(src, dst, send, recv, k).start()
    pltpu.make_async_copy(src.at[sq], dst.at[sq], own).start()


def rows_end(src, dst, send, recv, own):
    dp, sq, *_ = place()
    count = dst.shape[0]
    for k in range(1, count):
        copy = row_copy(src, dst, send, recv, k)
        copy.wait_send()
        landing(src, dst, send, recv, k).wait_recv()
    pltpu.make_async_copy(src.at[sq], dst.at[sq], own).wait()


def row_copy(src, dst, send, recv, k):
    dp, sq, *_ = place()
    count = dst.shape[0]
    to = lax.rem(sq + k, count)
    return remote(src.at[to], dst.at[sq], send.at[k - 1], recv.at[count - 1 - k], (dp, to))


def landing(src, dst, send, recv, k):
    dp, sq, *_ = place()
    origin = lax.rem(sq + k, dst.shape[0])
    return remote(src.at[sq], dst.at[origin], send.at[k - 1], recv.at[k - 1], (dp, origin))


def att_fwd_kernel(
    len_ref, qu_ref, qv_ref, k_ref, v_ref, t_ref, c_ref, ctx_ref, p_ref, c_all, send, recv, own, *, tq
):
    @pl.when(pl.program_id(0) == 0)
    def _():
        rows_begin(c_ref, c_all, send, recv, own)

    keys = k_ref.shape[0]
    span = keys + tq
    valid = lax.broadcasted_iota(jnp.int32, (1, keys), 1) < len_ref[0]

    @pl.loop(0, keys // tq)
    def _(i):
        rows = pl.ds(pl.multiple_of(i * tq, tq), tq)
        band = pl.ds(pl.multiple_of(keys - tq - i * tq, tq), span)
        for h in range(2):
            cols = slice(h * DH, (h + 1) * DH)
            content = dotf(qu_ref[rows, cols], k_ref[:, cols], NT)
            raw = dotf(qv_ref[rows, cols], t_ref[band, cols], NT)
            pos = pltpu.roll(raw, keys + 1, 1, stride=1, stride_axis=0)[:, :keys]
            s = jnp.where(valid, (content + pos) * 0.125, -1e30)
            e = jnp.exp(s - jnp.max(s, axis=1, keepdims=True))
            p = (e * (1.0 / jnp.sum(e, axis=1, keepdims=True))).astype(jnp.bfloat16)
            p_ref[h, rows, :] = p
            ctx_ref[rows, cols] = dotf(p, v_ref[:, cols]).astype(jnp.bfloat16)

    @pl.when(pl.program_id(0) == pl.num_programs(0) - 1)
    def _():
        rows_end(c_ref, c_all, send, recv, own)


def row_scratch(count):
    return [
        pltpu.SemaphoreType.DMA((count - 1,)),
        pltpu.SemaphoreType.DMA((count - 1,)),
        pltpu.SemaphoreType.DMA,
    ]


def att_fwd(length, qu, qv, k, v, table, cot, tq=384):
    rows, width = qu.shape
    blk = pl.BlockSpec((rows, 128), lambda h, *_: (0, h))
    tab = pl.BlockSpec((2 * rows, 128), lambda h, *_: (0, h))
    return pl.pallas_call(
        lambda *refs: att_fwd_kernel(*refs, tq=tq),
        grid_spec=pltpu.PrefetchScalarGridSpec(
            num_scalar_prefetch=1,
            grid=(width // 128,),
            in_specs=[blk] * 4 + [tab, pl.BlockSpec(memory_space=pltpu.VMEM)],
            out_specs=[
                blk,
                pl.BlockSpec((2, rows, rows), lambda h, *_: (h, 0, 0)),
                pl.BlockSpec(memory_space=pl.ANY),
            ],
            scratch_shapes=row_scratch(cot.shape[0]),
        ),
        out_shape=[
            jax.ShapeDtypeStruct((rows, width), jnp.bfloat16),
            jax.ShapeDtypeStruct((width // DH, rows, rows), jnp.bfloat16),
            jax.ShapeDtypeStruct(cot.shape, cot.dtype),
        ],
        compiler_params=pltpu.CompilerParams(
            collective_id=4, has_side_effects=True, vmem_limit_bytes=VMEM_LIMIT
        ),
        name="att_fwd",
    )(length, qu, qv, k, v, table, cot)


def att_bwd_kernel(
    p_ref, g_ref, qu_ref, qv_ref, k_ref, v_ref, t_ref, m_ref,
    dqu_ref, dqv_ref, dk_ref, dv_ref, dt_ref, m_all, ds_sc, dt_sc, send, recv, own, *, tq,
):
    @pl.when(pl.program_id(0) == 0)
    def _():
        rows_begin(m_ref, m_all, send, recv, own)

    keys = k_ref.shape[0]
    span = keys + tq
    low = jnp.bfloat16
    flip = (
        lax.broadcasted_iota(jnp.int32, (tq, tq), 0) + lax.broadcasted_iota(jnp.int32, (tq, tq), 1) == tq - 1
    ).astype(low)
    pad = jnp.zeros((tq, tq), jnp.float32)
    dt_sc[...] = jnp.zeros_like(dt_sc)

    @pl.loop(0, keys // tq)
    def _(i):
        rows = pl.ds(pl.multiple_of(i * tq, tq), tq)
        band = pl.ds(pl.multiple_of(keys - tq - i * tq, tq), span)
        for h in range(2):
            cols = slice(h * DH, (h + 1) * DH)
            dp = dotf(g_ref[rows, cols], v_ref[:, cols], NT)
            pf = p_ref[h, rows, :].astype(jnp.float32)
            ds = (pf * (dp - jnp.sum(dp * pf, axis=1, keepdims=True))).astype(low)
            ds_sc[h, rows, :] = ds
            dqu_ref[rows, cols] = dotf(ds, k_ref[:, cols]) * 0.125
            back = jnp.concatenate([dotf(flip, ds), pad], axis=1)
            raw = pltpu.roll(back, 0, 1, stride=1, stride_axis=0).astype(low)
            dqv = dotf(raw, t_ref[band, cols]).astype(low)
            dqv_ref[rows, cols] = dotf(flip, dqv) * 0.125
            qv = dotf(flip, qv_ref[rows, cols]).astype(low)
            dt_sc[h, band, :] += dotf(raw, qv, TN)

    for h in range(2):
        cols = slice(h * DH, (h + 1) * DH)
        dt_ref[:, cols] = (dt_sc[h] * 0.125).astype(low)
        dk_ref[:, cols] = dotf(ds_sc[h], qu_ref[:, cols], TN) * 0.125
        dv_ref[:, cols] = dotf(p_ref[h], g_ref[:, cols], TN)

    @pl.when(pl.program_id(0) == pl.num_programs(0) - 1)
    def _():
        rows_end(m_ref, m_all, send, recv, own)


def att_bwd(p, g, qu, qv, k, v, table, mixed, tq=256):
    rows, width = qu.shape
    blk = pl.BlockSpec((rows, 128), lambda h: (0, h))
    tab = pl.BlockSpec((2 * rows, 128), lambda h: (0, h))
    out = jax.ShapeDtypeStruct((rows, width), jnp.float32)
    return pl.pallas_call(
        lambda *refs: att_bwd_kernel(*refs, tq=tq),
        grid=(width // 128,),
        in_specs=[pl.BlockSpec((2, rows, rows), lambda h: (h, 0, 0))] + [blk] * 5
        + [tab, pl.BlockSpec(memory_space=pltpu.VMEM)],
        out_specs=[blk] * 4 + [tab, pl.BlockSpec(memory_space=pl.ANY)],
        out_shape=[out] * 4
        + [
            jax.ShapeDtypeStruct((2 * rows, width), jnp.bfloat16),
            jax.ShapeDtypeStruct(mixed.shape, mixed.dtype),
        ],
        scratch_shapes=[pltpu.VMEM((2, rows, rows), jnp.bfloat16), pltpu.VMEM((2, 2 * rows, DH), jnp.float32)]
        + row_scratch(mixed.shape[0]),
        compiler_params=pltpu.CompilerParams(
            collective_id=5, has_side_effects=True, vmem_limit_bytes=VMEM_LIMIT
        ),
        name="att_bwd",
    )(p, g, qu, qv, k, v, table, mixed)


def position_table(length, width):
    offsets = (length - 1 - np.arange(2 * length)).astype(np.float32)
    half = width // 2
    steps = np.arange(half, dtype=np.float32) * np.float32(-2.0 * math.log(10000.0) / width)
    angles = (offsets[:, None] * np.exp(steps)[None, :]).astype(np.float64)
    table = np.concatenate([np.sin(angles), np.cos(angles)], axis=1)
    return jnp.asarray(table.astype(np.float32)).astype(jnp.bfloat16)


def shifted_sum(values, kernel_f, reverse):
    taps = kernel_f.shape[1]
    reach = (taps - 1) // 2
    padded = jnp.pad(values, ((reach, reach), (0, 0)))
    rows = values.shape[0]
    total = None
    for k in range(taps):
        at = taps - 1 - k if reverse else k
        term = padded[at : at + rows].astype(jnp.float32) * kernel_f[:, k]
        total = term if total is None else total + term
    return total


def tap_grads(values, grad, taps):
    reach = (taps - 1) // 2
    padded = jnp.pad(values, ((reach, reach), (0, 0)))
    rows = values.shape[0]
    grad_f = grad.astype(jnp.float32)
    return jnp.stack(
        [jnp.sum(padded[k : k + rows].astype(jnp.float32) * grad_f, axis=0) for k in range(taps)]
    )


def local_whole(
    frames,
    lengths,
    cotangent,
    gains,
    shifts,
    rel_bias,
    ffn_up,
    ffn_down,
    attn_in,
    attn_out,
    pos_proj,
    conv_in,
    depthwise,
    conv_out,
):
    low = jnp.bfloat16
    dp, sq = lax.axis_index("dp"), lax.axis_index("seq")
    count, width_rows, model = frames.shape
    length = count * 0 + width_rows * lax.axis_size("seq")
    taps = depthwise.shape[2]
    small = jnp.concatenate([gains[0], shifts[0], rel_bias[0]], axis=0).T
    small = jnp.concatenate([small, depthwise[0]], axis=1)
    small = jnp.pad(small, ((0, 0), (0, COLS[-1] - small.shape[1])))
    packed = jnp.concatenate(
        [ffn_up[0, 0], ffn_up[0, 1], attn_in[0], attn_out[0], pos_proj[0], conv_in[0], conv_out[0], small],
        axis=1,
    )
    w_all, down, f_all = gather_all(packed, ffn_down[0], frames.astype(low))
    cuts = np.cumsum((0,) + COLS)
    up_0, up_1, w_attn_in, w_attn_out, w_pos, w_conv_in, w_conv_out, small = (
        w_all[:, int(lo) : int(hi)] for lo, hi in zip(cuts[:-1], cuts[1:])
    )
    small = small.astype(jnp.float32).T
    gain, shift, rel = small[0:6], small[6:12], small[12:14]
    kernel_f = small[14 : 14 + taps].T
    own_length = lax.dynamic_slice_in_dim(lengths, dp * count + sq, 1)
    grid = lengths.reshape(lax.axis_size("dp"), MB, UTTS)
    per_batch = jnp.sum(grid, axis=(0, 2)).astype(jnp.float32)
    frame_count = lax.dynamic_slice_in_dim(per_batch, lax.div(sq, UTTS), 1)[0]
    mask = (jnp.arange(length, dtype=jnp.int32) < own_length[0]).astype(jnp.float32)[:, None]
    table_in = position_table(length, model)

    x0 = f_all.reshape(length, model).astype(jnp.float32)
    x1, kept_one = ffn_forward(x0, gain[0], shift[0], up_0, down[0])
    a1 = layer_norm(x1, gain[1], shift[1]).astype(low)
    proj = matmul_low(a1, w_attn_in)
    query = proj[:, :model]
    qu = (query + rel[0]).astype(low)
    qv = (query + rel[1]).astype(low)
    key = proj[:, model : 2 * model].astype(low)
    value = proj[:, 2 * model :].astype(low)
    table = matmul_low(table_in, w_pos).astype(low)
    ctx, probs, c_all = att_fwd(own_length, qu, qv, key, value, table, cotangent.astype(low))
    x2 = x1 + matmul_low(ctx, w_attn_out)

    a2 = layer_norm(x2, gain[2], shift[2]).astype(low)
    gate = matmul_low(a2, w_conv_in)
    gated = (glu_gate(gate) * mask).astype(low)
    depth = shifted_sum(gated, kernel_f, False)
    sums = jnp.stack([jnp.sum(depth * mask, axis=0), jnp.sum(depth * depth * mask, axis=0)])
    sums = batch_sum(sums, 2)
    mean = sums[0] / frame_count
    var = sums[1] / frame_count - mean * mean
    inv = lax.rsqrt(var + 1e-05)
    normal = (depth - mean) * inv * gain[5] + shift[5]
    active = jax.nn.silu(normal).astype(low)
    x3 = x2 + matmul_low(active, w_conv_out)
    x4, kept_two = ffn_forward(x3, gain[3], shift[3], up_1, down[1])
    mixed = layer_norm(x4, gain[4], shift[4])

    cot = c_all.reshape(length, model).astype(jnp.float32)
    grad, g_gain4, g_shift4 = jax.vjp(layer_norm, x4, gain[4], shift[4])[1](cot)
    grad, (g_gain3, g_shift3, g_up1, g_down1) = ffn_backward(
        grad, kept_two, gain[3], shift[3], up_1, down[1]
    )
    grad_b = grad.astype(low)
    g_conv_out = weight_grad(active, grad_b)
    grad_active = matmul_back(grad_b, w_conv_out)
    grad_normal = jax.vjp(jax.nn.silu, normal)[1](grad_active)[0]
    g_gain5 = jnp.sum(grad_normal * ((depth - mean) * inv), axis=0)
    g_shift5 = jnp.sum(grad_normal, axis=0)
    hat = grad_normal * gain[5]
    sums = batch_sum(jnp.stack([jnp.sum(hat, axis=0), jnp.sum(hat * depth, axis=0)]), 3)
    grad_var = -0.5 * inv * inv * inv * (sums[1] - mean * sums[0])
    grad_mean = -inv * sums[0] - 2.0 * mean * grad_var
    grad_depth = (
        hat * inv + mask * (grad_mean / frame_count + 2.0 * depth * grad_var / frame_count)
    ).astype(low)
    grad_gated = shifted_sum(grad_depth, kernel_f, True) * mask
    g_kernel = tap_grads(gated, grad_depth, taps)
    grad_gate = jax.vjp(glu_gate, gate)[1](grad_gated)[0].astype(low)
    g_conv_in = weight_grad(a2, grad_gate)
    grad_ln, g_gain2, g_shift2 = jax.vjp(layer_norm, x2, gain[2], shift[2])[1](
        matmul_back(grad_gate, w_conv_in)
    )
    grad = grad + grad_ln

    grad_b = grad.astype(low)
    g_attn_out = weight_grad(ctx, grad_b)
    grad_ctx = matmul_back(grad_b, w_attn_out).astype(low)
    dqu, dqv, dkey, dvalue, dtable, m_all = att_bwd(
        probs, grad_ctx, qu, qv, key, value, table, mixed.astype(low).reshape(frames.shape)
    )
    g_rel = jnp.stack([jnp.sum(dqu, axis=0), jnp.sum(dqv, axis=0)])
    grad_proj = jnp.concatenate([dqu + dqv, dkey, dvalue], axis=1).astype(low)
    g_pos = weight_grad(table_in, dtable)
    g_attn_in = weight_grad(a1, grad_proj)
    grad_ln, g_gain1, g_shift1 = jax.vjp(layer_norm, x1, gain[1], shift[1])[1](
        matmul_back(grad_proj, w_attn_in)
    )
    grad = grad + grad_ln
    grad, (g_gain0, g_shift0, g_up0, g_down0) = ffn_backward(
        grad, kept_one, gain[0], shift[0], up_0, down[0]
    )

    g_small = jnp.concatenate(
        [
            jnp.stack([g_gain0, g_gain1, g_gain2, g_gain3, g_gain4, g_gain5]),
            jnp.stack([g_shift0, g_shift1, g_shift2, g_shift3, g_shift4, g_shift5]),
            g_rel,
            g_kernel,
        ]
    )
    g_small = jnp.pad(g_small, ((0, COLS[-1] - g_small.shape[0]), (0, 0))).T
    g_packed = jnp.concatenate(
        [
            member.astype(low)
            for member in (g_up0, g_up1, g_attn_in, g_attn_out, g_pos, g_conv_in, g_conv_out, g_small)
        ],
        axis=1,
    )
    g_down = jnp.stack([g_down0, g_down1]).astype(low)
    w_sum, d_sum, g_all = scatter_all(g_packed, g_down, grad.astype(low).reshape(frames.shape))
    parts = [w_sum[:, int(lo) : int(hi)] for lo, hi in zip(cuts[:-1], cuts[1:])]
    tail = parts[7][:, : 14 + taps]
    rows = tail[:, :14].T
    return (
        m_all.astype(jnp.float32),
        g_all.astype(jnp.float32),
        rows[None, 0:6],
        rows[None, 6:12],
        rows[None, 12:14],
        jnp.stack([parts[0], parts[1]])[None],
        d_sum[None],
        parts[2][None],
        parts[3][None],
        parts[4][None],
        parts[5][None],
        tail[None, :, 14:],
        parts[6][None],
    )


def solution(mesh):
    body = local_whole if fits_whole(mesh) else local_general
    in_specs = (
        P("dp", "seq", None),
        P(),
        P("dp", "seq", None),
        P(None, None, ("dp", "seq")),
        P(None, None, ("dp", "seq")),
        P(None, None, ("dp", "seq")),
        P(None, None, ("dp", "seq"), None),
        P(None, None, ("dp", "seq"), None),
        P(None, ("dp", "seq"), None),
        P(None, ("dp", "seq"), None),
        P(None, ("dp", "seq"), None),
        P(None, ("dp", "seq"), None),
        P(None, ("dp", "seq"), None),
        P(None, ("dp", "seq"), None),
    )
    out_specs = (
        P("dp", "seq", None),
        P("dp", "seq", None),
        P(None, None, ("dp", "seq")),
        P(None, None, ("dp", "seq")),
        P(None, None, ("dp", "seq")),
        P(None, None, ("dp", "seq"), None),
        P(None, None, ("dp", "seq"), None),
        P(None, ("dp", "seq"), None),
        P(None, ("dp", "seq"), None),
        P(None, ("dp", "seq"), None),
        P(None, ("dp", "seq"), None),
        P(None, ("dp", "seq"), None),
        P(None, ("dp", "seq"), None),
    )
    return jax.shard_map(body, mesh=mesh, in_specs=in_specs, out_specs=out_specs, check_vma=False)
```

```python
import math

import jax
import jax.numpy as jnp
import numpy as np
from jax import lax
from jax.experimental import pallas as pl
from jax.experimental.pallas import tpu as pltpu
from jax.sharding import PartitionSpec as P

H = 8
DH = 64
NL = 1
MB = 2


HIGHEST_PREC = lax.Precision.HIGHEST


def extended(cells, sides, width):
    for axis, dim in sides:
        count = lax.axis_size(axis)
        ends = count - 1
        head = lax.slice_in_dim(cells, 0, width, axis=dim)
        tail = lax.slice_in_dim(cells, cells.shape[dim] - width, cells.shape[dim], axis=dim)
        cells = jnp.concatenate(
            [
                lax.ppermute(tail, axis, [(i, (i + 1) % count) for i in range(ends)]),
                cells,
                lax.ppermute(head, axis, [((i + 1) % count, i) for i in range(ends)]),
            ],
            axis=dim,
        )
    return cells


def layer_norm(values, gain_row, shift_row):
    centred = values - jnp.mean(values, axis=-1, keepdims=True)
    spread = jnp.mean(centred * centred, axis=-1, keepdims=True)
    return centred * lax.rsqrt(spread + 1e-05) * gain_row + shift_row


def sinusoid(offsets, model_width):
    half_width = model_width // 2
    frequency = jnp.exp(
        jnp.arange(half_width, dtype=jnp.float32) * (-2.0 * math.log(10000.0) / model_width)
    )
    angles = offsets.astype(jnp.float32)[:, None] * frequency[None, :]
    return jnp.concatenate([jnp.sin(angles), jnp.cos(angles)], axis=1)


def skew_rows(raw_pos, key_count):
    row_count = raw_pos.shape[-2]
    col_count = raw_pos.shape[-1]
    lead = raw_pos.shape[:-2]
    flat_rows = raw_pos.reshape(lead + (row_count * col_count,))
    flat_rows = flat_rows[..., row_count - 1 : row_count - 1 + row_count * (col_count - 1)]
    return flat_rows.reshape(lead + (row_count, col_count - 1))[..., :key_count]


def skew_back(grad_skew, raw_shape, key_count):
    zero_raw = jnp.zeros(raw_shape, jnp.float32)
    return jax.vjp(lambda raw_pos: skew_rows(raw_pos, key_count), zero_raw)[1](grad_skew)[0]


def glu_gate(gate_pair):
    half_width = gate_pair.shape[-1] // 2
    return gate_pair[..., :half_width] * jax.nn.sigmoid(gate_pair[..., half_width:])


def matmul_low(left, right):
    return jnp.dot(left, right, preferred_element_type=jnp.float32)


def matmul_back(grad_low, weight):
    return lax.dot_general(
        grad_low, weight, (((1,), (1,)), ((), ())), preferred_element_type=jnp.float32
    )


def weight_grad(inputs_low, grad_low):
    return lax.dot_general(
        inputs_low, grad_low, (((0,), (0,)), ((), ())), preferred_element_type=jnp.float32
    )


def ffn_forward(row_data, gain_row, shift_row, w_up, w_down):
    normed_b = layer_norm(row_data, gain_row, shift_row).astype(jnp.bfloat16)
    hidden = matmul_low(normed_b, w_up)
    active_b = jax.nn.silu(hidden).astype(jnp.bfloat16)
    branch = matmul_low(active_b, w_down)
    return (row_data + 0.5 * branch, (row_data, normed_b, hidden, active_b))


def ffn_backward(grad_rows, kept_data, gain_row, shift_row, w_up, w_down):
    row_data, normed_b, hidden, active_b = kept_data
    grad_out_b = (0.5 * grad_rows).astype(jnp.bfloat16)
    g_down = weight_grad(active_b, grad_out_b)
    grad_active = matmul_back(grad_out_b, w_down)
    grad_hidden_b = jax.vjp(jax.nn.silu, hidden)[1](grad_active)[0].astype(jnp.bfloat16)
    g_up = weight_grad(normed_b, grad_hidden_b)
    grad_normed = matmul_back(grad_hidden_b, w_up)
    grad_ln, g_gain, g_shift = jax.vjp(layer_norm, row_data, gain_row, shift_row)[1](grad_normed)
    return (grad_rows + grad_ln, (g_gain, g_shift, g_up, g_down))


def attention_logits(query_u_b, query_v_b, key_heads, pos_heads, key_valid):
    content = jnp.einsum(
        "ufhd,ulhd->uhfl", query_u_b, key_heads, preferred_element_type=jnp.float32
    )
    raw_pos = jnp.einsum("ufhd,whd->uhfw", query_v_b, pos_heads, preferred_element_type=jnp.float32)
    logits = (content + skew_rows(raw_pos, key_heads.shape[1])) * 0.125
    return jnp.where(key_valid[:, None, None, :], logits, -1e30)


def attn_forward(
    row_data,
    utt_count,
    gain_row,
    shift_row,
    bias_u,
    bias_v,
    w_in,
    w_out,
    w_pos,
    key_valid,
    pos_table_b,
):
    model_width = row_data.shape[1]
    frame_len = row_data.shape[0] // utt_count
    normed_b = layer_norm(row_data, gain_row, shift_row).astype(jnp.bfloat16)
    proj_rows = matmul_low(normed_b, w_in)
    query_rows = proj_rows[:, :model_width].reshape(utt_count, frame_len, H, DH)
    key_b = (
        proj_rows[:, model_width : 2 * model_width]
        .astype(jnp.bfloat16)
        .reshape(utt_count, frame_len, model_width)
    )
    value_b = (
        proj_rows[:, 2 * model_width :]
        .astype(jnp.bfloat16)
        .reshape(utt_count, frame_len, model_width)
    )
    all_keys, all_values = (
        lax.all_gather(key_b, "seq", axis=1, tiled=True),
        lax.all_gather(value_b, "seq", axis=1, tiled=True),
    )
    key_heads = all_keys.reshape(utt_count, -1, H, DH)
    value_heads = all_values.reshape(utt_count, -1, H, DH)
    query_u_b = (query_rows + bias_u.reshape(H, DH)).astype(jnp.bfloat16)
    query_v_b = (query_rows + bias_v.reshape(H, DH)).astype(jnp.bfloat16)
    pos_heads = matmul_low(pos_table_b, w_pos).astype(jnp.bfloat16).reshape(-1, H, DH)
    logits = attention_logits(query_u_b, query_v_b, key_heads, pos_heads, key_valid)
    top_score = jnp.max(logits, axis=-1, keepdims=True)
    exp_scores = jnp.exp(logits - top_score)
    row_total = jnp.sum(exp_scores, axis=-1, keepdims=True)
    prob_b = (exp_scores / row_total).astype(jnp.bfloat16)
    log_total = top_score + jnp.log(row_total)
    context = jnp.einsum("uhfl,ulhd->ufhd", prob_b, value_heads, preferred_element_type=jnp.float32)
    context_b = context.astype(jnp.bfloat16).reshape(-1, model_width)
    branch = matmul_low(context_b, w_out)
    kept_data = (
        row_data,
        normed_b,
        query_u_b,
        query_v_b,
        key_heads,
        value_heads,
        pos_heads,
        log_total,
        context_b,
    )
    return (row_data + branch, kept_data)


def attn_backward(grad_rows, kept_data, gain_row, shift_row, w_in, w_out, key_valid, pos_table_b):
    (
        row_data,
        normed_b,
        query_u_b,
        query_v_b,
        key_heads,
        value_heads,
        pos_heads,
        log_total,
        context_b,
    ) = kept_data
    utt_count = query_u_b.shape[0]
    frame_len = query_u_b.shape[1]
    model_width = row_data.shape[1]
    key_len = key_heads.shape[1]
    grad_out_b = grad_rows.astype(jnp.bfloat16)
    g_out = weight_grad(context_b, grad_out_b)
    grad_context_b = (
        matmul_back(grad_out_b, w_out).astype(jnp.bfloat16).reshape(utt_count, frame_len, H, DH)
    )
    logits = attention_logits(query_u_b, query_v_b, key_heads, pos_heads, key_valid)
    prob_rows = jnp.exp(logits - log_total)
    grad_probs = jnp.einsum(
        "ufhd,ulhd->uhfl", grad_context_b, value_heads, preferred_element_type=jnp.float32
    )
    inner_sum = jnp.sum(grad_probs * prob_rows, axis=-1, keepdims=True)
    grad_logits_b = (prob_rows * (grad_probs - inner_sum)).astype(jnp.bfloat16) * 0.125
    grad_query_u = jnp.einsum(
        "uhfl,ulhd->ufhd", grad_logits_b, key_heads, preferred_element_type=jnp.float32
    )
    raw_shape = (utt_count, H, frame_len, pos_heads.shape[0])
    grad_raw_b = skew_back(grad_logits_b.astype(jnp.float32), raw_shape, key_len).astype(
        jnp.bfloat16
    )
    grad_query_v = jnp.einsum(
        "uhfw,whd->ufhd", grad_raw_b, pos_heads, preferred_element_type=jnp.float32
    )
    grad_pos = jnp.einsum(
        "uhfw,ufhd->whd", grad_raw_b, query_v_b, preferred_element_type=jnp.float32
    )
    grad_pos = grad_pos.reshape(-1, model_width)
    g_pos = lax.dot_general(
        pos_table_b.astype(jnp.float32),
        grad_pos,
        (((0,), (0,)), ((), ())),
        precision=HIGHEST_PREC,
        preferred_element_type=jnp.float32,
    )
    prob_b = prob_rows.astype(jnp.bfloat16)
    grad_values = jnp.einsum(
        "uhfl,ufhd->ulhd", prob_b, grad_context_b, preferred_element_type=jnp.float32
    )
    grad_keys = jnp.einsum(
        "uhfl,ufhd->ulhd", grad_logits_b, query_u_b, preferred_element_type=jnp.float32
    )
    own_keys, own_values = (
        lax.psum_scatter(
            grad_keys.reshape(utt_count, key_len, model_width),
            "seq",
            scatter_dimension=1,
            tiled=True,
        ),
        lax.psum_scatter(
            grad_values.reshape(utt_count, key_len, model_width),
            "seq",
            scatter_dimension=1,
            tiled=True,
        ),
    )
    g_bias_u = jnp.sum(grad_query_u, axis=(0, 1)).reshape(-1)
    g_bias_v = jnp.sum(grad_query_v, axis=(0, 1)).reshape(-1)
    grad_proj_b = jnp.concatenate(
        [
            (grad_query_u + grad_query_v).reshape(-1, model_width),
            own_keys.reshape(-1, model_width),
            own_values.reshape(-1, model_width),
        ],
        axis=1,
    ).astype(jnp.bfloat16)
    g_in = weight_grad(normed_b, grad_proj_b)
    grad_normed = matmul_back(grad_proj_b, w_in)
    grad_ln, g_gain, g_shift = jax.vjp(layer_norm, row_data, gain_row, shift_row)[1](grad_normed)
    return (grad_rows + grad_ln, (g_gain, g_shift, g_bias_u, g_bias_v, g_in, g_out, g_pos))


def conv_forward(
    row_data,
    utt_count,
    gain_row,
    shift_row,
    w_in,
    kernel,
    bn_gain,
    bn_shift,
    w_out,
    frame_mask,
    frame_count,
):
    model_width = row_data.shape[1]
    frame_len = row_data.shape[0] // utt_count
    normed_b = layer_norm(row_data, gain_row, shift_row).astype(jnp.bfloat16)
    gate_pair = matmul_low(normed_b, w_in)
    mask_rows = frame_mask.reshape(-1, 1)
    gated_b = (
        (glu_gate(gate_pair) * mask_rows)
        .astype(jnp.bfloat16)
        .reshape(utt_count, frame_len, model_width)
    )
    halo_reach = (kernel.shape[1] - 1) // 2
    padded = extended(gated_b, (("seq", 1),), halo_reach)
    kernel_f = kernel.astype(jnp.float32)
    depth_out = padded[:, 0:frame_len].astype(jnp.float32) * kernel_f[:, 0]
    for tap_idx in range(1, kernel.shape[1]):
        depth_out = (
            depth_out
            + padded[:, tap_idx : tap_idx + frame_len].astype(jnp.float32) * kernel_f[:, tap_idx]
        )
    weight_mask = frame_mask[:, :, None]
    sum_local = jnp.sum(depth_out * weight_mask, axis=(0, 1))
    square_local = jnp.sum(depth_out * depth_out * weight_mask, axis=(0, 1))
    sum_all, square_all = lax.psum((sum_local, square_local), ("dp", "seq"))
    mean_val = sum_all / frame_count
    variance = square_all / frame_count - mean_val * mean_val
    inv_std = lax.rsqrt(variance + 1e-05)
    normal = (depth_out - mean_val) * inv_std * bn_gain + bn_shift
    active_b = jax.nn.silu(normal).astype(jnp.bfloat16).reshape(-1, model_width)
    branch = matmul_low(active_b, w_out)
    kept_data = (
        row_data,
        normed_b,
        gate_pair,
        padded,
        depth_out,
        mean_val,
        inv_std,
        normal,
        active_b,
    )
    return (row_data + branch, kept_data)


def conv_backward(
    grad_rows, kept_data, gain_row, shift_row, w_in, kernel, bn_gain, w_out, frame_mask, frame_count
):
    row_data, normed_b, gate_pair, padded, depth_out, mean_val, inv_std, normal, active_b = (
        kept_data
    )
    frame_len = depth_out.shape[1]
    model_width = depth_out.shape[2]
    grad_out_b = grad_rows.astype(jnp.bfloat16)
    g_out = weight_grad(active_b, grad_out_b)
    grad_active = matmul_back(grad_out_b, w_out).reshape(depth_out.shape)
    grad_normal = jax.vjp(jax.nn.silu, normal)[1](grad_active)[0]
    centred_hat = (depth_out - mean_val) * inv_std
    g_bn_gain = jnp.sum(grad_normal * centred_hat, axis=(0, 1))
    g_bn_shift = jnp.sum(grad_normal, axis=(0, 1))
    grad_hat = grad_normal * bn_gain
    part_one = jnp.sum(grad_hat, axis=(0, 1))
    part_two = jnp.sum(grad_hat * depth_out, axis=(0, 1))
    part_one, part_two = lax.psum((part_one, part_two), ("dp", "seq"))
    grad_inv = part_two - mean_val * part_one
    grad_var = -0.5 * inv_std * inv_std * inv_std * grad_inv
    grad_mean = -inv_std * part_one - 2.0 * mean_val * grad_var
    weight_mask = frame_mask[:, :, None]
    grad_depth_b = (
        grad_hat * inv_std
        + weight_mask * (grad_mean / frame_count + 2.0 * depth_out * grad_var / frame_count)
    ).astype(jnp.bfloat16)
    halo_reach = (kernel.shape[1] - 1) // 2
    grad_padded = extended(grad_depth_b, (("seq", 1),), halo_reach)
    kernel_f = kernel.astype(jnp.float32)
    grad_depth_f = grad_depth_b.astype(jnp.float32)
    grad_gated = jnp.zeros(depth_out.shape, jnp.float32)
    kernel_cols = []
    for tap_idx in range(kernel.shape[1]):
        begin_at = 2 * halo_reach - tap_idx
        grad_gated = (
            grad_gated
            + grad_padded[:, begin_at : begin_at + frame_len].astype(jnp.float32)
            * kernel_f[:, tap_idx]
        )
        kernel_cols.append(
            jnp.sum(
                padded[:, tap_idx : tap_idx + frame_len].astype(jnp.float32) * grad_depth_f,
                axis=(0, 1),
            )
        )
    g_kernel = jnp.stack(kernel_cols, axis=1)
    grad_gate_b = jax.vjp(glu_gate, gate_pair)[1](
        (grad_gated * weight_mask).reshape(-1, model_width)
    )[0]
    grad_gate_b = grad_gate_b.astype(jnp.bfloat16)
    g_in = weight_grad(normed_b, grad_gate_b)
    grad_normed = matmul_back(grad_gate_b, w_in)
    grad_ln, g_gain, g_shift = jax.vjp(layer_norm, row_data, gain_row, shift_row)[1](grad_normed)
    return (grad_rows + grad_ln, (g_gain, g_shift, g_in, g_kernel, g_bn_gain, g_bn_shift, g_out))


def layer_forward(values, weights, frame_mask, key_valid, frame_count, pos_table_b):
    (
        gain_set,
        shift_set,
        rel_set,
        up_pair,
        down_pair,
        attn_in_w,
        attn_out_w,
        pos_w,
        conv_in_w,
        kernel,
        conv_out_w,
    ) = weights
    gain_f = gain_set.astype(jnp.float32)
    shift_f = shift_set.astype(jnp.float32)
    rel_f = rel_set.astype(jnp.float32)
    utt_count = values.shape[0]
    row_data = values.reshape(-1, values.shape[2])
    row_data, kept_one = ffn_forward(row_data, gain_f[0], shift_f[0], up_pair[0], down_pair[0])
    row_data, kept_attn = attn_forward(
        row_data,
        utt_count,
        gain_f[1],
        shift_f[1],
        rel_f[0],
        rel_f[1],
        attn_in_w,
        attn_out_w,
        pos_w,
        key_valid,
        pos_table_b,
    )
    row_data, kept_conv = conv_forward(
        row_data,
        utt_count,
        gain_f[2],
        shift_f[2],
        conv_in_w,
        kernel,
        gain_f[5],
        shift_f[5],
        conv_out_w,
        frame_mask,
        frame_count,
    )
    row_data, kept_two = ffn_forward(row_data, gain_f[3], shift_f[3], up_pair[1], down_pair[1])
    result = layer_norm(row_data, gain_f[4], shift_f[4])
    return (result.reshape(values.shape), (kept_one, kept_attn, kept_conv, kept_two, row_data))


def layer_backward(
    grad_values, kept_data, weights, frame_mask, key_valid, frame_count, pos_table_b
):
    (
        gain_set,
        shift_set,
        rel_set,
        up_pair,
        down_pair,
        attn_in_w,
        attn_out_w,
        pos_w,
        conv_in_w,
        kernel,
        conv_out_w,
    ) = weights
    gain_f = gain_set.astype(jnp.float32)
    shift_f = shift_set.astype(jnp.float32)
    kept_one, kept_attn, kept_conv, kept_two, last_rows = kept_data
    grad_rows = grad_values.reshape(-1, grad_values.shape[2])
    grad_rows, g_gain_last, g_shift_last = jax.vjp(layer_norm, last_rows, gain_f[4], shift_f[4])[1](
        grad_rows
    )
    grad_rows, two_grads = ffn_backward(
        grad_rows, kept_two, gain_f[3], shift_f[3], up_pair[1], down_pair[1]
    )
    grad_rows, conv_grads = conv_backward(
        grad_rows,
        kept_conv,
        gain_f[2],
        shift_f[2],
        conv_in_w,
        kernel,
        gain_f[5],
        conv_out_w,
        frame_mask,
        frame_count,
    )
    grad_rows, attn_grads = attn_backward(
        grad_rows, kept_attn, gain_f[1], shift_f[1], attn_in_w, attn_out_w, key_valid, pos_table_b
    )
    grad_rows, one_grads = ffn_backward(
        grad_rows, kept_one, gain_f[0], shift_f[0], up_pair[0], down_pair[0]
    )
    grad_gains = jnp.stack(
        [one_grads[0], attn_grads[0], conv_grads[0], two_grads[0], g_gain_last, conv_grads[4]]
    )
    grad_shifts = jnp.stack(
        [one_grads[1], attn_grads[1], conv_grads[1], two_grads[1], g_shift_last, conv_grads[5]]
    )
    grad_rel = jnp.stack([attn_grads[2], attn_grads[3]])
    grad_up = jnp.stack([one_grads[2], two_grads[2]])
    grad_down = jnp.stack([one_grads[3], two_grads[3]])
    layer_grads = (
        grad_gains,
        grad_shifts,
        grad_rel,
        grad_up,
        grad_down,
        attn_grads[4],
        attn_grads[5],
        attn_grads[6],
        conv_grads[2],
        conv_grads[3],
        conv_grads[6],
    )
    return (grad_rows.reshape(grad_values.shape), layer_grads)


def gather_forward(shards, layer_idx):
    pieces = tuple((member[layer_idx] for member in shards))
    return (
        lax.all_gather(pieces[0], ("dp", "seq"), axis=1, tiled=True),
        lax.all_gather(pieces[1], ("dp", "seq"), axis=1, tiled=True),
        lax.all_gather(pieces[2], ("dp", "seq"), axis=1, tiled=True),
        lax.all_gather(pieces[3], ("dp", "seq"), axis=1, tiled=True),
        lax.all_gather(pieces[4], ("dp", "seq"), axis=1, tiled=True),
        lax.all_gather(pieces[5], ("dp", "seq"), axis=0, tiled=True),
        lax.all_gather(pieces[6], ("dp", "seq"), axis=0, tiled=True),
        lax.all_gather(pieces[7], ("dp", "seq"), axis=0, tiled=True),
        lax.all_gather(pieces[8], ("dp", "seq"), axis=0, tiled=True),
        lax.all_gather(pieces[9], ("dp", "seq"), axis=0, tiled=True),
        lax.all_gather(pieces[10], ("dp", "seq"), axis=0, tiled=True),
    )


def gather_backward(shards, layer_idx):
    pieces = tuple((member[layer_idx] for member in shards))
    return (
        lax.all_gather(pieces[0], ("dp", "seq"), axis=1, tiled=True),
        lax.all_gather(pieces[1], ("dp", "seq"), axis=1, tiled=True),
        lax.all_gather(pieces[2], ("dp", "seq"), axis=1, tiled=True),
        lax.all_gather(pieces[3], ("dp", "seq"), axis=1, tiled=True),
        lax.all_gather(pieces[4], ("dp", "seq"), axis=1, tiled=True),
        lax.all_gather(pieces[5], ("dp", "seq"), axis=0, tiled=True),
        lax.all_gather(pieces[6], ("dp", "seq"), axis=0, tiled=True),
        lax.all_gather(pieces[7], ("dp", "seq"), axis=0, tiled=True),
        lax.all_gather(pieces[8], ("dp", "seq"), axis=0, tiled=True),
        lax.all_gather(pieces[9], ("dp", "seq"), axis=0, tiled=True),
        lax.all_gather(pieces[10], ("dp", "seq"), axis=0, tiled=True),
    )


def local_general(
    frames,
    lengths,
    cotangent,
    gains,
    shifts,
    rel_bias,
    ffn_up,
    ffn_down,
    attn_in,
    attn_out,
    pos_proj,
    conv_in,
    depthwise,
    conv_out,
):
    shards = (
        gains,
        shifts,
        rel_bias,
        ffn_up,
        ffn_down,
        attn_in,
        attn_out,
        pos_proj,
        conv_in,
        depthwise,
        conv_out,
    )
    groups = lax.axis_size("dp")
    seq_devices = lax.axis_size("seq")
    local_utts = frames.shape[0]
    frame_len = frames.shape[1]
    model_width = frames.shape[2]
    utt_per = local_utts // MB
    length = frame_len * seq_devices
    seq_start = lax.axis_index("seq") * frame_len
    first_utt = lax.axis_index("dp") * local_utts
    own_lengths = lax.dynamic_slice_in_dim(lengths, first_utt, local_utts)
    lengths_grid = lengths.reshape(groups, MB, utt_per)
    offsets = seq_start + frame_len - 1 - jnp.arange(length + frame_len - 1, dtype=jnp.int32)
    pos_table_b = sinusoid(offsets, model_width).astype(jnp.bfloat16)
    frame_pos = seq_start + jnp.arange(frame_len, dtype=jnp.int32)
    key_pos = jnp.arange(length, dtype=jnp.int32)
    result_list = []
    grad_list = []
    full_sums = [None] * NL
    for micro_idx in range(MB):
        lens_here = own_lengths[micro_idx * utt_per : (micro_idx + 1) * utt_per]
        frame_mask = (frame_pos[None, :] < lens_here[:, None]).astype(jnp.float32)
        key_valid = key_pos[None, :] < lens_here[:, None]
        frame_count = jnp.sum(lengths_grid[:, micro_idx]).astype(jnp.float32)
        values = frames[micro_idx * utt_per : (micro_idx + 1) * utt_per]
        held_weights = []
        layer_idx = 0
        weights = gather_forward(shards, layer_idx)
        values, kept_data = layer_forward(
            values, weights, frame_mask, key_valid, frame_count, pos_table_b
        )
        saved_acts = [kept_data]
        held_weights.append(weights)
        result_list.append(values)
        grad_values = cotangent[micro_idx * utt_per : (micro_idx + 1) * utt_per]
        for layer_idx in reversed(range(NL)):
            weights = gather_backward(shards, layer_idx)
            grad_values, layer_grads = layer_backward(
                grad_values,
                saved_acts[layer_idx],
                weights,
                frame_mask,
                key_valid,
                frame_count,
                pos_table_b,
            )
            if full_sums[layer_idx] is None:
                full_sums[layer_idx] = layer_grads
            else:
                full_sums[layer_idx] = jax.tree.map(jnp.add, full_sums[layer_idx], layer_grads)
        grad_list.append(grad_values)
    stacked = tuple((jnp.stack([full_sums[0][member]]) for member in range(11)))
    final_grads = (
        lax.psum_scatter(stacked[0], ("dp", "seq"), scatter_dimension=2, tiled=True),
        lax.psum_scatter(stacked[1], ("dp", "seq"), scatter_dimension=2, tiled=True),
        lax.psum_scatter(stacked[2], ("dp", "seq"), scatter_dimension=2, tiled=True),
        lax.psum_scatter(stacked[3], ("dp", "seq"), scatter_dimension=2, tiled=True),
        lax.psum_scatter(stacked[4], ("dp", "seq"), scatter_dimension=2, tiled=True),
        lax.psum_scatter(stacked[5], ("dp", "seq"), scatter_dimension=1, tiled=True),
        lax.psum_scatter(stacked[6], ("dp", "seq"), scatter_dimension=1, tiled=True),
        lax.psum_scatter(stacked[7], ("dp", "seq"), scatter_dimension=1, tiled=True),
        lax.psum_scatter(stacked[8], ("dp", "seq"), scatter_dimension=1, tiled=True),
        lax.psum_scatter(stacked[9], ("dp", "seq"), scatter_dimension=1, tiled=True),
        lax.psum_scatter(stacked[10], ("dp", "seq"), scatter_dimension=1, tiled=True),
    )
    mixed = jnp.concatenate(result_list, axis=0)
    grad_frames = jnp.concatenate(grad_list, axis=0)
    return (
        mixed,
        grad_frames,
        final_grads[0],
        final_grads[1],
        final_grads[2],
        final_grads[3],
        final_grads[4],
        final_grads[5],
        final_grads[6],
        final_grads[7],
        final_grads[8],
        final_grads[9],
        final_grads[10],
    )


NT = (((1,), (1,)), ((), ()))
TN = (((0,), (0,)), ((), ()))
NN = (((1,), (0,)), ((), ()))
MESH = pl.DeviceIdType.MESH
UTTS = 4
SMALL = 128
VMEM_LIMIT = 60 * 1024 * 1024


def fits_whole(mesh):
    return mesh.shape["dp"] == 4 and mesh.shape["seq"] == MB * UTTS


def dotf(left, right, dims=NN):
    return lax.dot_general(left, right, dims, preferred_element_type=jnp.float32)


def place():
    dp = lax.axis_index("dp")
    sq = lax.axis_index("seq")
    return dp, sq, lax.div(dp, 2), lax.rem(dp, 2), lax.div(sq, 2), lax.rem(sq, 2)


def flip_if(value, bit):
    return 1 - value if bit else value


def partners():
    dp, sq, x, c, z, y = place()
    even = c == 0
    core = (x * 2 + 1 - c, sq)
    xdev = ((1 - x) * 2 + c, sq)
    ydev = (dp, z * 2 + 1 - y)
    first = (jnp.where(even, ydev[0], xdev[0]), jnp.where(even, ydev[1], xdev[1]))
    second = (jnp.where(even, xdev[0], ydev[0]), jnp.where(even, xdev[1], ydev[1]))
    return core, xdev, first, second


def rank_of(color, a, b, k):
    _, _, x, _, z, y = place()
    even = color == 0
    xx = jnp.where(even, x + a * (1 - 2 * x), x + b * (1 - 2 * x))
    yy = jnp.where(even, y + b * (1 - 2 * y), y + a * (1 - 2 * y))
    return xx * 16 + color * 8 + lax.rem(z + k, 4) * 2 + yy


def greet(devices):
    barrier = pltpu.get_barrier_semaphore()
    for device in devices:
        pl.semaphore_signal(barrier, inc=1, device_id=device, device_id_type=MESH)
    pl.semaphore_wait(barrier, len(devices))


def seq_peers(dp, sq, count):
    return [(dp, lax.rem(sq + k, count)) for k in range(1, count)]


def remote(src, dst, send, recv, device):
    return pltpu.make_async_remote_copy(
        src_ref=src, dst_ref=dst, send_sem=send, recv_sem=recv, device_id=device, device_id_type=MESH
    )


def alternate(a, b, k):
    return a * 8 + b * 4 + k


def gather_steps(w_ref, d_ref, w_all, d_all, send, recv, own):
    wr, dr = w_ref.shape[0], d_ref.shape[0]
    started = []

    def blocks(rank):
        return (
            w_all.at[pl.ds(pl.multiple_of(rank * wr, 16), wr), :],
            d_all.at[pl.ds(pl.multiple_of(rank * dr, 16), dr), :],
        )

    def pair(group, target, slot, landing_slot, mine, other):
        dp, sq, _, c, z, y = place()
        core, _, first, second = partners()
        device = {"core": core, "first": first, "second": second}.get(target)
        if device is None:
            device = (dp, lax.rem(z + target, 4) * 2 + y)
        w_dst, d_dst = blocks(rank_of(1 - c if other else c, *group))
        w_src, d_src = (w_ref, d_ref) if mine else (w_dst, d_dst)
        return (
            remote(w_src, w_dst, send.at[0, slot], recv.at[0, landing_slot], device),
            remote(d_src, d_dst, send.at[1, slot], recv.at[1, landing_slot], device),
        )

    def ship(group, target, slot, landing_slot, mine=False):
        spec = (group, target, slot, landing_slot, mine, False)
        for copy in pair(*spec):
            copy.start()
        started.append(spec)

    def arrive(group, other=False):
        for copy in pair(group, "core", 0, alternate(*group) + (16 if other else 0), False, other):
            copy.wait_recv()

    def to_core(group, mine=False):
        spot = 16 + alternate(*group)
        ship(group, "core", spot, spot, mine)

    def own_copies():
        _, _, _, c, _, _ = place()
        w_own, d_own = blocks(rank_of(c, 0, 0, 0))
        return (
            pltpu.make_async_copy(w_ref, w_own, own.at[0]),
            pltpu.make_async_copy(d_ref, d_own, own.at[1]),
        )

    def begin():
        mine = (0, 0, 0)
        ship(mine, "second", 15, 8, mine=True)
        ship(mine, "first", 3, 4, mine=True)
        for k in (1, 3, 2):
            ship(mine, k, k - 1, 4 - k, mine=True)
        to_core(mine, mine=True)
        for copy in own_copies():
            copy.start()

    def along(k):
        group = (0, 0, k)
        arrive(group)
        ship(group, "second", 8 + k - 1, 8 + k)
        ship(group, "first", 4 + k - 1, 4 + k)
        to_core(group)

    def across(k):
        group = (0, 1, k)
        arrive(group)
        ship(group, "second", 11 + k, 12 + k)
        to_core(group)

    def over(k):
        for b in (0, 1):
            group = (1, b, k)
            arrive(group)
            to_core(group)

    def finish():
        for k in (0, 1, 3, 2):
            for a, b in ((0, 0), (0, 1), (1, 0), (1, 1)):
                arrive((a, b, k), other=True)
        for copy in own_copies():
            copy.wait()
        for spec in started:
            for copy in pair(*spec):
                copy.wait_send()

    return begin, along, across, over, finish


def meeting(count):
    dp, sq, *_ = place()
    core, xdev, _, _ = partners()
    greet(seq_peers(dp, sq, count) + [core, xdev])


def tree_scratch():
    return [
        pltpu.SemaphoreType.DMA((2, 32)),
        pltpu.SemaphoreType.DMA((2, 32)),
        pltpu.SemaphoreType.DMA((2,)),
    ]


def gather_kernel(w_ref, d_ref, f_ref, w_all, d_all, f_all, send, recv, own, row_send, row_recv, row_own):
    meeting(f_ref.shape[0])
    begin, along, across, over, finish = gather_steps(w_ref, d_ref, w_all, d_all, send, recv, own)
    begin()
    rows_begin(f_ref, f_all, row_send, row_recv, row_own)
    across(0)
    along(1)
    across(1)
    over(0)
    along(3)
    across(3)
    over(1)
    along(2)
    across(2)
    over(3)
    over(2)
    finish()
    rows_end(f_ref, f_all, row_send, row_recv, row_own)


def gathered(w, d):
    return [
        jax.ShapeDtypeStruct((w.shape[0] * 32, w.shape[1]), w.dtype),
        jax.ShapeDtypeStruct((d.shape[0] * 32, d.shape[1]), d.dtype),
    ]


def gather_all(w, d, f):
    vm = pl.BlockSpec(memory_space=pltpu.VMEM)
    hbm = pl.BlockSpec(memory_space=pl.ANY)
    return pl.pallas_call(
        gather_kernel,
        in_specs=[vm] * 3,
        out_specs=[hbm] * 3,
        out_shape=gathered(w, d) + [jax.ShapeDtypeStruct(f.shape, f.dtype)],
        scratch_shapes=tree_scratch() + row_scratch(f.shape[0]),
        compiler_params=pltpu.CompilerParams(collective_id=0, has_side_effects=True),
        name="gather_all",
    )(w, d, f)


def scatter_steps(w_ref, d_ref, w_out, d_out, bufs, send, recv):
    w0, d0, w1, d1, w2, d2, w3, d3 = bufs
    wr, dr = w_out.shape[0], d_out.shape[0]

    def rows(rank, size):
        return pl.ds(pl.multiple_of(rank * size, 16), size)

    def group_rank(slot, other):
        _, _, _, c, _, _ = place()
        color = 1 - c if other else c
        return rank_of(color, lax.div(slot, 8), lax.rem(lax.div(slot, 4), 2), lax.rem(slot, 4))

    def core_copies(slot):
        core = partners()[0]
        rank = group_rank(slot, True)
        return (
            remote(w_ref.at[rows(rank, wr), :], w0.at[slot], send.at[0, slot], recv.at[0, slot], core),
            remote(d_ref.at[rows(rank, dr), :], d0.at[slot], send.at[1, slot], recv.at[1, slot], core),
        )

    def second_copies(slot):
        to = partners()[3]
        return (
            remote(w0.at[8 + slot], w1.at[slot], send.at[0, 16 + slot], recv.at[0, 16 + slot], to),
            remote(d0.at[8 + slot], d1.at[slot], send.at[1, 16 + slot], recv.at[1, 16 + slot], to),
        )

    def first_copies(slot):
        to = partners()[2]
        return (
            remote(w0.at[4 + slot], w2.at[slot], send.at[0, 24 + slot], recv.at[0, 24 + slot], to),
            remote(d0.at[4 + slot], d2.at[slot], send.at[1, 24 + slot], recv.at[1, 24 + slot], to),
        )

    def z_copies(k):
        dp, _, _, _, z, y = place()
        to = (dp, lax.rem(z + k, 4) * 2 + y)
        return (
            remote(w0.at[k], w3.at[3 - k], send.at[0, 27 + k], recv.at[0, 31 - k], to),
            remote(d0.at[k], d3.at[3 - k], send.at[1, 27 + k], recv.at[1, 31 - k], to),
        )

    def start(copies):
        for copy in copies:
            copy.start()

    def landed(copies):
        for copy in copies:
            copy.wait_recv()

    def sent(copies):
        for copy in copies:
            copy.wait_send()

    def add(slot, w, d):
        f = jnp.float32
        w0[slot] = (w0[slot].astype(f) + w.astype(f)).astype(jnp.bfloat16)
        d0[slot] = (d0[slot].astype(f) + d.astype(f)).astype(jnp.bfloat16)

    def begin():
        @pl.loop(0, 16)
        def _(step):
            start(core_copies(15 - step))

    def take(slot):
        landed(core_copies(slot))
        rank = group_rank(slot, False)
        add(slot, w_ref[rows(rank, wr), :], d_ref[rows(rank, dr), :])

    def far(lo, hi):
        @pl.loop(lo, hi)
        def _(step):
            take(15 - step)
            start(second_copies(7 - step))

    def near(lo, hi):
        @pl.loop(lo, hi)
        def _(step):
            take(7 - step)

    def pass_first(lo, hi):
        @pl.loop(lo, hi)
        def _(step):
            slot = 7 - step
            landed(second_copies(slot))
            add(slot, w1[slot], d1[slot])
            start(first_copies(slot - 4))

    def join_second():
        @pl.loop(0, 3)
        def _(step):
            slot = 3 - step
            landed(second_copies(slot))
            add(slot, w1[slot], d1[slot])

    def pass_along(lo, hi):
        @pl.loop(lo, hi)
        def _(step):
            slot = 3 - step
            landed(first_copies(slot))
            add(slot, w2[slot], d2[slot])
            start(z_copies(slot))

    def total(base, parts):
        value = base.astype(jnp.float32)
        for part in parts:
            value = value + part.astype(jnp.float32)
        return value

    def finish():
        landed(second_copies(0))
        landed(first_copies(0))
        for k in (1, 2, 3):
            landed(z_copies(k))
        w_out[...] = total(w0[0], (w1[0], w2[0], w3[0], w3[1], w3[2]))
        d_out[...] = total(d0[0], (d1[0], d2[0], d3[0], d3[1], d3[2]))

        @pl.loop(0, 16)
        def _(slot):
            sent(core_copies(slot))

        @pl.loop(0, 8)
        def _(slot):
            sent(second_copies(slot))

        @pl.loop(0, 4)
        def _(slot):
            sent(first_copies(slot))

        for k in (1, 2, 3):
            sent(z_copies(k))

    return begin, far, near, pass_first, join_second, pass_along, finish


def scatter_scratch(w, d):
    bf = jnp.bfloat16
    scratch = []
    for n in (16, 8, 4, 3):
        scratch += [
            pltpu.VMEM((n, w.shape[0] // 32, w.shape[1]), bf),
            pltpu.VMEM((n, d.shape[0] // 32, d.shape[1]), bf),
        ]
    return scratch + tree_scratch()[:2]


def scattered(w, d):
    return [
        jax.ShapeDtypeStruct((w.shape[0] // 32, w.shape[1]), jnp.float32),
        jax.ShapeDtypeStruct((d.shape[0] // 32, d.shape[1]), jnp.float32),
    ]


def scatter_kernel(w_ref, d_ref, g_ref, w_out, d_out, g_all, *scratch):
    bufs, (send, recv, row_send, row_recv, row_own) = scratch[:8], scratch[8:]
    meeting(g_ref.shape[0])
    begin, far, near, pass_first, join_second, pass_along, finish = scatter_steps(
        w_ref, d_ref, w_out, d_out, bufs, send, recv
    )
    begin()
    far(0, 8)
    rows_begin(g_ref, g_all, row_send, row_recv, row_own)
    near(0, 4)
    pass_first(0, 4)
    near(4, 8)
    join_second()
    pass_along(0, 3)
    finish()
    rows_end(g_ref, g_all, row_send, row_recv, row_own)


def scatter_all(w, d, g):
    vm = pl.BlockSpec(memory_space=pltpu.VMEM)
    hbm = pl.BlockSpec(memory_space=pl.ANY)
    return pl.pallas_call(
        scatter_kernel,
        in_specs=[vm] * 3,
        out_specs=[vm, vm, hbm],
        out_shape=scattered(w, d) + [jax.ShapeDtypeStruct(g.shape, g.dtype)],
        scratch_shapes=scatter_scratch(w, d) + row_scratch(g.shape[0]),
        compiler_params=pltpu.CompilerParams(
            collective_id=1, has_side_effects=True, vmem_limit_bytes=VMEM_LIMIT
        ),
        name="scatter_all",
    )(w, d, g)


def batch_sum_kernel(s_ref, o_ref, buf, send, recv):
    dp, sq, *_ = place()
    base = lax.div(sq, UTTS) * UTTS
    me = dp * UTTS + lax.rem(sq, UTTS)
    size = buf.shape[0]

    def device(j):
        r = lax.rem(me + j, size)
        return (lax.div(r, UTTS), base + lax.rem(r, UTTS))

    def copy(j):
        return remote(s_ref, buf.at[me], send.at[j - 1], recv.at[size - 1 - j], device(j))

    greet([device(j) for j in range(1, size)])
    for j in range(1, size):
        copy(j).start()
    buf[me] = s_ref[...]
    for j in range(1, size):
        remote(s_ref, buf.at[lax.rem(me + j, size)], send.at[j - 1], recv.at[j - 1], device(j)).wait_recv()
    o_ref[...] = jnp.sum(buf[...], axis=0)
    for j in range(1, size):
        copy(j).wait_send()


def batch_sum(sums, ident):
    vm = pl.BlockSpec(memory_space=pltpu.VMEM)
    size = 4 * UTTS
    return pl.pallas_call(
        batch_sum_kernel,
        in_specs=[vm],
        out_specs=vm,
        out_shape=jax.ShapeDtypeStruct(sums.shape, jnp.float32),
        scratch_shapes=[
            pltpu.VMEM((size,) + sums.shape, jnp.float32),
            pltpu.SemaphoreType.DMA((size - 1,)),
            pltpu.SemaphoreType.DMA((size - 1,)),
        ],
        compiler_params=pltpu.CompilerParams(collective_id=ident, has_side_effects=True),
        name="batch_sum",
    )(sums)


def rows_begin(src, dst, send, recv, own):
    _, sq, *_ = place()
    for k in range(1, dst.shape[0]):
        row_copy(src, dst, send, recv, k).start()
    pltpu.make_async_copy(src.at[sq], dst.at[sq], own).start()


def rows_end(src, dst, send, recv, own):
    dp, sq, *_ = place()
    count = dst.shape[0]
    for k in range(1, count):
        copy = row_copy(src, dst, send, recv, k)
        copy.wait_send()
        landing(src, dst, send, recv, k).wait_recv()
    pltpu.make_async_copy(src.at[sq], dst.at[sq], own).wait()


def row_copy(src, dst, send, recv, k):
    dp, sq, *_ = place()
    count = dst.shape[0]
    to = lax.rem(sq + k, count)
    return remote(src.at[to], dst.at[sq], send.at[k - 1], recv.at[count - 1 - k], (dp, to))


def landing(src, dst, send, recv, k):
    dp, sq, *_ = place()
    origin = lax.rem(sq + k, dst.shape[0])
    return remote(src.at[sq], dst.at[origin], send.at[k - 1], recv.at[k - 1], (dp, origin))


def att_fwd_kernel(
    len_ref, qu_ref, qv_ref, k_ref, v_ref, t_ref, c_ref, w_ref, d_ref,
    ctx_ref, p_ref, c_all, w_all, d_all,
    send, recv, own, row_send, row_recv, row_own, *, tq,
):
    begin, along, across, over, finish = gather_steps(w_ref, d_ref, w_all, d_all, send, recv, own)

    def open_up():
        meeting(c_ref.shape[0])
        begin()
        rows_begin(c_ref, c_all, row_send, row_recv, row_own)

    def both(*steps):
        def run():
            for step, k in steps:
                step(k)

        return run

    plan = {
        0: open_up,
        2: both((across, 0), (along, 1)),
        3: both((along, 3), (across, 1)),
        4: both((along, 2), (across, 3), (over, 0)),
        5: both((across, 2), (over, 1)),
        7: both((over, 3)),
        8: both((over, 2)),
    }
    keys = k_ref.shape[0]
    span = keys + tq
    valid = lax.broadcasted_iota(jnp.int32, (1, keys), 1) < len_ref[0]

    def block(i):
        time = pl.program_id(0) * (keys // tq) + i
        for at, step in plan.items():
            pl.when(time == at)(step)
        rows = pl.ds(pl.multiple_of(i * tq, tq), tq)
        band = pl.ds(pl.multiple_of(keys - tq - i * tq, tq), span)
        for h in range(2):
            cols = slice(h * DH, (h + 1) * DH)
            content = dotf(qu_ref[rows, cols], k_ref[:, cols], NT)
            raw = dotf(qv_ref[rows, cols], t_ref[band, cols], NT)
            pos = pltpu.roll(raw, keys + 1, 1, stride=1, stride_axis=0)[:, :keys]
            s = jnp.where(valid, (content + pos) * 0.125, -1e30)
            e = jnp.exp(s - jnp.max(s, axis=1, keepdims=True))
            p = (e * (1.0 / jnp.sum(e, axis=1, keepdims=True))).astype(jnp.bfloat16)
            p_ref[h, rows, :] = p
            ctx_ref[rows, cols] = dotf(p, v_ref[:, cols]).astype(jnp.bfloat16)

    pl.loop(0, keys // tq)(block)

    @pl.when(pl.program_id(0) == pl.num_programs(0) - 1)
    def _():
        finish()
        rows_end(c_ref, c_all, row_send, row_recv, row_own)


def row_scratch(count):
    return [
        pltpu.SemaphoreType.DMA((count - 1,)),
        pltpu.SemaphoreType.DMA((count - 1,)),
        pltpu.SemaphoreType.DMA,
    ]


def att_fwd(length, qu, qv, k, v, table, cot, w, d, tq=256):
    rows, width = qu.shape
    blk = pl.BlockSpec((rows, 128), lambda h, *_: (0, h))
    tab = pl.BlockSpec((2 * rows, 128), lambda h, *_: (0, h))
    return pl.pallas_call(
        lambda *refs: att_fwd_kernel(*refs, tq=tq),
        grid_spec=pltpu.PrefetchScalarGridSpec(
            num_scalar_prefetch=1,
            grid=(width // 128,),
            in_specs=[blk] * 4 + [tab] + [pl.BlockSpec(memory_space=pltpu.VMEM)] * 3,
            out_specs=[blk, pl.BlockSpec((2, rows, rows), lambda h, *_: (h, 0, 0))]
            + [pl.BlockSpec(memory_space=pl.ANY)] * 3,
            scratch_shapes=tree_scratch() + row_scratch(cot.shape[0]),
        ),
        out_shape=[
            jax.ShapeDtypeStruct((rows, width), jnp.bfloat16),
            jax.ShapeDtypeStruct((width // DH, rows, rows), jnp.bfloat16),
            jax.ShapeDtypeStruct(cot.shape, cot.dtype),
        ]
        + gathered(w, d),
        compiler_params=pltpu.CompilerParams(
            collective_id=4, has_side_effects=True, vmem_limit_bytes=VMEM_LIMIT
        ),
        name="att_fwd",
    )(length, qu, qv, k, v, table, cot, w, d)


def att_bwd_kernel(
    p_ref, g_ref, qu_ref, qv_ref, k_ref, v_ref, t_ref, m_ref, w_ref, d_ref,
    dqu_ref, dqv_ref, dk_ref, dv_ref, dt_ref, m_all, w_out, d_out, ds_sc, dt_sc, *scratch, tq,
):
    bufs, (send, recv, row_send, row_recv, row_own) = scratch[:8], scratch[8:]
    begin, far, near, pass_first, join_second, pass_along, finish = scatter_steps(
        w_ref, d_ref, w_out, d_out, bufs, send, recv
    )

    def open_up():
        meeting(m_ref.shape[0])
        begin()

    def rows_away():
        near(4, 8)
        rows_begin(m_ref, m_all, row_send, row_recv, row_own)

    plan = {
        0: open_up,
        1: lambda: far(0, 4),
        2: lambda: far(4, 8),
        3: lambda: near(0, 4),
        4: rows_away,
        5: lambda: pass_first(0, 2),
        6: lambda: pass_first(2, 4),
        7: join_second,
        8: lambda: pass_along(0, 2),
        9: lambda: pass_along(2, 3),
    }
    keys = k_ref.shape[0]
    span = keys + tq
    low = jnp.bfloat16
    flip = (
        lax.broadcasted_iota(jnp.int32, (tq, tq), 0) + lax.broadcasted_iota(jnp.int32, (tq, tq), 1) == tq - 1
    ).astype(low)
    pad = jnp.zeros((tq, tq), jnp.float32)
    dt_sc[...] = jnp.zeros_like(dt_sc)

    def block(i):
        time = pl.program_id(0) * (keys // tq) + i
        for at, step in plan.items():
            pl.when(time == at)(step)
        rows = pl.ds(pl.multiple_of(i * tq, tq), tq)
        band = pl.ds(pl.multiple_of(keys - tq - i * tq, tq), span)
        for h in range(2):
            cols = slice(h * DH, (h + 1) * DH)
            dp = dotf(g_ref[rows, cols], v_ref[:, cols], NT)
            pf = p_ref[h, rows, :].astype(jnp.float32)
            ds = (pf * (dp - jnp.sum(dp * pf, axis=1, keepdims=True))).astype(low)
            ds_sc[h, rows, :] = ds
            dqu_ref[rows, cols] = dotf(ds, k_ref[:, cols]) * 0.125
            back = jnp.concatenate([dotf(flip, ds), pad], axis=1)
            raw = pltpu.roll(back, 0, 1, stride=1, stride_axis=0).astype(low)
            dqv = dotf(raw, t_ref[band, cols]).astype(low)
            dqv_ref[rows, cols] = dotf(flip, dqv) * 0.125
            qv = dotf(flip, qv_ref[rows, cols]).astype(low)
            dt_sc[h, band, :] += dotf(raw, qv, TN)

    pl.loop(0, keys // tq)(block)

    for h in range(2):
        cols = slice(h * DH, (h + 1) * DH)
        dt_ref[:, cols] = (dt_sc[h] * 0.125).astype(low)
        dk_ref[:, cols] = dotf(ds_sc[h], qu_ref[:, cols], TN) * 0.125
        dv_ref[:, cols] = dotf(p_ref[h], g_ref[:, cols], TN)

    @pl.when(pl.program_id(0) == pl.num_programs(0) - 1)
    def _():
        finish()
        rows_end(m_ref, m_all, row_send, row_recv, row_own)


def att_bwd(p, g, qu, qv, k, v, table, mixed, w, d, tq=256):
    vm = pl.BlockSpec(memory_space=pltpu.VMEM)
    rows, width = qu.shape
    blk = pl.BlockSpec((rows, 128), lambda h: (0, h))
    tab = pl.BlockSpec((2 * rows, 128), lambda h: (0, h))
    out = jax.ShapeDtypeStruct((rows, width), jnp.float32)
    return pl.pallas_call(
        lambda *refs: att_bwd_kernel(*refs, tq=tq),
        grid=(width // 128,),
        in_specs=[pl.BlockSpec((2, rows, rows), lambda h: (h, 0, 0))] + [blk] * 5
        + [tab, vm, vm, vm],
        out_specs=[blk] * 4 + [tab, pl.BlockSpec(memory_space=pl.ANY), vm, vm],
        out_shape=[out] * 4
        + [
            jax.ShapeDtypeStruct((2 * rows, width), jnp.bfloat16),
            jax.ShapeDtypeStruct(mixed.shape, mixed.dtype),
        ]
        + scattered(w, d),
        scratch_shapes=[pltpu.VMEM((2, rows, rows), jnp.bfloat16), pltpu.VMEM((2, 2 * rows, DH), jnp.float32)]
        + scatter_scratch(w, d)
        + row_scratch(mixed.shape[0]),
        compiler_params=pltpu.CompilerParams(
            collective_id=5, has_side_effects=True, vmem_limit_bytes=VMEM_LIMIT
        ),
        name="att_bwd",
    )(p, g, qu, qv, k, v, table, mixed, w, d)


def position_table(length, width):
    offsets = (length - 1 - np.arange(2 * length)).astype(np.float32)
    half = width // 2
    steps = np.arange(half, dtype=np.float32) * np.float32(-2.0 * math.log(10000.0) / width)
    angles = (offsets[:, None] * np.exp(steps)[None, :]).astype(np.float64)
    table = np.concatenate([np.sin(angles), np.cos(angles)], axis=1)
    return jnp.asarray(table.astype(np.float32)).astype(jnp.bfloat16)


def shifted_sum(values, kernel_f, reverse):
    taps = kernel_f.shape[1]
    reach = (taps - 1) // 2
    padded = jnp.pad(values, ((reach, reach), (0, 0)))
    rows = values.shape[0]
    total = None
    for k in range(taps):
        at = taps - 1 - k if reverse else k
        term = padded[at : at + rows].astype(jnp.float32) * kernel_f[:, k]
        total = term if total is None else total + term
    return total


def tap_grads(values, grad, taps):
    reach = (taps - 1) // 2
    padded = jnp.pad(values, ((reach, reach), (0, 0)))
    rows = values.shape[0]
    grad_f = grad.astype(jnp.float32)
    return jnp.stack(
        [jnp.sum(padded[k : k + rows].astype(jnp.float32) * grad_f, axis=0) for k in range(taps)]
    )


def columns(*members):
    return [0] + [int(v) for v in np.cumsum([member.shape[1] for member in members])]


def split(values, cuts):
    return [values[:, lo:hi] for lo, hi in zip(cuts[:-1], cuts[1:])]


def local_whole(
    frames,
    lengths,
    cotangent,
    gains,
    shifts,
    rel_bias,
    ffn_up,
    ffn_down,
    attn_in,
    attn_out,
    pos_proj,
    conv_in,
    depthwise,
    conv_out,
):
    low = jnp.bfloat16
    dp, sq = lax.axis_index("dp"), lax.axis_index("seq")
    count, width_rows, model = frames.shape
    length = count * 0 + width_rows * lax.axis_size("seq")
    taps = depthwise.shape[2]
    small = jnp.concatenate([gains[0], shifts[0], rel_bias[0]], axis=0).T
    small = jnp.concatenate([small, depthwise[0]], axis=1)
    small = jnp.pad(small, ((0, 0), (0, SMALL - small.shape[1])))
    early = jnp.concatenate([ffn_up[0, 0], attn_in[0], pos_proj[0], small], axis=1)
    late = jnp.concatenate([ffn_up[0, 1], attn_out[0], conv_in[0], conv_out[0]], axis=1)
    cuts_early = columns(ffn_up[0, 0], attn_in[0], pos_proj[0], small)
    cuts_late = columns(ffn_up[0, 1], attn_out[0], conv_in[0], conv_out[0])
    w_all, down_0, f_all = gather_all(early, ffn_down[0, 0], frames.astype(low))
    up_0, w_attn_in, w_pos, small = split(w_all, cuts_early)
    small = small.astype(jnp.float32).T
    gain, shift, rel = small[0:6], small[6:12], small[12:14]
    kernel_f = small[14 : 14 + taps].T
    own_length = lax.dynamic_slice_in_dim(lengths, dp * count + sq, 1)
    grid = lengths.reshape(lax.axis_size("dp"), MB, UTTS)
    per_batch = jnp.sum(grid, axis=(0, 2)).astype(jnp.float32)
    frame_count = lax.dynamic_slice_in_dim(per_batch, lax.div(sq, UTTS), 1)[0]
    mask = (jnp.arange(length, dtype=jnp.int32) < own_length[0]).astype(jnp.float32)[:, None]
    table_in = position_table(length, model)

    x0 = f_all.reshape(length, model).astype(jnp.float32)
    x1, kept_one = ffn_forward(x0, gain[0], shift[0], up_0, down_0)
    a1 = layer_norm(x1, gain[1], shift[1]).astype(low)
    proj = matmul_low(a1, w_attn_in)
    query = proj[:, :model]
    qu = (query + rel[0]).astype(low)
    qv = (query + rel[1]).astype(low)
    key = proj[:, model : 2 * model].astype(low)
    value = proj[:, 2 * model :].astype(low)
    table = matmul_low(table_in, w_pos).astype(low)
    ctx, probs, c_all, w_all, down_1 = att_fwd(
        own_length, qu, qv, key, value, table, cotangent.astype(low), late, ffn_down[0, 1]
    )
    up_1, w_attn_out, w_conv_in, w_conv_out = split(w_all, cuts_late)
    x2 = x1 + matmul_low(ctx, w_attn_out)

    a2 = layer_norm(x2, gain[2], shift[2]).astype(low)
    gate = matmul_low(a2, w_conv_in)
    gated = (glu_gate(gate) * mask).astype(low)
    depth = shifted_sum(gated, kernel_f, False)
    sums = jnp.stack([jnp.sum(depth * mask, axis=0), jnp.sum(depth * depth * mask, axis=0)])
    sums = batch_sum(sums, 2)
    mean = sums[0] / frame_count
    var = sums[1] / frame_count - mean * mean
    inv = lax.rsqrt(var + 1e-05)
    normal = (depth - mean) * inv * gain[5] + shift[5]
    active = jax.nn.silu(normal).astype(low)
    x3 = x2 + matmul_low(active, w_conv_out)
    x4, kept_two = ffn_forward(x3, gain[3], shift[3], up_1, down_1)
    mixed = layer_norm(x4, gain[4], shift[4])

    cot = c_all.reshape(length, model).astype(jnp.float32)
    grad, g_gain4, g_shift4 = jax.vjp(layer_norm, x4, gain[4], shift[4])[1](cot)
    grad, (g_gain3, g_shift3, g_up1, g_down1) = ffn_backward(
        grad, kept_two, gain[3], shift[3], up_1, down_1
    )
    grad_b = grad.astype(low)
    g_conv_out = weight_grad(active, grad_b)
    grad_active = matmul_back(grad_b, w_conv_out)
    grad_normal = jax.vjp(jax.nn.silu, normal)[1](grad_active)[0]
    g_gain5 = jnp.sum(grad_normal * ((depth - mean) * inv), axis=0)
    g_shift5 = jnp.sum(grad_normal, axis=0)
    hat = grad_normal * gain[5]
    sums = batch_sum(jnp.stack([jnp.sum(hat, axis=0), jnp.sum(hat * depth, axis=0)]), 3)
    grad_var = -0.5 * inv * inv * inv * (sums[1] - mean * sums[0])
    grad_mean = -inv * sums[0] - 2.0 * mean * grad_var
    grad_depth = (
        hat * inv + mask * (grad_mean / frame_count + 2.0 * depth * grad_var / frame_count)
    ).astype(low)
    grad_gated = shifted_sum(grad_depth, kernel_f, True) * mask
    g_kernel = tap_grads(gated, grad_depth, taps)
    grad_gate = jax.vjp(glu_gate, gate)[1](grad_gated)[0].astype(low)
    g_conv_in = weight_grad(a2, grad_gate)
    grad_ln, g_gain2, g_shift2 = jax.vjp(layer_norm, x2, gain[2], shift[2])[1](
        matmul_back(grad_gate, w_conv_in)
    )
    grad = grad + grad_ln

    grad_b = grad.astype(low)
    g_attn_out = weight_grad(ctx, grad_b)
    grad_ctx = matmul_back(grad_b, w_attn_out).astype(low)
    g_late = jnp.concatenate(
        [member.astype(low) for member in (g_up1, g_attn_out, g_conv_in, g_conv_out)], axis=1
    )
    dqu, dqv, dkey, dvalue, dtable, m_all, late_sum, down1_sum = att_bwd(
        probs,
        grad_ctx,
        qu,
        qv,
        key,
        value,
        table,
        mixed.astype(low).reshape(frames.shape),
        g_late,
        g_down1.astype(low),
    )
    g_rel = jnp.stack([jnp.sum(dqu, axis=0), jnp.sum(dqv, axis=0)])
    grad_proj = jnp.concatenate([dqu + dqv, dkey, dvalue], axis=1).astype(low)
    g_pos = weight_grad(table_in, dtable)
    g_attn_in = weight_grad(a1, grad_proj)
    grad_ln, g_gain1, g_shift1 = jax.vjp(layer_norm, x1, gain[1], shift[1])[1](
        matmul_back(grad_proj, w_attn_in)
    )
    grad = grad + grad_ln
    grad, (g_gain0, g_shift0, g_up0, g_down0) = ffn_backward(
        grad, kept_one, gain[0], shift[0], up_0, down_0
    )

    g_small = jnp.concatenate(
        [
            jnp.stack([g_gain0, g_gain1, g_gain2, g_gain3, g_gain4, g_gain5]),
            jnp.stack([g_shift0, g_shift1, g_shift2, g_shift3, g_shift4, g_shift5]),
            g_rel,
            g_kernel,
        ]
    )
    g_small = jnp.pad(g_small, ((0, SMALL - g_small.shape[0]), (0, 0))).T
    g_early = jnp.concatenate(
        [member.astype(low) for member in (g_up0, g_attn_in, g_pos, g_small)], axis=1
    )
    early_sum, down0_sum, g_all = scatter_all(
        g_early, g_down0.astype(low), grad.astype(low).reshape(frames.shape)
    )
    s_up0, s_attn_in, s_pos, tail = split(early_sum, cuts_early)
    s_up1, s_attn_out, s_conv_in, s_conv_out = split(late_sum, cuts_late)
    rows = tail[:, :14].T
    return (
        m_all.astype(jnp.float32),
        g_all.astype(jnp.float32),
        rows[None, 0:6],
        rows[None, 6:12],
        rows[None, 12:14],
        jnp.stack([s_up0, s_up1])[None],
        jnp.stack([down0_sum, down1_sum])[None],
        s_attn_in[None],
        s_attn_out[None],
        s_pos[None],
        s_conv_in[None],
        tail[None, :, 14 : 14 + taps],
        s_conv_out[None],
    )


def solution(mesh):
    body = local_whole if fits_whole(mesh) else local_general
    in_specs = (
        P("dp", "seq", None),
        P(),
        P("dp", "seq", None),
        P(None, None, ("dp", "seq")),
        P(None, None, ("dp", "seq")),
        P(None, None, ("dp", "seq")),
        P(None, None, ("dp", "seq"), None),
        P(None, None, ("dp", "seq"), None),
        P(None, ("dp", "seq"), None),
        P(None, ("dp", "seq"), None),
        P(None, ("dp", "seq"), None),
        P(None, ("dp", "seq"), None),
        P(None, ("dp", "seq"), None),
        P(None, ("dp", "seq"), None),
    )
    out_specs = (
        P("dp", "seq", None),
        P("dp", "seq", None),
        P(None, None, ("dp", "seq")),
        P(None, None, ("dp", "seq")),
        P(None, None, ("dp", "seq")),
        P(None, None, ("dp", "seq"), None),
        P(None, None, ("dp", "seq"), None),
        P(None, ("dp", "seq"), None),
        P(None, ("dp", "seq"), None),
        P(None, ("dp", "seq"), None),
        P(None, ("dp", "seq"), None),
        P(None, ("dp", "seq"), None),
        P(None, ("dp", "seq"), None),
    )
    return jax.shard_map(body, mesh=mesh, in_specs=in_specs, out_specs=out_specs, check_vma=False)
```

```python
import math

import jax
import jax.numpy as jnp
import numpy as np
from jax import lax
from jax.experimental import pallas as pl
from jax.experimental.pallas import tpu as pltpu
from jax.sharding import PartitionSpec as P

H = 8
DH = 64
NL = 1
MB = 2


HIGHEST_PREC = lax.Precision.HIGHEST


def extended(cells, sides, width):
    for axis, dim in sides:
        count = lax.axis_size(axis)
        ends = count - 1
        head = lax.slice_in_dim(cells, 0, width, axis=dim)
        tail = lax.slice_in_dim(cells, cells.shape[dim] - width, cells.shape[dim], axis=dim)
        cells = jnp.concatenate(
            [
                lax.ppermute(tail, axis, [(i, (i + 1) % count) for i in range(ends)]),
                cells,
                lax.ppermute(head, axis, [((i + 1) % count, i) for i in range(ends)]),
            ],
            axis=dim,
        )
    return cells


def layer_norm(values, gain_row, shift_row):
    centred = values - jnp.mean(values, axis=-1, keepdims=True)
    spread = jnp.mean(centred * centred, axis=-1, keepdims=True)
    return centred * lax.rsqrt(spread + 1e-05) * gain_row + shift_row


def sinusoid(offsets, model_width):
    half_width = model_width // 2
    frequency = jnp.exp(
        jnp.arange(half_width, dtype=jnp.float32) * (-2.0 * math.log(10000.0) / model_width)
    )
    angles = offsets.astype(jnp.float32)[:, None] * frequency[None, :]
    return jnp.concatenate([jnp.sin(angles), jnp.cos(angles)], axis=1)


def skew_rows(raw_pos, key_count):
    row_count = raw_pos.shape[-2]
    col_count = raw_pos.shape[-1]
    lead = raw_pos.shape[:-2]
    flat_rows = raw_pos.reshape(lead + (row_count * col_count,))
    flat_rows = flat_rows[..., row_count - 1 : row_count - 1 + row_count * (col_count - 1)]
    return flat_rows.reshape(lead + (row_count, col_count - 1))[..., :key_count]


def skew_back(grad_skew, raw_shape, key_count):
    zero_raw = jnp.zeros(raw_shape, jnp.float32)
    return jax.vjp(lambda raw_pos: skew_rows(raw_pos, key_count), zero_raw)[1](grad_skew)[0]


def glu_gate(gate_pair):
    half_width = gate_pair.shape[-1] // 2
    return gate_pair[..., :half_width] * jax.nn.sigmoid(gate_pair[..., half_width:])


def matmul_low(left, right):
    return jnp.dot(left, right, preferred_element_type=jnp.float32)


def matmul_back(grad_low, weight):
    return lax.dot_general(
        grad_low, weight, (((1,), (1,)), ((), ())), preferred_element_type=jnp.float32
    )


def weight_grad(inputs_low, grad_low):
    return lax.dot_general(
        inputs_low, grad_low, (((0,), (0,)), ((), ())), preferred_element_type=jnp.float32
    )


def ffn_forward(row_data, gain_row, shift_row, w_up, w_down):
    normed_b = layer_norm(row_data, gain_row, shift_row).astype(jnp.bfloat16)
    hidden = matmul_low(normed_b, w_up)
    active_b = jax.nn.silu(hidden).astype(jnp.bfloat16)
    branch = matmul_low(active_b, w_down)
    return (row_data + 0.5 * branch, (row_data, normed_b, hidden, active_b))


def ffn_backward(grad_rows, kept_data, gain_row, shift_row, w_up, w_down):
    row_data, normed_b, hidden, active_b = kept_data
    grad_out_b = (0.5 * grad_rows).astype(jnp.bfloat16)
    g_down = weight_grad(active_b, grad_out_b)
    grad_active = matmul_back(grad_out_b, w_down)
    grad_hidden_b = jax.vjp(jax.nn.silu, hidden)[1](grad_active)[0].astype(jnp.bfloat16)
    g_up = weight_grad(normed_b, grad_hidden_b)
    grad_normed = matmul_back(grad_hidden_b, w_up)
    grad_ln, g_gain, g_shift = jax.vjp(layer_norm, row_data, gain_row, shift_row)[1](grad_normed)
    return (grad_rows + grad_ln, (g_gain, g_shift, g_up, g_down))


def attention_logits(query_u_b, query_v_b, key_heads, pos_heads, key_valid):
    content = jnp.einsum(
        "ufhd,ulhd->uhfl", query_u_b, key_heads, preferred_element_type=jnp.float32
    )
    raw_pos = jnp.einsum("ufhd,whd->uhfw", query_v_b, pos_heads, preferred_element_type=jnp.float32)
    logits = (content + skew_rows(raw_pos, key_heads.shape[1])) * 0.125
    return jnp.where(key_valid[:, None, None, :], logits, -1e30)


def attn_forward(
    row_data,
    utt_count,
    gain_row,
    shift_row,
    bias_u,
    bias_v,
    w_in,
    w_out,
    w_pos,
    key_valid,
    pos_table_b,
):
    model_width = row_data.shape[1]
    frame_len = row_data.shape[0] // utt_count
    normed_b = layer_norm(row_data, gain_row, shift_row).astype(jnp.bfloat16)
    proj_rows = matmul_low(normed_b, w_in)
    query_rows = proj_rows[:, :model_width].reshape(utt_count, frame_len, H, DH)
    key_b = (
        proj_rows[:, model_width : 2 * model_width]
        .astype(jnp.bfloat16)
        .reshape(utt_count, frame_len, model_width)
    )
    value_b = (
        proj_rows[:, 2 * model_width :]
        .astype(jnp.bfloat16)
        .reshape(utt_count, frame_len, model_width)
    )
    all_keys, all_values = (
        lax.all_gather(key_b, "seq", axis=1, tiled=True),
        lax.all_gather(value_b, "seq", axis=1, tiled=True),
    )
    key_heads = all_keys.reshape(utt_count, -1, H, DH)
    value_heads = all_values.reshape(utt_count, -1, H, DH)
    query_u_b = (query_rows + bias_u.reshape(H, DH)).astype(jnp.bfloat16)
    query_v_b = (query_rows + bias_v.reshape(H, DH)).astype(jnp.bfloat16)
    pos_heads = matmul_low(pos_table_b, w_pos).astype(jnp.bfloat16).reshape(-1, H, DH)
    logits = attention_logits(query_u_b, query_v_b, key_heads, pos_heads, key_valid)
    top_score = jnp.max(logits, axis=-1, keepdims=True)
    exp_scores = jnp.exp(logits - top_score)
    row_total = jnp.sum(exp_scores, axis=-1, keepdims=True)
    prob_b = (exp_scores / row_total).astype(jnp.bfloat16)
    log_total = top_score + jnp.log(row_total)
    context = jnp.einsum("uhfl,ulhd->ufhd", prob_b, value_heads, preferred_element_type=jnp.float32)
    context_b = context.astype(jnp.bfloat16).reshape(-1, model_width)
    branch = matmul_low(context_b, w_out)
    kept_data = (
        row_data,
        normed_b,
        query_u_b,
        query_v_b,
        key_heads,
        value_heads,
        pos_heads,
        log_total,
        context_b,
    )
    return (row_data + branch, kept_data)


def attn_backward(grad_rows, kept_data, gain_row, shift_row, w_in, w_out, key_valid, pos_table_b):
    (
        row_data,
        normed_b,
        query_u_b,
        query_v_b,
        key_heads,
        value_heads,
        pos_heads,
        log_total,
        context_b,
    ) = kept_data
    utt_count = query_u_b.shape[0]
    frame_len = query_u_b.shape[1]
    model_width = row_data.shape[1]
    key_len = key_heads.shape[1]
    grad_out_b = grad_rows.astype(jnp.bfloat16)
    g_out = weight_grad(context_b, grad_out_b)
    grad_context_b = (
        matmul_back(grad_out_b, w_out).astype(jnp.bfloat16).reshape(utt_count, frame_len, H, DH)
    )
    logits = attention_logits(query_u_b, query_v_b, key_heads, pos_heads, key_valid)
    prob_rows = jnp.exp(logits - log_total)
    grad_probs = jnp.einsum(
        "ufhd,ulhd->uhfl", grad_context_b, value_heads, preferred_element_type=jnp.float32
    )
    inner_sum = jnp.sum(grad_probs * prob_rows, axis=-1, keepdims=True)
    grad_logits_b = (prob_rows * (grad_probs - inner_sum)).astype(jnp.bfloat16) * 0.125
    grad_query_u = jnp.einsum(
        "uhfl,ulhd->ufhd", grad_logits_b, key_heads, preferred_element_type=jnp.float32
    )
    raw_shape = (utt_count, H, frame_len, pos_heads.shape[0])
    grad_raw_b = skew_back(grad_logits_b.astype(jnp.float32), raw_shape, key_len).astype(
        jnp.bfloat16
    )
    grad_query_v = jnp.einsum(
        "uhfw,whd->ufhd", grad_raw_b, pos_heads, preferred_element_type=jnp.float32
    )
    grad_pos = jnp.einsum(
        "uhfw,ufhd->whd", grad_raw_b, query_v_b, preferred_element_type=jnp.float32
    )
    grad_pos = grad_pos.reshape(-1, model_width)
    g_pos = lax.dot_general(
        pos_table_b.astype(jnp.float32),
        grad_pos,
        (((0,), (0,)), ((), ())),
        precision=HIGHEST_PREC,
        preferred_element_type=jnp.float32,
    )
    prob_b = prob_rows.astype(jnp.bfloat16)
    grad_values = jnp.einsum(
        "uhfl,ufhd->ulhd", prob_b, grad_context_b, preferred_element_type=jnp.float32
    )
    grad_keys = jnp.einsum(
        "uhfl,ufhd->ulhd", grad_logits_b, query_u_b, preferred_element_type=jnp.float32
    )
    own_keys, own_values = (
        lax.psum_scatter(
            grad_keys.reshape(utt_count, key_len, model_width),
            "seq",
            scatter_dimension=1,
            tiled=True,
        ),
        lax.psum_scatter(
            grad_values.reshape(utt_count, key_len, model_width),
            "seq",
            scatter_dimension=1,
            tiled=True,
        ),
    )
    g_bias_u = jnp.sum(grad_query_u, axis=(0, 1)).reshape(-1)
    g_bias_v = jnp.sum(grad_query_v, axis=(0, 1)).reshape(-1)
    grad_proj_b = jnp.concatenate(
        [
            (grad_query_u + grad_query_v).reshape(-1, model_width),
            own_keys.reshape(-1, model_width),
            own_values.reshape(-1, model_width),
        ],
        axis=1,
    ).astype(jnp.bfloat16)
    g_in = weight_grad(normed_b, grad_proj_b)
    grad_normed = matmul_back(grad_proj_b, w_in)
    grad_ln, g_gain, g_shift = jax.vjp(layer_norm, row_data, gain_row, shift_row)[1](grad_normed)
    return (grad_rows + grad_ln, (g_gain, g_shift, g_bias_u, g_bias_v, g_in, g_out, g_pos))


def conv_forward(
    row_data,
    utt_count,
    gain_row,
    shift_row,
    w_in,
    kernel,
    bn_gain,
    bn_shift,
    w_out,
    frame_mask,
    frame_count,
):
    model_width = row_data.shape[1]
    frame_len = row_data.shape[0] // utt_count
    normed_b = layer_norm(row_data, gain_row, shift_row).astype(jnp.bfloat16)
    gate_pair = matmul_low(normed_b, w_in)
    mask_rows = frame_mask.reshape(-1, 1)
    gated_b = (
        (glu_gate(gate_pair) * mask_rows)
        .astype(jnp.bfloat16)
        .reshape(utt_count, frame_len, model_width)
    )
    halo_reach = (kernel.shape[1] - 1) // 2
    padded = extended(gated_b, (("seq", 1),), halo_reach)
    kernel_f = kernel.astype(jnp.float32)
    depth_out = padded[:, 0:frame_len].astype(jnp.float32) * kernel_f[:, 0]
    for tap_idx in range(1, kernel.shape[1]):
        depth_out = (
            depth_out
            + padded[:, tap_idx : tap_idx + frame_len].astype(jnp.float32) * kernel_f[:, tap_idx]
        )
    weight_mask = frame_mask[:, :, None]
    sum_local = jnp.sum(depth_out * weight_mask, axis=(0, 1))
    square_local = jnp.sum(depth_out * depth_out * weight_mask, axis=(0, 1))
    sum_all, square_all = lax.psum((sum_local, square_local), ("dp", "seq"))
    mean_val = sum_all / frame_count
    variance = square_all / frame_count - mean_val * mean_val
    inv_std = lax.rsqrt(variance + 1e-05)
    normal = (depth_out - mean_val) * inv_std * bn_gain + bn_shift
    active_b = jax.nn.silu(normal).astype(jnp.bfloat16).reshape(-1, model_width)
    branch = matmul_low(active_b, w_out)
    kept_data = (
        row_data,
        normed_b,
        gate_pair,
        padded,
        depth_out,
        mean_val,
        inv_std,
        normal,
        active_b,
    )
    return (row_data + branch, kept_data)


def conv_backward(
    grad_rows, kept_data, gain_row, shift_row, w_in, kernel, bn_gain, w_out, frame_mask, frame_count
):
    row_data, normed_b, gate_pair, padded, depth_out, mean_val, inv_std, normal, active_b = (
        kept_data
    )
    frame_len = depth_out.shape[1]
    model_width = depth_out.shape[2]
    grad_out_b = grad_rows.astype(jnp.bfloat16)
    g_out = weight_grad(active_b, grad_out_b)
    grad_active = matmul_back(grad_out_b, w_out).reshape(depth_out.shape)
    grad_normal = jax.vjp(jax.nn.silu, normal)[1](grad_active)[0]
    centred_hat = (depth_out - mean_val) * inv_std
    g_bn_gain = jnp.sum(grad_normal * centred_hat, axis=(0, 1))
    g_bn_shift = jnp.sum(grad_normal, axis=(0, 1))
    grad_hat = grad_normal * bn_gain
    part_one = jnp.sum(grad_hat, axis=(0, 1))
    part_two = jnp.sum(grad_hat * depth_out, axis=(0, 1))
    part_one, part_two = lax.psum((part_one, part_two), ("dp", "seq"))
    grad_inv = part_two - mean_val * part_one
    grad_var = -0.5 * inv_std * inv_std * inv_std * grad_inv
    grad_mean = -inv_std * part_one - 2.0 * mean_val * grad_var
    weight_mask = frame_mask[:, :, None]
    grad_depth_b = (
        grad_hat * inv_std
        + weight_mask * (grad_mean / frame_count + 2.0 * depth_out * grad_var / frame_count)
    ).astype(jnp.bfloat16)
    halo_reach = (kernel.shape[1] - 1) // 2
    grad_padded = extended(grad_depth_b, (("seq", 1),), halo_reach)
    kernel_f = kernel.astype(jnp.float32)
    grad_depth_f = grad_depth_b.astype(jnp.float32)
    grad_gated = jnp.zeros(depth_out.shape, jnp.float32)
    kernel_cols = []
    for tap_idx in range(kernel.shape[1]):
        begin_at = 2 * halo_reach - tap_idx
        grad_gated = (
            grad_gated
            + grad_padded[:, begin_at : begin_at + frame_len].astype(jnp.float32)
            * kernel_f[:, tap_idx]
        )
        kernel_cols.append(
            jnp.sum(
                padded[:, tap_idx : tap_idx + frame_len].astype(jnp.float32) * grad_depth_f,
                axis=(0, 1),
            )
        )
    g_kernel = jnp.stack(kernel_cols, axis=1)
    grad_gate_b = jax.vjp(glu_gate, gate_pair)[1](
        (grad_gated * weight_mask).reshape(-1, model_width)
    )[0]
    grad_gate_b = grad_gate_b.astype(jnp.bfloat16)
    g_in = weight_grad(normed_b, grad_gate_b)
    grad_normed = matmul_back(grad_gate_b, w_in)
    grad_ln, g_gain, g_shift = jax.vjp(layer_norm, row_data, gain_row, shift_row)[1](grad_normed)
    return (grad_rows + grad_ln, (g_gain, g_shift, g_in, g_kernel, g_bn_gain, g_bn_shift, g_out))


def layer_forward(values, weights, frame_mask, key_valid, frame_count, pos_table_b):
    (
        gain_set,
        shift_set,
        rel_set,
        up_pair,
        down_pair,
        attn_in_w,
        attn_out_w,
        pos_w,
        conv_in_w,
        kernel,
        conv_out_w,
    ) = weights
    gain_f = gain_set.astype(jnp.float32)
    shift_f = shift_set.astype(jnp.float32)
    rel_f = rel_set.astype(jnp.float32)
    utt_count = values.shape[0]
    row_data = values.reshape(-1, values.shape[2])
    row_data, kept_one = ffn_forward(row_data, gain_f[0], shift_f[0], up_pair[0], down_pair[0])
    row_data, kept_attn = attn_forward(
        row_data,
        utt_count,
        gain_f[1],
        shift_f[1],
        rel_f[0],
        rel_f[1],
        attn_in_w,
        attn_out_w,
        pos_w,
        key_valid,
        pos_table_b,
    )
    row_data, kept_conv = conv_forward(
        row_data,
        utt_count,
        gain_f[2],
        shift_f[2],
        conv_in_w,
        kernel,
        gain_f[5],
        shift_f[5],
        conv_out_w,
        frame_mask,
        frame_count,
    )
    row_data, kept_two = ffn_forward(row_data, gain_f[3], shift_f[3], up_pair[1], down_pair[1])
    result = layer_norm(row_data, gain_f[4], shift_f[4])
    return (result.reshape(values.shape), (kept_one, kept_attn, kept_conv, kept_two, row_data))


def layer_backward(
    grad_values, kept_data, weights, frame_mask, key_valid, frame_count, pos_table_b
):
    (
        gain_set,
        shift_set,
        rel_set,
        up_pair,
        down_pair,
        attn_in_w,
        attn_out_w,
        pos_w,
        conv_in_w,
        kernel,
        conv_out_w,
    ) = weights
    gain_f = gain_set.astype(jnp.float32)
    shift_f = shift_set.astype(jnp.float32)
    kept_one, kept_attn, kept_conv, kept_two, last_rows = kept_data
    grad_rows = grad_values.reshape(-1, grad_values.shape[2])
    grad_rows, g_gain_last, g_shift_last = jax.vjp(layer_norm, last_rows, gain_f[4], shift_f[4])[1](
        grad_rows
    )
    grad_rows, two_grads = ffn_backward(
        grad_rows, kept_two, gain_f[3], shift_f[3], up_pair[1], down_pair[1]
    )
    grad_rows, conv_grads = conv_backward(
        grad_rows,
        kept_conv,
        gain_f[2],
        shift_f[2],
        conv_in_w,
        kernel,
        gain_f[5],
        conv_out_w,
        frame_mask,
        frame_count,
    )
    grad_rows, attn_grads = attn_backward(
        grad_rows, kept_attn, gain_f[1], shift_f[1], attn_in_w, attn_out_w, key_valid, pos_table_b
    )
    grad_rows, one_grads = ffn_backward(
        grad_rows, kept_one, gain_f[0], shift_f[0], up_pair[0], down_pair[0]
    )
    grad_gains = jnp.stack(
        [one_grads[0], attn_grads[0], conv_grads[0], two_grads[0], g_gain_last, conv_grads[4]]
    )
    grad_shifts = jnp.stack(
        [one_grads[1], attn_grads[1], conv_grads[1], two_grads[1], g_shift_last, conv_grads[5]]
    )
    grad_rel = jnp.stack([attn_grads[2], attn_grads[3]])
    grad_up = jnp.stack([one_grads[2], two_grads[2]])
    grad_down = jnp.stack([one_grads[3], two_grads[3]])
    layer_grads = (
        grad_gains,
        grad_shifts,
        grad_rel,
        grad_up,
        grad_down,
        attn_grads[4],
        attn_grads[5],
        attn_grads[6],
        conv_grads[2],
        conv_grads[3],
        conv_grads[6],
    )
    return (grad_rows.reshape(grad_values.shape), layer_grads)


def gather_forward(shards, layer_idx):
    pieces = tuple((member[layer_idx] for member in shards))
    return (
        lax.all_gather(pieces[0], ("dp", "seq"), axis=1, tiled=True),
        lax.all_gather(pieces[1], ("dp", "seq"), axis=1, tiled=True),
        lax.all_gather(pieces[2], ("dp", "seq"), axis=1, tiled=True),
        lax.all_gather(pieces[3], ("dp", "seq"), axis=1, tiled=True),
        lax.all_gather(pieces[4], ("dp", "seq"), axis=1, tiled=True),
        lax.all_gather(pieces[5], ("dp", "seq"), axis=0, tiled=True),
        lax.all_gather(pieces[6], ("dp", "seq"), axis=0, tiled=True),
        lax.all_gather(pieces[7], ("dp", "seq"), axis=0, tiled=True),
        lax.all_gather(pieces[8], ("dp", "seq"), axis=0, tiled=True),
        lax.all_gather(pieces[9], ("dp", "seq"), axis=0, tiled=True),
        lax.all_gather(pieces[10], ("dp", "seq"), axis=0, tiled=True),
    )


def gather_backward(shards, layer_idx):
    pieces = tuple((member[layer_idx] for member in shards))
    return (
        lax.all_gather(pieces[0], ("dp", "seq"), axis=1, tiled=True),
        lax.all_gather(pieces[1], ("dp", "seq"), axis=1, tiled=True),
        lax.all_gather(pieces[2], ("dp", "seq"), axis=1, tiled=True),
        lax.all_gather(pieces[3], ("dp", "seq"), axis=1, tiled=True),
        lax.all_gather(pieces[4], ("dp", "seq"), axis=1, tiled=True),
        lax.all_gather(pieces[5], ("dp", "seq"), axis=0, tiled=True),
        lax.all_gather(pieces[6], ("dp", "seq"), axis=0, tiled=True),
        lax.all_gather(pieces[7], ("dp", "seq"), axis=0, tiled=True),
        lax.all_gather(pieces[8], ("dp", "seq"), axis=0, tiled=True),
        lax.all_gather(pieces[9], ("dp", "seq"), axis=0, tiled=True),
        lax.all_gather(pieces[10], ("dp", "seq"), axis=0, tiled=True),
    )


def local_general(
    frames,
    lengths,
    cotangent,
    gains,
    shifts,
    rel_bias,
    ffn_up,
    ffn_down,
    attn_in,
    attn_out,
    pos_proj,
    conv_in,
    depthwise,
    conv_out,
):
    shards = (
        gains,
        shifts,
        rel_bias,
        ffn_up,
        ffn_down,
        attn_in,
        attn_out,
        pos_proj,
        conv_in,
        depthwise,
        conv_out,
    )
    groups = lax.axis_size("dp")
    seq_devices = lax.axis_size("seq")
    local_utts = frames.shape[0]
    frame_len = frames.shape[1]
    model_width = frames.shape[2]
    utt_per = local_utts // MB
    length = frame_len * seq_devices
    seq_start = lax.axis_index("seq") * frame_len
    first_utt = lax.axis_index("dp") * local_utts
    own_lengths = lax.dynamic_slice_in_dim(lengths, first_utt, local_utts)
    lengths_grid = lengths.reshape(groups, MB, utt_per)
    offsets = seq_start + frame_len - 1 - jnp.arange(length + frame_len - 1, dtype=jnp.int32)
    pos_table_b = sinusoid(offsets, model_width).astype(jnp.bfloat16)
    frame_pos = seq_start + jnp.arange(frame_len, dtype=jnp.int32)
    key_pos = jnp.arange(length, dtype=jnp.int32)
    result_list = []
    grad_list = []
    full_sums = [None] * NL
    for micro_idx in range(MB):
        lens_here = own_lengths[micro_idx * utt_per : (micro_idx + 1) * utt_per]
        frame_mask = (frame_pos[None, :] < lens_here[:, None]).astype(jnp.float32)
        key_valid = key_pos[None, :] < lens_here[:, None]
        frame_count = jnp.sum(lengths_grid[:, micro_idx]).astype(jnp.float32)
        values = frames[micro_idx * utt_per : (micro_idx + 1) * utt_per]
        held_weights = []
        layer_idx = 0
        weights = gather_forward(shards, layer_idx)
        values, kept_data = layer_forward(
            values, weights, frame_mask, key_valid, frame_count, pos_table_b
        )
        saved_acts = [kept_data]
        held_weights.append(weights)
        result_list.append(values)
        grad_values = cotangent[micro_idx * utt_per : (micro_idx + 1) * utt_per]
        for layer_idx in reversed(range(NL)):
            weights = gather_backward(shards, layer_idx)
            grad_values, layer_grads = layer_backward(
                grad_values,
                saved_acts[layer_idx],
                weights,
                frame_mask,
                key_valid,
                frame_count,
                pos_table_b,
            )
            if full_sums[layer_idx] is None:
                full_sums[layer_idx] = layer_grads
            else:
                full_sums[layer_idx] = jax.tree.map(jnp.add, full_sums[layer_idx], layer_grads)
        grad_list.append(grad_values)
    stacked = tuple((jnp.stack([full_sums[0][member]]) for member in range(11)))
    final_grads = (
        lax.psum_scatter(stacked[0], ("dp", "seq"), scatter_dimension=2, tiled=True),
        lax.psum_scatter(stacked[1], ("dp", "seq"), scatter_dimension=2, tiled=True),
        lax.psum_scatter(stacked[2], ("dp", "seq"), scatter_dimension=2, tiled=True),
        lax.psum_scatter(stacked[3], ("dp", "seq"), scatter_dimension=2, tiled=True),
        lax.psum_scatter(stacked[4], ("dp", "seq"), scatter_dimension=2, tiled=True),
        lax.psum_scatter(stacked[5], ("dp", "seq"), scatter_dimension=1, tiled=True),
        lax.psum_scatter(stacked[6], ("dp", "seq"), scatter_dimension=1, tiled=True),
        lax.psum_scatter(stacked[7], ("dp", "seq"), scatter_dimension=1, tiled=True),
        lax.psum_scatter(stacked[8], ("dp", "seq"), scatter_dimension=1, tiled=True),
        lax.psum_scatter(stacked[9], ("dp", "seq"), scatter_dimension=1, tiled=True),
        lax.psum_scatter(stacked[10], ("dp", "seq"), scatter_dimension=1, tiled=True),
    )
    mixed = jnp.concatenate(result_list, axis=0)
    grad_frames = jnp.concatenate(grad_list, axis=0)
    return (
        mixed,
        grad_frames,
        final_grads[0],
        final_grads[1],
        final_grads[2],
        final_grads[3],
        final_grads[4],
        final_grads[5],
        final_grads[6],
        final_grads[7],
        final_grads[8],
        final_grads[9],
        final_grads[10],
    )


NT = (((1,), (1,)), ((), ()))
TN = (((0,), (0,)), ((), ()))
NN = (((1,), (0,)), ((), ()))
MESH = pl.DeviceIdType.MESH
UTTS = 4
SMALL = 128
VMEM_LIMIT = 60 * 1024 * 1024


def fits_whole(mesh):
    return mesh.shape["dp"] == 4 and mesh.shape["seq"] == MB * UTTS


def dotf(left, right, dims=NN):
    return lax.dot_general(left, right, dims, preferred_element_type=jnp.float32)


def place():
    dp = lax.axis_index("dp")
    sq = lax.axis_index("seq")
    return dp, sq, lax.div(dp, 2), lax.rem(dp, 2), lax.div(sq, 2), lax.rem(sq, 2)


def flip_if(value, bit):
    return 1 - value if bit else value


def partners():
    dp, sq, x, c, z, y = place()
    even = c == 0
    core = (x * 2 + 1 - c, sq)
    xdev = ((1 - x) * 2 + c, sq)
    ydev = (dp, z * 2 + 1 - y)
    first = (jnp.where(even, ydev[0], xdev[0]), jnp.where(even, ydev[1], xdev[1]))
    second = (jnp.where(even, xdev[0], ydev[0]), jnp.where(even, xdev[1], ydev[1]))
    return core, xdev, first, second


def rank_of(color, a, b, k):
    _, _, x, _, z, y = place()
    even = color == 0
    xx = jnp.where(even, x + a * (1 - 2 * x), x + b * (1 - 2 * x))
    yy = jnp.where(even, y + b * (1 - 2 * y), y + a * (1 - 2 * y))
    return xx * 16 + color * 8 + lax.rem(z + k, 4) * 2 + yy


def greet(devices):
    barrier = pltpu.get_barrier_semaphore()
    for device in devices:
        pl.semaphore_signal(barrier, inc=1, device_id=device, device_id_type=MESH)
    pl.semaphore_wait(barrier, len(devices))


def seq_peers(dp, sq, count):
    return [(dp, lax.rem(sq + k, count)) for k in range(1, count)]


def remote(src, dst, send, recv, device):
    return pltpu.make_async_remote_copy(
        src_ref=src, dst_ref=dst, send_sem=send, recv_sem=recv, device_id=device, device_id_type=MESH
    )


def alternate(a, b, k):
    return a * 8 + b * 4 + k


def gather_steps(w_ref, d_ref, w_all, d_all, send, recv, own):
    wr, dr = w_ref.shape[0], d_ref.shape[0]
    started = []

    def blocks(rank):
        return (
            w_all.at[pl.ds(pl.multiple_of(rank * wr, 16), wr), :],
            d_all.at[pl.ds(pl.multiple_of(rank * dr, 16), dr), :],
        )

    def pair(group, target, slot, landing_slot, mine, other):
        dp, sq, _, c, z, y = place()
        core, _, first, second = partners()
        device = {"core": core, "first": first, "second": second}.get(target)
        if device is None:
            device = (dp, lax.rem(z + target, 4) * 2 + y)
        w_dst, d_dst = blocks(rank_of(1 - c if other else c, *group))
        w_src, d_src = (w_ref, d_ref) if mine else (w_dst, d_dst)
        return (
            remote(w_src, w_dst, send.at[0, slot], recv.at[0, landing_slot], device),
            remote(d_src, d_dst, send.at[1, slot], recv.at[1, landing_slot], device),
        )

    def ship(group, target, slot, landing_slot, mine=False):
        spec = (group, target, slot, landing_slot, mine, False)
        for copy in pair(*spec):
            copy.start()
        started.append(spec)

    def arrive(group, other=False):
        for copy in pair(group, "core", 0, alternate(*group) + (16 if other else 0), False, other):
            copy.wait_recv()

    def to_core(group, mine=False):
        spot = 16 + alternate(*group)
        ship(group, "core", spot, spot, mine)

    def own_copies():
        _, _, _, c, _, _ = place()
        w_own, d_own = blocks(rank_of(c, 0, 0, 0))
        return (
            pltpu.make_async_copy(w_ref, w_own, own.at[0]),
            pltpu.make_async_copy(d_ref, d_own, own.at[1]),
        )

    def begin():
        mine = (0, 0, 0)
        ship(mine, "second", 15, 8, mine=True)
        ship(mine, "first", 3, 4, mine=True)
        for k in (1, 3, 2):
            ship(mine, k, k - 1, 4 - k, mine=True)
        to_core(mine, mine=True)
        for copy in own_copies():
            copy.start()

    def along(k):
        group = (0, 0, k)
        arrive(group)
        ship(group, "second", 8 + k - 1, 8 + k)
        ship(group, "first", 4 + k - 1, 4 + k)
        to_core(group)

    def across(k):
        group = (0, 1, k)
        arrive(group)
        ship(group, "second", 11 + k, 12 + k)
        to_core(group)

    def over(k):
        for b in (0, 1):
            group = (1, b, k)
            arrive(group)
            to_core(group)

    def finish():
        for k in (0, 1, 3, 2):
            for a, b in ((0, 0), (0, 1), (1, 0), (1, 1)):
                arrive((a, b, k), other=True)
        for copy in own_copies():
            copy.wait()
        for spec in started:
            for copy in pair(*spec):
                copy.wait_send()

    return begin, along, across, over, finish


def meeting(count):
    dp, sq, *_ = place()
    core, xdev, _, _ = partners()
    greet(seq_peers(dp, sq, count) + [core, xdev])


def tree_scratch():
    return [
        pltpu.SemaphoreType.DMA((2, 32)),
        pltpu.SemaphoreType.DMA((2, 32)),
        pltpu.SemaphoreType.DMA((2,)),
    ]


def gather_kernel(w_ref, d_ref, f_ref, w_all, d_all, f_all, send, recv, own, row_send, row_recv, row_own):
    meeting(f_ref.shape[0])
    begin, along, across, over, finish = gather_steps(w_ref, d_ref, w_all, d_all, send, recv, own)
    begin()
    rows_begin(f_ref, f_all, row_send, row_recv, row_own)
    across(0)
    along(1)
    across(1)
    over(0)
    along(3)
    across(3)
    over(1)
    along(2)
    across(2)
    over(3)
    over(2)
    finish()
    rows_end(f_ref, f_all, row_send, row_recv, row_own)


def gathered(w, d):
    return [
        jax.ShapeDtypeStruct((w.shape[0] * 32, w.shape[1]), w.dtype),
        jax.ShapeDtypeStruct((d.shape[0] * 32, d.shape[1]), d.dtype),
    ]


def gather_all(w, d, f):
    vm = pl.BlockSpec(memory_space=pltpu.VMEM)
    hbm = pl.BlockSpec(memory_space=pl.ANY)
    return pl.pallas_call(
        gather_kernel,
        in_specs=[vm] * 3,
        out_specs=[hbm] * 3,
        out_shape=gathered(w, d) + [jax.ShapeDtypeStruct(f.shape, f.dtype)],
        scratch_shapes=tree_scratch() + row_scratch(f.shape[0]),
        compiler_params=pltpu.CompilerParams(collective_id=0, has_side_effects=True),
        name="gather_all",
    )(w, d, f)


def scatter_steps(w_ref, d_ref, w_out, d_out, bufs, send, recv):
    w0, d0, w1, d1, w2, d2, w3, d3 = bufs
    wr, dr = w_out.shape[0], d_out.shape[0]

    def rows(rank, size):
        return pl.ds(pl.multiple_of(rank * size, 16), size)

    def group_rank(slot, other):
        _, _, _, c, _, _ = place()
        color = 1 - c if other else c
        return rank_of(color, lax.div(slot, 8), lax.rem(lax.div(slot, 4), 2), lax.rem(slot, 4))

    def core_copies(slot):
        core = partners()[0]
        rank = group_rank(slot, True)
        return (
            remote(w_ref.at[rows(rank, wr), :], w0.at[slot], send.at[0, slot], recv.at[0, slot], core),
            remote(d_ref.at[rows(rank, dr), :], d0.at[slot], send.at[1, slot], recv.at[1, slot], core),
        )

    def second_copies(slot):
        to = partners()[3]
        return (
            remote(w0.at[8 + slot], w1.at[slot], send.at[0, 16 + slot], recv.at[0, 16 + slot], to),
            remote(d0.at[8 + slot], d1.at[slot], send.at[1, 16 + slot], recv.at[1, 16 + slot], to),
        )

    def first_copies(slot):
        to = partners()[2]
        return (
            remote(w0.at[4 + slot], w2.at[slot], send.at[0, 24 + slot], recv.at[0, 24 + slot], to),
            remote(d0.at[4 + slot], d2.at[slot], send.at[1, 24 + slot], recv.at[1, 24 + slot], to),
        )

    def z_copies(k):
        dp, _, _, _, z, y = place()
        to = (dp, lax.rem(z + k, 4) * 2 + y)
        return (
            remote(w0.at[k], w3.at[3 - k], send.at[0, 27 + k], recv.at[0, 31 - k], to),
            remote(d0.at[k], d3.at[3 - k], send.at[1, 27 + k], recv.at[1, 31 - k], to),
        )

    def start(copies):
        for copy in copies:
            copy.start()

    def landed(copies):
        for copy in copies:
            copy.wait_recv()

    def sent(copies):
        for copy in copies:
            copy.wait_send()

    def add(slot, w, d):
        f = jnp.float32
        w0[slot] = (w0[slot].astype(f) + w.astype(f)).astype(jnp.bfloat16)
        d0[slot] = (d0[slot].astype(f) + d.astype(f)).astype(jnp.bfloat16)

    def begin():
        @pl.loop(0, 16)
        def _(step):
            start(core_copies(15 - step))

    def take(slot):
        landed(core_copies(slot))
        rank = group_rank(slot, False)
        add(slot, w_ref[rows(rank, wr), :], d_ref[rows(rank, dr), :])

    def far(lo, hi):
        @pl.loop(lo, hi)
        def _(step):
            take(15 - step)
            start(second_copies(7 - step))

    def near(lo, hi):
        @pl.loop(lo, hi)
        def _(step):
            take(7 - step)

    def pass_first(lo, hi):
        @pl.loop(lo, hi)
        def _(step):
            slot = 7 - step
            landed(second_copies(slot))
            add(slot, w1[slot], d1[slot])
            start(first_copies(slot - 4))

    def join_second():
        @pl.loop(0, 3)
        def _(step):
            slot = 3 - step
            landed(second_copies(slot))
            add(slot, w1[slot], d1[slot])

    def pass_along(lo, hi):
        @pl.loop(lo, hi)
        def _(step):
            slot = 3 - step
            landed(first_copies(slot))
            add(slot, w2[slot], d2[slot])
            start(z_copies(slot))

    def total(base, parts):
        value = base.astype(jnp.float32)
        for part in parts:
            value = value + part.astype(jnp.float32)
        return value

    def finish():
        landed(second_copies(0))
        landed(first_copies(0))
        for k in (1, 2, 3):
            landed(z_copies(k))
        w_out[...] = total(w0[0], (w1[0], w2[0], w3[0], w3[1], w3[2]))
        d_out[...] = total(d0[0], (d1[0], d2[0], d3[0], d3[1], d3[2]))

        @pl.loop(0, 16)
        def _(slot):
            sent(core_copies(slot))

        @pl.loop(0, 8)
        def _(slot):
            sent(second_copies(slot))

        @pl.loop(0, 4)
        def _(slot):
            sent(first_copies(slot))

        for k in (1, 2, 3):
            sent(z_copies(k))

    return begin, far, near, pass_first, join_second, pass_along, finish


def scatter_scratch(w, d):
    bf = jnp.bfloat16
    scratch = []
    for n in (16, 8, 4, 3):
        scratch += [
            pltpu.VMEM((n, w.shape[0] // 32, w.shape[1]), bf),
            pltpu.VMEM((n, d.shape[0] // 32, d.shape[1]), bf),
        ]
    return scratch + tree_scratch()[:2]


def scattered(w, d):
    return [
        jax.ShapeDtypeStruct((w.shape[0] // 32, w.shape[1]), jnp.float32),
        jax.ShapeDtypeStruct((d.shape[0] // 32, d.shape[1]), jnp.float32),
    ]


def scatter_kernel(w_ref, d_ref, g_ref, w_out, d_out, g_all, *scratch):
    bufs, (send, recv, row_send, row_recv, row_own) = scratch[:8], scratch[8:]
    meeting(g_ref.shape[0])
    begin, far, near, pass_first, join_second, pass_along, finish = scatter_steps(
        w_ref, d_ref, w_out, d_out, bufs, send, recv
    )
    begin()
    far(0, 8)
    rows_begin(g_ref, g_all, row_send, row_recv, row_own)
    near(0, 4)
    pass_first(0, 4)
    near(4, 8)
    join_second()
    pass_along(0, 3)
    finish()
    rows_end(g_ref, g_all, row_send, row_recv, row_own)


def scatter_all(w, d, g):
    vm = pl.BlockSpec(memory_space=pltpu.VMEM)
    hbm = pl.BlockSpec(memory_space=pl.ANY)
    return pl.pallas_call(
        scatter_kernel,
        in_specs=[vm] * 3,
        out_specs=[vm, vm, hbm],
        out_shape=scattered(w, d) + [jax.ShapeDtypeStruct(g.shape, g.dtype)],
        scratch_shapes=scatter_scratch(w, d) + row_scratch(g.shape[0]),
        compiler_params=pltpu.CompilerParams(
            collective_id=1, has_side_effects=True, vmem_limit_bytes=VMEM_LIMIT
        ),
        name="scatter_all",
    )(w, d, g)


def batch_sum_kernel(s_ref, o_ref, buf, send, recv):
    dp, sq, *_ = place()
    base = lax.div(sq, UTTS) * UTTS
    me = dp * UTTS + lax.rem(sq, UTTS)
    size = buf.shape[0]

    def device(j):
        r = lax.rem(me + j, size)
        return (lax.div(r, UTTS), base + lax.rem(r, UTTS))

    def copy(j):
        return remote(s_ref, buf.at[me], send.at[j - 1], recv.at[size - 1 - j], device(j))

    greet([device(j) for j in range(1, size)])
    for j in range(1, size):
        copy(j).start()
    buf[me] = s_ref[...]
    for j in range(1, size):
        remote(s_ref, buf.at[lax.rem(me + j, size)], send.at[j - 1], recv.at[j - 1], device(j)).wait_recv()
    o_ref[...] = jnp.sum(buf[...], axis=0)
    for j in range(1, size):
        copy(j).wait_send()


def batch_sum(sums, ident):
    vm = pl.BlockSpec(memory_space=pltpu.VMEM)
    size = 4 * UTTS
    return pl.pallas_call(
        batch_sum_kernel,
        in_specs=[vm],
        out_specs=vm,
        out_shape=jax.ShapeDtypeStruct(sums.shape, jnp.float32),
        scratch_shapes=[
            pltpu.VMEM((size,) + sums.shape, jnp.float32),
            pltpu.SemaphoreType.DMA((size - 1,)),
            pltpu.SemaphoreType.DMA((size - 1,)),
        ],
        compiler_params=pltpu.CompilerParams(collective_id=ident, has_side_effects=True),
        name="batch_sum",
    )(sums)


def rows_begin(src, dst, send, recv, own):
    _, sq, *_ = place()
    for k in range(1, dst.shape[0]):
        row_copy(src, dst, send, recv, k).start()
    pltpu.make_async_copy(src.at[sq], dst.at[sq], own).start()


def rows_end(src, dst, send, recv, own):
    dp, sq, *_ = place()
    count = dst.shape[0]
    for k in range(1, count):
        copy = row_copy(src, dst, send, recv, k)
        copy.wait_send()
        landing(src, dst, send, recv, k).wait_recv()
    pltpu.make_async_copy(src.at[sq], dst.at[sq], own).wait()


def row_copy(src, dst, send, recv, k):
    dp, sq, *_ = place()
    count = dst.shape[0]
    to = lax.rem(sq + k, count)
    return remote(src.at[to], dst.at[sq], send.at[k - 1], recv.at[count - 1 - k], (dp, to))


def landing(src, dst, send, recv, k):
    dp, sq, *_ = place()
    origin = lax.rem(sq + k, dst.shape[0])
    return remote(src.at[sq], dst.at[origin], send.at[k - 1], recv.at[k - 1], (dp, origin))


def norm_parts(rows):
    centred = rows - jnp.mean(rows, axis=1, keepdims=True)
    return centred, lax.rsqrt(jnp.mean(centred * centred, axis=1, keepdims=True) + 1e-05)


def norm(rows, gain, shift):
    centred, inv = norm_parts(rows)
    return centred * inv * gain + shift


def silu(h):
    return h * (1.0 / (1.0 + jnp.exp(-h)))


def front_kernel(
    len_ref, f_ref, in_ref, pos_ref, up_ref, small_ref, down_ref, table_ref, c_ref, w_ref, d_ref,
    ctx_ref, p_ref, x1_ref, qu_ref, qv_ref, k_ref, v_ref, t_ref, sm_ref, c_all, w_all, d_all,
    send, recv, own, row_send, row_recv, row_own, *, tq, tile,
):
    low = jnp.bfloat16
    keys, model = f_ref.shape
    span = keys + tq
    steps = keys // tq
    begin, along, across, over, finish = gather_steps(w_ref, d_ref, w_all, d_all, send, recv, own)

    def dense(i):
        rows = pl.ds(pl.multiple_of(i * tile, tile), tile)
        x0 = f_ref[rows, :].astype(jnp.float32)
        a0 = norm(x0, sm_ref[0:1, :], sm_ref[6:7, :]).astype(low)
        z = silu(dotf(a0, up_ref[...])).astype(low)
        x1 = x0 + 0.5 * dotf(z, down_ref[...])
        x1_ref[rows, :] = x1
        a1 = norm(x1, sm_ref[1:2, :], sm_ref[7:8, :]).astype(low)
        query = dotf(a1, in_ref[:, :model])
        qu_ref[rows, :] = (query + sm_ref[12:13, :]).astype(low)
        qv_ref[rows, :] = (query + sm_ref[13:14, :]).astype(low)
        k_ref[rows, :] = dotf(a1, in_ref[:, model : 2 * model]).astype(low)
        v_ref[rows, :] = dotf(a1, in_ref[:, 2 * model :]).astype(low)

    @pl.when(pl.program_id(0) == 0)
    def _():
        meeting(c_ref.shape[0])
        begin()
        rows_begin(c_ref, c_all, row_send, row_recv, row_own)
        sm_ref[...] = small_ref[...].astype(jnp.float32).T

        @pl.loop(0, 2 * keys // tile)
        def _(i):
            rows = pl.ds(pl.multiple_of(i * tile, tile), tile)
            t_ref[rows, :] = dotf(table_ref[rows, :], pos_ref[...]).astype(low)

        @pl.loop(0, keys // tile)
        def _(i):
            dense(i)

            @pl.when(i == 0)
            def _():
                across(0)
                along(1)

            @pl.when(i == 1)
            def _():
                along(3)
                across(1)

            @pl.when(i == 2)
            def _():
                along(2)

    plan = {1: ((across, 3), (over, 0)), 3: ((across, 2),), 5: ((over, 1),), 8: ((over, 3),), 11: ((over, 2),)}
    valid = lax.broadcasted_iota(jnp.int32, (1, keys), 1) < len_ref[0]
    base = pl.program_id(0) * 128

    @pl.loop(0, steps)
    def _(i):
        time = pl.program_id(0) * steps + i
        for at, todo in plan.items():

            @pl.when(time == at)
            def _():
                for step, k in todo:
                    step(k)

        rows = pl.ds(pl.multiple_of(i * tq, tq), tq)
        band = pl.ds(pl.multiple_of(keys - tq - i * tq, tq), span)
        pair = pl.ds(pl.multiple_of(base, 128), 128)
        qu, qv, k, v, t = qu_ref[rows, pair], qv_ref[rows, pair], k_ref[:, pair], v_ref[:, pair], t_ref[band, pair]
        for h in range(2):
            cols = slice(h * DH, (h + 1) * DH)
            content = dotf(qu[:, cols], k[:, cols], NT)
            raw = dotf(qv[:, cols], t[:, cols], NT)
            pos = pltpu.roll(raw, keys + 1, 1, stride=1, stride_axis=0)[:, :keys]
            s = jnp.where(valid, (content + pos) * 0.125, -1e30)
            e = jnp.exp(s - jnp.max(s, axis=1, keepdims=True))
            p = (e * (1.0 / jnp.sum(e, axis=1, keepdims=True))).astype(low)
            p_ref[h, rows, :] = p
            ctx_ref[rows, cols] = dotf(p, v[:, cols]).astype(low)

    @pl.when(pl.program_id(0) == pl.num_programs(0) - 1)
    def _():
        finish()
        rows_end(c_ref, c_all, row_send, row_recv, row_own)


def row_scratch(count):
    return [
        pltpu.SemaphoreType.DMA((count - 1,)),
        pltpu.SemaphoreType.DMA((count - 1,)),
        pltpu.SemaphoreType.DMA,
    ]


def front(length, f, w_early, cuts, down, table_in, cot, w, d, tq=256, tile=256):
    rows, model = f.shape
    low = jnp.bfloat16
    vm = pl.BlockSpec(memory_space=pltpu.VMEM)
    hbm = pl.BlockSpec(memory_space=pl.ANY)

    def window(lo, hi):
        return pl.BlockSpec((w_early.shape[0], hi - lo), lambda h, *_: (0, lo // (hi - lo)), pipeline_mode=pl.Buffered(1))

    one = jax.ShapeDtypeStruct((rows, model), low)
    return pl.pallas_call(
        lambda *refs: front_kernel(*refs, tq=tq, tile=tile),
        grid_spec=pltpu.PrefetchScalarGridSpec(
            num_scalar_prefetch=1,
            grid=(model // 128,),
            in_specs=[vm] + [window(lo, hi) for lo, hi in zip(cuts[:-1], cuts[1:])] + [vm] * 5,
            out_specs=[
                pl.BlockSpec((rows, 128), lambda h, *_: (0, h)),
                pl.BlockSpec((2, rows, rows), lambda h, *_: (h, 0, 0)),
            ]
            + [vm] * 7
            + [hbm] * 3,
            scratch_shapes=tree_scratch() + row_scratch(cot.shape[0]),
        ),
        out_shape=[
            one,
            jax.ShapeDtypeStruct((model // DH, rows, rows), low),
            jax.ShapeDtypeStruct((rows, model), jnp.float32),
            one,
            one,
            one,
            one,
            jax.ShapeDtypeStruct((2 * rows, model), low),
            jax.ShapeDtypeStruct((SMALL, model), jnp.float32),
            jax.ShapeDtypeStruct(cot.shape, cot.dtype),
        ]
        + gathered(w, d),
        compiler_params=pltpu.CompilerParams(
            collective_id=4, has_side_effects=True, vmem_limit_bytes=VMEM_LIMIT
        ),
        name="front",
    )(length, f, *[w_early] * (len(cuts) - 1), down, table_in, cot, w, d)


def norm_back(rows, gain, grad):
    centred, inv = norm_parts(rows)
    hat = centred * inv
    scaled = grad * gain
    inner = jnp.mean(scaled * hat, axis=1, keepdims=True)
    out = inv * (scaled - jnp.mean(scaled, axis=1, keepdims=True) - hat * inner)
    return out, hat, jnp.sum(grad * hat, axis=0, keepdims=True)


def back_kernel(
    p_ref, g_ref, qu_ref, qv_ref, k_ref, v_ref, t_ref,
    m_ref, w_ref, d_ref, x1_ref, f_ref, grad_ref, sm_ref, gs_ref, in_ref, up_ref, down_ref, table_ref,
    ge_ref, gd_ref, rows_ref, m_all, w_out, d_out,
    ds_sc, dt_sc, dproj_sc, dtab_sc, z_sc, dh_sc, a0_sc, a1_sc, go_sc, gs_sc, *scratch, tq, tile,
):
    bufs, (send, recv, row_send, row_recv, row_own) = scratch[:8], scratch[8:]
    begin, far, near, pass_first, join_second, pass_along, finish = scatter_steps(
        w_ref, d_ref, w_out, d_out, bufs, send, recv
    )
    low = jnp.bfloat16
    keys = k_ref.shape[0]
    model = f_ref.shape[1]
    span = keys + tq
    steps = keys // tq

    def open_up():
        meeting(m_ref.shape[0])
        begin()
        gs_sc[...] = gs_ref[...]

    def rows_away():
        near(4, 8)
        rows_begin(m_ref, m_all, row_send, row_recv, row_own)

    plan = {
        0: open_up,
        1: lambda: far(0, 4),
        2: lambda: far(4, 8),
        3: lambda: near(0, 4),
        4: rows_away,
        5: lambda: pass_first(0, 2),
        6: lambda: pass_first(2, 4),
        9: join_second,
        10: lambda: pass_along(0, 2),
        11: lambda: pass_along(2, 3),
    }
    flip = (
        lax.broadcasted_iota(jnp.int32, (tq, tq), 0) + lax.broadcasted_iota(jnp.int32, (tq, tq), 1) == tq - 1
    ).astype(low)
    pad = jnp.zeros((tq, tq), jnp.float32)
    dt_sc[...] = jnp.zeros_like(dt_sc)
    base = pl.program_id(0) * 128

    def at(offset):
        return pl.ds(pl.multiple_of(base + offset, 128), 128)

    @pl.loop(0, steps)
    def _(i):
        time = pl.program_id(0) * steps + i
        for moment, step in plan.items():
            pl.when(time == moment)(step)
        rows = pl.ds(pl.multiple_of(i * tq, tq), tq)
        band = pl.ds(pl.multiple_of(keys - tq - i * tq, tq), span)
        sides = []
        for h in range(2):
            cols = slice(h * DH, (h + 1) * DH)
            dp = dotf(g_ref[rows, cols], v_ref[:, cols], NT)
            pf = p_ref[h, rows, :].astype(jnp.float32)
            ds = (pf * (dp - jnp.sum(dp * pf, axis=1, keepdims=True))).astype(low)
            ds_sc[h, rows, :] = ds
            dqu = dotf(ds, k_ref[:, cols]) * 0.125
            turned = jnp.concatenate([dotf(flip, ds), pad], axis=1)
            raw = pltpu.roll(turned, 0, 1, stride=1, stride_axis=0).astype(low)
            dqv = dotf(flip, dotf(raw, t_ref[band, cols]).astype(low)) * 0.125
            qv = dotf(flip, qv_ref[rows, cols]).astype(low)
            dt_sc[h, band, :] += dotf(raw, qv, TN)
            sides.append((dqu, dqv))
        dqu, dqv = (jnp.concatenate(both, axis=1) for both in zip(*sides))
        gs_sc[12:13, at(0)] += jnp.sum(dqu, axis=0, keepdims=True)
        gs_sc[13:14, at(0)] += jnp.sum(dqv, axis=0, keepdims=True)
        dproj_sc[rows, at(0)] = (dqu + dqv).astype(low)

    halves = []
    for h in range(2):
        cols = slice(h * DH, (h + 1) * DH)
        halves.append(
            (
                dt_sc[h] * 0.125,
                dotf(ds_sc[h], qu_ref[:, cols], TN) * 0.125,
                dotf(p_ref[h], g_ref[:, cols], TN),
            )
        )
    dtab, dk, dv = (jnp.concatenate(both, axis=1).astype(low) for both in zip(*halves))
    dtab_sc[:, at(0)] = dtab
    dproj_sc[:, at(model)] = dk
    dproj_sc[:, at(2 * model)] = dv

    @pl.when(pl.program_id(0) == pl.num_programs(0) - 1)
    def _():
        @pl.loop(0, keys // tile)
        def _(i):
            rows = pl.ds(pl.multiple_of(i * tile, tile), tile)
            dn = dotf(dproj_sc[rows, :], in_ref[...], NT)
            dx, hat, dgain = norm_back(x1_ref[rows, :], sm_ref[1:2, :], dn)
            gs_sc[1:2, :] += dgain
            gs_sc[7:8, :] += jnp.sum(dn, axis=0, keepdims=True)
            a1_sc[rows, :] = (hat * sm_ref[1:2, :] + sm_ref[7:8, :]).astype(low)
            grad = grad_ref[rows, :] + dx
            go = (0.5 * grad).astype(low)
            go_sc[rows, :] = go
            x0 = f_ref[rows, :].astype(jnp.float32)
            a0 = norm(x0, sm_ref[0:1, :], sm_ref[6:7, :]).astype(low)
            a0_sc[rows, :] = a0
            h = dotf(a0, up_ref[...])
            sig = 1.0 / (1.0 + jnp.exp(-h))
            z_sc[rows, :] = (h * sig).astype(low)
            dh = (dotf(go, down_ref[...], NT) * (sig * (1.0 + h * (1.0 - sig)))).astype(low)
            dh_sc[rows, :] = dh
            dn = dotf(dh, up_ref[...], NT)
            dx, _, dgain = norm_back(x0, sm_ref[0:1, :], dn)
            gs_sc[0:1, :] += dgain
            gs_sc[6:7, :] += jnp.sum(dn, axis=0, keepdims=True)
            rows_ref[rows, :] = (grad + dx).astype(low)

        width = model

        @pl.loop(0, 3)
        def _(j):
            cols = pl.ds(pl.multiple_of(j * width, width), width)
            ge_ref[:, cols] = dotf(a1_sc[...], dproj_sc[:, cols], TN).astype(low)

        ge_ref[:, 3 * width : 4 * width] = dotf(table_ref[...], dtab_sc[...], TN).astype(low)

        @pl.loop(0, 4)
        def _(j):
            cols = pl.ds(pl.multiple_of(j * width, width), width)
            ge_ref[:, pl.ds(pl.multiple_of((j + 4) * width, width), width)] = dotf(
                a0_sc[...], dh_sc[:, cols], TN
            ).astype(low)
            gd_ref[cols, :] = dotf(z_sc[:, cols], go_sc[...], TN).astype(low)

        ge_ref[:, 8 * width :] = gs_sc[...].T.astype(low)
        finish()
        rows_end(m_ref, m_all, row_send, row_recv, row_own)


def back(
    p, g, qu, qv, k, v, table, mixed, w, d, x1, f, grad, small, g_small, w_early, cuts, down, table_in, tq=256, tile=256
):
    rows, model = qu.shape
    low = jnp.bfloat16
    vm = pl.BlockSpec(memory_space=pltpu.VMEM)
    blk = pl.BlockSpec((rows, 128), lambda h: (0, h))
    tab = pl.BlockSpec((2 * rows, 128), lambda h: (0, h))

    def window(j):
        lo, hi = cuts[j], cuts[j + 1]
        return pl.BlockSpec((w_early.shape[0], hi - lo), lambda h: (0, lo // (hi - lo)), pipeline_mode=pl.Buffered(1))

    hidden = down.shape[0]
    return pl.pallas_call(
        lambda *refs: back_kernel(*refs, tq=tq, tile=tile),
        grid=(model // 128,),
        in_specs=[pl.BlockSpec((2, rows, rows), lambda h: (h, 0, 0))]
        + [blk] * 5
        + [tab]
        + [vm] * 8
        + [window(0), window(2), vm, vm],
        out_specs=[vm] * 3 + [pl.BlockSpec(memory_space=pl.ANY), vm, vm],
        out_shape=[
            jax.ShapeDtypeStruct(w_early.shape, low),
            jax.ShapeDtypeStruct(down.shape, low),
            jax.ShapeDtypeStruct((rows, model), low),
            jax.ShapeDtypeStruct(mixed.shape, mixed.dtype),
        ]
        + scattered(w, d),
        scratch_shapes=[
            pltpu.VMEM((2, rows, rows), low),
            pltpu.VMEM((2, 2 * rows, DH), jnp.float32),
            pltpu.VMEM((rows, 3 * model), low),
            pltpu.VMEM((2 * rows, model), low),
            pltpu.VMEM((rows, hidden), low),
            pltpu.VMEM((rows, hidden), low),
            pltpu.VMEM((rows, model), low),
            pltpu.VMEM((rows, model), low),
            pltpu.VMEM((rows, model), low),
            pltpu.VMEM((SMALL, model), jnp.float32),
        ]
        + scatter_scratch(w, d)
        + row_scratch(mixed.shape[0]),
        compiler_params=pltpu.CompilerParams(
            collective_id=5, has_side_effects=True, vmem_limit_bytes=63 * 1024 * 1024
        ),
        name="back",
    )(p, g, qu, qv, k, v, table, mixed, w, d, x1, f, grad, small, g_small, w_early, w_early, down, table_in)


def position_table(length, width):
    offsets = (length - 1 - np.arange(2 * length)).astype(np.float32)
    half = width // 2
    steps = np.arange(half, dtype=np.float32) * np.float32(-2.0 * math.log(10000.0) / width)
    angles = (offsets[:, None] * np.exp(steps)[None, :]).astype(np.float64)
    table = np.concatenate([np.sin(angles), np.cos(angles)], axis=1)
    return jnp.asarray(table.astype(np.float32)).astype(jnp.bfloat16)


def shifted_sum(values, kernel_f, reverse):
    taps = kernel_f.shape[1]
    reach = (taps - 1) // 2
    padded = jnp.pad(values, ((reach, reach), (0, 0)))
    rows = values.shape[0]
    total = None
    for k in range(taps):
        at = taps - 1 - k if reverse else k
        term = padded[at : at + rows].astype(jnp.float32) * kernel_f[:, k]
        total = term if total is None else total + term
    return total


def tap_grads(values, grad, taps):
    reach = (taps - 1) // 2
    padded = jnp.pad(values, ((reach, reach), (0, 0)))
    rows = values.shape[0]
    grad_f = grad.astype(jnp.float32)
    return jnp.stack(
        [jnp.sum(padded[k : k + rows].astype(jnp.float32) * grad_f, axis=0) for k in range(taps)]
    )


def columns(*members):
    return [0] + [int(v) for v in np.cumsum([member.shape[1] for member in members])]


def split(values, cuts):
    return [values[:, lo:hi] for lo, hi in zip(cuts[:-1], cuts[1:])]


def local_whole(
    frames,
    lengths,
    cotangent,
    gains,
    shifts,
    rel_bias,
    ffn_up,
    ffn_down,
    attn_in,
    attn_out,
    pos_proj,
    conv_in,
    depthwise,
    conv_out,
):
    low = jnp.bfloat16
    dp, sq = lax.axis_index("dp"), lax.axis_index("seq")
    count, width_rows, model = frames.shape
    length = count * 0 + width_rows * lax.axis_size("seq")
    taps = depthwise.shape[2]
    small = jnp.concatenate([gains[0], shifts[0], rel_bias[0]], axis=0).T
    small = jnp.concatenate([small, depthwise[0]], axis=1)
    small = jnp.pad(small, ((0, 0), (0, SMALL - small.shape[1])))
    early = jnp.concatenate([attn_in[0], pos_proj[0], ffn_up[0, 0], small], axis=1)
    late = jnp.concatenate([ffn_up[0, 1], attn_out[0], conv_in[0], conv_out[0]], axis=1)
    cuts_early = columns(attn_in[0], pos_proj[0], ffn_up[0, 0], small)
    cuts_late = columns(ffn_up[0, 1], attn_out[0], conv_in[0], conv_out[0])
    w_early, down_0, f_all = gather_all(early, ffn_down[0, 0], frames.astype(low))
    own_length = lax.dynamic_slice_in_dim(lengths, dp * count + sq, 1)
    grid = lengths.reshape(lax.axis_size("dp"), MB, UTTS)
    per_batch = jnp.sum(grid, axis=(0, 2)).astype(jnp.float32)
    frame_count = lax.dynamic_slice_in_dim(per_batch, lax.div(sq, UTTS), 1)[0]
    mask = (jnp.arange(length, dtype=jnp.int32) < own_length[0]).astype(jnp.float32)[:, None]
    table_in = position_table(length, model)

    ctx, probs, x1, qu, qv, key, value, table, small, c_all, w_all, down_1 = front(
        own_length,
        f_all.reshape(length, model),
        w_early,
        cuts_early,
        down_0,
        table_in,
        cotangent.astype(low),
        late,
        ffn_down[0, 1],
    )
    gain, shift = small[0:6], small[6:12]
    kernel_f = small[14 : 14 + taps].T
    up_1, w_attn_out, w_conv_in, w_conv_out = split(w_all, cuts_late)
    x2 = x1 + matmul_low(ctx, w_attn_out)

    a2 = layer_norm(x2, gain[2], shift[2]).astype(low)
    gate = matmul_low(a2, w_conv_in)
    gated = (glu_gate(gate) * mask).astype(low)
    depth = shifted_sum(gated, kernel_f, False)
    sums = jnp.stack([jnp.sum(depth * mask, axis=0), jnp.sum(depth * depth * mask, axis=0)])
    sums = batch_sum(sums, 2)
    mean = sums[0] / frame_count
    var = sums[1] / frame_count - mean * mean
    inv = lax.rsqrt(var + 1e-05)
    normal = (depth - mean) * inv * gain[5] + shift[5]
    active = jax.nn.silu(normal).astype(low)
    x3 = x2 + matmul_low(active, w_conv_out)
    x4, kept_two = ffn_forward(x3, gain[3], shift[3], up_1, down_1)
    mixed = layer_norm(x4, gain[4], shift[4])

    cot = c_all.reshape(length, model).astype(jnp.float32)
    grad, g_gain4, g_shift4 = jax.vjp(layer_norm, x4, gain[4], shift[4])[1](cot)
    grad, (g_gain3, g_shift3, g_up1, g_down1) = ffn_backward(
        grad, kept_two, gain[3], shift[3], up_1, down_1
    )
    grad_b = grad.astype(low)
    g_conv_out = weight_grad(active, grad_b)
    grad_active = matmul_back(grad_b, w_conv_out)
    grad_normal = jax.vjp(jax.nn.silu, normal)[1](grad_active)[0]
    g_gain5 = jnp.sum(grad_normal * ((depth - mean) * inv), axis=0)
    g_shift5 = jnp.sum(grad_normal, axis=0)
    hat = grad_normal * gain[5]
    sums = batch_sum(jnp.stack([jnp.sum(hat, axis=0), jnp.sum(hat * depth, axis=0)]), 3)
    grad_var = -0.5 * inv * inv * inv * (sums[1] - mean * sums[0])
    grad_mean = -inv * sums[0] - 2.0 * mean * grad_var
    grad_depth = (
        hat * inv + mask * (grad_mean / frame_count + 2.0 * depth * grad_var / frame_count)
    ).astype(low)
    grad_gated = shifted_sum(grad_depth, kernel_f, True) * mask
    g_kernel = tap_grads(gated, grad_depth, taps)
    grad_gate = jax.vjp(glu_gate, gate)[1](grad_gated)[0].astype(low)
    g_conv_in = weight_grad(a2, grad_gate)
    grad_ln, g_gain2, g_shift2 = jax.vjp(layer_norm, x2, gain[2], shift[2])[1](
        matmul_back(grad_gate, w_conv_in)
    )
    grad = grad + grad_ln

    grad_b = grad.astype(low)
    g_attn_out = weight_grad(ctx, grad_b)
    grad_ctx = matmul_back(grad_b, w_attn_out).astype(low)
    g_late = jnp.concatenate(
        [member.astype(low) for member in (g_up1, g_attn_out, g_conv_in, g_conv_out)], axis=1
    )
    none = jnp.zeros((2, model), jnp.float32)
    g_small = jnp.concatenate(
        [
            none,
            jnp.stack([g_gain2, g_gain3, g_gain4, g_gain5]),
            none,
            jnp.stack([g_shift2, g_shift3, g_shift4, g_shift5]),
            none,
            g_kernel,
        ]
    )
    g_small = jnp.pad(g_small, ((0, SMALL - g_small.shape[0]), (0, 0)))
    g_early, g_down0, grad, m_all, late_sum, down1_sum = back(
        probs,
        grad_ctx,
        qu,
        qv,
        key,
        value,
        table,
        mixed.astype(low).reshape(frames.shape),
        g_late,
        g_down1.astype(low),
        x1,
        f_all.reshape(length, model),
        grad,
        small,
        g_small,
        w_early,
        cuts_early,
        down_0,
        table_in,
    )
    early_sum, down0_sum, g_all = scatter_all(g_early, g_down0, grad.reshape(frames.shape))
    s_attn_in, s_pos, s_up0, tail = split(early_sum, cuts_early)
    s_up1, s_attn_out, s_conv_in, s_conv_out = split(late_sum, cuts_late)
    rows = tail[:, :14].T
    return (
        m_all.astype(jnp.float32),
        g_all.astype(jnp.float32),
        rows[None, 0:6],
        rows[None, 6:12],
        rows[None, 12:14],
        jnp.stack([s_up0, s_up1])[None],
        jnp.stack([down0_sum, down1_sum])[None],
        s_attn_in[None],
        s_attn_out[None],
        s_pos[None],
        s_conv_in[None],
        tail[None, :, 14 : 14 + taps],
        s_conv_out[None],
    )


def solution(mesh):
    body = local_whole if fits_whole(mesh) else local_general
    in_specs = (
        P("dp", "seq", None),
        P(),
        P("dp", "seq", None),
        P(None, None, ("dp", "seq")),
        P(None, None, ("dp", "seq")),
        P(None, None, ("dp", "seq")),
        P(None, None, ("dp", "seq"), None),
        P(None, None, ("dp", "seq"), None),
        P(None, ("dp", "seq"), None),
        P(None, ("dp", "seq"), None),
        P(None, ("dp", "seq"), None),
        P(None, ("dp", "seq"), None),
        P(None, ("dp", "seq"), None),
        P(None, ("dp", "seq"), None),
    )
    out_specs = (
        P("dp", "seq", None),
        P("dp", "seq", None),
        P(None, None, ("dp", "seq")),
        P(None, None, ("dp", "seq")),
        P(None, None, ("dp", "seq")),
        P(None, None, ("dp", "seq"), None),
        P(None, None, ("dp", "seq"), None),
        P(None, ("dp", "seq"), None),
        P(None, ("dp", "seq"), None),
        P(None, ("dp", "seq"), None),
        P(None, ("dp", "seq"), None),
        P(None, ("dp", "seq"), None),
        P(None, ("dp", "seq"), None),
    )
    return jax.shard_map(body, mesh=mesh, in_specs=in_specs, out_specs=out_specs, check_vma=False)
```

```python
import math

import jax
import jax.numpy as jnp
import numpy as np
from jax import lax
from jax.experimental import pallas as pl
from jax.experimental.pallas import tpu as pltpu
from jax.sharding import PartitionSpec as P

H = 8
DH = 64
NL = 1
MB = 2


HIGHEST_PREC = lax.Precision.HIGHEST


def extended(cells, sides, width):
    for axis, dim in sides:
        count = lax.axis_size(axis)
        ends = count - 1
        head = lax.slice_in_dim(cells, 0, width, axis=dim)
        tail = lax.slice_in_dim(cells, cells.shape[dim] - width, cells.shape[dim], axis=dim)
        cells = jnp.concatenate(
            [
                lax.ppermute(tail, axis, [(i, (i + 1) % count) for i in range(ends)]),
                cells,
                lax.ppermute(head, axis, [((i + 1) % count, i) for i in range(ends)]),
            ],
            axis=dim,
        )
    return cells


def layer_norm(values, gain_row, shift_row):
    centred = values - jnp.mean(values, axis=-1, keepdims=True)
    spread = jnp.mean(centred * centred, axis=-1, keepdims=True)
    return centred * lax.rsqrt(spread + 1e-05) * gain_row + shift_row


def sinusoid(offsets, model_width):
    half_width = model_width // 2
    frequency = jnp.exp(
        jnp.arange(half_width, dtype=jnp.float32) * (-2.0 * math.log(10000.0) / model_width)
    )
    angles = offsets.astype(jnp.float32)[:, None] * frequency[None, :]
    return jnp.concatenate([jnp.sin(angles), jnp.cos(angles)], axis=1)


def skew_rows(raw_pos, key_count):
    row_count = raw_pos.shape[-2]
    col_count = raw_pos.shape[-1]
    lead = raw_pos.shape[:-2]
    flat_rows = raw_pos.reshape(lead + (row_count * col_count,))
    flat_rows = flat_rows[..., row_count - 1 : row_count - 1 + row_count * (col_count - 1)]
    return flat_rows.reshape(lead + (row_count, col_count - 1))[..., :key_count]


def skew_back(grad_skew, raw_shape, key_count):
    zero_raw = jnp.zeros(raw_shape, jnp.float32)
    return jax.vjp(lambda raw_pos: skew_rows(raw_pos, key_count), zero_raw)[1](grad_skew)[0]


def glu_gate(gate_pair):
    half_width = gate_pair.shape[-1] // 2
    return gate_pair[..., :half_width] * jax.nn.sigmoid(gate_pair[..., half_width:])


def matmul_low(left, right):
    return jnp.dot(left, right, preferred_element_type=jnp.float32)


def matmul_back(grad_low, weight):
    return lax.dot_general(
        grad_low, weight, (((1,), (1,)), ((), ())), preferred_element_type=jnp.float32
    )


def weight_grad(inputs_low, grad_low):
    return lax.dot_general(
        inputs_low, grad_low, (((0,), (0,)), ((), ())), preferred_element_type=jnp.float32
    )


def ffn_forward(row_data, gain_row, shift_row, w_up, w_down):
    normed_b = layer_norm(row_data, gain_row, shift_row).astype(jnp.bfloat16)
    hidden = matmul_low(normed_b, w_up)
    active_b = jax.nn.silu(hidden).astype(jnp.bfloat16)
    branch = matmul_low(active_b, w_down)
    return (row_data + 0.5 * branch, (row_data, normed_b, hidden, active_b))


def ffn_backward(grad_rows, kept_data, gain_row, shift_row, w_up, w_down):
    row_data, normed_b, hidden, active_b = kept_data
    grad_out_b = (0.5 * grad_rows).astype(jnp.bfloat16)
    g_down = weight_grad(active_b, grad_out_b)
    grad_active = matmul_back(grad_out_b, w_down)
    grad_hidden_b = jax.vjp(jax.nn.silu, hidden)[1](grad_active)[0].astype(jnp.bfloat16)
    g_up = weight_grad(normed_b, grad_hidden_b)
    grad_normed = matmul_back(grad_hidden_b, w_up)
    grad_ln, g_gain, g_shift = jax.vjp(layer_norm, row_data, gain_row, shift_row)[1](grad_normed)
    return (grad_rows + grad_ln, (g_gain, g_shift, g_up, g_down))


def attention_logits(query_u_b, query_v_b, key_heads, pos_heads, key_valid):
    content = jnp.einsum(
        "ufhd,ulhd->uhfl", query_u_b, key_heads, preferred_element_type=jnp.float32
    )
    raw_pos = jnp.einsum("ufhd,whd->uhfw", query_v_b, pos_heads, preferred_element_type=jnp.float32)
    logits = (content + skew_rows(raw_pos, key_heads.shape[1])) * 0.125
    return jnp.where(key_valid[:, None, None, :], logits, -1e30)


def attn_forward(
    row_data,
    utt_count,
    gain_row,
    shift_row,
    bias_u,
    bias_v,
    w_in,
    w_out,
    w_pos,
    key_valid,
    pos_table_b,
):
    model_width = row_data.shape[1]
    frame_len = row_data.shape[0] // utt_count
    normed_b = layer_norm(row_data, gain_row, shift_row).astype(jnp.bfloat16)
    proj_rows = matmul_low(normed_b, w_in)
    query_rows = proj_rows[:, :model_width].reshape(utt_count, frame_len, H, DH)
    key_b = (
        proj_rows[:, model_width : 2 * model_width]
        .astype(jnp.bfloat16)
        .reshape(utt_count, frame_len, model_width)
    )
    value_b = (
        proj_rows[:, 2 * model_width :]
        .astype(jnp.bfloat16)
        .reshape(utt_count, frame_len, model_width)
    )
    all_keys, all_values = (
        lax.all_gather(key_b, "seq", axis=1, tiled=True),
        lax.all_gather(value_b, "seq", axis=1, tiled=True),
    )
    key_heads = all_keys.reshape(utt_count, -1, H, DH)
    value_heads = all_values.reshape(utt_count, -1, H, DH)
    query_u_b = (query_rows + bias_u.reshape(H, DH)).astype(jnp.bfloat16)
    query_v_b = (query_rows + bias_v.reshape(H, DH)).astype(jnp.bfloat16)
    pos_heads = matmul_low(pos_table_b, w_pos).astype(jnp.bfloat16).reshape(-1, H, DH)
    logits = attention_logits(query_u_b, query_v_b, key_heads, pos_heads, key_valid)
    top_score = jnp.max(logits, axis=-1, keepdims=True)
    exp_scores = jnp.exp(logits - top_score)
    row_total = jnp.sum(exp_scores, axis=-1, keepdims=True)
    prob_b = (exp_scores / row_total).astype(jnp.bfloat16)
    log_total = top_score + jnp.log(row_total)
    context = jnp.einsum("uhfl,ulhd->ufhd", prob_b, value_heads, preferred_element_type=jnp.float32)
    context_b = context.astype(jnp.bfloat16).reshape(-1, model_width)
    branch = matmul_low(context_b, w_out)
    kept_data = (
        row_data,
        normed_b,
        query_u_b,
        query_v_b,
        key_heads,
        value_heads,
        pos_heads,
        log_total,
        context_b,
    )
    return (row_data + branch, kept_data)


def attn_backward(grad_rows, kept_data, gain_row, shift_row, w_in, w_out, key_valid, pos_table_b):
    (
        row_data,
        normed_b,
        query_u_b,
        query_v_b,
        key_heads,
        value_heads,
        pos_heads,
        log_total,
        context_b,
    ) = kept_data
    utt_count = query_u_b.shape[0]
    frame_len = query_u_b.shape[1]
    model_width = row_data.shape[1]
    key_len = key_heads.shape[1]
    grad_out_b = grad_rows.astype(jnp.bfloat16)
    g_out = weight_grad(context_b, grad_out_b)
    grad_context_b = (
        matmul_back(grad_out_b, w_out).astype(jnp.bfloat16).reshape(utt_count, frame_len, H, DH)
    )
    logits = attention_logits(query_u_b, query_v_b, key_heads, pos_heads, key_valid)
    prob_rows = jnp.exp(logits - log_total)
    grad_probs = jnp.einsum(
        "ufhd,ulhd->uhfl", grad_context_b, value_heads, preferred_element_type=jnp.float32
    )
    inner_sum = jnp.sum(grad_probs * prob_rows, axis=-1, keepdims=True)
    grad_logits_b = (prob_rows * (grad_probs - inner_sum)).astype(jnp.bfloat16) * 0.125
    grad_query_u = jnp.einsum(
        "uhfl,ulhd->ufhd", grad_logits_b, key_heads, preferred_element_type=jnp.float32
    )
    raw_shape = (utt_count, H, frame_len, pos_heads.shape[0])
    grad_raw_b = skew_back(grad_logits_b.astype(jnp.float32), raw_shape, key_len).astype(
        jnp.bfloat16
    )
    grad_query_v = jnp.einsum(
        "uhfw,whd->ufhd", grad_raw_b, pos_heads, preferred_element_type=jnp.float32
    )
    grad_pos = jnp.einsum(
        "uhfw,ufhd->whd", grad_raw_b, query_v_b, preferred_element_type=jnp.float32
    )
    grad_pos = grad_pos.reshape(-1, model_width)
    g_pos = lax.dot_general(
        pos_table_b.astype(jnp.float32),
        grad_pos,
        (((0,), (0,)), ((), ())),
        precision=HIGHEST_PREC,
        preferred_element_type=jnp.float32,
    )
    prob_b = prob_rows.astype(jnp.bfloat16)
    grad_values = jnp.einsum(
        "uhfl,ufhd->ulhd", prob_b, grad_context_b, preferred_element_type=jnp.float32
    )
    grad_keys = jnp.einsum(
        "uhfl,ufhd->ulhd", grad_logits_b, query_u_b, preferred_element_type=jnp.float32
    )
    own_keys, own_values = (
        lax.psum_scatter(
            grad_keys.reshape(utt_count, key_len, model_width),
            "seq",
            scatter_dimension=1,
            tiled=True,
        ),
        lax.psum_scatter(
            grad_values.reshape(utt_count, key_len, model_width),
            "seq",
            scatter_dimension=1,
            tiled=True,
        ),
    )
    g_bias_u = jnp.sum(grad_query_u, axis=(0, 1)).reshape(-1)
    g_bias_v = jnp.sum(grad_query_v, axis=(0, 1)).reshape(-1)
    grad_proj_b = jnp.concatenate(
        [
            (grad_query_u + grad_query_v).reshape(-1, model_width),
            own_keys.reshape(-1, model_width),
            own_values.reshape(-1, model_width),
        ],
        axis=1,
    ).astype(jnp.bfloat16)
    g_in = weight_grad(normed_b, grad_proj_b)
    grad_normed = matmul_back(grad_proj_b, w_in)
    grad_ln, g_gain, g_shift = jax.vjp(layer_norm, row_data, gain_row, shift_row)[1](grad_normed)
    return (grad_rows + grad_ln, (g_gain, g_shift, g_bias_u, g_bias_v, g_in, g_out, g_pos))


def conv_forward(
    row_data,
    utt_count,
    gain_row,
    shift_row,
    w_in,
    kernel,
    bn_gain,
    bn_shift,
    w_out,
    frame_mask,
    frame_count,
):
    model_width = row_data.shape[1]
    frame_len = row_data.shape[0] // utt_count
    normed_b = layer_norm(row_data, gain_row, shift_row).astype(jnp.bfloat16)
    gate_pair = matmul_low(normed_b, w_in)
    mask_rows = frame_mask.reshape(-1, 1)
    gated_b = (
        (glu_gate(gate_pair) * mask_rows)
        .astype(jnp.bfloat16)
        .reshape(utt_count, frame_len, model_width)
    )
    halo_reach = (kernel.shape[1] - 1) // 2
    padded = extended(gated_b, (("seq", 1),), halo_reach)
    kernel_f = kernel.astype(jnp.float32)
    depth_out = padded[:, 0:frame_len].astype(jnp.float32) * kernel_f[:, 0]
    for tap_idx in range(1, kernel.shape[1]):
        depth_out = (
            depth_out
            + padded[:, tap_idx : tap_idx + frame_len].astype(jnp.float32) * kernel_f[:, tap_idx]
        )
    weight_mask = frame_mask[:, :, None]
    sum_local = jnp.sum(depth_out * weight_mask, axis=(0, 1))
    square_local = jnp.sum(depth_out * depth_out * weight_mask, axis=(0, 1))
    sum_all, square_all = lax.psum((sum_local, square_local), ("dp", "seq"))
    mean_val = sum_all / frame_count
    variance = square_all / frame_count - mean_val * mean_val
    inv_std = lax.rsqrt(variance + 1e-05)
    normal = (depth_out - mean_val) * inv_std * bn_gain + bn_shift
    active_b = jax.nn.silu(normal).astype(jnp.bfloat16).reshape(-1, model_width)
    branch = matmul_low(active_b, w_out)
    kept_data = (
        row_data,
        normed_b,
        gate_pair,
        padded,
        depth_out,
        mean_val,
        inv_std,
        normal,
        active_b,
    )
    return (row_data + branch, kept_data)


def conv_backward(
    grad_rows, kept_data, gain_row, shift_row, w_in, kernel, bn_gain, w_out, frame_mask, frame_count
):
    row_data, normed_b, gate_pair, padded, depth_out, mean_val, inv_std, normal, active_b = (
        kept_data
    )
    frame_len = depth_out.shape[1]
    model_width = depth_out.shape[2]
    grad_out_b = grad_rows.astype(jnp.bfloat16)
    g_out = weight_grad(active_b, grad_out_b)
    grad_active = matmul_back(grad_out_b, w_out).reshape(depth_out.shape)
    grad_normal = jax.vjp(jax.nn.silu, normal)[1](grad_active)[0]
    centred_hat = (depth_out - mean_val) * inv_std
    g_bn_gain = jnp.sum(grad_normal * centred_hat, axis=(0, 1))
    g_bn_shift = jnp.sum(grad_normal, axis=(0, 1))
    grad_hat = grad_normal * bn_gain
    part_one = jnp.sum(grad_hat, axis=(0, 1))
    part_two = jnp.sum(grad_hat * depth_out, axis=(0, 1))
    part_one, part_two = lax.psum((part_one, part_two), ("dp", "seq"))
    grad_inv = part_two - mean_val * part_one
    grad_var = -0.5 * inv_std * inv_std * inv_std * grad_inv
    grad_mean = -inv_std * part_one - 2.0 * mean_val * grad_var
    weight_mask = frame_mask[:, :, None]
    grad_depth_b = (
        grad_hat * inv_std
        + weight_mask * (grad_mean / frame_count + 2.0 * depth_out * grad_var / frame_count)
    ).astype(jnp.bfloat16)
    halo_reach = (kernel.shape[1] - 1) // 2
    grad_padded = extended(grad_depth_b, (("seq", 1),), halo_reach)
    kernel_f = kernel.astype(jnp.float32)
    grad_depth_f = grad_depth_b.astype(jnp.float32)
    grad_gated = jnp.zeros(depth_out.shape, jnp.float32)
    kernel_cols = []
    for tap_idx in range(kernel.shape[1]):
        begin_at = 2 * halo_reach - tap_idx
        grad_gated = (
            grad_gated
            + grad_padded[:, begin_at : begin_at + frame_len].astype(jnp.float32)
            * kernel_f[:, tap_idx]
        )
        kernel_cols.append(
            jnp.sum(
                padded[:, tap_idx : tap_idx + frame_len].astype(jnp.float32) * grad_depth_f,
                axis=(0, 1),
            )
        )
    g_kernel = jnp.stack(kernel_cols, axis=1)
    grad_gate_b = jax.vjp(glu_gate, gate_pair)[1](
        (grad_gated * weight_mask).reshape(-1, model_width)
    )[0]
    grad_gate_b = grad_gate_b.astype(jnp.bfloat16)
    g_in = weight_grad(normed_b, grad_gate_b)
    grad_normed = matmul_back(grad_gate_b, w_in)
    grad_ln, g_gain, g_shift = jax.vjp(layer_norm, row_data, gain_row, shift_row)[1](grad_normed)
    return (grad_rows + grad_ln, (g_gain, g_shift, g_in, g_kernel, g_bn_gain, g_bn_shift, g_out))


def layer_forward(values, weights, frame_mask, key_valid, frame_count, pos_table_b):
    (
        gain_set,
        shift_set,
        rel_set,
        up_pair,
        down_pair,
        attn_in_w,
        attn_out_w,
        pos_w,
        conv_in_w,
        kernel,
        conv_out_w,
    ) = weights
    gain_f = gain_set.astype(jnp.float32)
    shift_f = shift_set.astype(jnp.float32)
    rel_f = rel_set.astype(jnp.float32)
    utt_count = values.shape[0]
    row_data = values.reshape(-1, values.shape[2])
    row_data, kept_one = ffn_forward(row_data, gain_f[0], shift_f[0], up_pair[0], down_pair[0])
    row_data, kept_attn = attn_forward(
        row_data,
        utt_count,
        gain_f[1],
        shift_f[1],
        rel_f[0],
        rel_f[1],
        attn_in_w,
        attn_out_w,
        pos_w,
        key_valid,
        pos_table_b,
    )
    row_data, kept_conv = conv_forward(
        row_data,
        utt_count,
        gain_f[2],
        shift_f[2],
        conv_in_w,
        kernel,
        gain_f[5],
        shift_f[5],
        conv_out_w,
        frame_mask,
        frame_count,
    )
    row_data, kept_two = ffn_forward(row_data, gain_f[3], shift_f[3], up_pair[1], down_pair[1])
    result = layer_norm(row_data, gain_f[4], shift_f[4])
    return (result.reshape(values.shape), (kept_one, kept_attn, kept_conv, kept_two, row_data))


def layer_backward(
    grad_values, kept_data, weights, frame_mask, key_valid, frame_count, pos_table_b
):
    (
        gain_set,
        shift_set,
        rel_set,
        up_pair,
        down_pair,
        attn_in_w,
        attn_out_w,
        pos_w,
        conv_in_w,
        kernel,
        conv_out_w,
    ) = weights
    gain_f = gain_set.astype(jnp.float32)
    shift_f = shift_set.astype(jnp.float32)
    kept_one, kept_attn, kept_conv, kept_two, last_rows = kept_data
    grad_rows = grad_values.reshape(-1, grad_values.shape[2])
    grad_rows, g_gain_last, g_shift_last = jax.vjp(layer_norm, last_rows, gain_f[4], shift_f[4])[1](
        grad_rows
    )
    grad_rows, two_grads = ffn_backward(
        grad_rows, kept_two, gain_f[3], shift_f[3], up_pair[1], down_pair[1]
    )
    grad_rows, conv_grads = conv_backward(
        grad_rows,
        kept_conv,
        gain_f[2],
        shift_f[2],
        conv_in_w,
        kernel,
        gain_f[5],
        conv_out_w,
        frame_mask,
        frame_count,
    )
    grad_rows, attn_grads = attn_backward(
        grad_rows, kept_attn, gain_f[1], shift_f[1], attn_in_w, attn_out_w, key_valid, pos_table_b
    )
    grad_rows, one_grads = ffn_backward(
        grad_rows, kept_one, gain_f[0], shift_f[0], up_pair[0], down_pair[0]
    )
    grad_gains = jnp.stack(
        [one_grads[0], attn_grads[0], conv_grads[0], two_grads[0], g_gain_last, conv_grads[4]]
    )
    grad_shifts = jnp.stack(
        [one_grads[1], attn_grads[1], conv_grads[1], two_grads[1], g_shift_last, conv_grads[5]]
    )
    grad_rel = jnp.stack([attn_grads[2], attn_grads[3]])
    grad_up = jnp.stack([one_grads[2], two_grads[2]])
    grad_down = jnp.stack([one_grads[3], two_grads[3]])
    layer_grads = (
        grad_gains,
        grad_shifts,
        grad_rel,
        grad_up,
        grad_down,
        attn_grads[4],
        attn_grads[5],
        attn_grads[6],
        conv_grads[2],
        conv_grads[3],
        conv_grads[6],
    )
    return (grad_rows.reshape(grad_values.shape), layer_grads)


def gather_forward(shards, layer_idx):
    pieces = tuple((member[layer_idx] for member in shards))
    return (
        lax.all_gather(pieces[0], ("dp", "seq"), axis=1, tiled=True),
        lax.all_gather(pieces[1], ("dp", "seq"), axis=1, tiled=True),
        lax.all_gather(pieces[2], ("dp", "seq"), axis=1, tiled=True),
        lax.all_gather(pieces[3], ("dp", "seq"), axis=1, tiled=True),
        lax.all_gather(pieces[4], ("dp", "seq"), axis=1, tiled=True),
        lax.all_gather(pieces[5], ("dp", "seq"), axis=0, tiled=True),
        lax.all_gather(pieces[6], ("dp", "seq"), axis=0, tiled=True),
        lax.all_gather(pieces[7], ("dp", "seq"), axis=0, tiled=True),
        lax.all_gather(pieces[8], ("dp", "seq"), axis=0, tiled=True),
        lax.all_gather(pieces[9], ("dp", "seq"), axis=0, tiled=True),
        lax.all_gather(pieces[10], ("dp", "seq"), axis=0, tiled=True),
    )


def gather_backward(shards, layer_idx):
    pieces = tuple((member[layer_idx] for member in shards))
    return (
        lax.all_gather(pieces[0], ("dp", "seq"), axis=1, tiled=True),
        lax.all_gather(pieces[1], ("dp", "seq"), axis=1, tiled=True),
        lax.all_gather(pieces[2], ("dp", "seq"), axis=1, tiled=True),
        lax.all_gather(pieces[3], ("dp", "seq"), axis=1, tiled=True),
        lax.all_gather(pieces[4], ("dp", "seq"), axis=1, tiled=True),
        lax.all_gather(pieces[5], ("dp", "seq"), axis=0, tiled=True),
        lax.all_gather(pieces[6], ("dp", "seq"), axis=0, tiled=True),
        lax.all_gather(pieces[7], ("dp", "seq"), axis=0, tiled=True),
        lax.all_gather(pieces[8], ("dp", "seq"), axis=0, tiled=True),
        lax.all_gather(pieces[9], ("dp", "seq"), axis=0, tiled=True),
        lax.all_gather(pieces[10], ("dp", "seq"), axis=0, tiled=True),
    )


def local_general(
    frames,
    lengths,
    cotangent,
    gains,
    shifts,
    rel_bias,
    ffn_up,
    ffn_down,
    attn_in,
    attn_out,
    pos_proj,
    conv_in,
    depthwise,
    conv_out,
):
    shards = (
        gains,
        shifts,
        rel_bias,
        ffn_up,
        ffn_down,
        attn_in,
        attn_out,
        pos_proj,
        conv_in,
        depthwise,
        conv_out,
    )
    groups = lax.axis_size("dp")
    seq_devices = lax.axis_size("seq")
    local_utts = frames.shape[0]
    frame_len = frames.shape[1]
    model_width = frames.shape[2]
    utt_per = local_utts // MB
    length = frame_len * seq_devices
    seq_start = lax.axis_index("seq") * frame_len
    first_utt = lax.axis_index("dp") * local_utts
    own_lengths = lax.dynamic_slice_in_dim(lengths, first_utt, local_utts)
    lengths_grid = lengths.reshape(groups, MB, utt_per)
    offsets = seq_start + frame_len - 1 - jnp.arange(length + frame_len - 1, dtype=jnp.int32)
    pos_table_b = sinusoid(offsets, model_width).astype(jnp.bfloat16)
    frame_pos = seq_start + jnp.arange(frame_len, dtype=jnp.int32)
    key_pos = jnp.arange(length, dtype=jnp.int32)
    result_list = []
    grad_list = []
    full_sums = [None] * NL
    for micro_idx in range(MB):
        lens_here = own_lengths[micro_idx * utt_per : (micro_idx + 1) * utt_per]
        frame_mask = (frame_pos[None, :] < lens_here[:, None]).astype(jnp.float32)
        key_valid = key_pos[None, :] < lens_here[:, None]
        frame_count = jnp.sum(lengths_grid[:, micro_idx]).astype(jnp.float32)
        values = frames[micro_idx * utt_per : (micro_idx + 1) * utt_per]
        held_weights = []
        layer_idx = 0
        weights = gather_forward(shards, layer_idx)
        values, kept_data = layer_forward(
            values, weights, frame_mask, key_valid, frame_count, pos_table_b
        )
        saved_acts = [kept_data]
        held_weights.append(weights)
        result_list.append(values)
        grad_values = cotangent[micro_idx * utt_per : (micro_idx + 1) * utt_per]
        for layer_idx in reversed(range(NL)):
            weights = gather_backward(shards, layer_idx)
            grad_values, layer_grads = layer_backward(
                grad_values,
                saved_acts[layer_idx],
                weights,
                frame_mask,
                key_valid,
                frame_count,
                pos_table_b,
            )
            if full_sums[layer_idx] is None:
                full_sums[layer_idx] = layer_grads
            else:
                full_sums[layer_idx] = jax.tree.map(jnp.add, full_sums[layer_idx], layer_grads)
        grad_list.append(grad_values)
    stacked = tuple((jnp.stack([full_sums[0][member]]) for member in range(11)))
    final_grads = (
        lax.psum_scatter(stacked[0], ("dp", "seq"), scatter_dimension=2, tiled=True),
        lax.psum_scatter(stacked[1], ("dp", "seq"), scatter_dimension=2, tiled=True),
        lax.psum_scatter(stacked[2], ("dp", "seq"), scatter_dimension=2, tiled=True),
        lax.psum_scatter(stacked[3], ("dp", "seq"), scatter_dimension=2, tiled=True),
        lax.psum_scatter(stacked[4], ("dp", "seq"), scatter_dimension=2, tiled=True),
        lax.psum_scatter(stacked[5], ("dp", "seq"), scatter_dimension=1, tiled=True),
        lax.psum_scatter(stacked[6], ("dp", "seq"), scatter_dimension=1, tiled=True),
        lax.psum_scatter(stacked[7], ("dp", "seq"), scatter_dimension=1, tiled=True),
        lax.psum_scatter(stacked[8], ("dp", "seq"), scatter_dimension=1, tiled=True),
        lax.psum_scatter(stacked[9], ("dp", "seq"), scatter_dimension=1, tiled=True),
        lax.psum_scatter(stacked[10], ("dp", "seq"), scatter_dimension=1, tiled=True),
    )
    mixed = jnp.concatenate(result_list, axis=0)
    grad_frames = jnp.concatenate(grad_list, axis=0)
    return (
        mixed,
        grad_frames,
        final_grads[0],
        final_grads[1],
        final_grads[2],
        final_grads[3],
        final_grads[4],
        final_grads[5],
        final_grads[6],
        final_grads[7],
        final_grads[8],
        final_grads[9],
        final_grads[10],
    )


NT = (((1,), (1,)), ((), ()))
TN = (((0,), (0,)), ((), ()))
NN = (((1,), (0,)), ((), ()))
MESH = pl.DeviceIdType.MESH
UTTS = 4
SMALL = 128
STRIP = 64
VMEM_LIMIT = 60 * 1024 * 1024


def fits_whole(mesh):
    return mesh.shape["dp"] == 4 and mesh.shape["seq"] == MB * UTTS


def dotf(left, right, dims=NN):
    return lax.dot_general(left, right, dims, preferred_element_type=jnp.float32)


def place():
    dp = lax.axis_index("dp")
    sq = lax.axis_index("seq")
    return dp, sq, lax.div(dp, 2), lax.rem(dp, 2), lax.div(sq, 2), lax.rem(sq, 2)


def flip_if(value, bit):
    return 1 - value if bit else value


def partners():
    dp, sq, x, c, z, y = place()
    even = c == 0
    core = (x * 2 + 1 - c, sq)
    xdev = ((1 - x) * 2 + c, sq)
    ydev = (dp, z * 2 + 1 - y)
    first = (jnp.where(even, ydev[0], xdev[0]), jnp.where(even, ydev[1], xdev[1]))
    second = (jnp.where(even, xdev[0], ydev[0]), jnp.where(even, xdev[1], ydev[1]))
    return core, xdev, first, second


def rank_of(color, a, b, k):
    _, _, x, _, z, y = place()
    even = color == 0
    xx = jnp.where(even, x + a * (1 - 2 * x), x + b * (1 - 2 * x))
    yy = jnp.where(even, y + b * (1 - 2 * y), y + a * (1 - 2 * y))
    return xx * 16 + color * 8 + lax.rem(z + k, 4) * 2 + yy


def greet(devices):
    barrier = pltpu.get_barrier_semaphore()
    for device in devices:
        pl.semaphore_signal(barrier, inc=1, device_id=device, device_id_type=MESH)
    pl.semaphore_wait(barrier, len(devices))


def seq_peers(dp, sq, count):
    return [(dp, lax.rem(sq + k, count)) for k in range(1, count)]


def remote(src, dst, send, recv, device):
    return pltpu.make_async_remote_copy(
        src_ref=src, dst_ref=dst, send_sem=send, recv_sem=recv, device_id=device, device_id_type=MESH
    )


def alternate(a, b, k):
    return a * 8 + b * 4 + k


def gather_steps(w_ref, d_ref, w_all, d_all, send, recv, own):
    wr, dr = w_ref.shape[0], d_ref.shape[0]
    started = []

    def blocks(rank):
        return (
            w_all.at[pl.ds(pl.multiple_of(rank * wr, 16), wr), :],
            d_all.at[pl.ds(pl.multiple_of(rank * dr, 16), dr), :],
        )

    def pair(group, target, slot, landing_slot, mine, other):
        dp, sq, _, c, z, y = place()
        core, _, first, second = partners()
        device = {"core": core, "first": first, "second": second}.get(target)
        if device is None:
            device = (dp, lax.rem(z + target, 4) * 2 + y)
        w_dst, d_dst = blocks(rank_of(1 - c if other else c, *group))
        w_src, d_src = (w_ref, d_ref) if mine else (w_dst, d_dst)
        return (
            remote(w_src, w_dst, send.at[0, slot], recv.at[0, landing_slot], device),
            remote(d_src, d_dst, send.at[1, slot], recv.at[1, landing_slot], device),
        )

    def ship(group, target, slot, landing_slot, mine=False):
        spec = (group, target, slot, landing_slot, mine, False)
        for copy in pair(*spec):
            copy.start()
        started.append(spec)

    def arrive(group, other=False):
        for copy in pair(group, "core", 0, alternate(*group) + (16 if other else 0), False, other):
            copy.wait_recv()

    def to_core(group, mine=False):
        spot = 16 + alternate(*group)
        ship(group, "core", spot, spot, mine)

    def own_copies():
        _, _, _, c, _, _ = place()
        w_own, d_own = blocks(rank_of(c, 0, 0, 0))
        return (
            pltpu.make_async_copy(w_ref, w_own, own.at[0]),
            pltpu.make_async_copy(d_ref, d_own, own.at[1]),
        )

    def begin():
        mine = (0, 0, 0)
        ship(mine, "second", 15, 8, mine=True)
        ship(mine, "first", 3, 4, mine=True)
        for k in (1, 3, 2):
            ship(mine, k, k - 1, 4 - k, mine=True)
        to_core(mine, mine=True)
        for copy in own_copies():
            copy.start()

    def along(k):
        group = (0, 0, k)
        arrive(group)
        ship(group, "second", 8 + k - 1, 8 + k)
        ship(group, "first", 4 + k - 1, 4 + k)
        to_core(group)

    def across(k):
        group = (0, 1, k)
        arrive(group)
        ship(group, "second", 11 + k, 12 + k)
        to_core(group)

    def over(k):
        for b in (0, 1):
            group = (1, b, k)
            arrive(group)
            to_core(group)

    def finish():
        for k in (0, 1, 3, 2):
            for a, b in ((0, 0), (0, 1), (1, 0), (1, 1)):
                arrive((a, b, k), other=True)
        for copy in own_copies():
            copy.wait()
        for spec in started:
            for copy in pair(*spec):
                copy.wait_send()

    return begin, along, across, over, finish


def meeting(count):
    dp, sq, *_ = place()
    core, xdev, _, _ = partners()
    greet(seq_peers(dp, sq, count) + [core, xdev])


def tree_scratch():
    return [
        pltpu.SemaphoreType.DMA((2, 32)),
        pltpu.SemaphoreType.DMA((2, 32)),
        pltpu.SemaphoreType.DMA((2,)),
    ]


def gather_kernel(w_ref, d_ref, f_ref, w_all, d_all, f_all, send, recv, own, row_send, row_recv, row_own):
    meeting(f_ref.shape[0])
    begin, along, across, over, finish = gather_steps(w_ref, d_ref, w_all, d_all, send, recv, own)
    begin()
    rows_begin(f_ref, f_all, row_send, row_recv, row_own)
    across(0)
    along(1)
    across(1)
    over(0)
    along(3)
    across(3)
    over(1)
    along(2)
    across(2)
    over(3)
    over(2)
    finish()
    rows_end(f_ref, f_all, row_send, row_recv, row_own)


def gathered(w, d):
    return [
        jax.ShapeDtypeStruct((w.shape[0] * 32, w.shape[1]), w.dtype),
        jax.ShapeDtypeStruct((d.shape[0] * 32, d.shape[1]), d.dtype),
    ]


def gather_all(w, d, f):
    vm = pl.BlockSpec(memory_space=pltpu.VMEM)
    hbm = pl.BlockSpec(memory_space=pl.ANY)
    return pl.pallas_call(
        gather_kernel,
        in_specs=[vm] * 3,
        out_specs=[hbm] * 3,
        out_shape=gathered(w, d) + [jax.ShapeDtypeStruct(f.shape, f.dtype)],
        scratch_shapes=tree_scratch() + row_scratch(f.shape[0]),
        compiler_params=pltpu.CompilerParams(collective_id=0, has_side_effects=True),
        name="gather_all",
    )(w, d, f)


def scatter_steps(w_ref, d_ref, w_out, d_out, bufs, send, recv):
    w0, d0, w1, d1, w2, d2, w3, d3 = bufs
    wr, dr = w_out.shape[0], d_out.shape[0]

    def rows(rank, size):
        return pl.ds(pl.multiple_of(rank * size, 16), size)

    def group_rank(slot, other):
        _, _, _, c, _, _ = place()
        color = 1 - c if other else c
        return rank_of(color, lax.div(slot, 8), lax.rem(lax.div(slot, 4), 2), lax.rem(slot, 4))

    def core_copies(slot):
        core = partners()[0]
        rank = group_rank(slot, True)
        return (
            remote(w_ref.at[rows(rank, wr), :], w0.at[slot], send.at[0, slot], recv.at[0, slot], core),
            remote(d_ref.at[rows(rank, dr), :], d0.at[slot], send.at[1, slot], recv.at[1, slot], core),
        )

    def second_copies(slot):
        to = partners()[3]
        return (
            remote(w0.at[8 + slot], w1.at[slot], send.at[0, 16 + slot], recv.at[0, 16 + slot], to),
            remote(d0.at[8 + slot], d1.at[slot], send.at[1, 16 + slot], recv.at[1, 16 + slot], to),
        )

    def first_copies(slot):
        to = partners()[2]
        return (
            remote(w0.at[4 + slot], w2.at[slot], send.at[0, 24 + slot], recv.at[0, 24 + slot], to),
            remote(d0.at[4 + slot], d2.at[slot], send.at[1, 24 + slot], recv.at[1, 24 + slot], to),
        )

    def z_copies(k):
        dp, _, _, _, z, y = place()
        to = (dp, lax.rem(z + k, 4) * 2 + y)
        return (
            remote(w0.at[k], w3.at[3 - k], send.at[0, 27 + k], recv.at[0, 31 - k], to),
            remote(d0.at[k], d3.at[3 - k], send.at[1, 27 + k], recv.at[1, 31 - k], to),
        )

    def start(copies):
        for copy in copies:
            copy.start()

    def landed(copies):
        for copy in copies:
            copy.wait_recv()

    def sent(copies):
        for copy in copies:
            copy.wait_send()

    def add(slot, w, d):
        f = jnp.float32
        w0[slot] = (w0[slot].astype(f) + w.astype(f)).astype(jnp.bfloat16)
        d0[slot] = (d0[slot].astype(f) + d.astype(f)).astype(jnp.bfloat16)

    def begin():
        @pl.loop(0, 16)
        def _(step):
            start(core_copies(15 - step))

    def take(slot):
        landed(core_copies(slot))
        rank = group_rank(slot, False)
        add(slot, w_ref[rows(rank, wr), :], d_ref[rows(rank, dr), :])

    def far(lo, hi):
        @pl.loop(lo, hi)
        def _(step):
            take(15 - step)
            start(second_copies(7 - step))

    def near(lo, hi):
        @pl.loop(lo, hi)
        def _(step):
            take(7 - step)

    def pass_first(lo, hi):
        @pl.loop(lo, hi)
        def _(step):
            slot = 7 - step
            landed(second_copies(slot))
            add(slot, w1[slot], d1[slot])
            start(first_copies(slot - 4))

    def join_second():
        @pl.loop(0, 3)
        def _(step):
            slot = 3 - step
            landed(second_copies(slot))
            add(slot, w1[slot], d1[slot])

    def pass_along(lo, hi):
        @pl.loop(lo, hi)
        def _(step):
            slot = 3 - step
            landed(first_copies(slot))
            add(slot, w2[slot], d2[slot])
            start(z_copies(slot))

    def total(base, parts):
        value = base.astype(jnp.float32)
        for part in parts:
            value = value + part.astype(jnp.float32)
        return value

    def finish():
        landed(second_copies(0))
        landed(first_copies(0))
        for k in (1, 2, 3):
            landed(z_copies(k))
        w_out[...] = total(w0[0], (w1[0], w2[0], w3[0], w3[1], w3[2]))
        d_out[...] = total(d0[0], (d1[0], d2[0], d3[0], d3[1], d3[2]))

        @pl.loop(0, 16)
        def _(slot):
            sent(core_copies(slot))

        @pl.loop(0, 8)
        def _(slot):
            sent(second_copies(slot))

        @pl.loop(0, 4)
        def _(slot):
            sent(first_copies(slot))

        for k in (1, 2, 3):
            sent(z_copies(k))

    return begin, far, near, pass_first, join_second, pass_along, finish


def scatter_scratch(w, d):
    bf = jnp.bfloat16
    scratch = []
    for n in (16, 8, 4, 3):
        scratch += [
            pltpu.VMEM((n, w.shape[0] // 32, w.shape[1]), bf),
            pltpu.VMEM((n, d.shape[0] // 32, d.shape[1]), bf),
        ]
    return scratch + tree_scratch()[:2]


def scattered(w, d):
    return [
        jax.ShapeDtypeStruct((w.shape[0] // 32, w.shape[1]), jnp.float32),
        jax.ShapeDtypeStruct((d.shape[0] // 32, d.shape[1]), jnp.float32),
    ]


def scatter_kernel(w_ref, d_ref, g_ref, w_out, d_out, g_all, *scratch):
    bufs, (send, recv, row_send, row_recv, row_own) = scratch[:8], scratch[8:]
    meeting(g_ref.shape[0])
    begin, far, near, pass_first, join_second, pass_along, finish = scatter_steps(
        w_ref, d_ref, w_out, d_out, bufs, send, recv
    )
    begin()
    far(0, 8)
    rows_begin(g_ref, g_all, row_send, row_recv, row_own)
    near(0, 4)
    pass_first(0, 4)
    near(4, 8)
    join_second()
    pass_along(0, 3)
    finish()
    rows_end(g_ref, g_all, row_send, row_recv, row_own)


def scatter_all(w, d, g):
    vm = pl.BlockSpec(memory_space=pltpu.VMEM)
    hbm = pl.BlockSpec(memory_space=pl.ANY)
    return pl.pallas_call(
        scatter_kernel,
        in_specs=[vm] * 3,
        out_specs=[vm, vm, hbm],
        out_shape=scattered(w, d) + [jax.ShapeDtypeStruct(g.shape, g.dtype)],
        scratch_shapes=scatter_scratch(w, d) + row_scratch(g.shape[0]),
        compiler_params=pltpu.CompilerParams(
            collective_id=1, has_side_effects=True, vmem_limit_bytes=VMEM_LIMIT
        ),
        name="scatter_all",
    )(w, d, g)


def rows_begin(src, dst, send, recv, own):
    _, sq, *_ = place()
    for k in range(1, dst.shape[0]):
        row_copy(src, dst, send, recv, k).start()
    pltpu.make_async_copy(src.at[sq], dst.at[sq], own).start()


def rows_end(src, dst, send, recv, own):
    dp, sq, *_ = place()
    count = dst.shape[0]
    for k in range(1, count):
        copy = row_copy(src, dst, send, recv, k)
        copy.wait_send()
        landing(src, dst, send, recv, k).wait_recv()
    pltpu.make_async_copy(src.at[sq], dst.at[sq], own).wait()


def row_copy(src, dst, send, recv, k):
    dp, sq, *_ = place()
    count = dst.shape[0]
    to = lax.rem(sq + k, count)
    return remote(src.at[to], dst.at[sq], send.at[k - 1], recv.at[count - 1 - k], (dp, to))


def landing(src, dst, send, recv, k):
    dp, sq, *_ = place()
    origin = lax.rem(sq + k, dst.shape[0])
    return remote(src.at[sq], dst.at[origin], send.at[k - 1], recv.at[k - 1], (dp, origin))


def norm_parts(rows):
    centred = rows - jnp.mean(rows, axis=1, keepdims=True)
    return centred, lax.rsqrt(jnp.mean(centred * centred, axis=1, keepdims=True) + 1e-05)


def norm(rows, gain, shift):
    centred, inv = norm_parts(rows)
    return centred * inv * gain + shift


def silu(h):
    return h * (1.0 / (1.0 + jnp.exp(-h)))


def front_kernel(
    len_ref, f_ref, in_ref, pos_ref, up_ref, small_ref, down_ref, table_ref, c_ref, w_ref, d_ref,
    ctx_ref, p_ref, x1_ref, qu_ref, qv_ref, k_ref, v_ref, t_ref, sm_ref, c_all, w_all, d_all,
    send, recv, own, row_send, row_recv, row_own, *, tq, tile,
):
    low = jnp.bfloat16
    keys, model = f_ref.shape
    span = keys + tq
    steps = keys // tq
    begin, along, across, over, finish = gather_steps(w_ref, d_ref, w_all, d_all, send, recv, own)

    def dense(i):
        rows = pl.ds(pl.multiple_of(i * tile, tile), tile)
        x0 = f_ref[rows, :].astype(jnp.float32)
        a0 = norm(x0, sm_ref[0:1, :], sm_ref[6:7, :]).astype(low)
        z = silu(dotf(a0, up_ref[...])).astype(low)
        x1 = x0 + 0.5 * dotf(z, down_ref[...])
        x1_ref[rows, :] = x1
        a1 = norm(x1, sm_ref[1:2, :], sm_ref[7:8, :]).astype(low)
        query = dotf(a1, in_ref[:, :model])
        qu_ref[rows, :] = (query + sm_ref[12:13, :]).astype(low)
        qv_ref[rows, :] = (query + sm_ref[13:14, :]).astype(low)
        k_ref[rows, :] = dotf(a1, in_ref[:, model : 2 * model]).astype(low)
        v_ref[rows, :] = dotf(a1, in_ref[:, 2 * model :]).astype(low)

    @pl.when(pl.program_id(0) == 0)
    def _():
        meeting(c_ref.shape[0])
        begin()
        rows_begin(c_ref, c_all, row_send, row_recv, row_own)
        sm_ref[...] = small_ref[...].astype(jnp.float32).T

        @pl.loop(0, 2 * keys // tile)
        def _(i):
            rows = pl.ds(pl.multiple_of(i * tile, tile), tile)
            t_ref[rows, :] = dotf(table_ref[rows, :], pos_ref[...]).astype(low)

        @pl.loop(0, keys // tile)
        def _(i):
            dense(i)

            @pl.when(i == 0)
            def _():
                across(0)
                along(1)

            @pl.when(i == 1)
            def _():
                along(3)
                across(1)

            @pl.when(i == 2)
            def _():
                along(2)

    plan = {1: ((across, 3), (over, 0)), 3: ((across, 2),), 5: ((over, 1),), 8: ((over, 3),), 11: ((over, 2),)}
    dp, sq, *_ = place()
    valid = lax.broadcasted_iota(jnp.int32, (1, keys), 1) < len_ref[dp * (MB * UTTS) + sq]
    base = pl.program_id(0) * 128

    @pl.loop(0, steps)
    def _(i):
        time = pl.program_id(0) * steps + i
        for at, todo in plan.items():

            @pl.when(time == at)
            def _():
                for step, k in todo:
                    step(k)

        rows = pl.ds(pl.multiple_of(i * tq, tq), tq)
        band = pl.ds(pl.multiple_of(keys - tq - i * tq, tq), span)
        pair = pl.ds(pl.multiple_of(base, 128), 128)
        qu, qv, k, v, t = qu_ref[rows, pair], qv_ref[rows, pair], k_ref[:, pair], v_ref[:, pair], t_ref[band, pair]
        for h in range(2):
            cols = slice(h * DH, (h + 1) * DH)
            content = dotf(qu[:, cols], k[:, cols], NT)
            raw = dotf(qv[:, cols], t[:, cols], NT)
            pos = pltpu.roll(raw, keys + 1, 1, stride=1, stride_axis=0)[:, :keys]
            s = jnp.where(valid, (content + pos) * 0.125, -1e30)
            e = jnp.exp(s - jnp.max(s, axis=1, keepdims=True))
            p = (e * (1.0 / jnp.sum(e, axis=1, keepdims=True))).astype(low)
            p_ref[h, rows, :] = p
            ctx_ref[rows, cols] = dotf(p, v[:, cols]).astype(low)

    @pl.when(pl.program_id(0) == pl.num_programs(0) - 1)
    def _():
        finish()
        rows_end(c_ref, c_all, row_send, row_recv, row_own)


def row_scratch(count):
    return [
        pltpu.SemaphoreType.DMA((count - 1,)),
        pltpu.SemaphoreType.DMA((count - 1,)),
        pltpu.SemaphoreType.DMA,
    ]


def front(length, f, w_early, cuts, down, table_in, cot, w, d, tq=256, tile=256):
    rows, model = f.shape
    low = jnp.bfloat16
    vm = pl.BlockSpec(memory_space=pltpu.VMEM)
    hbm = pl.BlockSpec(memory_space=pl.ANY)

    def window(lo, hi):
        return pl.BlockSpec((w_early.shape[0], hi - lo), lambda h, *_: (0, lo // (hi - lo)), pipeline_mode=pl.Buffered(1))

    one = jax.ShapeDtypeStruct((rows, model), low)
    return pl.pallas_call(
        lambda *refs: front_kernel(*refs, tq=tq, tile=tile),
        grid_spec=pltpu.PrefetchScalarGridSpec(
            num_scalar_prefetch=1,
            grid=(model // 128,),
            in_specs=[vm] + [window(lo, hi) for lo, hi in zip(cuts[:-1], cuts[1:])] + [vm] * 5,
            out_specs=[
                pl.BlockSpec((rows, 128), lambda h, *_: (0, h)),
                pl.BlockSpec((2, rows, rows), lambda h, *_: (h, 0, 0)),
            ]
            + [vm] * 7
            + [hbm] * 3,
            scratch_shapes=tree_scratch() + row_scratch(cot.shape[0]),
        ),
        out_shape=[
            one,
            jax.ShapeDtypeStruct((model // DH, rows, rows), low),
            jax.ShapeDtypeStruct((rows, model), jnp.float32),
            one,
            one,
            one,
            one,
            jax.ShapeDtypeStruct((2 * rows, model), low),
            jax.ShapeDtypeStruct((SMALL, model), jnp.float32),
            jax.ShapeDtypeStruct(cot.shape, cot.dtype),
        ]
        + gathered(w, d),
        compiler_params=pltpu.CompilerParams(
            collective_id=4, has_side_effects=True, vmem_limit_bytes=VMEM_LIMIT
        ),
        name="front",
    )(length, f, *[w_early] * (len(cuts) - 1), down, table_in, cot, w, d)


def norm_back(rows, gain, grad):
    centred, inv = norm_parts(rows)
    hat = centred * inv
    scaled = grad * gain
    inner = jnp.mean(scaled * hat, axis=1, keepdims=True)
    out = inv * (scaled - jnp.mean(scaled, axis=1, keepdims=True) - hat * inner)
    return out, hat, jnp.sum(grad * hat, axis=0, keepdims=True)


def back_kernel(
    p_ref, g_ref, qu_ref, qv_ref, k_ref, v_ref, t_ref,
    m_ref, w_ref, d_ref, x1_ref, f_ref, grad_ref, sm_ref, gs_ref, in_ref, up_ref, down_ref, table_ref,
    ge_ref, gd_ref, rows_ref, m_all, w_out, d_out,
    ds_sc, dt_sc, dproj_sc, dtab_sc, z_sc, dh_sc, a0_sc, a1_sc, go_sc, gs_sc, *scratch, tq, tile,
):
    bufs, (send, recv, row_send, row_recv, row_own) = scratch[:8], scratch[8:]
    begin, far, near, pass_first, join_second, pass_along, finish = scatter_steps(
        w_ref, d_ref, w_out, d_out, bufs, send, recv
    )
    low = jnp.bfloat16
    keys = k_ref.shape[0]
    model = f_ref.shape[1]
    span = keys + tq
    steps = keys // tq

    def open_up():
        meeting(m_ref.shape[0])
        begin()
        gs_sc[...] = gs_ref[...]

    def rows_away():
        near(4, 8)
        rows_begin(m_ref, m_all, row_send, row_recv, row_own)

    plan = {
        0: open_up,
        1: lambda: far(0, 4),
        2: lambda: far(4, 8),
        3: lambda: near(0, 4),
        4: rows_away,
        5: lambda: pass_first(0, 2),
        6: lambda: pass_first(2, 4),
        9: join_second,
        10: lambda: pass_along(0, 2),
        11: lambda: pass_along(2, 3),
    }
    flip = (
        lax.broadcasted_iota(jnp.int32, (tq, tq), 0) + lax.broadcasted_iota(jnp.int32, (tq, tq), 1) == tq - 1
    ).astype(low)
    pad = jnp.zeros((tq, tq), jnp.float32)
    dt_sc[...] = jnp.zeros_like(dt_sc)
    base = pl.program_id(0) * 128

    def at(offset):
        return pl.ds(pl.multiple_of(base + offset, 128), 128)

    @pl.loop(0, steps)
    def _(i):
        time = pl.program_id(0) * steps + i
        for moment, step in plan.items():
            pl.when(time == moment)(step)
        rows = pl.ds(pl.multiple_of(i * tq, tq), tq)
        band = pl.ds(pl.multiple_of(keys - tq - i * tq, tq), span)
        sides = []
        for h in range(2):
            cols = slice(h * DH, (h + 1) * DH)
            dp = dotf(g_ref[rows, cols], v_ref[:, cols], NT)
            pf = p_ref[h, rows, :].astype(jnp.float32)
            ds = (pf * (dp - jnp.sum(dp * pf, axis=1, keepdims=True))).astype(low)
            ds_sc[h, rows, :] = ds
            dqu = dotf(ds, k_ref[:, cols]) * 0.125
            turned = jnp.concatenate([dotf(flip, ds), pad], axis=1)
            raw = pltpu.roll(turned, 0, 1, stride=1, stride_axis=0).astype(low)
            dqv = dotf(flip, dotf(raw, t_ref[band, cols]).astype(low)) * 0.125
            qv = dotf(flip, qv_ref[rows, cols]).astype(low)
            dt_sc[h, band, :] += dotf(raw, qv, TN)
            sides.append((dqu, dqv))
        dqu, dqv = (jnp.concatenate(both, axis=1) for both in zip(*sides))
        gs_sc[12:13, at(0)] += jnp.sum(dqu, axis=0, keepdims=True)
        gs_sc[13:14, at(0)] += jnp.sum(dqv, axis=0, keepdims=True)
        dproj_sc[rows, at(0)] = (dqu + dqv).astype(low)

    halves = []
    for h in range(2):
        cols = slice(h * DH, (h + 1) * DH)
        halves.append(
            (
                dt_sc[h] * 0.125,
                dotf(ds_sc[h], qu_ref[:, cols], TN) * 0.125,
                dotf(p_ref[h], g_ref[:, cols], TN),
            )
        )
    dtab, dk, dv = (jnp.concatenate(both, axis=1).astype(low) for both in zip(*halves))
    dtab_sc[:, at(0)] = dtab
    dproj_sc[:, at(model)] = dk
    dproj_sc[:, at(2 * model)] = dv

    @pl.when(pl.program_id(0) == pl.num_programs(0) - 1)
    def _():
        @pl.loop(0, keys // tile)
        def _(i):
            rows = pl.ds(pl.multiple_of(i * tile, tile), tile)
            dn = dotf(dproj_sc[rows, :], in_ref[...], NT)
            dx, hat, dgain = norm_back(x1_ref[rows, :], sm_ref[1:2, :], dn)
            gs_sc[1:2, :] += dgain
            gs_sc[7:8, :] += jnp.sum(dn, axis=0, keepdims=True)
            a1_sc[rows, :] = (hat * sm_ref[1:2, :] + sm_ref[7:8, :]).astype(low)
            grad = grad_ref[rows, :] + dx
            go = (0.5 * grad).astype(low)
            go_sc[rows, :] = go
            x0 = f_ref[rows, :].astype(jnp.float32)
            a0 = norm(x0, sm_ref[0:1, :], sm_ref[6:7, :]).astype(low)
            a0_sc[rows, :] = a0
            h = dotf(a0, up_ref[...])
            sig = 1.0 / (1.0 + jnp.exp(-h))
            z_sc[rows, :] = (h * sig).astype(low)
            dh = (dotf(go, down_ref[...], NT) * (sig * (1.0 + h * (1.0 - sig)))).astype(low)
            dh_sc[rows, :] = dh
            dn = dotf(dh, up_ref[...], NT)
            dx, _, dgain = norm_back(x0, sm_ref[0:1, :], dn)
            gs_sc[0:1, :] += dgain
            gs_sc[6:7, :] += jnp.sum(dn, axis=0, keepdims=True)
            rows_ref[rows, :] = (grad + dx).astype(low)

        width = model

        @pl.loop(0, 3)
        def _(j):
            cols = pl.ds(pl.multiple_of(j * width, width), width)
            ge_ref[:, cols] = dotf(a1_sc[...], dproj_sc[:, cols], TN).astype(low)

        ge_ref[:, 3 * width : 4 * width] = dotf(table_ref[...], dtab_sc[...], TN).astype(low)

        @pl.loop(0, 4)
        def _(j):
            cols = pl.ds(pl.multiple_of(j * width, width), width)
            ge_ref[:, pl.ds(pl.multiple_of((j + 4) * width, width), width)] = dotf(
                a0_sc[...], dh_sc[:, cols], TN
            ).astype(low)
            gd_ref[cols, :] = dotf(z_sc[:, cols], go_sc[...], TN).astype(low)

        ge_ref[:, 8 * width :] = gs_sc[...].T.astype(low)
        finish()
        rows_end(m_ref, m_all, row_send, row_recv, row_own)


def back(
    p, g, qu, qv, k, v, table, mixed, w, d, x1, f, grad, small, g_small, w_early, cuts, down, table_in, tq=256, tile=256
):
    rows, model = qu.shape
    low = jnp.bfloat16
    vm = pl.BlockSpec(memory_space=pltpu.VMEM)
    blk = pl.BlockSpec((rows, 128), lambda h: (0, h))
    tab = pl.BlockSpec((2 * rows, 128), lambda h: (0, h))

    def window(j):
        lo, hi = cuts[j], cuts[j + 1]
        return pl.BlockSpec((w_early.shape[0], hi - lo), lambda h: (0, lo // (hi - lo)), pipeline_mode=pl.Buffered(1))

    hidden = down.shape[0]
    return pl.pallas_call(
        lambda *refs: back_kernel(*refs, tq=tq, tile=tile),
        grid=(model // 128,),
        in_specs=[pl.BlockSpec((2, rows, rows), lambda h: (h, 0, 0))]
        + [blk] * 5
        + [tab]
        + [vm] * 8
        + [window(0), window(2), vm, vm],
        out_specs=[vm] * 3 + [pl.BlockSpec(memory_space=pl.ANY), vm, vm],
        out_shape=[
            jax.ShapeDtypeStruct(w_early.shape, low),
            jax.ShapeDtypeStruct(down.shape, low),
            jax.ShapeDtypeStruct((rows, model), low),
            jax.ShapeDtypeStruct(mixed.shape, mixed.dtype),
        ]
        + scattered(w, d),
        scratch_shapes=[
            pltpu.VMEM((2, rows, rows), low),
            pltpu.VMEM((2, 2 * rows, DH), jnp.float32),
            pltpu.VMEM((rows, 3 * model), low),
            pltpu.VMEM((2 * rows, model), low),
            pltpu.VMEM((rows, hidden), low),
            pltpu.VMEM((rows, hidden), low),
            pltpu.VMEM((rows, model), low),
            pltpu.VMEM((rows, model), low),
            pltpu.VMEM((rows, model), low),
            pltpu.VMEM((SMALL, model), jnp.float32),
        ]
        + scatter_scratch(w, d)
        + row_scratch(mixed.shape[0]),
        compiler_params=pltpu.CompilerParams(
            collective_id=5, has_side_effects=True, vmem_limit_bytes=63 * 1024 * 1024
        ),
        name="back",
    )(p, g, qu, qv, k, v, table, mixed, w, d, x1, f, grad, small, g_small, w_early, w_early, down, table_in)


def sigmoid(h):
    return 1.0 / (1.0 + jnp.exp(-h))


def middle_kernel(
    len_ref, ctx_ref, x1_ref, w_ref, down_ref, cot_ref, sm_ref,
    mixed_ref, grad_ref, gctx_ref, gw_ref, gd_ref, gs_ref,
    x2_sc, a2_sc, gate_sc, gl_sc, dep_sc, act_sc, a3_sc, z_sc, dh_sc, go_sc, gob_sc, e_sc, dd_sc, tap_sc, win_sc,
    part_sc, peer_sc, send, recv, *, tile, taps,
):
    low = jnp.bfloat16
    f32 = jnp.float32
    length, model = x1_ref.shape
    hidden = down_ref.shape[0]
    reach = (taps - 1) // 2
    edge = gl_sc.shape[0] - length
    half = edge // 2
    dp, sq, *_ = place()
    batch = lax.div(sq, UTTS)
    me = dp * UTTS + lax.rem(sq, UTTS)
    size = peer_sc.shape[1]
    valid = len_ref[dp * (MB * UTTS) + sq]
    frames = jnp.int32(0)
    for group in range(4):
        for u in range(UTTS):
            frames = frames + len_ref[group * (MB * UTTS) + batch * UTTS + u]
    per = 1.0 / jnp.full((1, model), frames, jnp.int32).astype(f32)
    up_w = w_ref.at[:, :hidden]
    out_w = w_ref.at[:, hidden : hidden + model]
    gate_w = w_ref.at[:, hidden + model : hidden + 3 * model]
    conv_w = w_ref.at[:, hidden + 3 * model :]

    def peer(j):
        r = lax.rem(me + j, size)
        return (lax.div(r, UTTS), batch * UTTS + lax.rem(r, UTTS))

    barrier = pltpu.get_barrier_semaphore()
    for j in range(1, size):
        pl.semaphore_signal(barrier, inc=1, device_id=peer(j), device_id_type=MESH)

    def give(which, j):
        return remote(
            part_sc.at[which], peer_sc.at[which, me], send.at[which, j - 1], recv.at[which, size - 1 - j], peer(j)
        )

    def give_all(which):
        for j in range(1, size):
            give(which, j).start()
        peer_sc[which, me] = part_sc[which]

    def take_all(which):
        for j in range(1, size):
            remote(
                part_sc.at[which],
                peer_sc.at[which, lax.rem(me + j, size)],
                send.at[which, j - 1],
                recv.at[which, j - 1],
                peer(j),
            ).wait_recv()
        for j in range(1, size):
            give(which, j).wait_send()
        return jnp.sum(peer_sc[which], axis=0)

    def row_of(i):
        return pl.ds(pl.multiple_of(i * tile, tile), tile)

    def inner_of(i):
        return pl.ds(pl.multiple_of(i * tile + half, 8), tile)

    def mask_of(i):
        return (lax.broadcasted_iota(jnp.int32, (tile, 1), 0) + i * tile < valid).astype(f32)

    def total(rows):
        return jnp.sum(rows, axis=0, keepdims=True)

    def row(r):
        return sm_ref[r : r + 1, :]

    gs_ref[...] = jnp.zeros_like(gs_ref)
    part_sc[...] = jnp.zeros_like(part_sc)
    for pad_sc in (gl_sc, dd_sc):
        pad_sc[:half, :] = jnp.zeros((half, model), f32)
        pad_sc[half + length :, :] = jnp.zeros((half, model), f32)

    tiles = length // tile

    @pl.loop(0, tiles)
    def _(i):
        rows = row_of(i)
        x2 = x1_ref[rows, :] + dotf(ctx_ref[rows, :], out_w[...])
        x2_sc[rows, :] = x2
        a2 = norm(x2, row(2), row(8)).astype(low)
        a2_sc[rows, :] = a2
        gate = dotf(a2, gate_w[...])
        gate_sc[rows, :] = gate
        gl = (gate[:, :model] * sigmoid(gate[:, model:]) * mask_of(i)).astype(low)
        gl_sc[inner_of(i), :] = gl.astype(f32)

    strip = STRIP

    def depthwise(src, lanes, base, backward):
        win_sc[...] = src[pl.ds(base, strip + edge), lanes]
        acc = jnp.zeros((strip, 128), f32)
        for k in range(taps):
            shift = half + (reach - k if backward else k - reach)
            acc = acc + win_sc[shift : shift + strip, :] * sm_ref[14 + k : 15 + k, lanes]
        return acc

    for c in range(model // 128):
        lanes = slice(c * 128, (c + 1) * 128)

        @pl.loop(0, length // strip)
        def _(i):
            base = pl.multiple_of(i * strip, strip)
            dep = depthwise(gl_sc, lanes, base, False)
            dep_sc[pl.ds(base, strip), lanes] = dep
            mask = (lax.broadcasted_iota(jnp.int32, (strip, 1), 0) + base < valid).astype(f32)
            kept = dep * mask
            part_sc[0, 0:1, lanes] += total(kept)
            part_sc[0, 1:2, lanes] += total(kept * dep)

    pl.semaphore_wait(barrier, size - 1)
    give_all(0)
    sums = take_all(0)
    mean = sums[0:1] * per
    inv = lax.rsqrt(sums[1:2] * per - mean * mean + 1e-05)

    @pl.loop(0, tiles)
    def _(i):
        rows = row_of(i)
        dep = dep_sc[rows, :]
        hatn = (dep - mean) * inv
        normal = hatn * row(5) + row(11)
        sgn = sigmoid(normal)
        act = (normal * sgn).astype(low)
        act_sc[rows, :] = act
        x3 = x2_sc[rows, :] + dotf(act, conv_w[...])
        a3 = norm(x3, row(3), row(9)).astype(low)
        a3_sc[rows, :] = a3
        h = dotf(a3, up_w[...])
        sig = sigmoid(h)
        z = (h * sig).astype(low)
        z_sc[rows, :] = z
        x4 = x3 + 0.5 * dotf(z, down_ref[...])
        mixed_ref[rows, :] = norm(x4, row(4), row(10)).astype(low)
        cot = cot_ref[rows, :].astype(f32)
        grad, _, dgain = norm_back(x4, row(4), cot)
        gs_ref[4:5, :] += dgain
        gs_ref[10:11, :] += total(cot)
        go = (0.5 * grad).astype(low)
        go_sc[rows, :] = go
        dh = (dotf(go, down_ref[...], NT) * (sig * (1.0 + h * (1.0 - sig)))).astype(low)
        dh_sc[rows, :] = dh
        dn = dotf(dh, up_w[...], NT)
        dx, _, dgain = norm_back(x3, row(3), dn)
        gs_ref[3:4, :] += dgain
        gs_ref[9:10, :] += total(dn)
        grad = grad + dx
        grad_ref[rows, :] = grad
        gob = grad.astype(low)
        gob_sc[rows, :] = gob
        dnormal = dotf(gob, conv_w[...], NT) * (sgn * (1.0 + normal * (1.0 - sgn)))
        gs_ref[5:6, :] += total(dnormal * hatn)
        gs_ref[11:12, :] += total(dnormal)
        e = dnormal * row(5)
        e_sc[rows, :] = e
        part_sc[1, 0:1, :] += total(e)
        part_sc[1, 1:2, :] += total(e * dep)

    give_all(1)

    @pl.loop(0, hidden // model)
    def _(j):
        cols = pl.ds(pl.multiple_of(j * model, model), model)
        gw_ref[:, cols] = dotf(a3_sc[...], dh_sc[:, cols], TN).astype(low)
        gd_ref[cols, :] = dotf(z_sc[:, cols], go_sc[...], TN).astype(low)

    gw_ref[:, hidden + 3 * model :] = dotf(act_sc[...], gob_sc[...], TN).astype(low)
    sums = take_all(1)
    dvar = -0.5 * inv * inv * inv * (sums[1:2] - mean * sums[0:1])
    dmean = -inv * sums[0:1] - 2.0 * mean * dvar

    @pl.loop(0, tiles)
    def _(i):
        rows = row_of(i)
        dd = e_sc[rows, :] * inv + mask_of(i) * (dmean * per + 2.0 * dep_sc[rows, :] * dvar * per)
        dd_sc[inner_of(i), :] = dd.astype(low).astype(f32)

    for c in range(model // 128):
        lanes = slice(c * 128, (c + 1) * 128)
        tap_sc[...] = jnp.zeros_like(tap_sc)

        @pl.loop(0, length // strip)
        def _(i):
            base = pl.multiple_of(i * strip, strip)
            e_sc[pl.ds(base, strip), lanes] = depthwise(dd_sc, lanes, base, True)
            dd = dd_sc[pl.ds(pl.multiple_of(base + half, 8), strip), lanes]
            win_sc[...] = gl_sc[pl.ds(base, strip + edge), lanes]
            for k in range(taps):
                prod = win_sc[half + k - reach : half + k - reach + strip, :] * dd
                tap_sc[k] += jnp.sum(prod.reshape(strip // 8, 8, 128), axis=0)

        gs_ref[14 : 14 + taps, lanes] = jnp.sum(tap_sc[...], axis=1)

    @pl.loop(0, tiles)
    def _(i):
        rows = row_of(i)
        dgl = e_sc[rows, :] * mask_of(i)
        ga = gate_sc[rows, :model]
        sb = sigmoid(gate_sc[rows, model:])
        dgate = jnp.concatenate([dgl * sb, dgl * ga * sb * (1.0 - sb)], axis=1).astype(low)
        dh_sc[rows, : 2 * model] = dgate
        dn = dotf(dgate, gate_w[...], NT)
        dx, _, dgain = norm_back(x2_sc[rows, :], row(2), dn)
        gs_ref[2:3, :] += dgain
        gs_ref[8:9, :] += total(dn)
        grad = grad_ref[rows, :] + dx
        grad_ref[rows, :] = grad
        gob = grad.astype(low)
        gob_sc[rows, :] = gob
        gctx_ref[rows, :] = dotf(gob, out_w[...], NT).astype(low)

    gw_ref[:, hidden + model : hidden + 3 * model] = dotf(a2_sc[...], dh_sc[:, : 2 * model], TN).astype(low)
    gw_ref[:, hidden : hidden + model] = dotf(ctx_ref[...], gob_sc[...], TN).astype(low)


def middle(lengths, ctx, x1, w, down, cot, small, taps, tile=256):
    rows, model = x1.shape
    hidden = down.shape[0]
    low = jnp.bfloat16
    f32 = jnp.float32
    vm = pl.BlockSpec(memory_space=pltpu.VMEM)
    size = 4 * UTTS
    half = -(-(taps - 1) // 2 // 8) * 8
    wide = pltpu.VMEM((rows, model), f32)
    thin = pltpu.VMEM((rows, model), low)
    padded = pltpu.VMEM((rows + 2 * half, model), f32)
    return pl.pallas_call(
        lambda *refs: middle_kernel(*refs, tile=tile, taps=taps),
        in_specs=[pl.BlockSpec(memory_space=pltpu.SMEM)] + [vm] * 6,
        out_specs=[vm] * 6,
        out_shape=[
            jax.ShapeDtypeStruct((rows, model), low),
            jax.ShapeDtypeStruct((rows, model), f32),
            jax.ShapeDtypeStruct((rows, model), low),
            jax.ShapeDtypeStruct(w.shape, low),
            jax.ShapeDtypeStruct(down.shape, low),
            jax.ShapeDtypeStruct((SMALL, model), f32),
        ],
        scratch_shapes=[
            wide,
            thin,
            pltpu.VMEM((rows, 2 * model), f32),
            padded,
            wide,
            thin,
            thin,
            pltpu.VMEM((rows, hidden), low),
            pltpu.VMEM((rows, hidden), low),
            thin,
            thin,
            wide,
            padded,
            pltpu.VMEM((taps, 8, 128), f32),
            pltpu.VMEM((STRIP + 2 * half, 128), f32),
            pltpu.VMEM((2, 2, model), f32),
            pltpu.VMEM((2, size, 2, model), f32),
            pltpu.SemaphoreType.DMA((2, size - 1)),
            pltpu.SemaphoreType.DMA((2, size - 1)),
        ],
        compiler_params=pltpu.CompilerParams(
            collective_id=2, has_side_effects=True, vmem_limit_bytes=63 * 1024 * 1024
        ),
        name="middle",
    )(lengths, ctx, x1, w, down, cot, small)


def position_table(length, width):
    offsets = (length - 1 - np.arange(2 * length)).astype(np.float32)
    half = width // 2
    steps = np.arange(half, dtype=np.float32) * np.float32(-2.0 * math.log(10000.0) / width)
    angles = (offsets[:, None] * np.exp(steps)[None, :]).astype(np.float64)
    table = np.concatenate([np.sin(angles), np.cos(angles)], axis=1)
    return jnp.asarray(table.astype(np.float32)).astype(jnp.bfloat16)


def columns(*members):
    return [0] + [int(v) for v in np.cumsum([member.shape[1] for member in members])]


def split(values, cuts):
    return [values[:, lo:hi] for lo, hi in zip(cuts[:-1], cuts[1:])]


def local_whole(
    frames,
    lengths,
    cotangent,
    gains,
    shifts,
    rel_bias,
    ffn_up,
    ffn_down,
    attn_in,
    attn_out,
    pos_proj,
    conv_in,
    depthwise,
    conv_out,
):
    low = jnp.bfloat16
    _, width_rows, model = frames.shape
    length = width_rows * lax.axis_size("seq")
    taps = depthwise.shape[2]
    small = jnp.concatenate([gains[0], shifts[0], rel_bias[0]], axis=0).T
    small = jnp.concatenate([small, depthwise[0]], axis=1)
    small = jnp.pad(small, ((0, 0), (0, SMALL - small.shape[1])))
    early = jnp.concatenate([attn_in[0], pos_proj[0], ffn_up[0, 0], small], axis=1)
    late = jnp.concatenate([ffn_up[0, 1], attn_out[0], conv_in[0], conv_out[0]], axis=1)
    cuts_early = columns(attn_in[0], pos_proj[0], ffn_up[0, 0], small)
    cuts_late = columns(ffn_up[0, 1], attn_out[0], conv_in[0], conv_out[0])
    w_early, down_0, f_all = gather_all(early, ffn_down[0, 0], frames.astype(low))
    table_in = position_table(length, model)

    ctx, probs, x1, qu, qv, key, value, table, small, c_all, w_late, down_1 = front(
        lengths,
        f_all.reshape(length, model),
        w_early,
        cuts_early,
        down_0,
        table_in,
        cotangent.astype(low),
        late,
        ffn_down[0, 1],
    )
    mixed, grad, grad_ctx, g_late, g_down1, g_small = middle(
        lengths, ctx, x1, w_late, down_1, c_all.reshape(length, model), small, taps
    )
    g_early, g_down0, grad, m_all, late_sum, down1_sum = back(
        probs,
        grad_ctx,
        qu,
        qv,
        key,
        value,
        table,
        mixed.reshape(frames.shape),
        g_late,
        g_down1,
        x1,
        f_all.reshape(length, model),
        grad,
        small,
        g_small,
        w_early,
        cuts_early,
        down_0,
        table_in,
    )
    early_sum, down0_sum, g_all = scatter_all(g_early, g_down0, grad.reshape(frames.shape))
    s_attn_in, s_pos, s_up0, tail = split(early_sum, cuts_early)
    s_up1, s_attn_out, s_conv_in, s_conv_out = split(late_sum, cuts_late)
    rows = tail[:, :14].T
    return (
        m_all.astype(jnp.float32),
        g_all.astype(jnp.float32),
        rows[None, 0:6],
        rows[None, 6:12],
        rows[None, 12:14],
        jnp.stack([s_up0, s_up1])[None],
        jnp.stack([down0_sum, down1_sum])[None],
        s_attn_in[None],
        s_attn_out[None],
        s_pos[None],
        s_conv_in[None],
        tail[None, :, 14 : 14 + taps],
        s_conv_out[None],
    )


def solution(mesh):
    body = local_whole if fits_whole(mesh) else local_general
    in_specs = (
        P("dp", "seq", None),
        P(),
        P("dp", "seq", None),
        P(None, None, ("dp", "seq")),
        P(None, None, ("dp", "seq")),
        P(None, None, ("dp", "seq")),
        P(None, None, ("dp", "seq"), None),
        P(None, None, ("dp", "seq"), None),
        P(None, ("dp", "seq"), None),
        P(None, ("dp", "seq"), None),
        P(None, ("dp", "seq"), None),
        P(None, ("dp", "seq"), None),
        P(None, ("dp", "seq"), None),
        P(None, ("dp", "seq"), None),
    )
    out_specs = (
        P("dp", "seq", None),
        P("dp", "seq", None),
        P(None, None, ("dp", "seq")),
        P(None, None, ("dp", "seq")),
        P(None, None, ("dp", "seq")),
        P(None, None, ("dp", "seq"), None),
        P(None, None, ("dp", "seq"), None),
        P(None, ("dp", "seq"), None),
        P(None, ("dp", "seq"), None),
        P(None, ("dp", "seq"), None),
        P(None, ("dp", "seq"), None),
        P(None, ("dp", "seq"), None),
        P(None, ("dp", "seq"), None),
    )
    return jax.shard_map(body, mesh=mesh, in_specs=in_specs, out_specs=out_specs, check_vma=False)
```

```python
import math

import jax
import jax.numpy as jnp
import numpy as np
from jax import lax
from jax.experimental import pallas as pl
from jax.experimental.pallas import tpu as pltpu
from jax.sharding import PartitionSpec as P

H = 8
DH = 64
NL = 1
MB = 2


HIGHEST_PREC = lax.Precision.HIGHEST


def extended(cells, sides, width):
    for axis, dim in sides:
        count = lax.axis_size(axis)
        ends = count - 1
        head = lax.slice_in_dim(cells, 0, width, axis=dim)
        tail = lax.slice_in_dim(cells, cells.shape[dim] - width, cells.shape[dim], axis=dim)
        cells = jnp.concatenate(
            [
                lax.ppermute(tail, axis, [(i, (i + 1) % count) for i in range(ends)]),
                cells,
                lax.ppermute(head, axis, [((i + 1) % count, i) for i in range(ends)]),
            ],
            axis=dim,
        )
    return cells


def layer_norm(values, gain_row, shift_row):
    centred = values - jnp.mean(values, axis=-1, keepdims=True)
    spread = jnp.mean(centred * centred, axis=-1, keepdims=True)
    return centred * lax.rsqrt(spread + 1e-05) * gain_row + shift_row


def sinusoid(offsets, model_width):
    half_width = model_width // 2
    frequency = jnp.exp(
        jnp.arange(half_width, dtype=jnp.float32) * (-2.0 * math.log(10000.0) / model_width)
    )
    angles = offsets.astype(jnp.float32)[:, None] * frequency[None, :]
    return jnp.concatenate([jnp.sin(angles), jnp.cos(angles)], axis=1)


def skew_rows(raw_pos, key_count):
    row_count = raw_pos.shape[-2]
    col_count = raw_pos.shape[-1]
    lead = raw_pos.shape[:-2]
    flat_rows = raw_pos.reshape(lead + (row_count * col_count,))
    flat_rows = flat_rows[..., row_count - 1 : row_count - 1 + row_count * (col_count - 1)]
    return flat_rows.reshape(lead + (row_count, col_count - 1))[..., :key_count]


def skew_back(grad_skew, raw_shape, key_count):
    zero_raw = jnp.zeros(raw_shape, jnp.float32)
    return jax.vjp(lambda raw_pos: skew_rows(raw_pos, key_count), zero_raw)[1](grad_skew)[0]


def glu_gate(gate_pair):
    half_width = gate_pair.shape[-1] // 2
    return gate_pair[..., :half_width] * jax.nn.sigmoid(gate_pair[..., half_width:])


def matmul_low(left, right):
    return jnp.dot(left, right, preferred_element_type=jnp.float32)


def matmul_back(grad_low, weight):
    return lax.dot_general(
        grad_low, weight, (((1,), (1,)), ((), ())), preferred_element_type=jnp.float32
    )


def weight_grad(inputs_low, grad_low):
    return lax.dot_general(
        inputs_low, grad_low, (((0,), (0,)), ((), ())), preferred_element_type=jnp.float32
    )


def ffn_forward(row_data, gain_row, shift_row, w_up, w_down):
    normed_b = layer_norm(row_data, gain_row, shift_row).astype(jnp.bfloat16)
    hidden = matmul_low(normed_b, w_up)
    active_b = jax.nn.silu(hidden).astype(jnp.bfloat16)
    branch = matmul_low(active_b, w_down)
    return (row_data + 0.5 * branch, (row_data, normed_b, hidden, active_b))


def ffn_backward(grad_rows, kept_data, gain_row, shift_row, w_up, w_down):
    row_data, normed_b, hidden, active_b = kept_data
    grad_out_b = (0.5 * grad_rows).astype(jnp.bfloat16)
    g_down = weight_grad(active_b, grad_out_b)
    grad_active = matmul_back(grad_out_b, w_down)
    grad_hidden_b = jax.vjp(jax.nn.silu, hidden)[1](grad_active)[0].astype(jnp.bfloat16)
    g_up = weight_grad(normed_b, grad_hidden_b)
    grad_normed = matmul_back(grad_hidden_b, w_up)
    grad_ln, g_gain, g_shift = jax.vjp(layer_norm, row_data, gain_row, shift_row)[1](grad_normed)
    return (grad_rows + grad_ln, (g_gain, g_shift, g_up, g_down))


def attention_logits(query_u_b, query_v_b, key_heads, pos_heads, key_valid):
    content = jnp.einsum(
        "ufhd,ulhd->uhfl", query_u_b, key_heads, preferred_element_type=jnp.float32
    )
    raw_pos = jnp.einsum("ufhd,whd->uhfw", query_v_b, pos_heads, preferred_element_type=jnp.float32)
    logits = (content + skew_rows(raw_pos, key_heads.shape[1])) * 0.125
    return jnp.where(key_valid[:, None, None, :], logits, -1e30)


def attn_forward(
    row_data,
    utt_count,
    gain_row,
    shift_row,
    bias_u,
    bias_v,
    w_in,
    w_out,
    w_pos,
    key_valid,
    pos_table_b,
):
    model_width = row_data.shape[1]
    frame_len = row_data.shape[0] // utt_count
    normed_b = layer_norm(row_data, gain_row, shift_row).astype(jnp.bfloat16)
    proj_rows = matmul_low(normed_b, w_in)
    query_rows = proj_rows[:, :model_width].reshape(utt_count, frame_len, H, DH)
    key_b = (
        proj_rows[:, model_width : 2 * model_width]
        .astype(jnp.bfloat16)
        .reshape(utt_count, frame_len, model_width)
    )
    value_b = (
        proj_rows[:, 2 * model_width :]
        .astype(jnp.bfloat16)
        .reshape(utt_count, frame_len, model_width)
    )
    all_keys, all_values = (
        lax.all_gather(key_b, "seq", axis=1, tiled=True),
        lax.all_gather(value_b, "seq", axis=1, tiled=True),
    )
    key_heads = all_keys.reshape(utt_count, -1, H, DH)
    value_heads = all_values.reshape(utt_count, -1, H, DH)
    query_u_b = (query_rows + bias_u.reshape(H, DH)).astype(jnp.bfloat16)
    query_v_b = (query_rows + bias_v.reshape(H, DH)).astype(jnp.bfloat16)
    pos_heads = matmul_low(pos_table_b, w_pos).astype(jnp.bfloat16).reshape(-1, H, DH)
    logits = attention_logits(query_u_b, query_v_b, key_heads, pos_heads, key_valid)
    top_score = jnp.max(logits, axis=-1, keepdims=True)
    exp_scores = jnp.exp(logits - top_score)
    row_total = jnp.sum(exp_scores, axis=-1, keepdims=True)
    prob_b = (exp_scores / row_total).astype(jnp.bfloat16)
    log_total = top_score + jnp.log(row_total)
    context = jnp.einsum("uhfl,ulhd->ufhd", prob_b, value_heads, preferred_element_type=jnp.float32)
    context_b = context.astype(jnp.bfloat16).reshape(-1, model_width)
    branch = matmul_low(context_b, w_out)
    kept_data = (
        row_data,
        normed_b,
        query_u_b,
        query_v_b,
        key_heads,
        value_heads,
        pos_heads,
        log_total,
        context_b,
    )
    return (row_data + branch, kept_data)


def attn_backward(grad_rows, kept_data, gain_row, shift_row, w_in, w_out, key_valid, pos_table_b):
    (
        row_data,
        normed_b,
        query_u_b,
        query_v_b,
        key_heads,
        value_heads,
        pos_heads,
        log_total,
        context_b,
    ) = kept_data
    utt_count = query_u_b.shape[0]
    frame_len = query_u_b.shape[1]
    model_width = row_data.shape[1]
    key_len = key_heads.shape[1]
    grad_out_b = grad_rows.astype(jnp.bfloat16)
    g_out = weight_grad(context_b, grad_out_b)
    grad_context_b = (
        matmul_back(grad_out_b, w_out).astype(jnp.bfloat16).reshape(utt_count, frame_len, H, DH)
    )
    logits = attention_logits(query_u_b, query_v_b, key_heads, pos_heads, key_valid)
    prob_rows = jnp.exp(logits - log_total)
    grad_probs = jnp.einsum(
        "ufhd,ulhd->uhfl", grad_context_b, value_heads, preferred_element_type=jnp.float32
    )
    inner_sum = jnp.sum(grad_probs * prob_rows, axis=-1, keepdims=True)
    grad_logits_b = (prob_rows * (grad_probs - inner_sum)).astype(jnp.bfloat16) * 0.125
    grad_query_u = jnp.einsum(
        "uhfl,ulhd->ufhd", grad_logits_b, key_heads, preferred_element_type=jnp.float32
    )
    raw_shape = (utt_count, H, frame_len, pos_heads.shape[0])
    grad_raw_b = skew_back(grad_logits_b.astype(jnp.float32), raw_shape, key_len).astype(
        jnp.bfloat16
    )
    grad_query_v = jnp.einsum(
        "uhfw,whd->ufhd", grad_raw_b, pos_heads, preferred_element_type=jnp.float32
    )
    grad_pos = jnp.einsum(
        "uhfw,ufhd->whd", grad_raw_b, query_v_b, preferred_element_type=jnp.float32
    )
    grad_pos = grad_pos.reshape(-1, model_width)
    g_pos = lax.dot_general(
        pos_table_b.astype(jnp.float32),
        grad_pos,
        (((0,), (0,)), ((), ())),
        precision=HIGHEST_PREC,
        preferred_element_type=jnp.float32,
    )
    prob_b = prob_rows.astype(jnp.bfloat16)
    grad_values = jnp.einsum(
        "uhfl,ufhd->ulhd", prob_b, grad_context_b, preferred_element_type=jnp.float32
    )
    grad_keys = jnp.einsum(
        "uhfl,ufhd->ulhd", grad_logits_b, query_u_b, preferred_element_type=jnp.float32
    )
    own_keys, own_values = (
        lax.psum_scatter(
            grad_keys.reshape(utt_count, key_len, model_width),
            "seq",
            scatter_dimension=1,
            tiled=True,
        ),
        lax.psum_scatter(
            grad_values.reshape(utt_count, key_len, model_width),
            "seq",
            scatter_dimension=1,
            tiled=True,
        ),
    )
    g_bias_u = jnp.sum(grad_query_u, axis=(0, 1)).reshape(-1)
    g_bias_v = jnp.sum(grad_query_v, axis=(0, 1)).reshape(-1)
    grad_proj_b = jnp.concatenate(
        [
            (grad_query_u + grad_query_v).reshape(-1, model_width),
            own_keys.reshape(-1, model_width),
            own_values.reshape(-1, model_width),
        ],
        axis=1,
    ).astype(jnp.bfloat16)
    g_in = weight_grad(normed_b, grad_proj_b)
    grad_normed = matmul_back(grad_proj_b, w_in)
    grad_ln, g_gain, g_shift = jax.vjp(layer_norm, row_data, gain_row, shift_row)[1](grad_normed)
    return (grad_rows + grad_ln, (g_gain, g_shift, g_bias_u, g_bias_v, g_in, g_out, g_pos))


def conv_forward(
    row_data,
    utt_count,
    gain_row,
    shift_row,
    w_in,
    kernel,
    bn_gain,
    bn_shift,
    w_out,
    frame_mask,
    frame_count,
):
    model_width = row_data.shape[1]
    frame_len = row_data.shape[0] // utt_count
    normed_b = layer_norm(row_data, gain_row, shift_row).astype(jnp.bfloat16)
    gate_pair = matmul_low(normed_b, w_in)
    mask_rows = frame_mask.reshape(-1, 1)
    gated_b = (
        (glu_gate(gate_pair) * mask_rows)
        .astype(jnp.bfloat16)
        .reshape(utt_count, frame_len, model_width)
    )
    halo_reach = (kernel.shape[1] - 1) // 2
    padded = extended(gated_b, (("seq", 1),), halo_reach)
    kernel_f = kernel.astype(jnp.float32)
    depth_out = padded[:, 0:frame_len].astype(jnp.float32) * kernel_f[:, 0]
    for tap_idx in range(1, kernel.shape[1]):
        depth_out = (
            depth_out
            + padded[:, tap_idx : tap_idx + frame_len].astype(jnp.float32) * kernel_f[:, tap_idx]
        )
    weight_mask = frame_mask[:, :, None]
    sum_local = jnp.sum(depth_out * weight_mask, axis=(0, 1))
    square_local = jnp.sum(depth_out * depth_out * weight_mask, axis=(0, 1))
    sum_all, square_all = lax.psum((sum_local, square_local), ("dp", "seq"))
    mean_val = sum_all / frame_count
    variance = square_all / frame_count - mean_val * mean_val
    inv_std = lax.rsqrt(variance + 1e-05)
    normal = (depth_out - mean_val) * inv_std * bn_gain + bn_shift
    active_b = jax.nn.silu(normal).astype(jnp.bfloat16).reshape(-1, model_width)
    branch = matmul_low(active_b, w_out)
    kept_data = (
        row_data,
        normed_b,
        gate_pair,
        padded,
        depth_out,
        mean_val,
        inv_std,
        normal,
        active_b,
    )
    return (row_data + branch, kept_data)


def conv_backward(
    grad_rows, kept_data, gain_row, shift_row, w_in, kernel, bn_gain, w_out, frame_mask, frame_count
):
    row_data, normed_b, gate_pair, padded, depth_out, mean_val, inv_std, normal, active_b = (
        kept_data
    )
    frame_len = depth_out.shape[1]
    model_width = depth_out.shape[2]
    grad_out_b = grad_rows.astype(jnp.bfloat16)
    g_out = weight_grad(active_b, grad_out_b)
    grad_active = matmul_back(grad_out_b, w_out).reshape(depth_out.shape)
    grad_normal = jax.vjp(jax.nn.silu, normal)[1](grad_active)[0]
    centred_hat = (depth_out - mean_val) * inv_std
    g_bn_gain = jnp.sum(grad_normal * centred_hat, axis=(0, 1))
    g_bn_shift = jnp.sum(grad_normal, axis=(0, 1))
    grad_hat = grad_normal * bn_gain
    part_one = jnp.sum(grad_hat, axis=(0, 1))
    part_two = jnp.sum(grad_hat * depth_out, axis=(0, 1))
    part_one, part_two = lax.psum((part_one, part_two), ("dp", "seq"))
    grad_inv = part_two - mean_val * part_one
    grad_var = -0.5 * inv_std * inv_std * inv_std * grad_inv
    grad_mean = -inv_std * part_one - 2.0 * mean_val * grad_var
    weight_mask = frame_mask[:, :, None]
    grad_depth_b = (
        grad_hat * inv_std
        + weight_mask * (grad_mean / frame_count + 2.0 * depth_out * grad_var / frame_count)
    ).astype(jnp.bfloat16)
    halo_reach = (kernel.shape[1] - 1) // 2
    grad_padded = extended(grad_depth_b, (("seq", 1),), halo_reach)
    kernel_f = kernel.astype(jnp.float32)
    grad_depth_f = grad_depth_b.astype(jnp.float32)
    grad_gated = jnp.zeros(depth_out.shape, jnp.float32)
    kernel_cols = []
    for tap_idx in range(kernel.shape[1]):
        begin_at = 2 * halo_reach - tap_idx
        grad_gated = (
            grad_gated
            + grad_padded[:, begin_at : begin_at + frame_len].astype(jnp.float32)
            * kernel_f[:, tap_idx]
        )
        kernel_cols.append(
            jnp.sum(
                padded[:, tap_idx : tap_idx + frame_len].astype(jnp.float32) * grad_depth_f,
                axis=(0, 1),
            )
        )
    g_kernel = jnp.stack(kernel_cols, axis=1)
    grad_gate_b = jax.vjp(glu_gate, gate_pair)[1](
        (grad_gated * weight_mask).reshape(-1, model_width)
    )[0]
    grad_gate_b = grad_gate_b.astype(jnp.bfloat16)
    g_in = weight_grad(normed_b, grad_gate_b)
    grad_normed = matmul_back(grad_gate_b, w_in)
    grad_ln, g_gain, g_shift = jax.vjp(layer_norm, row_data, gain_row, shift_row)[1](grad_normed)
    return (grad_rows + grad_ln, (g_gain, g_shift, g_in, g_kernel, g_bn_gain, g_bn_shift, g_out))


def layer_forward(values, weights, frame_mask, key_valid, frame_count, pos_table_b):
    (
        gain_set,
        shift_set,
        rel_set,
        up_pair,
        down_pair,
        attn_in_w,
        attn_out_w,
        pos_w,
        conv_in_w,
        kernel,
        conv_out_w,
    ) = weights
    gain_f = gain_set.astype(jnp.float32)
    shift_f = shift_set.astype(jnp.float32)
    rel_f = rel_set.astype(jnp.float32)
    utt_count = values.shape[0]
    row_data = values.reshape(-1, values.shape[2])
    row_data, kept_one = ffn_forward(row_data, gain_f[0], shift_f[0], up_pair[0], down_pair[0])
    row_data, kept_attn = attn_forward(
        row_data,
        utt_count,
        gain_f[1],
        shift_f[1],
        rel_f[0],
        rel_f[1],
        attn_in_w,
        attn_out_w,
        pos_w,
        key_valid,
        pos_table_b,
    )
    row_data, kept_conv = conv_forward(
        row_data,
        utt_count,
        gain_f[2],
        shift_f[2],
        conv_in_w,
        kernel,
        gain_f[5],
        shift_f[5],
        conv_out_w,
        frame_mask,
        frame_count,
    )
    row_data, kept_two = ffn_forward(row_data, gain_f[3], shift_f[3], up_pair[1], down_pair[1])
    result = layer_norm(row_data, gain_f[4], shift_f[4])
    return (result.reshape(values.shape), (kept_one, kept_attn, kept_conv, kept_two, row_data))


def layer_backward(
    grad_values, kept_data, weights, frame_mask, key_valid, frame_count, pos_table_b
):
    (
        gain_set,
        shift_set,
        rel_set,
        up_pair,
        down_pair,
        attn_in_w,
        attn_out_w,
        pos_w,
        conv_in_w,
        kernel,
        conv_out_w,
    ) = weights
    gain_f = gain_set.astype(jnp.float32)
    shift_f = shift_set.astype(jnp.float32)
    kept_one, kept_attn, kept_conv, kept_two, last_rows = kept_data
    grad_rows = grad_values.reshape(-1, grad_values.shape[2])
    grad_rows, g_gain_last, g_shift_last = jax.vjp(layer_norm, last_rows, gain_f[4], shift_f[4])[1](
        grad_rows
    )
    grad_rows, two_grads = ffn_backward(
        grad_rows, kept_two, gain_f[3], shift_f[3], up_pair[1], down_pair[1]
    )
    grad_rows, conv_grads = conv_backward(
        grad_rows,
        kept_conv,
        gain_f[2],
        shift_f[2],
        conv_in_w,
        kernel,
        gain_f[5],
        conv_out_w,
        frame_mask,
        frame_count,
    )
    grad_rows, attn_grads = attn_backward(
        grad_rows, kept_attn, gain_f[1], shift_f[1], attn_in_w, attn_out_w, key_valid, pos_table_b
    )
    grad_rows, one_grads = ffn_backward(
        grad_rows, kept_one, gain_f[0], shift_f[0], up_pair[0], down_pair[0]
    )
    grad_gains = jnp.stack(
        [one_grads[0], attn_grads[0], conv_grads[0], two_grads[0], g_gain_last, conv_grads[4]]
    )
    grad_shifts = jnp.stack(
        [one_grads[1], attn_grads[1], conv_grads[1], two_grads[1], g_shift_last, conv_grads[5]]
    )
    grad_rel = jnp.stack([attn_grads[2], attn_grads[3]])
    grad_up = jnp.stack([one_grads[2], two_grads[2]])
    grad_down = jnp.stack([one_grads[3], two_grads[3]])
    layer_grads = (
        grad_gains,
        grad_shifts,
        grad_rel,
        grad_up,
        grad_down,
        attn_grads[4],
        attn_grads[5],
        attn_grads[6],
        conv_grads[2],
        conv_grads[3],
        conv_grads[6],
    )
    return (grad_rows.reshape(grad_values.shape), layer_grads)


def gather_forward(shards, layer_idx):
    pieces = tuple((member[layer_idx] for member in shards))
    return (
        lax.all_gather(pieces[0], ("dp", "seq"), axis=1, tiled=True),
        lax.all_gather(pieces[1], ("dp", "seq"), axis=1, tiled=True),
        lax.all_gather(pieces[2], ("dp", "seq"), axis=1, tiled=True),
        lax.all_gather(pieces[3], ("dp", "seq"), axis=1, tiled=True),
        lax.all_gather(pieces[4], ("dp", "seq"), axis=1, tiled=True),
        lax.all_gather(pieces[5], ("dp", "seq"), axis=0, tiled=True),
        lax.all_gather(pieces[6], ("dp", "seq"), axis=0, tiled=True),
        lax.all_gather(pieces[7], ("dp", "seq"), axis=0, tiled=True),
        lax.all_gather(pieces[8], ("dp", "seq"), axis=0, tiled=True),
        lax.all_gather(pieces[9], ("dp", "seq"), axis=0, tiled=True),
        lax.all_gather(pieces[10], ("dp", "seq"), axis=0, tiled=True),
    )


def gather_backward(shards, layer_idx):
    pieces = tuple((member[layer_idx] for member in shards))
    return (
        lax.all_gather(pieces[0], ("dp", "seq"), axis=1, tiled=True),
        lax.all_gather(pieces[1], ("dp", "seq"), axis=1, tiled=True),
        lax.all_gather(pieces[2], ("dp", "seq"), axis=1, tiled=True),
        lax.all_gather(pieces[3], ("dp", "seq"), axis=1, tiled=True),
        lax.all_gather(pieces[4], ("dp", "seq"), axis=1, tiled=True),
        lax.all_gather(pieces[5], ("dp", "seq"), axis=0, tiled=True),
        lax.all_gather(pieces[6], ("dp", "seq"), axis=0, tiled=True),
        lax.all_gather(pieces[7], ("dp", "seq"), axis=0, tiled=True),
        lax.all_gather(pieces[8], ("dp", "seq"), axis=0, tiled=True),
        lax.all_gather(pieces[9], ("dp", "seq"), axis=0, tiled=True),
        lax.all_gather(pieces[10], ("dp", "seq"), axis=0, tiled=True),
    )


def local_general(
    frames,
    lengths,
    cotangent,
    gains,
    shifts,
    rel_bias,
    ffn_up,
    ffn_down,
    attn_in,
    attn_out,
    pos_proj,
    conv_in,
    depthwise,
    conv_out,
):
    shards = (
        gains,
        shifts,
        rel_bias,
        ffn_up,
        ffn_down,
        attn_in,
        attn_out,
        pos_proj,
        conv_in,
        depthwise,
        conv_out,
    )
    groups = lax.axis_size("dp")
    seq_devices = lax.axis_size("seq")
    local_utts = frames.shape[0]
    frame_len = frames.shape[1]
    model_width = frames.shape[2]
    utt_per = local_utts // MB
    length = frame_len * seq_devices
    seq_start = lax.axis_index("seq") * frame_len
    first_utt = lax.axis_index("dp") * local_utts
    own_lengths = lax.dynamic_slice_in_dim(lengths, first_utt, local_utts)
    lengths_grid = lengths.reshape(groups, MB, utt_per)
    offsets = seq_start + frame_len - 1 - jnp.arange(length + frame_len - 1, dtype=jnp.int32)
    pos_table_b = sinusoid(offsets, model_width).astype(jnp.bfloat16)
    frame_pos = seq_start + jnp.arange(frame_len, dtype=jnp.int32)
    key_pos = jnp.arange(length, dtype=jnp.int32)
    result_list = []
    grad_list = []
    full_sums = [None] * NL
    for micro_idx in range(MB):
        lens_here = own_lengths[micro_idx * utt_per : (micro_idx + 1) * utt_per]
        frame_mask = (frame_pos[None, :] < lens_here[:, None]).astype(jnp.float32)
        key_valid = key_pos[None, :] < lens_here[:, None]
        frame_count = jnp.sum(lengths_grid[:, micro_idx]).astype(jnp.float32)
        values = frames[micro_idx * utt_per : (micro_idx + 1) * utt_per]
        held_weights = []
        layer_idx = 0
        weights = gather_forward(shards, layer_idx)
        values, kept_data = layer_forward(
            values, weights, frame_mask, key_valid, frame_count, pos_table_b
        )
        saved_acts = [kept_data]
        held_weights.append(weights)
        result_list.append(values)
        grad_values = cotangent[micro_idx * utt_per : (micro_idx + 1) * utt_per]
        for layer_idx in reversed(range(NL)):
            weights = gather_backward(shards, layer_idx)
            grad_values, layer_grads = layer_backward(
                grad_values,
                saved_acts[layer_idx],
                weights,
                frame_mask,
                key_valid,
                frame_count,
                pos_table_b,
            )
            if full_sums[layer_idx] is None:
                full_sums[layer_idx] = layer_grads
            else:
                full_sums[layer_idx] = jax.tree.map(jnp.add, full_sums[layer_idx], layer_grads)
        grad_list.append(grad_values)
    stacked = tuple((jnp.stack([full_sums[0][member]]) for member in range(11)))
    final_grads = (
        lax.psum_scatter(stacked[0], ("dp", "seq"), scatter_dimension=2, tiled=True),
        lax.psum_scatter(stacked[1], ("dp", "seq"), scatter_dimension=2, tiled=True),
        lax.psum_scatter(stacked[2], ("dp", "seq"), scatter_dimension=2, tiled=True),
        lax.psum_scatter(stacked[3], ("dp", "seq"), scatter_dimension=2, tiled=True),
        lax.psum_scatter(stacked[4], ("dp", "seq"), scatter_dimension=2, tiled=True),
        lax.psum_scatter(stacked[5], ("dp", "seq"), scatter_dimension=1, tiled=True),
        lax.psum_scatter(stacked[6], ("dp", "seq"), scatter_dimension=1, tiled=True),
        lax.psum_scatter(stacked[7], ("dp", "seq"), scatter_dimension=1, tiled=True),
        lax.psum_scatter(stacked[8], ("dp", "seq"), scatter_dimension=1, tiled=True),
        lax.psum_scatter(stacked[9], ("dp", "seq"), scatter_dimension=1, tiled=True),
        lax.psum_scatter(stacked[10], ("dp", "seq"), scatter_dimension=1, tiled=True),
    )
    mixed = jnp.concatenate(result_list, axis=0)
    grad_frames = jnp.concatenate(grad_list, axis=0)
    return (
        mixed,
        grad_frames,
        final_grads[0],
        final_grads[1],
        final_grads[2],
        final_grads[3],
        final_grads[4],
        final_grads[5],
        final_grads[6],
        final_grads[7],
        final_grads[8],
        final_grads[9],
        final_grads[10],
    )


NT = (((1,), (1,)), ((), ()))
TN = (((0,), (0,)), ((), ()))
NN = (((1,), (0,)), ((), ()))
MESH = pl.DeviceIdType.MESH
UTTS = 4
SMALL = 128
STRIP = 64
VMEM_LIMIT = 60 * 1024 * 1024


def fits_whole(mesh):
    return mesh.shape["dp"] == 4 and mesh.shape["seq"] == MB * UTTS


def dotf(left, right, dims=NN):
    return lax.dot_general(left, right, dims, preferred_element_type=jnp.float32)


def place():
    dp = lax.axis_index("dp")
    sq = lax.axis_index("seq")
    return dp, sq, lax.div(dp, 2), lax.rem(dp, 2), lax.div(sq, 2), lax.rem(sq, 2)


def flip_if(value, bit):
    return 1 - value if bit else value


def partners():
    dp, sq, x, c, z, y = place()
    even = c == 0
    core = (x * 2 + 1 - c, sq)
    xdev = ((1 - x) * 2 + c, sq)
    ydev = (dp, z * 2 + 1 - y)
    first = (jnp.where(even, ydev[0], xdev[0]), jnp.where(even, ydev[1], xdev[1]))
    second = (jnp.where(even, xdev[0], ydev[0]), jnp.where(even, xdev[1], ydev[1]))
    return core, xdev, first, second, ydev


def rank_of(color, a, b, k, fixed=False):
    _, _, x, _, z, y = place()
    even = jnp.logical_or(color == 0, fixed)
    xx = jnp.where(even, x + a * (1 - 2 * x), x + b * (1 - 2 * x))
    yy = jnp.where(even, y + b * (1 - 2 * y), y + a * (1 - 2 * y))
    return xx * 16 + color * 8 + lax.rem(z + k, 4) * 2 + yy


def greet(devices):
    barrier = pltpu.get_barrier_semaphore()
    for device in devices:
        pl.semaphore_signal(barrier, inc=1, device_id=device, device_id_type=MESH)
    pl.semaphore_wait(barrier, len(devices))


def seq_peers(dp, sq, count):
    return [(dp, lax.rem(sq + k, count)) for k in range(1, count)]


def remote(src, dst, send, recv, device):
    return pltpu.make_async_remote_copy(
        src_ref=src, dst_ref=dst, send_sem=send, recv_sem=recv, device_id=device, device_id_type=MESH
    )


def alternate(a, b, k):
    return a * 8 + b * 4 + k


def gather_steps(w_ref, d_ref, w_all, d_all, send, recv, own):
    wr, dr = w_ref.shape[0], d_ref.shape[0]
    started = []

    def blocks(w_rank, d_rank):
        return (
            w_all.at[pl.ds(pl.multiple_of(w_rank * wr, 16), wr), :],
            d_all.at[pl.ds(pl.multiple_of(d_rank * dr, 16), dr), :],
        )

    def pair(group, target, slot, landing_slot, mine, other):
        dp, sq, _, c, z, y = place()
        core, xdev, first, second, ydev = partners()
        along_z = (dp, lax.rem(z + target, 4) * 2 + y) if isinstance(target, int) else None
        w_to = {"core": core, "first": first, "second": second}.get(target, along_z)
        d_to = {"core": core, "first": ydev, "second": xdev}.get(target, along_z)
        color = 1 - c if other else c
        w_dst, d_dst = blocks(rank_of(color, *group), rank_of(color, *group, fixed=True))
        w_src, d_src = (w_ref, d_ref) if mine else (w_dst, d_dst)
        return (
            remote(w_src, w_dst, send.at[0, slot], recv.at[0, landing_slot], w_to),
            remote(d_src, d_dst, send.at[1, slot], recv.at[1, landing_slot], d_to),
        )

    def ship(group, target, slot, landing_slot, mine=False):
        spec = (group, target, slot, landing_slot, mine, False)
        for copy in pair(*spec):
            copy.start()
        started.append(spec)

    def arrive(group, other=False):
        for copy in pair(group, "core", 0, alternate(*group) + (16 if other else 0), False, other):
            copy.wait_recv()

    def to_core(group, mine=False):
        spot = 16 + alternate(*group)
        ship(group, "core", spot, spot, mine)

    def own_copies():
        _, _, _, c, _, _ = place()
        mine = rank_of(c, 0, 0, 0)
        w_own, d_own = blocks(mine, mine)
        return (
            pltpu.make_async_copy(w_ref, w_own, own.at[0]),
            pltpu.make_async_copy(d_ref, d_own, own.at[1]),
        )

    def begin():
        mine = (0, 0, 0)
        ship(mine, "second", 15, 8, mine=True)
        ship(mine, "first", 3, 4, mine=True)
        for k in (1, 3, 2):
            ship(mine, k, k - 1, 4 - k, mine=True)
        to_core(mine, mine=True)
        for copy in own_copies():
            copy.start()

    def along(k):
        group = (0, 0, k)
        arrive(group)
        ship(group, "second", 8 + k - 1, 8 + k)
        ship(group, "first", 4 + k - 1, 4 + k)
        to_core(group)

    def across(k):
        group = (0, 1, k)
        arrive(group)
        ship(group, "second", 11 + k, 12 + k)
        to_core(group)

    def over(k):
        for b in (0, 1):
            group = (1, b, k)
            arrive(group)
            to_core(group)

    def finish():
        for k in (0, 1, 3, 2):
            for a, b in ((0, 0), (0, 1), (1, 0), (1, 1)):
                arrive((a, b, k), other=True)
        for copy in own_copies():
            copy.wait()
        for spec in started:
            for copy in pair(*spec):
                copy.wait_send()

    return begin, along, across, over, finish


def meeting(count):
    dp, sq, *_ = place()
    core, xdev, *_ = partners()
    greet(seq_peers(dp, sq, count) + [core, xdev])


def tree_scratch():
    return [
        pltpu.SemaphoreType.DMA((2, 32)),
        pltpu.SemaphoreType.DMA((2, 32)),
        pltpu.SemaphoreType.DMA((2,)),
    ]


def gather_kernel(w_ref, d_ref, f_ref, w_all, d_all, f_all, send, recv, own, row_send, row_recv, row_own):
    meeting(f_ref.shape[0])
    begin, along, across, over, finish = gather_steps(w_ref, d_ref, w_all, d_all, send, recv, own)
    begin()
    across(0)
    along(1)
    along(3)
    across(1)
    along(2)
    rows_begin(f_ref, f_all, row_send, row_recv, row_own)
    across(3)
    over(0)
    across(2)
    over(1)
    over(3)
    over(2)
    finish()
    rows_end(f_ref, f_all, row_send, row_recv, row_own)


def gathered(w, d):
    return [
        jax.ShapeDtypeStruct((w.shape[0] * 32, w.shape[1]), w.dtype),
        jax.ShapeDtypeStruct((d.shape[0] * 32, d.shape[1]), d.dtype),
    ]


def gather_all(w, d, f):
    vm = pl.BlockSpec(memory_space=pltpu.VMEM)
    hbm = pl.BlockSpec(memory_space=pl.ANY)
    return pl.pallas_call(
        gather_kernel,
        in_specs=[vm] * 3,
        out_specs=[hbm] * 3,
        out_shape=gathered(w, d) + [jax.ShapeDtypeStruct(f.shape, f.dtype)],
        scratch_shapes=tree_scratch() + row_scratch(f.shape[0]),
        compiler_params=pltpu.CompilerParams(collective_id=0, has_side_effects=True),
        name="gather_all",
    )(w, d, f)


def scatter_steps(w_ref, d_ref, w_out, d_out, bufs, send, recv):
    w0, d0, w1, d1, w2, d2, w3, d3 = bufs
    wr, dr = w_out.shape[0], d_out.shape[0]

    def rows(rank, size):
        return pl.ds(pl.multiple_of(rank * size, 16), size)

    def group_ranks(slot, other):
        _, _, _, c, _, _ = place()
        group = (1 - c if other else c, lax.div(slot, 8), lax.rem(lax.div(slot, 4), 2), lax.rem(slot, 4))
        return rank_of(*group), rank_of(*group, fixed=True)

    def core_copies(slot):
        core = partners()[0]
        w_rank, d_rank = group_ranks(slot, True)
        return (
            remote(w_ref.at[rows(w_rank, wr), :], w0.at[slot], send.at[0, slot], recv.at[0, slot], core),
            remote(d_ref.at[rows(d_rank, dr), :], d0.at[slot], send.at[1, slot], recv.at[1, slot], core),
        )

    def second_copies(slot):
        _, xdev, _, to, _ = partners()
        return (
            remote(w0.at[8 + slot], w1.at[slot], send.at[0, 16 + slot], recv.at[0, 16 + slot], to),
            remote(d0.at[8 + slot], d1.at[slot], send.at[1, 16 + slot], recv.at[1, 16 + slot], xdev),
        )

    def first_copies(slot):
        _, _, to, _, ydev = partners()
        return (
            remote(w0.at[4 + slot], w2.at[slot], send.at[0, 24 + slot], recv.at[0, 24 + slot], to),
            remote(d0.at[4 + slot], d2.at[slot], send.at[1, 24 + slot], recv.at[1, 24 + slot], ydev),
        )

    def z_copies(k):
        dp, _, _, _, z, y = place()
        to = (dp, lax.rem(z + k, 4) * 2 + y)
        return (
            remote(w0.at[k], w3.at[3 - k], send.at[0, 27 + k], recv.at[0, 31 - k], to),
            remote(d0.at[k], d3.at[3 - k], send.at[1, 27 + k], recv.at[1, 31 - k], to),
        )

    def start(copies):
        for copy in copies:
            copy.start()

    def landed(copies):
        for copy in copies:
            copy.wait_recv()

    def sent(copies):
        for copy in copies:
            copy.wait_send()

    def add(slot, w, d):
        f = jnp.float32
        w0[slot] = (w0[slot].astype(f) + w.astype(f)).astype(jnp.bfloat16)
        d0[slot] = (d0[slot].astype(f) + d.astype(f)).astype(jnp.bfloat16)

    def begin():
        @pl.loop(0, 16)
        def _(step):
            start(core_copies(15 - step))

    def take(slot):
        landed(core_copies(slot))
        w_rank, d_rank = group_ranks(slot, False)
        add(slot, w_ref[rows(w_rank, wr), :], d_ref[rows(d_rank, dr), :])

    def far(lo, hi):
        @pl.loop(lo, hi)
        def _(step):
            take(15 - step)
            start(second_copies(7 - step))

    def near(lo, hi):
        @pl.loop(lo, hi)
        def _(step):
            take(7 - step)

    def pass_first(lo, hi):
        @pl.loop(lo, hi)
        def _(step):
            slot = 7 - step
            landed(second_copies(slot))
            add(slot, w1[slot], d1[slot])
            start(first_copies(slot - 4))

    def join_second():
        @pl.loop(0, 3)
        def _(step):
            slot = 3 - step
            landed(second_copies(slot))
            add(slot, w1[slot], d1[slot])

    def pass_along(lo, hi):
        @pl.loop(lo, hi)
        def _(step):
            slot = 3 - step
            landed(first_copies(slot))
            add(slot, w2[slot], d2[slot])
            start(z_copies(slot))

    def total(base, parts):
        value = base.astype(jnp.float32)
        for part in parts:
            value = value + part.astype(jnp.float32)
        return value

    def finish():
        landed(second_copies(0))
        landed(first_copies(0))
        for k in (1, 2, 3):
            landed(z_copies(k))
        w_out[...] = total(w0[0], (w1[0], w2[0], w3[0], w3[1], w3[2]))
        d_out[...] = total(d0[0], (d1[0], d2[0], d3[0], d3[1], d3[2]))

        @pl.loop(0, 16)
        def _(slot):
            sent(core_copies(slot))

        @pl.loop(0, 8)
        def _(slot):
            sent(second_copies(slot))

        @pl.loop(0, 4)
        def _(slot):
            sent(first_copies(slot))

        for k in (1, 2, 3):
            sent(z_copies(k))

    return begin, far, near, pass_first, join_second, pass_along, finish


def scatter_scratch(w, d):
    bf = jnp.bfloat16
    scratch = []
    for n in (16, 8, 4, 3):
        scratch += [
            pltpu.VMEM((n, w.shape[0] // 32, w.shape[1]), bf),
            pltpu.VMEM((n, d.shape[0] // 32, d.shape[1]), bf),
        ]
    return scratch + tree_scratch()[:2]


def scattered(w, d):
    return [
        jax.ShapeDtypeStruct((w.shape[0] // 32, w.shape[1]), jnp.float32),
        jax.ShapeDtypeStruct((d.shape[0] // 32, d.shape[1]), jnp.float32),
    ]


def scatter_kernel(w_ref, d_ref, g_ref, w_out, d_out, g_all, *scratch):
    bufs, (send, recv, row_send, row_recv, row_own) = scratch[:8], scratch[8:]
    meeting(g_ref.shape[0])
    begin, far, near, pass_first, join_second, pass_along, finish = scatter_steps(
        w_ref, d_ref, w_out, d_out, bufs, send, recv
    )
    begin()
    far(0, 8)
    rows_begin(g_ref, g_all, row_send, row_recv, row_own)
    near(0, 4)
    pass_first(0, 4)
    near(4, 8)
    join_second()
    pass_along(0, 3)
    finish()
    rows_end(g_ref, g_all, row_send, row_recv, row_own)


def scatter_all(w, d, g):
    vm = pl.BlockSpec(memory_space=pltpu.VMEM)
    hbm = pl.BlockSpec(memory_space=pl.ANY)
    return pl.pallas_call(
        scatter_kernel,
        in_specs=[vm] * 3,
        out_specs=[vm, vm, hbm],
        out_shape=scattered(w, d) + [jax.ShapeDtypeStruct(g.shape, g.dtype)],
        scratch_shapes=scatter_scratch(w, d) + row_scratch(g.shape[0]),
        compiler_params=pltpu.CompilerParams(
            collective_id=1, has_side_effects=True, vmem_limit_bytes=VMEM_LIMIT
        ),
        name="scatter_all",
    )(w, d, g)


def rows_begin(src, dst, send, recv, own):
    _, sq, *_ = place()
    for k in range(1, dst.shape[0]):
        row_copy(src, dst, send, recv, k).start()
    pltpu.make_async_copy(src.at[sq], dst.at[sq], own).start()


def rows_end(src, dst, send, recv, own):
    dp, sq, *_ = place()
    count = dst.shape[0]
    for k in range(1, count):
        copy = row_copy(src, dst, send, recv, k)
        copy.wait_send()
        landing(src, dst, send, recv, k).wait_recv()
    pltpu.make_async_copy(src.at[sq], dst.at[sq], own).wait()


def row_copy(src, dst, send, recv, k):
    dp, sq, *_ = place()
    count = dst.shape[0]
    to = lax.rem(sq + k, count)
    return remote(src.at[to], dst.at[sq], send.at[k - 1], recv.at[count - 1 - k], (dp, to))


def landing(src, dst, send, recv, k):
    dp, sq, *_ = place()
    origin = lax.rem(sq + k, dst.shape[0])
    return remote(src.at[sq], dst.at[origin], send.at[k - 1], recv.at[k - 1], (dp, origin))


def norm_parts(rows):
    centred = rows - jnp.mean(rows, axis=1, keepdims=True)
    return centred, lax.rsqrt(jnp.mean(centred * centred, axis=1, keepdims=True) + 1e-05)


def norm(rows, gain, shift):
    centred, inv = norm_parts(rows)
    return centred * inv * gain + shift


def silu(h):
    return h * (1.0 / (1.0 + jnp.exp(-h)))


def front_kernel(
    len_ref, f_ref, in_ref, pos_ref, up_ref, small_ref, down_ref, table_ref, c_ref, w_ref, d_ref,
    ctx_ref, p_ref, x1_ref, qu_ref, qv_ref, k_ref, v_ref, t_ref, sm_ref, c_all, w_all, d_all,
    send, recv, own, row_send, row_recv, row_own, *, tq, tile,
):
    low = jnp.bfloat16
    keys, model = f_ref.shape
    span = keys + tq
    steps = keys // tq
    begin, along, across, over, finish = gather_steps(w_ref, d_ref, w_all, d_all, send, recv, own)

    def dense(i):
        rows = pl.ds(pl.multiple_of(i * tile, tile), tile)
        x0 = f_ref[rows, :].astype(jnp.float32)
        a0 = norm(x0, sm_ref[0:1, :], sm_ref[6:7, :]).astype(low)
        z = silu(dotf(a0, up_ref[...])).astype(low)
        x1 = x0 + 0.5 * dotf(z, down_ref[...])
        x1_ref[rows, :] = x1
        a1 = norm(x1, sm_ref[1:2, :], sm_ref[7:8, :]).astype(low)
        query = dotf(a1, in_ref[:, :model])
        qu_ref[rows, :] = (query + sm_ref[12:13, :]).astype(low)
        qv_ref[rows, :] = (query + sm_ref[13:14, :]).astype(low)
        k_ref[rows, :] = dotf(a1, in_ref[:, model : 2 * model]).astype(low)
        v_ref[rows, :] = dotf(a1, in_ref[:, 2 * model :]).astype(low)

    @pl.when(pl.program_id(0) == 0)
    def _():
        meeting(c_ref.shape[0])
        begin()
        sm_ref[...] = small_ref[...].astype(jnp.float32).T

        @pl.loop(0, 2 * keys // tile)
        def _(i):
            rows = pl.ds(pl.multiple_of(i * tile, tile), tile)
            t_ref[rows, :] = dotf(table_ref[rows, :], pos_ref[...]).astype(low)

        @pl.loop(0, keys // tile)
        def _(i):
            dense(i)

            @pl.when(i == 0)
            def _():
                across(0)
                along(1)

            @pl.when(i == 1)
            def _():
                along(3)
                across(1)

            @pl.when(i == 2)
            def _():
                along(2)
                rows_begin(c_ref, c_all, row_send, row_recv, row_own)

    plan = {1: ((across, 3), (over, 0)), 3: ((across, 2),), 5: ((over, 1),), 8: ((over, 3),), 11: ((over, 2),)}
    dp, sq, *_ = place()
    valid = lax.broadcasted_iota(jnp.int32, (1, keys), 1) < len_ref[dp * (MB * UTTS) + sq]
    base = pl.program_id(0) * 128

    @pl.loop(0, steps)
    def _(i):
        time = pl.program_id(0) * steps + i
        for at, todo in plan.items():

            @pl.when(time == at)
            def _():
                for step, k in todo:
                    step(k)

        rows = pl.ds(pl.multiple_of(i * tq, tq), tq)
        band = pl.ds(pl.multiple_of(keys - tq - i * tq, tq), span)
        pair = pl.ds(pl.multiple_of(base, 128), 128)
        qu, qv, k, v, t = qu_ref[rows, pair], qv_ref[rows, pair], k_ref[:, pair], v_ref[:, pair], t_ref[band, pair]
        for h in range(2):
            cols = slice(h * DH, (h + 1) * DH)
            content = dotf(qu[:, cols], k[:, cols], NT)
            raw = dotf(qv[:, cols], t[:, cols], NT)
            pos = pltpu.roll(raw, keys + 1, 1, stride=1, stride_axis=0)[:, :keys]
            s = jnp.where(valid, (content + pos) * 0.125, -1e30)
            e = jnp.exp(s - jnp.max(s, axis=1, keepdims=True))
            p = (e * (1.0 / jnp.sum(e, axis=1, keepdims=True))).astype(low)
            p_ref[h, rows, :] = p
            ctx_ref[rows, cols] = dotf(p, v[:, cols]).astype(low)

    @pl.when(pl.program_id(0) == pl.num_programs(0) - 1)
    def _():
        finish()
        rows_end(c_ref, c_all, row_send, row_recv, row_own)


def row_scratch(count):
    return [
        pltpu.SemaphoreType.DMA((count - 1,)),
        pltpu.SemaphoreType.DMA((count - 1,)),
        pltpu.SemaphoreType.DMA,
    ]


def front(length, f, w_early, cuts, down, table_in, cot, w, d, tq=256, tile=256):
    rows, model = f.shape
    low = jnp.bfloat16
    vm = pl.BlockSpec(memory_space=pltpu.VMEM)
    hbm = pl.BlockSpec(memory_space=pl.ANY)

    def window(lo, hi):
        return pl.BlockSpec((w_early.shape[0], hi - lo), lambda h, *_: (0, lo // (hi - lo)), pipeline_mode=pl.Buffered(1))

    one = jax.ShapeDtypeStruct((rows, model), low)
    return pl.pallas_call(
        lambda *refs: front_kernel(*refs, tq=tq, tile=tile),
        grid_spec=pltpu.PrefetchScalarGridSpec(
            num_scalar_prefetch=1,
            grid=(model // 128,),
            in_specs=[vm] + [window(lo, hi) for lo, hi in zip(cuts[:-1], cuts[1:])] + [vm] * 5,
            out_specs=[
                pl.BlockSpec((rows, 128), lambda h, *_: (0, h)),
                pl.BlockSpec((2, rows, rows), lambda h, *_: (h, 0, 0)),
            ]
            + [vm] * 7
            + [hbm] * 3,
            scratch_shapes=tree_scratch() + row_scratch(cot.shape[0]),
        ),
        out_shape=[
            one,
            jax.ShapeDtypeStruct((model // DH, rows, rows), low),
            jax.ShapeDtypeStruct((rows, model), jnp.float32),
            one,
            one,
            one,
            one,
            jax.ShapeDtypeStruct((2 * rows, model), low),
            jax.ShapeDtypeStruct((SMALL, model), jnp.float32),
            jax.ShapeDtypeStruct(cot.shape, cot.dtype),
        ]
        + gathered(w, d),
        compiler_params=pltpu.CompilerParams(
            collective_id=4, has_side_effects=True, vmem_limit_bytes=VMEM_LIMIT
        ),
        name="front",
    )(length, f, *[w_early] * (len(cuts) - 1), down, table_in, cot, w, d)


def norm_back(rows, gain, grad):
    centred, inv = norm_parts(rows)
    hat = centred * inv
    scaled = grad * gain
    inner = jnp.mean(scaled * hat, axis=1, keepdims=True)
    out = inv * (scaled - jnp.mean(scaled, axis=1, keepdims=True) - hat * inner)
    return out, hat, jnp.sum(grad * hat, axis=0, keepdims=True)


def back_kernel(
    p_ref, g_ref, qu_ref, qv_ref, k_ref, v_ref, t_ref,
    m_ref, w_ref, d_ref, x1_ref, f_ref, grad_ref, sm_ref, gs_ref, in_ref, up_ref, down_ref, table_ref,
    ge_ref, gd_ref, rows_ref, m_all, w_out, d_out,
    ds_sc, dt_sc, dproj_sc, dtab_sc, z_sc, dh_sc, a0_sc, a1_sc, go_sc, gs_sc, *scratch, tq, tile,
):
    bufs, (send, recv, row_send, row_recv, row_own) = scratch[:8], scratch[8:]
    begin, far, near, pass_first, join_second, pass_along, finish = scatter_steps(
        w_ref, d_ref, w_out, d_out, bufs, send, recv
    )
    low = jnp.bfloat16
    keys = k_ref.shape[0]
    model = f_ref.shape[1]
    span = keys + tq
    steps = keys // tq

    def open_up():
        meeting(m_ref.shape[0])
        begin()
        gs_sc[...] = gs_ref[...]

    def rows_away():
        near(4, 8)
        rows_begin(m_ref, m_all, row_send, row_recv, row_own)

    plan = {
        0: open_up,
        1: lambda: far(0, 4),
        2: lambda: far(4, 8),
        3: lambda: near(0, 4),
        4: rows_away,
        5: lambda: pass_first(0, 2),
        6: lambda: pass_first(2, 4),
        9: join_second,
        10: lambda: pass_along(0, 2),
        11: lambda: pass_along(2, 3),
    }
    flip = (
        lax.broadcasted_iota(jnp.int32, (tq, tq), 0) + lax.broadcasted_iota(jnp.int32, (tq, tq), 1) == tq - 1
    ).astype(low)
    pad = jnp.zeros((tq, tq), jnp.float32)
    dt_sc[...] = jnp.zeros_like(dt_sc)
    base = pl.program_id(0) * 128

    def at(offset):
        return pl.ds(pl.multiple_of(base + offset, 128), 128)

    @pl.loop(0, steps)
    def _(i):
        time = pl.program_id(0) * steps + i
        for moment, step in plan.items():
            pl.when(time == moment)(step)
        rows = pl.ds(pl.multiple_of(i * tq, tq), tq)
        band = pl.ds(pl.multiple_of(keys - tq - i * tq, tq), span)
        sides = []
        for h in range(2):
            cols = slice(h * DH, (h + 1) * DH)
            dp = dotf(g_ref[rows, cols], v_ref[:, cols], NT)
            pf = p_ref[h, rows, :].astype(jnp.float32)
            ds = (pf * (dp - jnp.sum(dp * pf, axis=1, keepdims=True))).astype(low)
            ds_sc[h, rows, :] = ds
            dqu = dotf(ds, k_ref[:, cols]) * 0.125
            turned = jnp.concatenate([dotf(flip, ds), pad], axis=1)
            raw = pltpu.roll(turned, 0, 1, stride=1, stride_axis=0).astype(low)
            dqv = dotf(flip, dotf(raw, t_ref[band, cols]).astype(low)) * 0.125
            qv = dotf(flip, qv_ref[rows, cols]).astype(low)
            dt_sc[h, band, :] += dotf(raw, qv, TN)
            sides.append((dqu, dqv))
        dqu, dqv = (jnp.concatenate(both, axis=1) for both in zip(*sides))
        gs_sc[12:13, at(0)] += jnp.sum(dqu, axis=0, keepdims=True)
        gs_sc[13:14, at(0)] += jnp.sum(dqv, axis=0, keepdims=True)
        dproj_sc[rows, at(0)] = (dqu + dqv).astype(low)

    halves = []
    for h in range(2):
        cols = slice(h * DH, (h + 1) * DH)
        halves.append(
            (
                dt_sc[h] * 0.125,
                dotf(ds_sc[h], qu_ref[:, cols], TN) * 0.125,
                dotf(p_ref[h], g_ref[:, cols], TN),
            )
        )
    dtab, dk, dv = (jnp.concatenate(both, axis=1).astype(low) for both in zip(*halves))
    dtab_sc[:, at(0)] = dtab
    dproj_sc[:, at(model)] = dk
    dproj_sc[:, at(2 * model)] = dv

    @pl.when(pl.program_id(0) == pl.num_programs(0) - 1)
    def _():
        @pl.loop(0, keys // tile)
        def _(i):
            rows = pl.ds(pl.multiple_of(i * tile, tile), tile)
            dn = dotf(dproj_sc[rows, :], in_ref[...], NT)
            dx, hat, dgain = norm_back(x1_ref[rows, :], sm_ref[1:2, :], dn)
            gs_sc[1:2, :] += dgain
            gs_sc[7:8, :] += jnp.sum(dn, axis=0, keepdims=True)
            a1_sc[rows, :] = (hat * sm_ref[1:2, :] + sm_ref[7:8, :]).astype(low)
            grad = grad_ref[rows, :] + dx
            go = (0.5 * grad).astype(low)
            go_sc[rows, :] = go
            x0 = f_ref[rows, :].astype(jnp.float32)
            a0 = norm(x0, sm_ref[0:1, :], sm_ref[6:7, :]).astype(low)
            a0_sc[rows, :] = a0
            h = dotf(a0, up_ref[...])
            sig = 1.0 / (1.0 + jnp.exp(-h))
            z_sc[rows, :] = (h * sig).astype(low)
            dh = (dotf(go, down_ref[...], NT) * (sig * (1.0 + h * (1.0 - sig)))).astype(low)
            dh_sc[rows, :] = dh
            dn = dotf(dh, up_ref[...], NT)
            dx, _, dgain = norm_back(x0, sm_ref[0:1, :], dn)
            gs_sc[0:1, :] += dgain
            gs_sc[6:7, :] += jnp.sum(dn, axis=0, keepdims=True)
            rows_ref[rows, :] = (grad + dx).astype(low)

        width = model

        @pl.loop(0, 3)
        def _(j):
            cols = pl.ds(pl.multiple_of(j * width, width), width)
            ge_ref[:, cols] = dotf(a1_sc[...], dproj_sc[:, cols], TN).astype(low)

        ge_ref[:, 3 * width : 4 * width] = dotf(table_ref[...], dtab_sc[...], TN).astype(low)

        @pl.loop(0, 4)
        def _(j):
            cols = pl.ds(pl.multiple_of(j * width, width), width)
            ge_ref[:, pl.ds(pl.multiple_of((j + 4) * width, width), width)] = dotf(
                a0_sc[...], dh_sc[:, cols], TN
            ).astype(low)
            gd_ref[cols, :] = dotf(z_sc[:, cols], go_sc[...], TN).astype(low)

        ge_ref[:, 8 * width :] = gs_sc[...].T.astype(low)
        finish()
        rows_end(m_ref, m_all, row_send, row_recv, row_own)


def back(
    p, g, qu, qv, k, v, table, mixed, w, d, x1, f, grad, small, g_small, w_early, cuts, down, table_in, tq=256, tile=256
):
    rows, model = qu.shape
    low = jnp.bfloat16
    vm = pl.BlockSpec(memory_space=pltpu.VMEM)
    blk = pl.BlockSpec((rows, 128), lambda h: (0, h))
    tab = pl.BlockSpec((2 * rows, 128), lambda h: (0, h))

    def window(j):
        lo, hi = cuts[j], cuts[j + 1]
        return pl.BlockSpec((w_early.shape[0], hi - lo), lambda h: (0, lo // (hi - lo)), pipeline_mode=pl.Buffered(1))

    hidden = down.shape[0]
    return pl.pallas_call(
        lambda *refs: back_kernel(*refs, tq=tq, tile=tile),
        grid=(model // 128,),
        in_specs=[pl.BlockSpec((2, rows, rows), lambda h: (h, 0, 0))]
        + [blk] * 5
        + [tab]
        + [vm] * 8
        + [window(0), window(2), vm, vm],
        out_specs=[vm] * 3 + [pl.BlockSpec(memory_space=pl.ANY), vm, vm],
        out_shape=[
            jax.ShapeDtypeStruct(w_early.shape, low),
            jax.ShapeDtypeStruct(down.shape, low),
            jax.ShapeDtypeStruct((rows, model), low),
            jax.ShapeDtypeStruct(mixed.shape, mixed.dtype),
        ]
        + scattered(w, d),
        scratch_shapes=[
            pltpu.VMEM((2, rows, rows), low),
            pltpu.VMEM((2, 2 * rows, DH), jnp.float32),
            pltpu.VMEM((rows, 3 * model), low),
            pltpu.VMEM((2 * rows, model), low),
            pltpu.VMEM((rows, hidden), low),
            pltpu.VMEM((rows, hidden), low),
            pltpu.VMEM((rows, model), low),
            pltpu.VMEM((rows, model), low),
            pltpu.VMEM((rows, model), low),
            pltpu.VMEM((SMALL, model), jnp.float32),
        ]
        + scatter_scratch(w, d)
        + row_scratch(mixed.shape[0]),
        compiler_params=pltpu.CompilerParams(
            collective_id=5, has_side_effects=True, vmem_limit_bytes=63 * 1024 * 1024
        ),
        name="back",
    )(p, g, qu, qv, k, v, table, mixed, w, d, x1, f, grad, small, g_small, w_early, w_early, down, table_in)


def sigmoid(h):
    return 1.0 / (1.0 + jnp.exp(-h))


def middle_kernel(
    len_ref, ctx_ref, x1_ref, w_ref, down_ref, cot_ref, sm_ref,
    mixed_ref, grad_ref, gctx_ref, gw_ref, gd_ref, gs_ref,
    x2_sc, a2_sc, gate_sc, gl_sc, dep_sc, act_sc, a3_sc, z_sc, dh_sc, go_sc, gob_sc, e_sc, dd_sc, tap_sc, win_sc,
    part_sc, peer_sc, send, recv, *, tile, taps,
):
    low = jnp.bfloat16
    f32 = jnp.float32
    length, model = x1_ref.shape
    hidden = down_ref.shape[0]
    reach = (taps - 1) // 2
    edge = gl_sc.shape[0] - length
    half = edge // 2
    dp, sq, *_ = place()
    batch = lax.div(sq, UTTS)
    me = dp * UTTS + lax.rem(sq, UTTS)
    size = peer_sc.shape[1]
    valid = len_ref[dp * (MB * UTTS) + sq]
    frames = jnp.int32(0)
    for group in range(4):
        for u in range(UTTS):
            frames = frames + len_ref[group * (MB * UTTS) + batch * UTTS + u]
    per = 1.0 / jnp.full((1, model), frames, jnp.int32).astype(f32)
    up_w = w_ref.at[:, :hidden]
    out_w = w_ref.at[:, hidden : hidden + model]
    gate_w = w_ref.at[:, hidden + model : hidden + 3 * model]
    conv_w = w_ref.at[:, hidden + 3 * model :]

    def peer(j):
        r = lax.rem(me + j, size)
        return (lax.div(r, UTTS), batch * UTTS + lax.rem(r, UTTS))

    barrier = pltpu.get_barrier_semaphore()
    for j in range(1, size):
        pl.semaphore_signal(barrier, inc=1, device_id=peer(j), device_id_type=MESH)

    def give(which, j):
        return remote(
            part_sc.at[which], peer_sc.at[which, me], send.at[which, j - 1], recv.at[which, size - 1 - j], peer(j)
        )

    def give_all(which):
        for j in range(1, size):
            give(which, j).start()
        peer_sc[which, me] = part_sc[which]

    def take_all(which):
        for j in range(1, size):
            remote(
                part_sc.at[which],
                peer_sc.at[which, lax.rem(me + j, size)],
                send.at[which, j - 1],
                recv.at[which, j - 1],
                peer(j),
            ).wait_recv()
        for j in range(1, size):
            give(which, j).wait_send()
        return jnp.sum(peer_sc[which], axis=0)

    def row_of(i):
        return pl.ds(pl.multiple_of(i * tile, tile), tile)

    def inner_of(i):
        return pl.ds(pl.multiple_of(i * tile + half, 8), tile)

    def mask_of(i):
        return (lax.broadcasted_iota(jnp.int32, (tile, 1), 0) + i * tile < valid).astype(f32)

    def total(rows):
        return jnp.sum(rows, axis=0, keepdims=True)

    def row(r):
        return sm_ref[r : r + 1, :]

    gs_ref[...] = jnp.zeros_like(gs_ref)
    part_sc[...] = jnp.zeros_like(part_sc)
    for pad_sc in (gl_sc, dd_sc):
        pad_sc[:half, :] = jnp.zeros((half, model), f32)
        pad_sc[half + length :, :] = jnp.zeros((half, model), f32)

    tiles = length // tile

    @pl.loop(0, tiles)
    def _(i):
        rows = row_of(i)
        x2 = x1_ref[rows, :] + dotf(ctx_ref[rows, :], out_w[...])
        x2_sc[rows, :] = x2
        a2 = norm(x2, row(2), row(8)).astype(low)
        a2_sc[rows, :] = a2
        gate = dotf(a2, gate_w[...])
        gate_sc[rows, :] = gate
        gl = (gate[:, :model] * sigmoid(gate[:, model:]) * mask_of(i)).astype(low)
        gl_sc[inner_of(i), :] = gl.astype(f32)

    strip = STRIP

    def depthwise(src, lanes, base, backward):
        win_sc[...] = src[pl.ds(base, strip + edge), lanes]
        acc = jnp.zeros((strip, 128), f32)
        for k in range(taps):
            shift = half + (reach - k if backward else k - reach)
            acc = acc + win_sc[shift : shift + strip, :] * sm_ref[14 + k : 15 + k, lanes]
        return acc

    for c in range(model // 128):
        lanes = slice(c * 128, (c + 1) * 128)

        @pl.loop(0, length // strip)
        def _(i):
            base = pl.multiple_of(i * strip, strip)
            dep = depthwise(gl_sc, lanes, base, False)
            dep_sc[pl.ds(base, strip), lanes] = dep
            mask = (lax.broadcasted_iota(jnp.int32, (strip, 1), 0) + base < valid).astype(f32)
            kept = dep * mask
            part_sc[0, 0:1, lanes] += total(kept)
            part_sc[0, 1:2, lanes] += total(kept * dep)

    pl.semaphore_wait(barrier, size - 1)
    give_all(0)
    sums = take_all(0)
    mean = sums[0:1] * per
    inv = lax.rsqrt(sums[1:2] * per - mean * mean + 1e-05)

    @pl.loop(0, tiles)
    def _(i):
        rows = row_of(i)
        dep = dep_sc[rows, :]
        hatn = (dep - mean) * inv
        normal = hatn * row(5) + row(11)
        sgn = sigmoid(normal)
        act = (normal * sgn).astype(low)
        act_sc[rows, :] = act
        x3 = x2_sc[rows, :] + dotf(act, conv_w[...])
        a3 = norm(x3, row(3), row(9)).astype(low)
        a3_sc[rows, :] = a3
        h = dotf(a3, up_w[...])
        sig = sigmoid(h)
        z = (h * sig).astype(low)
        z_sc[rows, :] = z
        x4 = x3 + 0.5 * dotf(z, down_ref[...])
        mixed_ref[rows, :] = norm(x4, row(4), row(10)).astype(low)
        cot = cot_ref[rows, :].astype(f32)
        grad, _, dgain = norm_back(x4, row(4), cot)
        gs_ref[4:5, :] += dgain
        gs_ref[10:11, :] += total(cot)
        go = (0.5 * grad).astype(low)
        go_sc[rows, :] = go
        dh = (dotf(go, down_ref[...], NT) * (sig * (1.0 + h * (1.0 - sig)))).astype(low)
        dh_sc[rows, :] = dh
        dn = dotf(dh, up_w[...], NT)
        dx, _, dgain = norm_back(x3, row(3), dn)
        gs_ref[3:4, :] += dgain
        gs_ref[9:10, :] += total(dn)
        grad = grad + dx
        grad_ref[rows, :] = grad
        gob = grad.astype(low)
        gob_sc[rows, :] = gob
        dnormal = dotf(gob, conv_w[...], NT) * (sgn * (1.0 + normal * (1.0 - sgn)))
        gs_ref[5:6, :] += total(dnormal * hatn)
        gs_ref[11:12, :] += total(dnormal)
        e = dnormal * row(5)
        e_sc[rows, :] = e
        part_sc[1, 0:1, :] += total(e)
        part_sc[1, 1:2, :] += total(e * dep)

    give_all(1)

    @pl.loop(0, hidden // model)
    def _(j):
        cols = pl.ds(pl.multiple_of(j * model, model), model)
        gw_ref[:, cols] = dotf(a3_sc[...], dh_sc[:, cols], TN).astype(low)
        gd_ref[cols, :] = dotf(z_sc[:, cols], go_sc[...], TN).astype(low)

    gw_ref[:, hidden + 3 * model :] = dotf(act_sc[...], gob_sc[...], TN).astype(low)
    sums = take_all(1)
    dvar = -0.5 * inv * inv * inv * (sums[1:2] - mean * sums[0:1])
    dmean = -inv * sums[0:1] - 2.0 * mean * dvar

    @pl.loop(0, tiles)
    def _(i):
        rows = row_of(i)
        dd = e_sc[rows, :] * inv + mask_of(i) * (dmean * per + 2.0 * dep_sc[rows, :] * dvar * per)
        dd_sc[inner_of(i), :] = dd.astype(low).astype(f32)

    for c in range(model // 128):
        lanes = slice(c * 128, (c + 1) * 128)
        tap_sc[...] = jnp.zeros_like(tap_sc)

        @pl.loop(0, length // strip)
        def _(i):
            base = pl.multiple_of(i * strip, strip)
            e_sc[pl.ds(base, strip), lanes] = depthwise(dd_sc, lanes, base, True)
            dd = dd_sc[pl.ds(pl.multiple_of(base + half, 8), strip), lanes]
            win_sc[...] = gl_sc[pl.ds(base, strip + edge), lanes]
            for k in range(taps):
                prod = win_sc[half + k - reach : half + k - reach + strip, :] * dd
                tap_sc[k] += jnp.sum(prod.reshape(strip // 8, 8, 128), axis=0)

        gs_ref[14 : 14 + taps, lanes] = jnp.sum(tap_sc[...], axis=1)

    @pl.loop(0, tiles)
    def _(i):
        rows = row_of(i)
        dgl = e_sc[rows, :] * mask_of(i)
        ga = gate_sc[rows, :model]
        sb = sigmoid(gate_sc[rows, model:])
        dgate = jnp.concatenate([dgl * sb, dgl * ga * sb * (1.0 - sb)], axis=1).astype(low)
        dh_sc[rows, : 2 * model] = dgate
        dn = dotf(dgate, gate_w[...], NT)
        dx, _, dgain = norm_back(x2_sc[rows, :], row(2), dn)
        gs_ref[2:3, :] += dgain
        gs_ref[8:9, :] += total(dn)
        grad = grad_ref[rows, :] + dx
        grad_ref[rows, :] = grad
        gob = grad.astype(low)
        gob_sc[rows, :] = gob
        gctx_ref[rows, :] = dotf(gob, out_w[...], NT).astype(low)

    gw_ref[:, hidden + model : hidden + 3 * model] = dotf(a2_sc[...], dh_sc[:, : 2 * model], TN).astype(low)
    gw_ref[:, hidden : hidden + model] = dotf(ctx_ref[...], gob_sc[...], TN).astype(low)


def middle(lengths, ctx, x1, w, down, cot, small, taps, tile=256):
    rows, model = x1.shape
    hidden = down.shape[0]
    low = jnp.bfloat16
    f32 = jnp.float32
    vm = pl.BlockSpec(memory_space=pltpu.VMEM)
    size = 4 * UTTS
    half = -(-(taps - 1) // 2 // 8) * 8
    wide = pltpu.VMEM((rows, model), f32)
    thin = pltpu.VMEM((rows, model), low)
    padded = pltpu.VMEM((rows + 2 * half, model), f32)
    return pl.pallas_call(
        lambda *refs: middle_kernel(*refs, tile=tile, taps=taps),
        in_specs=[pl.BlockSpec(memory_space=pltpu.SMEM)] + [vm] * 6,
        out_specs=[vm] * 6,
        out_shape=[
            jax.ShapeDtypeStruct((rows, model), low),
            jax.ShapeDtypeStruct((rows, model), f32),
            jax.ShapeDtypeStruct((rows, model), low),
            jax.ShapeDtypeStruct(w.shape, low),
            jax.ShapeDtypeStruct(down.shape, low),
            jax.ShapeDtypeStruct((SMALL, model), f32),
        ],
        scratch_shapes=[
            wide,
            thin,
            pltpu.VMEM((rows, 2 * model), f32),
            padded,
            wide,
            thin,
            thin,
            pltpu.VMEM((rows, hidden), low),
            pltpu.VMEM((rows, hidden), low),
            thin,
            thin,
            wide,
            padded,
            pltpu.VMEM((taps, 8, 128), f32),
            pltpu.VMEM((STRIP + 2 * half, 128), f32),
            pltpu.VMEM((2, 2, model), f32),
            pltpu.VMEM((2, size, 2, model), f32),
            pltpu.SemaphoreType.DMA((2, size - 1)),
            pltpu.SemaphoreType.DMA((2, size - 1)),
        ],
        compiler_params=pltpu.CompilerParams(
            collective_id=2, has_side_effects=True, vmem_limit_bytes=63 * 1024 * 1024
        ),
        name="middle",
    )(lengths, ctx, x1, w, down, cot, small)


def position_table(length, width):
    offsets = (length - 1 - np.arange(2 * length)).astype(np.float32)
    half = width // 2
    steps = np.arange(half, dtype=np.float32) * np.float32(-2.0 * math.log(10000.0) / width)
    angles = (offsets[:, None] * np.exp(steps)[None, :]).astype(np.float64)
    table = np.concatenate([np.sin(angles), np.cos(angles)], axis=1)
    return jnp.asarray(table.astype(np.float32)).astype(jnp.bfloat16)


def pack_kernel(
    frames, cot, gains, shifts, rel, up, down, attn_in, attn_out, pos, conv_in, taps, conv_out,
    early, late, down_0, down_1, f_out, c_out, turn, table,
):
    low = jnp.bfloat16
    f32 = jnp.float32
    own = gains.shape[2]
    count = taps.shape[2]
    at = 0
    for piece in (attn_in[0], pos[0], up[0, 0]):
        early[:, at : at + piece.shape[1]] = piece
        at += piece.shape[1]
    table[...] = jnp.zeros_like(table)
    turn[...] = jnp.zeros_like(turn)
    turn[:own, :count] = taps[0].astype(f32)
    table[0:6, :own] = gains[0].astype(f32)
    table[6:12, :own] = shifts[0].astype(f32)
    table[12:14, :own] = rel[0].astype(f32)
    table[14 : 14 + count, :own] = turn[...].T[:count, :own]
    early[:, at:] = table[...].T[:own, :].astype(low)
    at = 0
    for piece in (up[0, 1], attn_out[0], conv_in[0], conv_out[0]):
        late[:, at : at + piece.shape[1]] = piece
        at += piece.shape[1]
    down_0[...] = down[0, 0]
    down_1[...] = down[0, 1]
    f_out[...] = frames[...].astype(low)
    c_out[...] = cot[...].astype(low)


def pack(frames, cot, *weights):
    low = jnp.bfloat16
    vm = pl.BlockSpec(memory_space=pltpu.VMEM)
    _, _, _, up, down, attn_in, attn_out, pos, conv_in, _, conv_out = weights
    own = attn_in.shape[1]
    early = attn_in.shape[2] + pos.shape[2] + up.shape[3] + SMALL
    late = up.shape[3] + attn_out.shape[2] + conv_in.shape[2] + conv_out.shape[2]
    shapes = [(own, early), (own, late), down.shape[2:], down.shape[2:], frames.shape, frames.shape]
    return pl.pallas_call(
        pack_kernel,
        in_specs=[vm] * 13,
        out_specs=[vm] * 6,
        out_shape=[jax.ShapeDtypeStruct(shape, low) for shape in shapes],
        scratch_shapes=[pltpu.VMEM((SMALL, SMALL), jnp.float32)] * 2,
        name="pack",
    )(frames, cot, *weights)


def unpack_kernel(
    early, late, down_0, down_1, m_rows, g_rows,
    mixed, grad, gains, shifts, rel, up, down, attn_in, attn_out, pos, conv_in, taps, conv_out, turn, table,
):
    f32 = jnp.float32
    own = early.shape[0]
    count = taps.shape[2]
    at = 0
    for piece in (attn_in, pos):
        piece[0] = early[:, at : at + piece.shape[2]]
        at += piece.shape[2]
    up[0, 0] = early[:, at : at + up.shape[3]]
    at += up.shape[3]
    turn[...] = jnp.zeros_like(turn)
    turn[:own, :] = early[:, at:]
    table[...] = turn[...].T
    gains[0] = table[0:6, :own]
    shifts[0] = table[6:12, :own]
    rel[0] = table[12:14, :own]
    turn[:count, :] = table[14 : 14 + count, :]
    taps[0] = turn[...].T[:own, :count]
    up[0, 1] = late[:, : up.shape[3]]
    at = up.shape[3]
    for piece in (attn_out, conv_in, conv_out):
        piece[0] = late[:, at : at + piece.shape[2]]
        at += piece.shape[2]
    down[0, 0] = down_0[...]
    down[0, 1] = down_1[...]
    mixed[...] = m_rows[...].astype(f32)
    grad[...] = g_rows[...].astype(f32)


def unpack(early, late, down_0, down_1, m_rows, g_rows, likes):
    vm = pl.BlockSpec(memory_space=pltpu.VMEM)
    shapes = [m_rows.shape, g_rows.shape] + [like.shape for like in likes]
    return pl.pallas_call(
        unpack_kernel,
        in_specs=[vm] * 6,
        out_specs=[vm] * 13,
        out_shape=[jax.ShapeDtypeStruct(shape, jnp.float32) for shape in shapes],
        scratch_shapes=[pltpu.VMEM((SMALL, SMALL), jnp.float32)] * 2,
        name="unpack",
    )(early, late, down_0, down_1, m_rows, g_rows)


def local_whole(
    frames,
    lengths,
    cotangent,
    gains,
    shifts,
    rel_bias,
    ffn_up,
    ffn_down,
    attn_in,
    attn_out,
    pos_proj,
    conv_in,
    depthwise,
    conv_out,
):
    weights = (
        gains, shifts, rel_bias, ffn_up, ffn_down, attn_in, attn_out, pos_proj, conv_in, depthwise, conv_out
    )
    _, width_rows, model = frames.shape
    length = width_rows * lax.axis_size("seq")
    taps = depthwise.shape[2]
    table_in = position_table(length, model)
    early, late, own_0, own_1, f_rows, c_rows = pack(frames, cotangent, *weights)
    sizes = (attn_in.shape[2], pos_proj.shape[2], ffn_up.shape[3], SMALL)
    cuts = [0] + [int(v) for v in np.cumsum(sizes)]
    w_early, down_0, f_all = gather_all(early, own_0, f_rows)
    f_all = f_all.reshape(length, model)
    ctx, probs, x1, qu, qv, key, value, table, small, c_all, w_late, down_1 = front(
        lengths, f_all, w_early, cuts, down_0, table_in, c_rows, late, own_1
    )
    mixed, grad, grad_ctx, g_late, g_down1, g_small = middle(
        lengths, ctx, x1, w_late, down_1, c_all.reshape(length, model), small, taps
    )
    g_early, g_down0, grad, m_all, late_sum, down1_sum = back(
        probs,
        grad_ctx,
        qu,
        qv,
        key,
        value,
        table,
        mixed.reshape(frames.shape),
        g_late,
        g_down1,
        x1,
        f_all,
        grad,
        small,
        g_small,
        w_early,
        cuts,
        down_0,
        table_in,
    )
    early_sum, down0_sum, g_all = scatter_all(g_early, g_down0, grad.reshape(frames.shape))
    return tuple(unpack(early_sum, late_sum, down0_sum, down1_sum, m_all, g_all, weights))


def solution(mesh):
    body = local_whole if fits_whole(mesh) else local_general
    in_specs = (
        P("dp", "seq", None),
        P(),
        P("dp", "seq", None),
        P(None, None, ("dp", "seq")),
        P(None, None, ("dp", "seq")),
        P(None, None, ("dp", "seq")),
        P(None, None, ("dp", "seq"), None),
        P(None, None, ("dp", "seq"), None),
        P(None, ("dp", "seq"), None),
        P(None, ("dp", "seq"), None),
        P(None, ("dp", "seq"), None),
        P(None, ("dp", "seq"), None),
        P(None, ("dp", "seq"), None),
        P(None, ("dp", "seq"), None),
    )
    out_specs = (
        P("dp", "seq", None),
        P("dp", "seq", None),
        P(None, None, ("dp", "seq")),
        P(None, None, ("dp", "seq")),
        P(None, None, ("dp", "seq")),
        P(None, None, ("dp", "seq"), None),
        P(None, None, ("dp", "seq"), None),
        P(None, ("dp", "seq"), None),
        P(None, ("dp", "seq"), None),
        P(None, ("dp", "seq"), None),
        P(None, ("dp", "seq"), None),
        P(None, ("dp", "seq"), None),
        P(None, ("dp", "seq"), None),
    )
    return jax.shard_map(body, mesh=mesh, in_specs=in_specs, out_specs=out_specs, check_vma=False)
```

```python
import math

import jax
import jax.numpy as jnp
import numpy as np
from jax import lax
from jax.experimental import pallas as pl
from jax.experimental.pallas import tpu as pltpu
from jax.sharding import PartitionSpec as P

H = 8
DH = 64
NL = 1
MB = 2


HIGHEST_PREC = lax.Precision.HIGHEST


def extended(cells, sides, width):
    for axis, dim in sides:
        count = lax.axis_size(axis)
        ends = count - 1
        head = lax.slice_in_dim(cells, 0, width, axis=dim)
        tail = lax.slice_in_dim(cells, cells.shape[dim] - width, cells.shape[dim], axis=dim)
        cells = jnp.concatenate(
            [
                lax.ppermute(tail, axis, [(i, (i + 1) % count) for i in range(ends)]),
                cells,
                lax.ppermute(head, axis, [((i + 1) % count, i) for i in range(ends)]),
            ],
            axis=dim,
        )
    return cells


def layer_norm(values, gain_row, shift_row):
    centred = values - jnp.mean(values, axis=-1, keepdims=True)
    spread = jnp.mean(centred * centred, axis=-1, keepdims=True)
    return centred * lax.rsqrt(spread + 1e-05) * gain_row + shift_row


def sinusoid(offsets, model_width):
    half_width = model_width // 2
    frequency = jnp.exp(
        jnp.arange(half_width, dtype=jnp.float32) * (-2.0 * math.log(10000.0) / model_width)
    )
    angles = offsets.astype(jnp.float32)[:, None] * frequency[None, :]
    return jnp.concatenate([jnp.sin(angles), jnp.cos(angles)], axis=1)


def skew_rows(raw_pos, key_count):
    row_count = raw_pos.shape[-2]
    col_count = raw_pos.shape[-1]
    lead = raw_pos.shape[:-2]
    flat_rows = raw_pos.reshape(lead + (row_count * col_count,))
    flat_rows = flat_rows[..., row_count - 1 : row_count - 1 + row_count * (col_count - 1)]
    return flat_rows.reshape(lead + (row_count, col_count - 1))[..., :key_count]


def skew_back(grad_skew, raw_shape, key_count):
    zero_raw = jnp.zeros(raw_shape, jnp.float32)
    return jax.vjp(lambda raw_pos: skew_rows(raw_pos, key_count), zero_raw)[1](grad_skew)[0]


def glu_gate(gate_pair):
    half_width = gate_pair.shape[-1] // 2
    return gate_pair[..., :half_width] * jax.nn.sigmoid(gate_pair[..., half_width:])


def matmul_low(left, right):
    return jnp.dot(left, right, preferred_element_type=jnp.float32)


def matmul_back(grad_low, weight):
    return lax.dot_general(
        grad_low, weight, (((1,), (1,)), ((), ())), preferred_element_type=jnp.float32
    )


def weight_grad(inputs_low, grad_low):
    return lax.dot_general(
        inputs_low, grad_low, (((0,), (0,)), ((), ())), preferred_element_type=jnp.float32
    )


def ffn_forward(row_data, gain_row, shift_row, w_up, w_down):
    normed_b = layer_norm(row_data, gain_row, shift_row).astype(jnp.bfloat16)
    hidden = matmul_low(normed_b, w_up)
    active_b = jax.nn.silu(hidden).astype(jnp.bfloat16)
    branch = matmul_low(active_b, w_down)
    return (row_data + 0.5 * branch, (row_data, normed_b, hidden, active_b))


def ffn_backward(grad_rows, kept_data, gain_row, shift_row, w_up, w_down):
    row_data, normed_b, hidden, active_b = kept_data
    grad_out_b = (0.5 * grad_rows).astype(jnp.bfloat16)
    g_down = weight_grad(active_b, grad_out_b)
    grad_active = matmul_back(grad_out_b, w_down)
    grad_hidden_b = jax.vjp(jax.nn.silu, hidden)[1](grad_active)[0].astype(jnp.bfloat16)
    g_up = weight_grad(normed_b, grad_hidden_b)
    grad_normed = matmul_back(grad_hidden_b, w_up)
    grad_ln, g_gain, g_shift = jax.vjp(layer_norm, row_data, gain_row, shift_row)[1](grad_normed)
    return (grad_rows + grad_ln, (g_gain, g_shift, g_up, g_down))


def attention_logits(query_u_b, query_v_b, key_heads, pos_heads, key_valid):
    content = jnp.einsum(
        "ufhd,ulhd->uhfl", query_u_b, key_heads, preferred_element_type=jnp.float32
    )
    raw_pos = jnp.einsum("ufhd,whd->uhfw", query_v_b, pos_heads, preferred_element_type=jnp.float32)
    logits = (content + skew_rows(raw_pos, key_heads.shape[1])) * 0.125
    return jnp.where(key_valid[:, None, None, :], logits, -1e30)


def attn_forward(
    row_data,
    utt_count,
    gain_row,
    shift_row,
    bias_u,
    bias_v,
    w_in,
    w_out,
    w_pos,
    key_valid,
    pos_table_b,
):
    model_width = row_data.shape[1]
    frame_len = row_data.shape[0] // utt_count
    normed_b = layer_norm(row_data, gain_row, shift_row).astype(jnp.bfloat16)
    proj_rows = matmul_low(normed_b, w_in)
    query_rows = proj_rows[:, :model_width].reshape(utt_count, frame_len, H, DH)
    key_b = (
        proj_rows[:, model_width : 2 * model_width]
        .astype(jnp.bfloat16)
        .reshape(utt_count, frame_len, model_width)
    )
    value_b = (
        proj_rows[:, 2 * model_width :]
        .astype(jnp.bfloat16)
        .reshape(utt_count, frame_len, model_width)
    )
    all_keys, all_values = (
        lax.all_gather(key_b, "seq", axis=1, tiled=True),
        lax.all_gather(value_b, "seq", axis=1, tiled=True),
    )
    key_heads = all_keys.reshape(utt_count, -1, H, DH)
    value_heads = all_values.reshape(utt_count, -1, H, DH)
    query_u_b = (query_rows + bias_u.reshape(H, DH)).astype(jnp.bfloat16)
    query_v_b = (query_rows + bias_v.reshape(H, DH)).astype(jnp.bfloat16)
    pos_heads = matmul_low(pos_table_b, w_pos).astype(jnp.bfloat16).reshape(-1, H, DH)
    logits = attention_logits(query_u_b, query_v_b, key_heads, pos_heads, key_valid)
    top_score = jnp.max(logits, axis=-1, keepdims=True)
    exp_scores = jnp.exp(logits - top_score)
    row_total = jnp.sum(exp_scores, axis=-1, keepdims=True)
    prob_b = (exp_scores / row_total).astype(jnp.bfloat16)
    log_total = top_score + jnp.log(row_total)
    context = jnp.einsum("uhfl,ulhd->ufhd", prob_b, value_heads, preferred_element_type=jnp.float32)
    context_b = context.astype(jnp.bfloat16).reshape(-1, model_width)
    branch = matmul_low(context_b, w_out)
    kept_data = (
        row_data,
        normed_b,
        query_u_b,
        query_v_b,
        key_heads,
        value_heads,
        pos_heads,
        log_total,
        context_b,
    )
    return (row_data + branch, kept_data)


def attn_backward(grad_rows, kept_data, gain_row, shift_row, w_in, w_out, key_valid, pos_table_b):
    (
        row_data,
        normed_b,
        query_u_b,
        query_v_b,
        key_heads,
        value_heads,
        pos_heads,
        log_total,
        context_b,
    ) = kept_data
    utt_count = query_u_b.shape[0]
    frame_len = query_u_b.shape[1]
    model_width = row_data.shape[1]
    key_len = key_heads.shape[1]
    grad_out_b = grad_rows.astype(jnp.bfloat16)
    g_out = weight_grad(context_b, grad_out_b)
    grad_context_b = (
        matmul_back(grad_out_b, w_out).astype(jnp.bfloat16).reshape(utt_count, frame_len, H, DH)
    )
    logits = attention_logits(query_u_b, query_v_b, key_heads, pos_heads, key_valid)
    prob_rows = jnp.exp(logits - log_total)
    grad_probs = jnp.einsum(
        "ufhd,ulhd->uhfl", grad_context_b, value_heads, preferred_element_type=jnp.float32
    )
    inner_sum = jnp.sum(grad_probs * prob_rows, axis=-1, keepdims=True)
    grad_logits_b = (prob_rows * (grad_probs - inner_sum)).astype(jnp.bfloat16) * 0.125
    grad_query_u = jnp.einsum(
        "uhfl,ulhd->ufhd", grad_logits_b, key_heads, preferred_element_type=jnp.float32
    )
    raw_shape = (utt_count, H, frame_len, pos_heads.shape[0])
    grad_raw_b = skew_back(grad_logits_b.astype(jnp.float32), raw_shape, key_len).astype(
        jnp.bfloat16
    )
    grad_query_v = jnp.einsum(
        "uhfw,whd->ufhd", grad_raw_b, pos_heads, preferred_element_type=jnp.float32
    )
    grad_pos = jnp.einsum(
        "uhfw,ufhd->whd", grad_raw_b, query_v_b, preferred_element_type=jnp.float32
    )
    grad_pos = grad_pos.reshape(-1, model_width)
    g_pos = lax.dot_general(
        pos_table_b.astype(jnp.float32),
        grad_pos,
        (((0,), (0,)), ((), ())),
        precision=HIGHEST_PREC,
        preferred_element_type=jnp.float32,
    )
    prob_b = prob_rows.astype(jnp.bfloat16)
    grad_values = jnp.einsum(
        "uhfl,ufhd->ulhd", prob_b, grad_context_b, preferred_element_type=jnp.float32
    )
    grad_keys = jnp.einsum(
        "uhfl,ufhd->ulhd", grad_logits_b, query_u_b, preferred_element_type=jnp.float32
    )
    own_keys, own_values = (
        lax.psum_scatter(
            grad_keys.reshape(utt_count, key_len, model_width),
            "seq",
            scatter_dimension=1,
            tiled=True,
        ),
        lax.psum_scatter(
            grad_values.reshape(utt_count, key_len, model_width),
            "seq",
            scatter_dimension=1,
            tiled=True,
        ),
    )
    g_bias_u = jnp.sum(grad_query_u, axis=(0, 1)).reshape(-1)
    g_bias_v = jnp.sum(grad_query_v, axis=(0, 1)).reshape(-1)
    grad_proj_b = jnp.concatenate(
        [
            (grad_query_u + grad_query_v).reshape(-1, model_width),
            own_keys.reshape(-1, model_width),
            own_values.reshape(-1, model_width),
        ],
        axis=1,
    ).astype(jnp.bfloat16)
    g_in = weight_grad(normed_b, grad_proj_b)
    grad_normed = matmul_back(grad_proj_b, w_in)
    grad_ln, g_gain, g_shift = jax.vjp(layer_norm, row_data, gain_row, shift_row)[1](grad_normed)
    return (grad_rows + grad_ln, (g_gain, g_shift, g_bias_u, g_bias_v, g_in, g_out, g_pos))


def conv_forward(
    row_data,
    utt_count,
    gain_row,
    shift_row,
    w_in,
    kernel,
    bn_gain,
    bn_shift,
    w_out,
    frame_mask,
    frame_count,
):
    model_width = row_data.shape[1]
    frame_len = row_data.shape[0] // utt_count
    normed_b = layer_norm(row_data, gain_row, shift_row).astype(jnp.bfloat16)
    gate_pair = matmul_low(normed_b, w_in)
    mask_rows = frame_mask.reshape(-1, 1)
    gated_b = (
        (glu_gate(gate_pair) * mask_rows)
        .astype(jnp.bfloat16)
        .reshape(utt_count, frame_len, model_width)
    )
    halo_reach = (kernel.shape[1] - 1) // 2
    padded = extended(gated_b, (("seq", 1),), halo_reach)
    kernel_f = kernel.astype(jnp.float32)
    depth_out = padded[:, 0:frame_len].astype(jnp.float32) * kernel_f[:, 0]
    for tap_idx in range(1, kernel.shape[1]):
        depth_out = (
            depth_out
            + padded[:, tap_idx : tap_idx + frame_len].astype(jnp.float32) * kernel_f[:, tap_idx]
        )
    weight_mask = frame_mask[:, :, None]
    sum_local = jnp.sum(depth_out * weight_mask, axis=(0, 1))
    square_local = jnp.sum(depth_out * depth_out * weight_mask, axis=(0, 1))
    sum_all, square_all = lax.psum((sum_local, square_local), ("dp", "seq"))
    mean_val = sum_all / frame_count
    variance = square_all / frame_count - mean_val * mean_val
    inv_std = lax.rsqrt(variance + 1e-05)
    normal = (depth_out - mean_val) * inv_std * bn_gain + bn_shift
    active_b = jax.nn.silu(normal).astype(jnp.bfloat16).reshape(-1, model_width)
    branch = matmul_low(active_b, w_out)
    kept_data = (
        row_data,
        normed_b,
        gate_pair,
        padded,
        depth_out,
        mean_val,
        inv_std,
        normal,
        active_b,
    )
    return (row_data + branch, kept_data)


def conv_backward(
    grad_rows, kept_data, gain_row, shift_row, w_in, kernel, bn_gain, w_out, frame_mask, frame_count
):
    row_data, normed_b, gate_pair, padded, depth_out, mean_val, inv_std, normal, active_b = (
        kept_data
    )
    frame_len = depth_out.shape[1]
    model_width = depth_out.shape[2]
    grad_out_b = grad_rows.astype(jnp.bfloat16)
    g_out = weight_grad(active_b, grad_out_b)
    grad_active = matmul_back(grad_out_b, w_out).reshape(depth_out.shape)
    grad_normal = jax.vjp(jax.nn.silu, normal)[1](grad_active)[0]
    centred_hat = (depth_out - mean_val) * inv_std
    g_bn_gain = jnp.sum(grad_normal * centred_hat, axis=(0, 1))
    g_bn_shift = jnp.sum(grad_normal, axis=(0, 1))
    grad_hat = grad_normal * bn_gain
    part_one = jnp.sum(grad_hat, axis=(0, 1))
    part_two = jnp.sum(grad_hat * depth_out, axis=(0, 1))
    part_one, part_two = lax.psum((part_one, part_two), ("dp", "seq"))
    grad_inv = part_two - mean_val * part_one
    grad_var = -0.5 * inv_std * inv_std * inv_std * grad_inv
    grad_mean = -inv_std * part_one - 2.0 * mean_val * grad_var
    weight_mask = frame_mask[:, :, None]
    grad_depth_b = (
        grad_hat * inv_std
        + weight_mask * (grad_mean / frame_count + 2.0 * depth_out * grad_var / frame_count)
    ).astype(jnp.bfloat16)
    halo_reach = (kernel.shape[1] - 1) // 2
    grad_padded = extended(grad_depth_b, (("seq", 1),), halo_reach)
    kernel_f = kernel.astype(jnp.float32)
    grad_depth_f = grad_depth_b.astype(jnp.float32)
    grad_gated = jnp.zeros(depth_out.shape, jnp.float32)
    kernel_cols = []
    for tap_idx in range(kernel.shape[1]):
        begin_at = 2 * halo_reach - tap_idx
        grad_gated = (
            grad_gated
            + grad_padded[:, begin_at : begin_at + frame_len].astype(jnp.float32)
            * kernel_f[:, tap_idx]
        )
        kernel_cols.append(
            jnp.sum(
                padded[:, tap_idx : tap_idx + frame_len].astype(jnp.float32) * grad_depth_f,
                axis=(0, 1),
            )
        )
    g_kernel = jnp.stack(kernel_cols, axis=1)
    grad_gate_b = jax.vjp(glu_gate, gate_pair)[1](
        (grad_gated * weight_mask).reshape(-1, model_width)
    )[0]
    grad_gate_b = grad_gate_b.astype(jnp.bfloat16)
    g_in = weight_grad(normed_b, grad_gate_b)
    grad_normed = matmul_back(grad_gate_b, w_in)
    grad_ln, g_gain, g_shift = jax.vjp(layer_norm, row_data, gain_row, shift_row)[1](grad_normed)
    return (grad_rows + grad_ln, (g_gain, g_shift, g_in, g_kernel, g_bn_gain, g_bn_shift, g_out))


def layer_forward(values, weights, frame_mask, key_valid, frame_count, pos_table_b):
    (
        gain_set,
        shift_set,
        rel_set,
        up_pair,
        down_pair,
        attn_in_w,
        attn_out_w,
        pos_w,
        conv_in_w,
        kernel,
        conv_out_w,
    ) = weights
    gain_f = gain_set.astype(jnp.float32)
    shift_f = shift_set.astype(jnp.float32)
    rel_f = rel_set.astype(jnp.float32)
    utt_count = values.shape[0]
    row_data = values.reshape(-1, values.shape[2])
    row_data, kept_one = ffn_forward(row_data, gain_f[0], shift_f[0], up_pair[0], down_pair[0])
    row_data, kept_attn = attn_forward(
        row_data,
        utt_count,
        gain_f[1],
        shift_f[1],
        rel_f[0],
        rel_f[1],
        attn_in_w,
        attn_out_w,
        pos_w,
        key_valid,
        pos_table_b,
    )
    row_data, kept_conv = conv_forward(
        row_data,
        utt_count,
        gain_f[2],
        shift_f[2],
        conv_in_w,
        kernel,
        gain_f[5],
        shift_f[5],
        conv_out_w,
        frame_mask,
        frame_count,
    )
    row_data, kept_two = ffn_forward(row_data, gain_f[3], shift_f[3], up_pair[1], down_pair[1])
    result = layer_norm(row_data, gain_f[4], shift_f[4])
    return (result.reshape(values.shape), (kept_one, kept_attn, kept_conv, kept_two, row_data))


def layer_backward(
    grad_values, kept_data, weights, frame_mask, key_valid, frame_count, pos_table_b
):
    (
        gain_set,
        shift_set,
        rel_set,
        up_pair,
        down_pair,
        attn_in_w,
        attn_out_w,
        pos_w,
        conv_in_w,
        kernel,
        conv_out_w,
    ) = weights
    gain_f = gain_set.astype(jnp.float32)
    shift_f = shift_set.astype(jnp.float32)
    kept_one, kept_attn, kept_conv, kept_two, last_rows = kept_data
    grad_rows = grad_values.reshape(-1, grad_values.shape[2])
    grad_rows, g_gain_last, g_shift_last = jax.vjp(layer_norm, last_rows, gain_f[4], shift_f[4])[1](
        grad_rows
    )
    grad_rows, two_grads = ffn_backward(
        grad_rows, kept_two, gain_f[3], shift_f[3], up_pair[1], down_pair[1]
    )
    grad_rows, conv_grads = conv_backward(
        grad_rows,
        kept_conv,
        gain_f[2],
        shift_f[2],
        conv_in_w,
        kernel,
        gain_f[5],
        conv_out_w,
        frame_mask,
        frame_count,
    )
    grad_rows, attn_grads = attn_backward(
        grad_rows, kept_attn, gain_f[1], shift_f[1], attn_in_w, attn_out_w, key_valid, pos_table_b
    )
    grad_rows, one_grads = ffn_backward(
        grad_rows, kept_one, gain_f[0], shift_f[0], up_pair[0], down_pair[0]
    )
    grad_gains = jnp.stack(
        [one_grads[0], attn_grads[0], conv_grads[0], two_grads[0], g_gain_last, conv_grads[4]]
    )
    grad_shifts = jnp.stack(
        [one_grads[1], attn_grads[1], conv_grads[1], two_grads[1], g_shift_last, conv_grads[5]]
    )
    grad_rel = jnp.stack([attn_grads[2], attn_grads[3]])
    grad_up = jnp.stack([one_grads[2], two_grads[2]])
    grad_down = jnp.stack([one_grads[3], two_grads[3]])
    layer_grads = (
        grad_gains,
        grad_shifts,
        grad_rel,
        grad_up,
        grad_down,
        attn_grads[4],
        attn_grads[5],
        attn_grads[6],
        conv_grads[2],
        conv_grads[3],
        conv_grads[6],
    )
    return (grad_rows.reshape(grad_values.shape), layer_grads)


def gather_forward(shards, layer_idx):
    pieces = tuple((member[layer_idx] for member in shards))
    return (
        lax.all_gather(pieces[0], ("dp", "seq"), axis=1, tiled=True),
        lax.all_gather(pieces[1], ("dp", "seq"), axis=1, tiled=True),
        lax.all_gather(pieces[2], ("dp", "seq"), axis=1, tiled=True),
        lax.all_gather(pieces[3], ("dp", "seq"), axis=1, tiled=True),
        lax.all_gather(pieces[4], ("dp", "seq"), axis=1, tiled=True),
        lax.all_gather(pieces[5], ("dp", "seq"), axis=0, tiled=True),
        lax.all_gather(pieces[6], ("dp", "seq"), axis=0, tiled=True),
        lax.all_gather(pieces[7], ("dp", "seq"), axis=0, tiled=True),
        lax.all_gather(pieces[8], ("dp", "seq"), axis=0, tiled=True),
        lax.all_gather(pieces[9], ("dp", "seq"), axis=0, tiled=True),
        lax.all_gather(pieces[10], ("dp", "seq"), axis=0, tiled=True),
    )


def gather_backward(shards, layer_idx):
    pieces = tuple((member[layer_idx] for member in shards))
    return (
        lax.all_gather(pieces[0], ("dp", "seq"), axis=1, tiled=True),
        lax.all_gather(pieces[1], ("dp", "seq"), axis=1, tiled=True),
        lax.all_gather(pieces[2], ("dp", "seq"), axis=1, tiled=True),
        lax.all_gather(pieces[3], ("dp", "seq"), axis=1, tiled=True),
        lax.all_gather(pieces[4], ("dp", "seq"), axis=1, tiled=True),
        lax.all_gather(pieces[5], ("dp", "seq"), axis=0, tiled=True),
        lax.all_gather(pieces[6], ("dp", "seq"), axis=0, tiled=True),
        lax.all_gather(pieces[7], ("dp", "seq"), axis=0, tiled=True),
        lax.all_gather(pieces[8], ("dp", "seq"), axis=0, tiled=True),
        lax.all_gather(pieces[9], ("dp", "seq"), axis=0, tiled=True),
        lax.all_gather(pieces[10], ("dp", "seq"), axis=0, tiled=True),
    )


def local_general(
    frames,
    lengths,
    cotangent,
    gains,
    shifts,
    rel_bias,
    ffn_up,
    ffn_down,
    attn_in,
    attn_out,
    pos_proj,
    conv_in,
    depthwise,
    conv_out,
):
    shards = (
        gains,
        shifts,
        rel_bias,
        ffn_up,
        ffn_down,
        attn_in,
        attn_out,
        pos_proj,
        conv_in,
        depthwise,
        conv_out,
    )
    groups = lax.axis_size("dp")
    seq_devices = lax.axis_size("seq")
    local_utts = frames.shape[0]
    frame_len = frames.shape[1]
    model_width = frames.shape[2]
    utt_per = local_utts // MB
    length = frame_len * seq_devices
    seq_start = lax.axis_index("seq") * frame_len
    first_utt = lax.axis_index("dp") * local_utts
    own_lengths = lax.dynamic_slice_in_dim(lengths, first_utt, local_utts)
    lengths_grid = lengths.reshape(groups, MB, utt_per)
    offsets = seq_start + frame_len - 1 - jnp.arange(length + frame_len - 1, dtype=jnp.int32)
    pos_table_b = sinusoid(offsets, model_width).astype(jnp.bfloat16)
    frame_pos = seq_start + jnp.arange(frame_len, dtype=jnp.int32)
    key_pos = jnp.arange(length, dtype=jnp.int32)
    result_list = []
    grad_list = []
    full_sums = [None] * NL
    for micro_idx in range(MB):
        lens_here = own_lengths[micro_idx * utt_per : (micro_idx + 1) * utt_per]
        frame_mask = (frame_pos[None, :] < lens_here[:, None]).astype(jnp.float32)
        key_valid = key_pos[None, :] < lens_here[:, None]
        frame_count = jnp.sum(lengths_grid[:, micro_idx]).astype(jnp.float32)
        values = frames[micro_idx * utt_per : (micro_idx + 1) * utt_per]
        held_weights = []
        layer_idx = 0
        weights = gather_forward(shards, layer_idx)
        values, kept_data = layer_forward(
            values, weights, frame_mask, key_valid, frame_count, pos_table_b
        )
        saved_acts = [kept_data]
        held_weights.append(weights)
        result_list.append(values)
        grad_values = cotangent[micro_idx * utt_per : (micro_idx + 1) * utt_per]
        for layer_idx in reversed(range(NL)):
            weights = gather_backward(shards, layer_idx)
            grad_values, layer_grads = layer_backward(
                grad_values,
                saved_acts[layer_idx],
                weights,
                frame_mask,
                key_valid,
                frame_count,
                pos_table_b,
            )
            if full_sums[layer_idx] is None:
                full_sums[layer_idx] = layer_grads
            else:
                full_sums[layer_idx] = jax.tree.map(jnp.add, full_sums[layer_idx], layer_grads)
        grad_list.append(grad_values)
    stacked = tuple((jnp.stack([full_sums[0][member]]) for member in range(11)))
    final_grads = (
        lax.psum_scatter(stacked[0], ("dp", "seq"), scatter_dimension=2, tiled=True),
        lax.psum_scatter(stacked[1], ("dp", "seq"), scatter_dimension=2, tiled=True),
        lax.psum_scatter(stacked[2], ("dp", "seq"), scatter_dimension=2, tiled=True),
        lax.psum_scatter(stacked[3], ("dp", "seq"), scatter_dimension=2, tiled=True),
        lax.psum_scatter(stacked[4], ("dp", "seq"), scatter_dimension=2, tiled=True),
        lax.psum_scatter(stacked[5], ("dp", "seq"), scatter_dimension=1, tiled=True),
        lax.psum_scatter(stacked[6], ("dp", "seq"), scatter_dimension=1, tiled=True),
        lax.psum_scatter(stacked[7], ("dp", "seq"), scatter_dimension=1, tiled=True),
        lax.psum_scatter(stacked[8], ("dp", "seq"), scatter_dimension=1, tiled=True),
        lax.psum_scatter(stacked[9], ("dp", "seq"), scatter_dimension=1, tiled=True),
        lax.psum_scatter(stacked[10], ("dp", "seq"), scatter_dimension=1, tiled=True),
    )
    mixed = jnp.concatenate(result_list, axis=0)
    grad_frames = jnp.concatenate(grad_list, axis=0)
    return (
        mixed,
        grad_frames,
        final_grads[0],
        final_grads[1],
        final_grads[2],
        final_grads[3],
        final_grads[4],
        final_grads[5],
        final_grads[6],
        final_grads[7],
        final_grads[8],
        final_grads[9],
        final_grads[10],
    )


NT = (((1,), (1,)), ((), ()))
TN = (((0,), (0,)), ((), ()))
NN = (((1,), (0,)), ((), ()))
MESH = pl.DeviceIdType.MESH
UTTS = 4
SMALL = 128
STRIP = 64
VMEM_LIMIT = 60 * 1024 * 1024


def fits_whole(mesh):
    return mesh.shape["dp"] == 4 and mesh.shape["seq"] == MB * UTTS


def dotf(left, right, dims=NN):
    return lax.dot_general(left, right, dims, preferred_element_type=jnp.float32)


def place():
    dp = lax.axis_index("dp")
    sq = lax.axis_index("seq")
    return dp, sq, lax.div(dp, 2), lax.rem(dp, 2), lax.div(sq, 2), lax.rem(sq, 2)


def flip_if(value, bit):
    return 1 - value if bit else value


def partners():
    dp, sq, x, c, z, y = place()
    even = c == 0
    core = (x * 2 + 1 - c, sq)
    xdev = ((1 - x) * 2 + c, sq)
    ydev = (dp, z * 2 + 1 - y)
    first = (jnp.where(even, ydev[0], xdev[0]), jnp.where(even, ydev[1], xdev[1]))
    second = (jnp.where(even, xdev[0], ydev[0]), jnp.where(even, xdev[1], ydev[1]))
    return core, xdev, first, second, ydev


def rank_of(color, a, b, k, fixed=False):
    _, _, x, _, z, y = place()
    even = jnp.logical_or(color == 0, fixed)
    xx = jnp.where(even, x + a * (1 - 2 * x), x + b * (1 - 2 * x))
    yy = jnp.where(even, y + b * (1 - 2 * y), y + a * (1 - 2 * y))
    return xx * 16 + color * 8 + lax.rem(z + k, 4) * 2 + yy


def greet(devices):
    barrier = pltpu.get_barrier_semaphore()
    for device in devices:
        pl.semaphore_signal(barrier, inc=1, device_id=device, device_id_type=MESH)
    pl.semaphore_wait(barrier, len(devices))


def seq_peers(dp, sq, count):
    return [(dp, lax.rem(sq + k, count)) for k in range(1, count)]


def remote(src, dst, send, recv, device):
    return pltpu.make_async_remote_copy(
        src_ref=src, dst_ref=dst, send_sem=send, recv_sem=recv, device_id=device, device_id_type=MESH
    )


def alternate(a, b, k):
    return a * 8 + b * 4 + k


def gather_steps(w_ref, d_ref, w_all, d_all, send, recv, own):
    wr, dr = w_ref.shape[0], d_ref.shape[0]
    started = []

    def blocks(w_rank, d_rank):
        return (
            w_all.at[pl.ds(pl.multiple_of(w_rank * wr, 16), wr), :],
            d_all.at[pl.ds(pl.multiple_of(d_rank * dr, 16), dr), :],
        )

    def pair(group, target, slot, landing_slot, mine, other):
        dp, sq, _, c, z, y = place()
        core, xdev, first, second, ydev = partners()
        along_z = (dp, lax.rem(z + target, 4) * 2 + y) if isinstance(target, int) else None
        w_to = {"core": core, "first": first, "second": second}.get(target, along_z)
        d_to = {"core": core, "first": ydev, "second": xdev}.get(target, along_z)
        color = 1 - c if other else c
        w_dst, d_dst = blocks(rank_of(color, *group), rank_of(color, *group, fixed=True))
        w_src, d_src = (w_ref, d_ref) if mine else (w_dst, d_dst)
        return (
            remote(w_src, w_dst, send.at[0, slot], recv.at[0, landing_slot], w_to),
            remote(d_src, d_dst, send.at[1, slot], recv.at[1, landing_slot], d_to),
        )

    def ship(group, target, slot, landing_slot, mine=False):
        spec = (group, target, slot, landing_slot, mine, False)
        for copy in pair(*spec):
            copy.start()
        started.append(spec)

    def arrive(group, other=False):
        for copy in pair(group, "core", 0, alternate(*group) + (16 if other else 0), False, other):
            copy.wait_recv()

    def to_core(group, mine=False):
        spot = 16 + alternate(*group)
        ship(group, "core", spot, spot, mine)

    def own_copies():
        _, _, _, c, _, _ = place()
        mine = rank_of(c, 0, 0, 0)
        w_own, d_own = blocks(mine, mine)
        return (
            pltpu.make_async_copy(w_ref, w_own, own.at[0]),
            pltpu.make_async_copy(d_ref, d_own, own.at[1]),
        )

    def begin():
        mine = (0, 0, 0)
        ship(mine, "second", 15, 8, mine=True)
        ship(mine, "first", 3, 4, mine=True)
        for k in (1, 3, 2):
            ship(mine, k, k - 1, 4 - k, mine=True)
        to_core(mine, mine=True)
        for copy in own_copies():
            copy.start()

    def along(k):
        group = (0, 0, k)
        arrive(group)
        ship(group, "second", 8 + k - 1, 8 + k)
        ship(group, "first", 4 + k - 1, 4 + k)
        to_core(group)

    def across(k):
        group = (0, 1, k)
        arrive(group)
        ship(group, "second", 11 + k, 12 + k)
        to_core(group)

    def over(k):
        for b in (0, 1):
            group = (1, b, k)
            arrive(group)
            to_core(group)

    def finish():
        for k in (0, 1, 3, 2):
            for a, b in ((0, 0), (0, 1), (1, 0), (1, 1)):
                arrive((a, b, k), other=True)
        for copy in own_copies():
            copy.wait()
        for spec in started:
            for copy in pair(*spec):
                copy.wait_send()

    return begin, along, across, over, finish


def meeting(count):
    dp, sq, *_ = place()
    core, xdev, *_ = partners()
    greet(seq_peers(dp, sq, count) + [core, xdev])


def tree_scratch():
    return [
        pltpu.SemaphoreType.DMA((2, 32)),
        pltpu.SemaphoreType.DMA((2, 32)),
        pltpu.SemaphoreType.DMA((2,)),
    ]


def gather_kernel(w_ref, d_ref, f_ref, w_all, d_all, f_all, send, recv, own, row_send, row_recv, row_own):
    meeting(f_ref.shape[0])
    begin, along, across, over, finish = gather_steps(w_ref, d_ref, w_all, d_all, send, recv, own)
    begin()
    across(0)
    along(1)
    along(3)
    across(1)
    along(2)
    rows_begin(f_ref, f_all, row_send, row_recv, row_own)
    across(3)
    over(0)
    across(2)
    over(1)
    over(3)
    over(2)
    finish()
    rows_end(f_ref, f_all, row_send, row_recv, row_own)


def gathered(w, d):
    return [
        jax.ShapeDtypeStruct((w.shape[0] * 32, w.shape[1]), w.dtype),
        jax.ShapeDtypeStruct((d.shape[0] * 32, d.shape[1]), d.dtype),
    ]


def gather_all(w, d, f):
    vm = pl.BlockSpec(memory_space=pltpu.VMEM)
    hbm = pl.BlockSpec(memory_space=pl.ANY)
    return pl.pallas_call(
        gather_kernel,
        in_specs=[vm] * 3,
        out_specs=[hbm] * 3,
        out_shape=gathered(w, d) + [jax.ShapeDtypeStruct(f.shape, f.dtype)],
        scratch_shapes=tree_scratch() + row_scratch(f.shape[0]),
        compiler_params=pltpu.CompilerParams(collective_id=0, has_side_effects=True),
        name="gather_all",
    )(w, d, f)


def scatter_steps(w_ref, d_ref, w_out, d_out, bufs, send, recv):
    w0, d0, w1, d1, w2, d2, w3, d3 = bufs
    wr, dr = w_out.shape[0], d_out.shape[0]

    def rows(rank, size):
        return pl.ds(pl.multiple_of(rank * size, 16), size)

    def group_ranks(slot, other):
        _, _, _, c, _, _ = place()
        group = (1 - c if other else c, lax.div(slot, 8), lax.rem(lax.div(slot, 4), 2), lax.rem(slot, 4))
        return rank_of(*group), rank_of(*group, fixed=True)

    def core_copies(slot):
        core = partners()[0]
        w_rank, d_rank = group_ranks(slot, True)
        return (
            remote(w_ref.at[rows(w_rank, wr), :], w0.at[slot], send.at[0, slot], recv.at[0, slot], core),
            remote(d_ref.at[rows(d_rank, dr), :], d0.at[slot], send.at[1, slot], recv.at[1, slot], core),
        )

    def second_copies(slot):
        _, xdev, _, to, _ = partners()
        return (
            remote(w0.at[8 + slot], w1.at[slot], send.at[0, 16 + slot], recv.at[0, 16 + slot], to),
            remote(d0.at[8 + slot], d1.at[slot], send.at[1, 16 + slot], recv.at[1, 16 + slot], xdev),
        )

    def first_copies(slot):
        _, _, to, _, ydev = partners()
        return (
            remote(w0.at[4 + slot], w2.at[slot], send.at[0, 24 + slot], recv.at[0, 24 + slot], to),
            remote(d0.at[4 + slot], d2.at[slot], send.at[1, 24 + slot], recv.at[1, 24 + slot], ydev),
        )

    def z_copies(k):
        dp, _, _, _, z, y = place()
        to = (dp, lax.rem(z + k, 4) * 2 + y)
        return (
            remote(w0.at[k], w3.at[3 - k], send.at[0, 27 + k], recv.at[0, 31 - k], to),
            remote(d0.at[k], d3.at[3 - k], send.at[1, 27 + k], recv.at[1, 31 - k], to),
        )

    def start(copies):
        for copy in copies:
            copy.start()

    def landed(copies):
        for copy in copies:
            copy.wait_recv()

    def sent(copies):
        for copy in copies:
            copy.wait_send()

    def add_to(buf, slot, more):
        buf[slot] = (buf[slot].astype(jnp.float32) + more.astype(jnp.float32)).astype(jnp.bfloat16)

    def add(slot, w, d):
        add_to(w0, slot, w)
        add_to(d0, slot, d)

    def spot_of(step):
        return (1 - lax.rem(step, 2)) * 4 + 3 - lax.div(step, 2)

    def begin(parts=(0, 1)):
        @pl.loop(0, 16)
        def _(step):
            copies = core_copies(8 * (1 - lax.div(step, 8)) + spot_of(lax.rem(step, 8)))
            for part in parts:
                copies[part].start()

    def take(slot, parts=(0, 1)):
        copies = core_copies(slot)
        w_rank, d_rank = group_ranks(slot, False)
        for part in parts:
            copies[part].wait_recv()
        if 0 in parts:
            add_to(w0, slot, w_ref[rows(w_rank, wr), :])
        if 1 in parts:
            add_to(d0, slot, d_ref[rows(d_rank, dr), :])

    def far(lo, hi, parts=(0, 1)):
        @pl.loop(lo, hi)
        def _(step):
            spot = spot_of(step)
            take(8 + spot, parts)
            copies = second_copies(spot)
            for part in parts:
                copies[part].start()

    def join(k):
        take(4 + k)
        landed(second_copies(4 + k))
        add(4 + k, w1[4 + k], d1[4 + k])
        start(first_copies(k))
        take(k)
        landed(second_copies(k))
        add(k, w1[k], d1[k])

    def onward(k):
        landed(first_copies(k))
        add(k, w2[k], d2[k])
        start(z_copies(k))

    def near(step):
        join(3 - step)

        @pl.when(step >= 1)
        def _():
            onward(4 - step)

    def total(base, parts):
        value = base.astype(jnp.float32)
        for part in parts:
            value = value + part.astype(jnp.float32)
        return value

    def finish():
        landed(first_copies(0))
        for k in (1, 2, 3):
            landed(z_copies(k))
        w_out[...] = total(w0[0], (w2[0], w3[0], w3[1], w3[2]))
        d_out[...] = total(d0[0], (d2[0], d3[0], d3[1], d3[2]))

        @pl.loop(0, 16)
        def _(slot):
            sent(core_copies(slot))

        @pl.loop(0, 8)
        def _(slot):
            sent(second_copies(slot))

        @pl.loop(0, 4)
        def _(slot):
            sent(first_copies(slot))

        for k in (1, 2, 3):
            sent(z_copies(k))

    return begin, far, near, finish


def scatter_scratch(w, d):
    bf = jnp.bfloat16
    scratch = []
    for n in (16, 8, 4, 3):
        scratch += [
            pltpu.VMEM((n, w.shape[0] // 32, w.shape[1]), bf),
            pltpu.VMEM((n, d.shape[0] // 32, d.shape[1]), bf),
        ]
    return scratch + tree_scratch()[:2]


def scattered(w, d):
    return [
        jax.ShapeDtypeStruct((w.shape[0] // 32, w.shape[1]), jnp.float32),
        jax.ShapeDtypeStruct((d.shape[0] // 32, d.shape[1]), jnp.float32),
    ]


def rows_begin(src, dst, send, recv, own):
    _, sq, *_ = place()
    for k in range(1, dst.shape[0]):
        row_copy(src, dst, send, recv, k).start()
    pltpu.make_async_copy(block_of(src, sq, dst), dst.at[sq], own).start()


def rows_end(src, dst, send, recv, own):
    dp, sq, *_ = place()
    count = dst.shape[0]
    for k in range(1, count):
        copy = row_copy(src, dst, send, recv, k)
        copy.wait_send()
        landing(src, dst, send, recv, k).wait_recv()
    pltpu.make_async_copy(block_of(src, sq, dst), dst.at[sq], own).wait()


def row_copy(src, dst, send, recv, k):
    dp, sq, *_ = place()
    count = dst.shape[0]
    to = lax.rem(sq + k, count)
    return remote(block_of(src, to, dst), dst.at[sq], send.at[k - 1], recv.at[count - 1 - k], (dp, to))


def block_of(src, index, dst):
    width = dst.shape[1]
    return src.at[pl.ds(pl.multiple_of(index * width, 16), width), :] if len(src.shape) == 2 else src.at[index]


def landing(src, dst, send, recv, k):
    dp, sq, *_ = place()
    origin = lax.rem(sq + k, dst.shape[0])
    return remote(block_of(src, sq, dst), dst.at[origin], send.at[k - 1], recv.at[k - 1], (dp, origin))


def norm_parts(rows):
    centred = rows - jnp.mean(rows, axis=1, keepdims=True)
    return centred, lax.rsqrt(jnp.mean(centred * centred, axis=1, keepdims=True) + 1e-05)


def norm(rows, gain, shift):
    centred, inv = norm_parts(rows)
    return centred * inv * gain + shift


def silu(h):
    return h * (1.0 / (1.0 + jnp.exp(-h)))


def front_kernel(
    len_ref, f_ref, in_ref, pos_ref, up_ref, small_ref, down_ref, table_ref, c_ref, w_ref, d_ref,
    ctx_ref, p_ref, x1_ref, qu_ref, qv_ref, k_ref, v_ref, t_ref, sm_ref, c_all, w_all, d_all,
    send, recv, own, row_send, row_recv, row_own, *, tq, tile,
):
    low = jnp.bfloat16
    keys, model = f_ref.shape
    span = keys + tq
    steps = keys // tq
    begin, along, across, over, finish = gather_steps(w_ref, d_ref, w_all, d_all, send, recv, own)

    def dense(i):
        rows = pl.ds(pl.multiple_of(i * tile, tile), tile)
        x0 = f_ref[rows, :].astype(jnp.float32)
        a0 = norm(x0, sm_ref[0:1, :], sm_ref[6:7, :]).astype(low)
        z = silu(dotf(a0, up_ref[...])).astype(low)
        x1 = x0 + 0.5 * dotf(z, down_ref[...])
        x1_ref[rows, :] = x1
        a1 = norm(x1, sm_ref[1:2, :], sm_ref[7:8, :]).astype(low)
        query = dotf(a1, in_ref[:, :model])
        qu_ref[rows, :] = (query + sm_ref[12:13, :]).astype(low)
        qv_ref[rows, :] = (query + sm_ref[13:14, :]).astype(low)
        k_ref[rows, :] = dotf(a1, in_ref[:, model : 2 * model]).astype(low)
        v_ref[rows, :] = dotf(a1, in_ref[:, 2 * model :]).astype(low)

    @pl.when(pl.program_id(0) == 0)
    def _():
        meeting(c_ref.shape[0])
        begin()
        sm_ref[...] = small_ref[...].astype(jnp.float32).T

        @pl.loop(0, 2 * keys // tile)
        def _(i):
            rows = pl.ds(pl.multiple_of(i * tile, tile), tile)
            t_ref[rows, :] = dotf(table_ref[rows, :], pos_ref[...]).astype(low)

        @pl.loop(0, keys // tile)
        def _(i):
            dense(i)

            @pl.when(i == 0)
            def _():
                across(0)
                along(1)

            @pl.when(i == 1)
            def _():
                along(3)
                across(1)

            @pl.when(i == 2)
            def _():
                along(2)
                rows_begin(c_ref, c_all, row_send, row_recv, row_own)

    plan = {1: ((across, 3), (over, 0)), 3: ((across, 2),), 5: ((over, 1),), 8: ((over, 3),), 11: ((over, 2),)}
    dp, sq, *_ = place()
    valid = lax.broadcasted_iota(jnp.int32, (1, keys), 1) < len_ref[dp * (MB * UTTS) + sq]
    base = pl.program_id(0) * 128

    @pl.loop(0, steps)
    def _(i):
        time = pl.program_id(0) * steps + i
        for at, todo in plan.items():

            @pl.when(time == at)
            def _():
                for step, k in todo:
                    step(k)

        rows = pl.ds(pl.multiple_of(i * tq, tq), tq)
        band = pl.ds(pl.multiple_of(keys - tq - i * tq, tq), span)
        pair = pl.ds(pl.multiple_of(base, 128), 128)
        qu, qv, k, v, t = qu_ref[rows, pair], qv_ref[rows, pair], k_ref[:, pair], v_ref[:, pair], t_ref[band, pair]
        for h in range(2):
            cols = slice(h * DH, (h + 1) * DH)
            content = dotf(qu[:, cols], k[:, cols], NT)
            raw = dotf(qv[:, cols], t[:, cols], NT)
            pos = pltpu.roll(raw, keys + 1, 1, stride=1, stride_axis=0)[:, :keys]
            s = jnp.where(valid, (content + pos) * 0.125, -1e30)
            e = jnp.exp(s - jnp.max(s, axis=1, keepdims=True))
            p = (e * (1.0 / jnp.sum(e, axis=1, keepdims=True))).astype(low)
            p_ref[h, rows, :] = p
            ctx_ref[rows, cols] = dotf(p, v[:, cols]).astype(low)

    @pl.when(pl.program_id(0) == pl.num_programs(0) - 1)
    def _():
        finish()
        rows_end(c_ref, c_all, row_send, row_recv, row_own)


def row_scratch(count):
    return [
        pltpu.SemaphoreType.DMA((count - 1,)),
        pltpu.SemaphoreType.DMA((count - 1,)),
        pltpu.SemaphoreType.DMA,
    ]


def front(length, f, w_early, cuts, down, table_in, cot, w, d, tq=256, tile=256):
    rows, model = f.shape
    low = jnp.bfloat16
    vm = pl.BlockSpec(memory_space=pltpu.VMEM)
    hbm = pl.BlockSpec(memory_space=pl.ANY)

    def window(lo, hi):
        return pl.BlockSpec((w_early.shape[0], hi - lo), lambda h, *_: (0, lo // (hi - lo)), pipeline_mode=pl.Buffered(1))

    one = jax.ShapeDtypeStruct((rows, model), low)
    return pl.pallas_call(
        lambda *refs: front_kernel(*refs, tq=tq, tile=tile),
        grid_spec=pltpu.PrefetchScalarGridSpec(
            num_scalar_prefetch=1,
            grid=(model // 128,),
            in_specs=[vm] + [window(lo, hi) for lo, hi in zip(cuts[:-1], cuts[1:])] + [vm] * 5,
            out_specs=[
                pl.BlockSpec((rows, 128), lambda h, *_: (0, h)),
                pl.BlockSpec((2, rows, rows), lambda h, *_: (h, 0, 0)),
            ]
            + [vm] * 7
            + [hbm] * 3,
            scratch_shapes=tree_scratch() + row_scratch(cot.shape[0]),
        ),
        out_shape=[
            one,
            jax.ShapeDtypeStruct((model // DH, rows, rows), low),
            jax.ShapeDtypeStruct((rows, model), jnp.float32),
            one,
            one,
            one,
            one,
            jax.ShapeDtypeStruct((2 * rows, model), low),
            jax.ShapeDtypeStruct((SMALL, model), jnp.float32),
            jax.ShapeDtypeStruct(cot.shape, cot.dtype),
        ]
        + gathered(w, d),
        compiler_params=pltpu.CompilerParams(
            collective_id=4, has_side_effects=True, vmem_limit_bytes=VMEM_LIMIT
        ),
        name="front",
    )(length, f, *[w_early] * (len(cuts) - 1), down, table_in, cot, w, d)


def norm_back(rows, gain, grad):
    centred, inv = norm_parts(rows)
    hat = centred * inv
    scaled = grad * gain
    inner = jnp.mean(scaled * hat, axis=1, keepdims=True)
    out = inv * (scaled - jnp.mean(scaled, axis=1, keepdims=True) - hat * inner)
    return out, hat, jnp.sum(grad * hat, axis=0, keepdims=True)


def back_kernel(
    p_ref, g_ref, qu_ref, qv_ref, k_ref, v_ref, t_ref,
    m_ref, w_ref, d_ref, x1_ref, f_ref, grad_ref, sm_ref, gs_ref, in_ref, up_ref, down_ref, table_ref,
    m_all, w_out, d_out, g_all, e_out, l_out,
    ge_ref, gd_ref, rows_ref, ds_sc, dt_sc, dproj_sc, dtab_sc, z_sc, dh_sc, a0_sc, a1_sc, go_sc, gs_sc, *scratch, tq, tile,
):
    bufs, (send, recv, send_2, recv_2), rows_m, rows_g = scratch[:8], scratch[8:12], scratch[12:15], scratch[15:]
    wide = w_ref.shape[1]
    trimmed = [buf.at[:, :, :wide] if j % 2 == 0 else buf for j, buf in enumerate(bufs)]
    begin, far, near, finish = scatter_steps(w_ref, d_ref, w_out, d_out, trimmed, send, recv)
    again = scatter_steps(ge_ref, gd_ref, e_out, l_out, bufs, send_2, recv_2)
    low = jnp.bfloat16
    keys = k_ref.shape[0]
    model = f_ref.shape[1]
    span = keys + tq
    steps = keys // tq

    def open_up():
        meeting(m_ref.shape[0])
        begin()
        gs_sc[...] = gs_ref[...]

    plan = {
        0: open_up,
        1: lambda: far(0, 4),
        2: lambda: far(4, 8),
        5: lambda: rows_begin(m_ref, m_all, *rows_m),
    }
    flip = (
        lax.broadcasted_iota(jnp.int32, (tq, tq), 0) + lax.broadcasted_iota(jnp.int32, (tq, tq), 1) == tq - 1
    ).astype(low)
    pad = jnp.zeros((tq, tq), jnp.float32)
    dt_sc[...] = jnp.zeros_like(dt_sc)
    base = pl.program_id(0) * 128

    def at(offset):
        return pl.ds(pl.multiple_of(base + offset, 128), 128)

    @pl.loop(0, steps)
    def _(i):
        time = pl.program_id(0) * steps + i
        for moment, step in plan.items():
            pl.when(time == moment)(step)
        due = jnp.logical_and(jnp.logical_and(time >= 4, time <= 10), lax.rem(time, 2) == 0)

        @pl.when(due)
        def _():
            near(lax.div(time, 2) - 2)

        rows = pl.ds(pl.multiple_of(i * tq, tq), tq)
        band = pl.ds(pl.multiple_of(keys - tq - i * tq, tq), span)
        sides = []
        for h in range(2):
            cols = slice(h * DH, (h + 1) * DH)
            dp = dotf(g_ref[rows, cols], v_ref[:, cols], NT)
            pf = p_ref[h, rows, :].astype(jnp.float32)
            ds = (pf * (dp - jnp.sum(dp * pf, axis=1, keepdims=True))).astype(low)
            ds_sc[h, rows, :] = ds
            dqu = dotf(ds, k_ref[:, cols]) * 0.125
            turned = jnp.concatenate([dotf(flip, ds), pad], axis=1)
            raw = pltpu.roll(turned, 0, 1, stride=1, stride_axis=0).astype(low)
            dqv = dotf(flip, dotf(raw, t_ref[band, cols]).astype(low)) * 0.125
            qv = dotf(flip, qv_ref[rows, cols]).astype(low)
            dt_sc[h, band, :] += dotf(raw, qv, TN)
            sides.append((dqu, dqv))
        dqu, dqv = (jnp.concatenate(both, axis=1) for both in zip(*sides))
        gs_sc[12:13, at(0)] += jnp.sum(dqu, axis=0, keepdims=True)
        gs_sc[13:14, at(0)] += jnp.sum(dqv, axis=0, keepdims=True)
        dproj_sc[rows, at(0)] = (dqu + dqv).astype(low)

    halves = []
    for h in range(2):
        cols = slice(h * DH, (h + 1) * DH)
        halves.append(
            (
                dt_sc[h] * 0.125,
                dotf(ds_sc[h], qu_ref[:, cols], TN) * 0.125,
                dotf(p_ref[h], g_ref[:, cols], TN),
            )
        )
    dtab, dk, dv = (jnp.concatenate(both, axis=1).astype(low) for both in zip(*halves))
    dtab_sc[:, at(0)] = dtab
    dproj_sc[:, at(model)] = dk
    dproj_sc[:, at(2 * model)] = dv

    @pl.when(pl.program_id(0) == pl.num_programs(0) - 1)
    def _():
        @pl.loop(0, keys // tile)
        def _(i):
            rows = pl.ds(pl.multiple_of(i * tile, tile), tile)
            dn = dotf(dproj_sc[rows, :], in_ref[...], NT)
            dx, hat, dgain = norm_back(x1_ref[rows, :], sm_ref[1:2, :], dn)
            gs_sc[1:2, :] += dgain
            gs_sc[7:8, :] += jnp.sum(dn, axis=0, keepdims=True)
            a1_sc[rows, :] = (hat * sm_ref[1:2, :] + sm_ref[7:8, :]).astype(low)
            grad = grad_ref[rows, :] + dx
            go = (0.5 * grad).astype(low)
            go_sc[rows, :] = go
            x0 = f_ref[rows, :].astype(jnp.float32)
            a0 = norm(x0, sm_ref[0:1, :], sm_ref[6:7, :]).astype(low)
            a0_sc[rows, :] = a0
            h = dotf(a0, up_ref[...])
            sig = 1.0 / (1.0 + jnp.exp(-h))
            z_sc[rows, :] = (h * sig).astype(low)
            dh = (dotf(go, down_ref[...], NT) * (sig * (1.0 + h * (1.0 - sig)))).astype(low)
            dh_sc[rows, :] = dh
            dn = dotf(dh, up_ref[...], NT)
            dx, _, dgain = norm_back(x0, sm_ref[0:1, :], dn)
            gs_sc[0:1, :] += dgain
            gs_sc[6:7, :] += jnp.sum(dn, axis=0, keepdims=True)
            rows_ref[rows, :] = (grad + dx).astype(low)

        rows_begin(rows_ref, g_all, *rows_g)
        width = model

        def piece(j):
            return pl.ds(pl.multiple_of(j * width, width), width)

        @pl.loop(0, 4)
        def _(j):
            gd_ref[piece(j), :] = dotf(z_sc[:, piece(j)], go_sc[...], TN).astype(low)

        finish()
        rows_end(m_ref, m_all, *rows_m)
        meeting(m_ref.shape[0])
        begin_2, far_2, near_2, end = again
        begin_2((1,))
        far_2(0, 4, (1,))

        @pl.loop(0, 3)
        def _(j):
            ge_ref[:, piece(j)] = dotf(a1_sc[...], dproj_sc[:, piece(j)], TN).astype(low)

        far_2(4, 8, (1,))
        ge_ref[:, 3 * width : 4 * width] = dotf(table_ref[...], dtab_sc[...], TN).astype(low)

        @pl.loop(0, 4)
        def _(j):
            ge_ref[:, piece(j + 4)] = dotf(a0_sc[...], dh_sc[:, piece(j)], TN).astype(low)

        ge_ref[:, 8 * width :] = gs_sc[...].T.astype(low)
        begin_2((0,))
        far_2(0, 8, (0,))
        pl.loop(0, 4)(near_2)
        end()
        rows_end(rows_ref, g_all, *rows_g)


def back(
    p, g, qu, qv, k, v, table, mixed, w, d, x1, f, grad, small, g_small, w_early, cuts, down, table_in, tq=256, tile=256
):
    rows, model = qu.shape
    low = jnp.bfloat16
    vm = pl.BlockSpec(memory_space=pltpu.VMEM)
    hbm = pl.BlockSpec(memory_space=pl.ANY)
    blk = pl.BlockSpec((rows, 128), lambda h: (0, h))
    tab = pl.BlockSpec((2 * rows, 128), lambda h: (0, h))

    def window(j):
        lo, hi = cuts[j], cuts[j + 1]
        return pl.BlockSpec((w_early.shape[0], hi - lo), lambda h: (0, lo // (hi - lo)), pipeline_mode=pl.Buffered(1))

    hidden = down.shape[0]
    return pl.pallas_call(
        lambda *refs: back_kernel(*refs, tq=tq, tile=tile),
        grid=(model // 128,),
        in_specs=[pl.BlockSpec((2, rows, rows), lambda h: (h, 0, 0))]
        + [blk] * 5
        + [tab]
        + [vm] * 8
        + [window(0), window(2), vm, vm],
        out_specs=[hbm, vm, vm, hbm, vm, vm],
        out_shape=[jax.ShapeDtypeStruct(mixed.shape, low)]
        + scattered(w, d)
        + [jax.ShapeDtypeStruct(mixed.shape, low)]
        + scattered(w_early, down),
        scratch_shapes=[
            pltpu.VMEM(w_early.shape, low),
            pltpu.VMEM(down.shape, low),
            pltpu.VMEM((rows, model), low),
            pltpu.VMEM((2, rows, rows), low),
            pltpu.VMEM((2, 2 * rows, DH), jnp.float32),
            pltpu.VMEM((rows, 3 * model), low),
            pltpu.VMEM((2 * rows, model), low),
            pltpu.VMEM((rows, hidden), low),
            pltpu.VMEM((rows, hidden), low),
            pltpu.VMEM((rows, model), low),
            pltpu.VMEM((rows, model), low),
            pltpu.VMEM((rows, model), low),
            pltpu.VMEM((SMALL, model), jnp.float32),
        ]
        + scatter_scratch(w_early, down)
        + tree_scratch()[:2]
        + row_scratch(mixed.shape[0])
        + row_scratch(mixed.shape[0]),
        compiler_params=pltpu.CompilerParams(
            collective_id=5, has_side_effects=True, vmem_limit_bytes=63 * 1024 * 1024
        ),
        name="back",
    )(p, g, qu, qv, k, v, table, mixed, w, d, x1, f, grad, small, g_small, w_early, w_early, down, table_in)


def sigmoid(h):
    return 1.0 / (1.0 + jnp.exp(-h))


def middle_kernel(
    len_ref, ctx_ref, x1_ref, w_ref, down_ref, cot_ref, sm_ref,
    mixed_ref, grad_ref, gctx_ref, gw_ref, gd_ref, gs_ref,
    x2_sc, a2_sc, gate_sc, gl_sc, dep_sc, act_sc, a3_sc, z_sc, dh_sc, go_sc, gob_sc, e_sc, dd_sc, tap_sc, win_sc,
    part_sc, peer_sc, send, recv, *, tile, taps,
):
    low = jnp.bfloat16
    f32 = jnp.float32
    length, model = x1_ref.shape
    hidden = down_ref.shape[0]
    reach = (taps - 1) // 2
    edge = gl_sc.shape[0] - length
    half = edge // 2
    dp, sq, *_ = place()
    batch = lax.div(sq, UTTS)
    me = dp * UTTS + lax.rem(sq, UTTS)
    size = peer_sc.shape[1]
    valid = len_ref[dp * (MB * UTTS) + sq]
    frames = jnp.int32(0)
    for group in range(4):
        for u in range(UTTS):
            frames = frames + len_ref[group * (MB * UTTS) + batch * UTTS + u]
    per = 1.0 / jnp.full((1, model), frames, jnp.int32).astype(f32)
    up_w = w_ref.at[:, :hidden]
    out_w = w_ref.at[:, hidden : hidden + model]
    gate_w = w_ref.at[:, hidden + model : hidden + 3 * model]
    conv_w = w_ref.at[:, hidden + 3 * model :]

    def peer(j):
        r = lax.rem(me + j, size)
        return (lax.div(r, UTTS), batch * UTTS + lax.rem(r, UTTS))

    barrier = pltpu.get_barrier_semaphore()
    for j in range(1, size):
        pl.semaphore_signal(barrier, inc=1, device_id=peer(j), device_id_type=MESH)

    def give(which, j):
        return remote(
            part_sc.at[which], peer_sc.at[which, me], send.at[which, j - 1], recv.at[which, size - 1 - j], peer(j)
        )

    def give_all(which):
        for j in range(1, size):
            give(which, j).start()
        peer_sc[which, me] = part_sc[which]

    def take_all(which):
        for j in range(1, size):
            remote(
                part_sc.at[which],
                peer_sc.at[which, lax.rem(me + j, size)],
                send.at[which, j - 1],
                recv.at[which, j - 1],
                peer(j),
            ).wait_recv()
        for j in range(1, size):
            give(which, j).wait_send()
        return jnp.sum(peer_sc[which], axis=0)

    def row_of(i):
        return pl.ds(pl.multiple_of(i * tile, tile), tile)

    def inner_of(i):
        return pl.ds(pl.multiple_of(i * tile + half, 8), tile)

    def mask_of(i):
        return (lax.broadcasted_iota(jnp.int32, (tile, 1), 0) + i * tile < valid).astype(f32)

    def total(rows):
        return jnp.sum(rows, axis=0, keepdims=True)

    def row(r):
        return sm_ref[r : r + 1, :]

    gs_ref[...] = jnp.zeros_like(gs_ref)
    part_sc[...] = jnp.zeros_like(part_sc)
    for pad_sc in (gl_sc, dd_sc):
        pad_sc[:half, :] = jnp.zeros((half, model), f32)
        pad_sc[half + length :, :] = jnp.zeros((half, model), f32)

    tiles = length // tile

    @pl.loop(0, tiles)
    def _(i):
        rows = row_of(i)
        x2 = x1_ref[rows, :] + dotf(ctx_ref[rows, :], out_w[...])
        x2_sc[rows, :] = x2
        a2 = norm(x2, row(2), row(8)).astype(low)
        a2_sc[rows, :] = a2
        gate = dotf(a2, gate_w[...])
        gate_sc[rows, :] = gate
        gl = (gate[:, :model] * sigmoid(gate[:, model:]) * mask_of(i)).astype(low)
        gl_sc[inner_of(i), :] = gl.astype(f32)

    strip = STRIP

    def depthwise(src, lanes, base, backward):
        win_sc[...] = src[pl.ds(base, strip + edge), lanes]
        acc = jnp.zeros((strip, 128), f32)
        for k in range(taps):
            shift = half + (reach - k if backward else k - reach)
            acc = acc + win_sc[shift : shift + strip, :] * sm_ref[14 + k : 15 + k, lanes]
        return acc

    for c in range(model // 128):
        lanes = slice(c * 128, (c + 1) * 128)

        @pl.loop(0, length // strip)
        def _(i):
            base = pl.multiple_of(i * strip, strip)
            dep = depthwise(gl_sc, lanes, base, False)
            dep_sc[pl.ds(base, strip), lanes] = dep
            mask = (lax.broadcasted_iota(jnp.int32, (strip, 1), 0) + base < valid).astype(f32)
            kept = dep * mask
            part_sc[0, 0:1, lanes] += total(kept)
            part_sc[0, 1:2, lanes] += total(kept * dep)

    pl.semaphore_wait(barrier, size - 1)
    give_all(0)
    sums = take_all(0)
    mean = sums[0:1] * per
    inv = lax.rsqrt(sums[1:2] * per - mean * mean + 1e-05)

    @pl.loop(0, tiles)
    def _(i):
        rows = row_of(i)
        dep = dep_sc[rows, :]
        hatn = (dep - mean) * inv
        normal = hatn * row(5) + row(11)
        sgn = sigmoid(normal)
        act = (normal * sgn).astype(low)
        act_sc[rows, :] = act
        x3 = x2_sc[rows, :] + dotf(act, conv_w[...])
        a3 = norm(x3, row(3), row(9)).astype(low)
        a3_sc[rows, :] = a3
        h = dotf(a3, up_w[...])
        sig = sigmoid(h)
        z = (h * sig).astype(low)
        z_sc[rows, :] = z
        x4 = x3 + 0.5 * dotf(z, down_ref[...])
        mixed_ref[rows, :] = norm(x4, row(4), row(10)).astype(low)
        cot = cot_ref[rows, :].astype(f32)
        grad, _, dgain = norm_back(x4, row(4), cot)
        gs_ref[4:5, :] += dgain
        gs_ref[10:11, :] += total(cot)
        go = (0.5 * grad).astype(low)
        go_sc[rows, :] = go
        dh = (dotf(go, down_ref[...], NT) * (sig * (1.0 + h * (1.0 - sig)))).astype(low)
        dh_sc[rows, :] = dh
        dn = dotf(dh, up_w[...], NT)
        dx, _, dgain = norm_back(x3, row(3), dn)
        gs_ref[3:4, :] += dgain
        gs_ref[9:10, :] += total(dn)
        grad = grad + dx
        grad_ref[rows, :] = grad
        gob = grad.astype(low)
        gob_sc[rows, :] = gob
        dnormal = dotf(gob, conv_w[...], NT) * (sgn * (1.0 + normal * (1.0 - sgn)))
        gs_ref[5:6, :] += total(dnormal * hatn)
        gs_ref[11:12, :] += total(dnormal)
        e = dnormal * row(5)
        e_sc[rows, :] = e
        part_sc[1, 0:1, :] += total(e)
        part_sc[1, 1:2, :] += total(e * dep)

    give_all(1)

    @pl.loop(0, hidden // model)
    def _(j):
        cols = pl.ds(pl.multiple_of(j * model, model), model)
        gw_ref[:, cols] = dotf(a3_sc[...], dh_sc[:, cols], TN).astype(low)
        gd_ref[cols, :] = dotf(z_sc[:, cols], go_sc[...], TN).astype(low)

    gw_ref[:, hidden + 3 * model :] = dotf(act_sc[...], gob_sc[...], TN).astype(low)
    sums = take_all(1)
    dvar = -0.5 * inv * inv * inv * (sums[1:2] - mean * sums[0:1])
    dmean = -inv * sums[0:1] - 2.0 * mean * dvar

    @pl.loop(0, tiles)
    def _(i):
        rows = row_of(i)
        dd = e_sc[rows, :] * inv + mask_of(i) * (dmean * per + 2.0 * dep_sc[rows, :] * dvar * per)
        dd_sc[inner_of(i), :] = dd.astype(low).astype(f32)

    for c in range(model // 128):
        lanes = slice(c * 128, (c + 1) * 128)
        tap_sc[...] = jnp.zeros_like(tap_sc)

        @pl.loop(0, length // strip)
        def _(i):
            base = pl.multiple_of(i * strip, strip)
            e_sc[pl.ds(base, strip), lanes] = depthwise(dd_sc, lanes, base, True)
            dd = dd_sc[pl.ds(pl.multiple_of(base + half, 8), strip), lanes]
            win_sc[...] = gl_sc[pl.ds(base, strip + edge), lanes]
            for k in range(taps):
                prod = win_sc[half + k - reach : half + k - reach + strip, :] * dd
                tap_sc[k] += jnp.sum(prod.reshape(strip // 8, 8, 128), axis=0)

        gs_ref[14 : 14 + taps, lanes] = jnp.sum(tap_sc[...], axis=1)

    @pl.loop(0, tiles)
    def _(i):
        rows = row_of(i)
        dgl = e_sc[rows, :] * mask_of(i)
        ga = gate_sc[rows, :model]
        sb = sigmoid(gate_sc[rows, model:])
        dgate = jnp.concatenate([dgl * sb, dgl * ga * sb * (1.0 - sb)], axis=1).astype(low)
        dh_sc[rows, : 2 * model] = dgate
        dn = dotf(dgate, gate_w[...], NT)
        dx, _, dgain = norm_back(x2_sc[rows, :], row(2), dn)
        gs_ref[2:3, :] += dgain
        gs_ref[8:9, :] += total(dn)
        grad = grad_ref[rows, :] + dx
        grad_ref[rows, :] = grad
        gob = grad.astype(low)
        gob_sc[rows, :] = gob
        gctx_ref[rows, :] = dotf(gob, out_w[...], NT).astype(low)

    gw_ref[:, hidden + model : hidden + 3 * model] = dotf(a2_sc[...], dh_sc[:, : 2 * model], TN).astype(low)
    gw_ref[:, hidden : hidden + model] = dotf(ctx_ref[...], gob_sc[...], TN).astype(low)


def middle(lengths, ctx, x1, w, down, cot, small, taps, tile=256):
    rows, model = x1.shape
    hidden = down.shape[0]
    low = jnp.bfloat16
    f32 = jnp.float32
    vm = pl.BlockSpec(memory_space=pltpu.VMEM)
    size = 4 * UTTS
    half = -(-(taps - 1) // 2 // 8) * 8
    wide = pltpu.VMEM((rows, model), f32)
    thin = pltpu.VMEM((rows, model), low)
    padded = pltpu.VMEM((rows + 2 * half, model), f32)
    return pl.pallas_call(
        lambda *refs: middle_kernel(*refs, tile=tile, taps=taps),
        in_specs=[pl.BlockSpec(memory_space=pltpu.SMEM)] + [vm] * 6,
        out_specs=[vm] * 6,
        out_shape=[
            jax.ShapeDtypeStruct((rows, model), low),
            jax.ShapeDtypeStruct((rows, model), f32),
            jax.ShapeDtypeStruct((rows, model), low),
            jax.ShapeDtypeStruct(w.shape, low),
            jax.ShapeDtypeStruct(down.shape, low),
            jax.ShapeDtypeStruct((SMALL, model), f32),
        ],
        scratch_shapes=[
            wide,
            thin,
            pltpu.VMEM((rows, 2 * model), f32),
            padded,
            wide,
            thin,
            thin,
            pltpu.VMEM((rows, hidden), low),
            pltpu.VMEM((rows, hidden), low),
            thin,
            thin,
            wide,
            padded,
            pltpu.VMEM((taps, 8, 128), f32),
            pltpu.VMEM((STRIP + 2 * half, 128), f32),
            pltpu.VMEM((2, 2, model), f32),
            pltpu.VMEM((2, size, 2, model), f32),
            pltpu.SemaphoreType.DMA((2, size - 1)),
            pltpu.SemaphoreType.DMA((2, size - 1)),
        ],
        compiler_params=pltpu.CompilerParams(
            collective_id=2, has_side_effects=True, vmem_limit_bytes=63 * 1024 * 1024
        ),
        name="middle",
    )(lengths, ctx, x1, w, down, cot, small)


def position_table(length, width):
    offsets = (length - 1 - np.arange(2 * length)).astype(np.float32)
    half = width // 2
    steps = np.arange(half, dtype=np.float32) * np.float32(-2.0 * math.log(10000.0) / width)
    angles = (offsets[:, None] * np.exp(steps)[None, :]).astype(np.float64)
    table = np.concatenate([np.sin(angles), np.cos(angles)], axis=1)
    return jnp.asarray(table.astype(np.float32)).astype(jnp.bfloat16)


def pack_kernel(
    frames, cot, gains, shifts, rel, up, down, attn_in, attn_out, pos, conv_in, taps, conv_out,
    early, late, down_0, down_1, f_out, c_out, turn, table,
):
    low = jnp.bfloat16
    f32 = jnp.float32
    own = gains.shape[2]
    count = taps.shape[2]
    at = 0
    for piece in (attn_in[0], pos[0], up[0, 0]):
        early[:, at : at + piece.shape[1]] = piece
        at += piece.shape[1]
    table[...] = jnp.zeros_like(table)
    turn[...] = jnp.zeros_like(turn)
    turn[:own, :count] = taps[0].astype(f32)
    table[0:6, :own] = gains[0].astype(f32)
    table[6:12, :own] = shifts[0].astype(f32)
    table[12:14, :own] = rel[0].astype(f32)
    table[14 : 14 + count, :own] = turn[...].T[:count, :own]
    early[:, at:] = table[...].T[:own, :].astype(low)
    at = 0
    for piece in (up[0, 1], attn_out[0], conv_in[0], conv_out[0]):
        late[:, at : at + piece.shape[1]] = piece
        at += piece.shape[1]
    down_0[...] = down[0, 0]
    down_1[...] = down[0, 1]
    f_out[...] = frames[...].astype(low)
    c_out[...] = cot[...].astype(low)


def pack(frames, cot, *weights):
    low = jnp.bfloat16
    vm = pl.BlockSpec(memory_space=pltpu.VMEM)
    _, _, _, up, down, attn_in, attn_out, pos, conv_in, _, conv_out = weights
    own = attn_in.shape[1]
    early = attn_in.shape[2] + pos.shape[2] + up.shape[3] + SMALL
    late = up.shape[3] + attn_out.shape[2] + conv_in.shape[2] + conv_out.shape[2]
    shapes = [(own, early), (own, late), down.shape[2:], down.shape[2:], frames.shape, frames.shape]
    return pl.pallas_call(
        pack_kernel,
        in_specs=[vm] * 13,
        out_specs=[vm] * 6,
        out_shape=[jax.ShapeDtypeStruct(shape, low) for shape in shapes],
        scratch_shapes=[pltpu.VMEM((SMALL, SMALL), jnp.float32)] * 2,
        name="pack",
    )(frames, cot, *weights)


def unpack_kernel(
    early, late, down_0, down_1, m_rows, g_rows,
    mixed, grad, gains, shifts, rel, up, down, attn_in, attn_out, pos, conv_in, taps, conv_out, turn, table,
):
    f32 = jnp.float32
    own = early.shape[0]
    count = taps.shape[2]
    at = 0
    for piece in (attn_in, pos):
        piece[0] = early[:, at : at + piece.shape[2]]
        at += piece.shape[2]
    up[0, 0] = early[:, at : at + up.shape[3]]
    at += up.shape[3]
    turn[...] = jnp.zeros_like(turn)
    turn[:own, :] = early[:, at:]
    table[...] = turn[...].T
    gains[0] = table[0:6, :own]
    shifts[0] = table[6:12, :own]
    rel[0] = table[12:14, :own]
    turn[:count, :] = table[14 : 14 + count, :]
    taps[0] = turn[...].T[:own, :count]
    up[0, 1] = late[:, : up.shape[3]]
    at = up.shape[3]
    for piece in (attn_out, conv_in, conv_out):
        piece[0] = late[:, at : at + piece.shape[2]]
        at += piece.shape[2]
    down[0, 0] = down_0[...]
    down[0, 1] = down_1[...]
    mixed[...] = m_rows[...].astype(f32)
    grad[...] = g_rows[...].astype(f32)


def unpack(early, late, down_0, down_1, m_rows, g_rows, likes):
    vm = pl.BlockSpec(memory_space=pltpu.VMEM)
    shapes = [m_rows.shape, g_rows.shape] + [like.shape for like in likes]
    return pl.pallas_call(
        unpack_kernel,
        in_specs=[vm] * 6,
        out_specs=[vm] * 13,
        out_shape=[jax.ShapeDtypeStruct(shape, jnp.float32) for shape in shapes],
        scratch_shapes=[pltpu.VMEM((SMALL, SMALL), jnp.float32)] * 2,
        name="unpack",
    )(early, late, down_0, down_1, m_rows, g_rows)


def local_whole(
    frames,
    lengths,
    cotangent,
    gains,
    shifts,
    rel_bias,
    ffn_up,
    ffn_down,
    attn_in,
    attn_out,
    pos_proj,
    conv_in,
    depthwise,
    conv_out,
):
    weights = (
        gains, shifts, rel_bias, ffn_up, ffn_down, attn_in, attn_out, pos_proj, conv_in, depthwise, conv_out
    )
    _, width_rows, model = frames.shape
    length = width_rows * lax.axis_size("seq")
    taps = depthwise.shape[2]
    table_in = position_table(length, model)
    early, late, own_0, own_1, f_rows, c_rows = pack(frames, cotangent, *weights)
    sizes = (attn_in.shape[2], pos_proj.shape[2], ffn_up.shape[3], SMALL)
    cuts = [0] + [int(v) for v in np.cumsum(sizes)]
    w_early, down_0, f_all = gather_all(early, own_0, f_rows)
    f_all = f_all.reshape(length, model)
    ctx, probs, x1, qu, qv, key, value, table, small, c_all, w_late, down_1 = front(
        lengths, f_all, w_early, cuts, down_0, table_in, c_rows, late, own_1
    )
    mixed, grad, grad_ctx, g_late, g_down1, g_small = middle(
        lengths, ctx, x1, w_late, down_1, c_all.reshape(length, model), small, taps
    )
    m_all, late_sum, down1_sum, g_all, early_sum, down0_sum = back(
        probs,
        grad_ctx,
        qu,
        qv,
        key,
        value,
        table,
        mixed.reshape(frames.shape),
        g_late,
        g_down1,
        x1,
        f_all,
        grad,
        small,
        g_small,
        w_early,
        cuts,
        down_0,
        table_in,
    )
    return tuple(unpack(early_sum, late_sum, down0_sum, down1_sum, m_all, g_all, weights))


def solution(mesh):
    body = local_whole if fits_whole(mesh) else local_general
    in_specs = (
        P("dp", "seq", None),
        P(),
        P("dp", "seq", None),
        P(None, None, ("dp", "seq")),
        P(None, None, ("dp", "seq")),
        P(None, None, ("dp", "seq")),
        P(None, None, ("dp", "seq"), None),
        P(None, None, ("dp", "seq"), None),
        P(None, ("dp", "seq"), None),
        P(None, ("dp", "seq"), None),
        P(None, ("dp", "seq"), None),
        P(None, ("dp", "seq"), None),
        P(None, ("dp", "seq"), None),
        P(None, ("dp", "seq"), None),
    )
    out_specs = (
        P("dp", "seq", None),
        P("dp", "seq", None),
        P(None, None, ("dp", "seq")),
        P(None, None, ("dp", "seq")),
        P(None, None, ("dp", "seq")),
        P(None, None, ("dp", "seq"), None),
        P(None, None, ("dp", "seq"), None),
        P(None, ("dp", "seq"), None),
        P(None, ("dp", "seq"), None),
        P(None, ("dp", "seq"), None),
        P(None, ("dp", "seq"), None),
        P(None, ("dp", "seq"), None),
        P(None, ("dp", "seq"), None),
    )
    return jax.shard_map(body, mesh=mesh, in_specs=in_specs, out_specs=out_specs, check_vma=False)
```
